32 devices in a mesh: dom: 16 (over z, x, core), grp: 2 (over y).
Axes of the slice: x: 2, y: 2, z: 4, core: 2. Of those that a mesh axis runs over, the one named last changes fastest.
Arguments:
- positions: float32 [3, 2, 16384], P(None, 'grp', 'dom'), as said below
- species: int32 [2, 16384], P('grp', 'dom'), may hold values from 0 to 3
- neighbours: int32 [48, 2, 16384], P(None, 'grp', 'dom'), may hold values from 0 to 16383, as said below
- slot_counts: int32 [2, 16384], P('grp', 'dom'), may hold values from 20 to 48, as said below
- structure: int32 [2, 16384], P('grp', 'dom'), may hold values from 0 to 511, as said below
- target_energy: float32 [2, 512], P('grp'), may hold values from -6 to 6
- radial_one: float32 [10, 12], replicated, may hold values from -6 to 6
- coupling_one: bfloat16 [4, 1960, 512], replicated, may hold values from -0.3125 to 0.3125
- coefficient_one: float32 [4, 512], replicated, may hold values from -0.25 to 0.25
- mixing: float32 [512, 4], replicated, may hold values from -0.375 to 0.375
- radial_two: float32 [10, 12], replicated, may hold values from -6 to 6
- coupling_two: bfloat16 [4, 1960, 512], replicated, may hold values from -0.3125 to 0.3125
- coefficient_two: float32 [4, 512], replicated, may hold values from -0.25 to 0.25
Outputs:
- energies: float32 [2, 512], P('grp')
- offsets: float32 [4], replicated
- forces: float32 [3, 2, 16384], P(None, 'grp', 'dom')
- radial_first: float32 [10, 12], replicated
- coefficient_first: float32 [4, 512], replicated
- mixing_gradient: float32 [512, 4], replicated
- radial_second: float32 [10, 12], replicated
- coefficient_second: float32 [4, 512], replicated
The draws below stay inside these ranges and needn't reach their ends.
Inputs may be any that keep to these rules, and one draw needn't show every extreme that they name: Atoms of one structure are consecutive within a group; structure numbers start at 0 in each group and rise by one, and every group holds exactly 512 structures; each structure holds a multiple of 8 atoms, from 8 to 4096. `neighbours`: each slot names another atom of the same structure; it lies in the same block of 1024 consecutive atoms of the group as the atom or in an adjacent block. An atom may be named in several slots of one atom. Slots k < slot_counts are live, the others are ignored. `positions`: any two atoms of one structure are 0.9 or more apart.
All inputs are finite; a program needn't handle non-finite values.
Results may differ from the reference program's by a relative error of at most 0.0085.
The reference program's roundings to bfloat16 on the way count: a program that leaves them out, or rounds other values in their place, can miss the bound.
Values sent between devices are 32-bit elements; how exact they have to be, the bound alone decides.
A program may use at most 320 MiB of HBM per device.

```python
import math
from functools import reduce
import jax
import jax.numpy as jnp
from jax import lax

NRAD = 12
NMAX = 10
LMAX = 6
LM = 49
SPECIES = 4
DENS = 1960
NINV = 512
FACTORS = 4
NBR = 48
MIN_NBR = 20
A_DEV = 1024
ATOMS_G = 16384
GROUPS = 2
SMAX = 512
N_DOM = 16


def structure_layout(key, group_at):
    group_key = jax.random.fold_in(jax.random.fold_in(key, 101), group_at)
    units_all = ATOMS_G // 8
    leading_units = min(512, units_all // 4)
    rest_units = units_all - leading_units
    picks = jax.random.permutation(jax.random.fold_in(group_key, 1), rest_units - 1)[:SMAX - 2] + 1
    cuts = jnp.sort(picks.astype(jnp.int32))
    boundaries = 8 * jnp.concatenate([jnp.array([leading_units], dtype=jnp.int32), leading_units + cuts, jnp.array([units_all], dtype=jnp.int32)])
    boundaries = boundaries.astype(jnp.int32)
    atom_index = jnp.arange(ATOMS_G, dtype=jnp.int32)
    labels = jnp.searchsorted(boundaries, atom_index, side='right').astype(jnp.int32)
    starts = jnp.where(labels > 0, boundaries[jnp.maximum(labels - 1, 0)], 0)
    finish = boundaries[labels]
    return (group_key, atom_index, labels, starts, finish - starts)


def over_groups(function_in, key, out_axis):
    return jax.vmap(lambda group_at: function_in(key, group_at), out_axes=out_axis)(jnp.arange(GROUPS, dtype=jnp.int32))


def structure_of(key, group_at):
    return structure_layout(key, group_at)[2]


def species_of(key, group_at):
    group_key, atom_index, labels, starts, extents = structure_layout(key, group_at)
    leading_species = jax.random.randint(jax.random.fold_in(group_key, 2), (SMAX,), 0, SPECIES)
    second_pick = jax.random.randint(jax.random.fold_in(group_key, 3), (ATOMS_G,), 0, 2)
    return ((leading_species[labels] + second_pick) % SPECIES).astype(jnp.int32)


def neighbours_of(key, group_at):
    group_key, atom_index, labels, starts, extents = structure_layout(key, group_at)
    lattice_moves = jax.random.randint(jax.random.fold_in(group_key, 4), (3, NBR, ATOMS_G), -1, 2)
    motionless = jnp.all(lattice_moves == 0, axis=0)
    step_x = jnp.where(motionless, 1, lattice_moves[0])
    offset = step_x + 4 * lattice_moves[1] + 16 * lattice_moves[2]
    rank_in = atom_index[None, :] - starts[None, :]
    wrapped = offset % extents[None, :]
    wrapped = jnp.where(wrapped == 0, 1, wrapped)
    within_small = starts[None, :] + (rank_in + wrapped) % extents[None, :]
    forward = atom_index[None, :] + offset
    inside = (forward >= starts[None, :]) & (forward < (starts + extents)[None, :])
    within_large = jnp.where(inside, forward, atom_index[None, :] - offset)
    return jnp.where(extents[None, :] <= A_DEV, within_small, within_large).astype(jnp.int32)


def counts_of(key, group_at):
    group_key = structure_layout(key, group_at)[0]
    counted = jax.random.randint(jax.random.fold_in(group_key, 5), (ATOMS_G,), MIN_NBR, NBR + 1)
    position_in = jnp.arange(ATOMS_G, dtype=jnp.int32) % A_DEV
    counted = jnp.where(position_in == 0, NBR, jnp.where(position_in == 1, MIN_NBR, counted))
    return counted.astype(jnp.int32)


def positions_of(key, group_at):
    group_key, atom_index, labels, starts, extents = structure_layout(key, group_at)
    rank_in = atom_index - starts
    lattice = jnp.stack([rank_in % 4, rank_in // 4 % 4, rank_in // 16]).astype(jnp.float32) * 1.5
    jitter_key = jax.random.fold_in(group_key, 6)
    jitter = jnp.clip(0.12 * jax.random.normal(jitter_key, (3, ATOMS_G), jnp.float32), -0.3, 0.3)
    return lattice + jitter


def draw_positions(key, part):
    return over_groups(positions_of, key, 1)


def draw_species(key, part):
    return over_groups(species_of, key, 0)


def draw_neighbours(key, part):
    return over_groups(neighbours_of, key, 1)


def draw_slot_counts(key, part):
    return over_groups(counts_of, key, 0)


def draw_structure(key, part):
    return over_groups(structure_of, key, 0)


def shard_levels(stream_key, dims, pieces, low, largest):
    def one(dim, parts):
        steps = jax.random.uniform(jax.random.fold_in(jax.random.fold_in(stream_key, 6), dim), (parts,), jnp.float32, low / len(pieces), largest / len(pieces))
        return jnp.repeat(jnp.exp(steps), dims[dim] // parts).reshape((-1,) + (1,) * (len(dims) - dim - 1))

    loudness = one(*pieces[0])
    for cut in pieces[1:]:
        loudness = loudness * one(*cut)
    return loudness


def bell_draw(key, dims, scale, limit, shards=(), kind=jnp.bfloat16):
    loudness = shard_levels(key, dims, shards, -0.22, 0.18) if shards else 1.0
    values = jax.random.normal(key, dims, jnp.float32) * scale * loudness
    return jnp.minimum(jnp.maximum(values, -limit), limit).astype(kind)


def setup_inputs(seed: int = 0) -> dict:
    streams_of = jax.random.split(jax.random.key(seed), 14)
    positions = draw_positions(jax.random.fold_in(streams_of[13], 71), 0)
    species = draw_species(jax.random.fold_in(streams_of[13], 71), 0)
    neighbours = draw_neighbours(jax.random.fold_in(streams_of[13], 71), 0)
    slot_counts = draw_slot_counts(jax.random.fold_in(streams_of[13], 71), 0)
    structure = draw_structure(jax.random.fold_in(streams_of[13], 71), 0)
    target_energy = bell_draw(streams_of[5], (GROUPS, SMAX), 1.0, 6.0, ((0, 2),), jnp.float32)
    radial_one = bell_draw(streams_of[6], (NMAX, NRAD), 1.0, 6.0, (), jnp.float32)
    coupling_one = bell_draw(streams_of[7], (FACTORS, DENS, NINV), (2.5 / (SPECIES * NMAX * LM) ** 0.5), 0.3125)
    coefficient_one = bell_draw(streams_of[8], (SPECIES, NINV), NINV ** -0.5, 0.25, (), jnp.float32)
    mixing = bell_draw(streams_of[9], (NINV, SPECIES), (NINV // 2) ** -0.5, 0.375, (), jnp.float32)
    radial_two = bell_draw(streams_of[10], (NMAX, NRAD), 1.0, 6.0, (), jnp.float32)
    coupling_two = bell_draw(streams_of[11], (FACTORS, DENS, NINV), (2.5 / (SPECIES * NMAX * LM) ** 0.5), 0.3125)
    coefficient_two = bell_draw(streams_of[12], (SPECIES, NINV), NINV ** -0.5, 0.25, (), jnp.float32)
    return {"positions": positions, "species": species, "neighbours": neighbours, "slot_counts": slot_counts, "structure": structure, "target_energy": target_energy, "radial_one": radial_one, "coupling_one": coupling_one, "coefficient_one": coefficient_one, "mixing": mixing, "radial_two": radial_two, "coupling_two": coupling_two, "coefficient_two": coefficient_two}


@jax.custom_vjp
def low(v):
    return lax.optimization_barrier(v.astype(jnp.bfloat16)).astype(jnp.float32)

@jax.custom_vjp
def low_back(v):
    return v

def low_keep(v):
    return (low(v), None)

def low_pass(kept, grad):
    return (grad,)

def back_keep(v):
    return (v, None)

def back_low(kept, grad):
    return (low(grad),)
low.defvjp(low_keep, low_pass)
low_back.defvjp(back_keep, back_low)
cutoff_radius = 5.0
density_scale = 0.17
norm_eps = 1e-05
ridge_weight = 0.1
highest = lax.Precision.HIGHEST

def double_factorial(number):
    result = 1.0
    while number > 1:
        result = result * number
        number = number - 2
    return result

def harmonics(unit_vec):
    coord_x, coord_y, coord_z = (unit_vec[0], unit_vec[1], unit_vec[2])
    cosines = [jnp.ones_like(coord_x)]
    sine_terms = [jnp.zeros_like(coord_x)]
    for degree in range(1, LMAX + 1):
        cosines.append(cosines[-1] * coord_x - sine_terms[-1] * coord_y)
        sine_terms.append(sine_terms[-1] * coord_x + cosines[-2] * coord_y)
    legendre = {}
    for azimuth in range(LMAX + 1):
        legendre[azimuth, azimuth] = jnp.full_like(coord_z, double_factorial(2 * azimuth - 1))
        if azimuth + 1 <= LMAX:
            legendre[azimuth + 1, azimuth] = (2 * azimuth + 1) * coord_z * legendre[azimuth, azimuth]
        for degree in range(azimuth + 2, LMAX + 1):
            legendre[degree, azimuth] = ((2 * degree - 1) * coord_z * legendre[degree - 1, azimuth] - (degree + azimuth - 1) * legendre[degree - 2, azimuth]) / (degree - azimuth)
    columns = []
    for degree in range(LMAX + 1):
        for signed in range(-degree, degree + 1):
            azimuth = abs(signed)
            factor = math.sqrt((2 * degree + 1) / (4 * math.pi) * math.factorial(degree - azimuth) / math.factorial(degree + azimuth))
            scaled_poly = factor * legendre[degree, azimuth]
            if signed == 0:
                columns.append(scaled_poly)
            elif signed > 0:
                columns.append(math.sqrt(2.0) * scaled_poly * cosines[azimuth])
            else:
                columns.append(math.sqrt(2.0) * scaled_poly * sine_terms[azimuth])
    return jnp.stack(columns)

def radial_basis(distance, radial_weight):
    scaled = 2.0 * distance / cutoff_radius - 1.0
    cutoff = jnp.where(distance < cutoff_radius, 0.5 * (jnp.cos(jnp.pi * distance / cutoff_radius) + 1.0), 0.0)
    cheb_terms = [jnp.ones_like(scaled), scaled]
    for degree in range(2, NRAD):
        cheb_terms.append(2.0 * scaled * cheb_terms[-1] - cheb_terms[-2])
    cheb_basis = jnp.stack(cheb_terms[:NRAD])
    return jnp.einsum('np,pka->nka', radial_weight, cheb_basis, precision=highest) * cutoff

def densities(centres, neighbour_sites, channel_weight, live_slots, radial_weight):
    offsets_vec = neighbour_sites - centres[:, None, :]
    distance = jnp.sqrt(lax.optimization_barrier(jnp.sum(offsets_vec * offsets_vec, axis=0)))
    unit_vec = offsets_vec / distance
    radial = radial_basis(distance, radial_weight)
    angular = harmonics(unit_vec)
    weighted = channel_weight * (live_slots * density_scale)
    mixed_terms = (weighted[:, None] * radial[None]).reshape(-1, radial.shape[1], radial.shape[2])
    dens_out = jnp.einsum('mka,lka->mla', mixed_terms, angular, precision=highest)
    return dens_out.reshape(-1, dens_out.shape[-1])

def feature_map(invariants, mixing):
    inverse_rms = lax.rsqrt(lax.optimization_barrier(jnp.mean(invariants * invariants, axis=0)) + norm_eps)
    return jnp.einsum('qk,qa->ka', mixing, invariants, precision=highest) * inverse_rms

def small_solve(matrix, vector):
    order_n = matrix.shape[0]
    rows_now = [matrix[row_at] for row_at in range(order_n)]
    rights_now = [vector[row_at] for row_at in range(order_n)]
    for pivot_at in range(order_n):
        for below_at in range(pivot_at + 1, order_n):
            ratio_now = rows_now[below_at][pivot_at] / rows_now[pivot_at][pivot_at]
            rows_now[below_at] = rows_now[below_at] - ratio_now * rows_now[pivot_at]
            rights_now[below_at] = rights_now[below_at] - ratio_now * rights_now[pivot_at]
    answer = [None] * order_n
    for row_at in range(order_n - 1, -1, -1):
        running = rights_now[row_at]
        for later_at in range(row_at + 1, order_n):
            running = running - rows_now[row_at][later_at] * answer[later_at]
        answer[row_at] = running / rows_now[row_at][row_at]
    return jnp.stack(answer)

def layer_block(centres, sites, weights_all, neighbour_block, count_block, onehot_block, radial_weight, coupling, coefficient):
    live_slots = (jnp.arange(NBR, dtype=jnp.int32)[:, None] < count_block[None, :]).astype(jnp.float32)
    dens_block = densities(centres, sites[:, neighbour_block], weights_all[:, neighbour_block], live_slots, radial_weight)
    factors = low_back(jnp.einsum('vdq,da->vqa', coupling, low(dens_block), precision=highest))
    invariants = reduce(lambda earlier, later: earlier * later, [factors[index_v] for index_v in range(FACTORS)])
    chosen = jnp.dot(coefficient.T, onehot_block, precision=highest)
    return (lax.optimization_barrier(jnp.sum(invariants * chosen, axis=0)), invariants)

def group_energy(params, inputs):
    radial_one, coupling_one, coefficient_one, mixing, radial_two, coupling_two, coefficient_two = params
    sites, species, neighbours, slot_counts = inputs
    labels = jnp.arange(SPECIES, dtype=jnp.int32)
    onehot = (species[None, :] == labels[:, None]).astype(jnp.float32)

    def blocked(array):
        return jnp.moveaxis(array.reshape(array.shape[:-1] + (N_DOM, A_DEV)), -2, 0)

    def unblock(array):
        return jnp.moveaxis(array, 0, -2).reshape(array.shape[1:-1] + (ATOMS_G,))
    block_inputs = (blocked(sites), blocked(neighbours), blocked(slot_counts), blocked(onehot))

    def first_layer(block_in):
        centres, neighbour_block, count_block, onehot_block = block_in
        energy_block, invariants = layer_block(centres, sites, onehot, neighbour_block, count_block, onehot_block, radial_one, coupling_one, coefficient_one)
        return (energy_block, feature_map(invariants, mixing))
    energy_one, features = lax.map(jax.checkpoint(first_layer), block_inputs)
    features_all = unblock(features)

    def second_layer(block_in):
        centres, neighbour_block, count_block, onehot_block = block_in
        return layer_block(centres, sites, features_all, neighbour_block, count_block, onehot_block, radial_two, coupling_two, coefficient_two)[0]
    energy_two = lax.map(jax.checkpoint(second_layer), block_inputs)
    return unblock(energy_one + energy_two)

def reference(positions, species, neighbours, slot_counts, structure, target_energy, radial_one, coupling_one, coefficient_one, mixing, radial_two, coupling_two, coefficient_two):
    coupling_first = coupling_one.astype(jnp.float32)
    coupling_second = coupling_two.astype(jnp.float32)
    group_sites = jnp.moveaxis(positions, 1, 0)
    group_neighbours = jnp.moveaxis(neighbours, 1, 0)

    def overall(sites, radial_a, coefficient_a, mixing_a, radial_b, coefficient_b):
        params = (radial_a, coupling_first, coefficient_a, mixing_a, radial_b, coupling_second, coefficient_b)
        site_energy = lax.map(lambda inputs: group_energy(params, inputs), (sites, species, group_neighbours, slot_counts))
        onehot_all = (species[..., None] == jnp.arange(SPECIES, dtype=jnp.int32)).astype(jnp.float32)
        energy_sum = jax.vmap(lambda values, segment_ids: jax.ops.segment_sum(values, segment_ids, num_segments=SMAX))(site_energy, structure)
        species_count = jax.vmap(lambda values, segment_ids: jax.ops.segment_sum(values, segment_ids, num_segments=SMAX))(onehot_all, structure)
        atom_total = jnp.maximum(lax.optimization_barrier(jnp.sum(species_count, axis=-1)), 1.0)
        fraction = species_count / atom_total[..., None]
        gram_matrix = jnp.einsum('gsc,gsd->cd', fraction, fraction, precision=highest) + ridge_weight * jnp.eye(SPECIES, dtype=jnp.float32)
        right_side = jnp.einsum('gsc,gs->c', fraction, target_energy, precision=highest)
        offsets = small_solve(gram_matrix, right_side)
        energies = energy_sum / atom_total + jnp.einsum('gsc,c->gs', fraction, offsets, precision=highest)
        return (site_energy, (energies, offsets))
    site_energy, pullback, extras = jax.vjp(overall, group_sites, radial_one, coefficient_one, mixing, radial_two, coefficient_two, has_aux=True)
    energies, offsets = extras
    grad_sites, radial_first, coefficient_first, mixing_gradient, radial_second, coefficient_second = pullback(jnp.ones_like(site_energy))
    forces = -jnp.moveaxis(grad_sites, 0, 1)
    return (energies, offsets, forces, radial_first, coefficient_first, mixing_gradient, radial_second, coefficient_second)
```

```python
from functools import partial, reduce
import math

import jax
import jax.numpy as jnp
from jax import lax
from jax.experimental import pallas as pl
from jax.experimental.pallas import tpu as pltpu
from jax.sharding import PartitionSpec as P

NRAD = 12
NMAX = 10
LMAX = 6
LM = 49
SPECIES = 4
CH = SPECIES * NMAX
DENS = CH * LM
NBR = 48
NPAD = 64
TILE = 128
LBLK = 7
WROWS = 4
NVAL = 7

cutoff_radius = 5.0
density_scale = 0.17
norm_eps = 1e-05
ridge_weight = 0.1
highest = lax.Precision.HIGHEST
f32 = jnp.float32
bf16 = jnp.bfloat16


def shift_pair(cells, axis):
    count = lax.axis_size(axis)
    ends = count - 1
    left = lax.ppermute(cells, axis, [(i, i + 1) for i in range(ends)])
    right = lax.ppermute(cells, axis, [(i + 1, i) for i in range(ends)])
    return left, right


def double_factorial(number):
    result = 1.0
    while number > 1:
        result = result * number
        number = number - 2
    return result


def norm_of(degree, azimuth):
    value = math.sqrt(
        (2 * degree + 1)
        / (4 * math.pi)
        * math.factorial(degree - azimuth)
        / math.factorial(degree + azimuth)
    )
    return value * (math.sqrt(2.0) if azimuth else 1.0)


def scaled_legendre(coord_z):
    table = {}
    for azimuth in range(LMAX + 1):
        table[azimuth, azimuth] = norm_of(azimuth, azimuth) * double_factorial(2 * azimuth - 1)
        if azimuth + 1 <= LMAX:
            ratio = norm_of(azimuth + 1, azimuth) / norm_of(azimuth, azimuth)
            table[azimuth + 1, azimuth] = coord_z * (
                (2 * azimuth + 1) * ratio * table[azimuth, azimuth]
            )
        for degree in range(azimuth + 2, LMAX + 1):
            gap = degree - azimuth
            first = (2 * degree - 1) / gap * norm_of(degree, azimuth) / norm_of(degree - 1, azimuth)
            second = (
                (degree + azimuth - 1) / gap * norm_of(degree, azimuth) / norm_of(degree - 2, azimuth)
            )
            table[degree, azimuth] = (first * coord_z) * table[degree - 1, azimuth] - (
                second * table[degree - 2, azimuth]
            )
    return table


def azimuth_powers(coord_x, coord_y):
    cosines = [None, coord_x]
    sines = [None, coord_y]
    for _ in range(2, LMAX + 1):
        cosines.append(cosines[-1] * coord_x - sines[-1] * coord_y)
        sines.append(sines[-1] * coord_x + cosines[-2] * coord_y)
    return cosines, sines


def fetch(tab_ref, names, hi, lo, row_low, row_high):
    def body(row, values):
        hit = hi == row
        out = []
        for name, value in zip(names, values):
            line = jnp.broadcast_to(tab_ref[pl.ds(name * 24 + row, 1), :], (8, TILE))
            got = jnp.take_along_axis(line, lo, axis=1, mode="promise_in_bounds")
            out.append(jnp.where(hit, got, value))
        return tuple(out)

    zero = jnp.zeros((8, TILE), f32)
    return lax.fori_loop(row_low, row_high + 1, body, tuple(zero for _ in names))


def edge_block(layer, tab_ref, cen_ref, idx_ref, wt_ref, block_at, row_low, row_high):
    base = pl.multiple_of(block_at * 8, 8)
    index = idx_ref[pl.ds(base, 8), :]
    weight = wt_ref[pl.ds(base, 8), :]
    hi = lax.shift_right_logical(index, 7)
    lo = lax.bitwise_and(index, 127)
    names = (0, 1, 2, 3) if layer == 1 else (0, 1, 2, 3, 4, 5, 6)
    values = fetch(tab_ref, names, hi, lo, row_low, row_high)
    live = weight > 0.0
    deltas = []
    for axis in range(3):
        centre = jnp.broadcast_to(cen_ref[pl.ds(axis, 1), :], (8, TILE))
        deltas.append(jnp.where(live, values[axis] - centre, 1.0))
    dist = jnp.sqrt(deltas[0] * deltas[0] + deltas[1] * deltas[1] + deltas[2] * deltas[2])
    inv = 1.0 / dist
    unit = [delta * inv for delta in deltas]
    if layer == 1:
        chan = [jnp.where(values[3] == float(c), 1.0, 0.0) for c in range(SPECIES)]
    else:
        chan = list(values[3:])
    return hi, lo, weight, dist, inv, unit, chan


def radial_terms(dist, rad_ref, with_slope):
    scaled = dist * (2.0 / cutoff_radius) - 1.0
    inside = dist < cutoff_radius
    angle = dist * (math.pi / cutoff_radius)
    cutoff = jnp.where(inside, 0.5 * (jnp.cos(angle) + 1.0), 0.0)
    cheb = [None, scaled]
    twice = 2.0 * scaled
    cheb.append(twice * scaled - 1.0)
    for _ in range(3, NRAD):
        cheb.append(twice * cheb[-1] - cheb[-2])
    basis = [cutoff] + [cutoff * cheb[p] for p in range(1, NRAD)]
    radial = []
    for n in range(NMAX):
        total = basis[0] * rad_ref[n, 0]
        for p in range(1, NRAD):
            total = total + basis[p] * rad_ref[n, p]
        radial.append(total)
    if not with_slope:
        return basis, radial, None
    slope_cut = jnp.where(inside, (-0.5 * math.pi / cutoff_radius) * jnp.sin(angle), 0.0)
    grad_scaled = cutoff * (2.0 / cutoff_radius)
    second = [None, None, twice]
    second[1] = jnp.ones_like(scaled)
    for _ in range(3, NRAD):
        second.append(twice * second[-1] - second[-2])
    slopes = [slope_cut, slope_cut * scaled + grad_scaled]
    for p in range(2, NRAD):
        slopes.append(slope_cut * cheb[p] + grad_scaled * (float(p) * second[p]))
    return basis, radial, slopes


def harmonic_list(unit):
    table = scaled_legendre(unit[2])
    cosines, sines = azimuth_powers(unit[0], unit[1])
    columns = []
    for degree in range(LMAX + 1):
        for signed in range(-degree, degree + 1):
            azimuth = abs(signed)
            poly = table[degree, azimuth]
            if signed == 0:
                columns.append(poly)
            elif signed > 0:
                columns.append(poly * cosines[azimuth])
            else:
                columns.append(poly * sines[azimuth])
    columns[0] = jnp.full_like(unit[2], columns[0])
    return columns


def density_kernel(layer, cnt_ref, row_ref, rad_ref, tab_ref, cen_ref, idx_ref, wt_ref, out_ref,
                   x_ref, y_ref, d_ref):
    tile = pl.program_id(0)
    count = cnt_ref[tile]
    row_low, row_high = row_ref[0, tile], row_ref[1, tile]
    blocks = lax.div(count + 7, 8)

    def edges(block_at, carry):
        base = pl.multiple_of(block_at * 8, 8)
        hi, lo, weight, dist, inv, unit, chan = edge_block(
            layer, tab_ref, cen_ref, idx_ref, wt_ref, block_at, row_low, row_high
        )
        _, radial, _ = radial_terms(dist, rad_ref, False)
        for c in range(SPECIES):
            scale = chan[c] * weight
            for n in range(NMAX):
                x_ref[pl.ds(base * CH + (c * NMAX + n), 8, stride=CH), :] = scale * radial[n]
        for at, column in enumerate(harmonic_list(unit)):
            y_ref[pl.ds(at * NPAD + base, 8), :] = column
        return carry

    lax.fori_loop(0, blocks, edges, 0)
    pairs = lax.div(count + 1, 2)

    def lm_block(block_at, carry):
        first = block_at * LBLK

        def slots(pair, acc):
            acc = list(acc)
            for part in range(2):
                slot = pair * 2 + part
                rows = [
                    x_ref[pl.ds(pl.multiple_of(slot * CH + 8 * j, 8), 8), :] for j in range(CH // 8)
                ]
                for at in range(LBLK):
                    line = jnp.broadcast_to(
                        y_ref[pl.ds((first + at) * NPAD + slot, 1), :], (8, TILE)
                    )
                    for j in range(CH // 8):
                        acc[at * (CH // 8) + j] = acc[at * (CH // 8) + j] + rows[j] * line
            return tuple(acc)

        zero = jnp.zeros((8, TILE), f32)
        acc = lax.fori_loop(0, pairs, slots, tuple(zero for _ in range(LBLK * (CH // 8))))
        for at in range(LBLK):
            for j in range(CH // 8):
                d_ref[pl.ds(8 * j * LM + first + at, 8, stride=LM), :] = acc[at * (CH // 8) + j]
        return carry

    lax.fori_loop(0, LM // LBLK, lm_block, 0)
    out_ref[...] = d_ref[...].astype(bf16)


def smem_spec():
    return pl.BlockSpec(memory_space=pltpu.SMEM)


def tile_spec(rows):
    return pl.BlockSpec((rows, TILE), lambda i: (0, i))


def whole_spec(shape):
    return pl.BlockSpec(shape, lambda i: tuple(0 for _ in shape))


def density_call(layer, counts, rows, radial, table, centres, index, weight):
    atoms = centres.shape[1]
    return pl.pallas_call(
        partial(density_kernel, layer),
        out_shape=jax.ShapeDtypeStruct((DENS, atoms), bf16),
        grid=(atoms // TILE,),
        in_specs=[
            smem_spec(),
            smem_spec(),
            smem_spec(),
            whole_spec(table.shape),
            tile_spec(8),
            tile_spec(NPAD),
            tile_spec(NPAD),
        ],
        out_specs=tile_spec(DENS),
        scratch_shapes=[
            pltpu.VMEM((NPAD * CH, TILE), f32),
            pltpu.VMEM((LM * NPAD, TILE), f32),
            pltpu.VMEM((DENS, TILE), f32),
        ],
        compiler_params=pltpu.CompilerParams(vmem_limit_bytes=48 << 20),
        name="density_%d" % layer,
    )(counts, rows, radial, table, centres, index, weight)


def backward_kernel(layer, cnt_ref, row_ref, rad_ref, tab_ref, cen_ref, idx_ref, wt_ref, dd_ref,
                    win_ref, own_ref, rgr_ref, x_ref, y_ref, gx_ref, gy_ref, val_ref):
    tile = pl.program_id(0)
    count = cnt_ref[tile]
    row_low, row_high = row_ref[0, tile], row_ref[1, tile]
    blocks = lax.div(count + 7, 8)
    chunks = lax.div(count + 31, 32)

    @pl.when(tile == 0)
    def _():
        win_ref[...] = jnp.zeros_like(win_ref)
        rgr_ref[...] = jnp.zeros_like(rgr_ref)

    def edges(block_at, carry):
        base = pl.multiple_of(block_at * 8, 8)
        hi, lo, weight, dist, inv, unit, chan = edge_block(
            layer, tab_ref, cen_ref, idx_ref, wt_ref, block_at, row_low, row_high
        )
        _, radial, _ = radial_terms(dist, rad_ref, False)
        for c in range(SPECIES):
            scale = chan[c] * weight
            for n in range(NMAX):
                x_ref[pl.ds((c * NMAX + n) * NPAD + base, 8), :] = scale * radial[n]
        for at, column in enumerate(harmonic_list(unit)):
            y_ref[pl.ds(at * NPAD + base, 8), :] = column
        return carry

    lax.fori_loop(0, chunks * 4, edges, 0)

    zero = jnp.zeros((8, TILE), f32)

    def chunk_body(chunk, carry):
        start = pl.multiple_of(chunk * 32, 32)

        def m_block(block_at, inner):
            def over_lm(lm, acc):
                acc = list(acc)
                lines = [
                    jnp.broadcast_to(dd_ref[pl.ds((block_at * 8 + i) * LM + lm, 1), :], (8, TILE))
                    for i in range(8)
                ]
                for kb in range(4):
                    col = y_ref[pl.ds(pl.multiple_of(lm * NPAD + start + 8 * kb, 8), 8), :]
                    for i in range(8):
                        acc[i * 4 + kb] = acc[i * 4 + kb] + lines[i] * col
                return tuple(acc)

            acc = lax.fori_loop(0, LM, over_lm, tuple(zero for _ in range(32)))
            for i in range(8):
                for kb in range(4):
                    at = pl.multiple_of((block_at * 8 + i) * NPAD + start + 8 * kb, 8)
                    gx_ref[pl.ds(at, 8), :] = acc[i * 4 + kb]
            return inner

        lax.fori_loop(0, CH // 8, m_block, 0)

        def lm_block(block_at, inner):
            def over_m(m, acc):
                acc = list(acc)
                lines = [
                    jnp.broadcast_to(dd_ref[pl.ds(m * LM + block_at * LBLK + i, 1), :], (8, TILE))
                    for i in range(LBLK)
                ]
                for kb in range(4):
                    col = x_ref[pl.ds(pl.multiple_of(m * NPAD + start + 8 * kb, 8), 8), :]
                    for i in range(LBLK):
                        acc[i * 4 + kb] = acc[i * 4 + kb] + lines[i] * col
                return tuple(acc)

            acc = lax.fori_loop(0, CH, over_m, tuple(zero for _ in range(LBLK * 4)))
            for i in range(LBLK):
                for kb in range(4):
                    at = pl.multiple_of((block_at * LBLK + i) * NPAD + start + 8 * kb, 8)
                    gy_ref[pl.ds(at, 8), :] = acc[i * 4 + kb]
            return inner

        lax.fori_loop(0, LM // LBLK, lm_block, 0)
        return carry

    lax.fori_loop(0, chunks, chunk_body, 0)

    def finish(block_at, own):
        base = pl.multiple_of(block_at * 8, 8)
        hi, lo, weight, dist, inv, unit, chan = edge_block(
            layer, tab_ref, cen_ref, idx_ref, wt_ref, block_at, row_low, row_high
        )
        basis, radial, slopes = radial_terms(dist, rad_ref, True)
        feat_grads = []
        radial_grads = [None] * NMAX
        for c in range(SPECIES):
            total = None
            for n in range(NMAX):
                grad = gx_ref[pl.ds((c * NMAX + n) * NPAD + base, 8), :]
                term = grad * radial[n]
                total = term if total is None else total + term
                piece = grad * chan[c]
                radial_grads[n] = piece if c == 0 else radial_grads[n] + piece
            feat_grads.append(total * weight)
        grad_r = None
        radial_grads = [grad * weight for grad in radial_grads]
        for p in range(NRAD):
            total = None
            for n in range(NMAX):
                at = (n * NRAD + p) * 8
                rgr_ref[pl.ds(at, 8), :] = rgr_ref[pl.ds(at, 8), :] + radial_grads[n] * basis[p]
                term = radial_grads[n] * rad_ref[n, p]
                total = term if total is None else total + term
            term = total * slopes[p]
            grad_r = term if grad_r is None else grad_r + term
        table = scaled_legendre(unit[2])
        cosines, sines = azimuth_powers(unit[0], unit[1])
        grad_x = grad_y = grad_z = None

        def plus(total, term):
            return term if total is None else total + term

        for azimuth in range(LMAX + 1):
            grad_cos = grad_sin = None
            for degree in range(azimuth, LMAX + 1):
                at = degree * degree + degree
                up = gy_ref[pl.ds((at + azimuth) * NPAD + base, 8), :]
                poly = table[degree, azimuth]
                if azimuth:
                    down = gy_ref[pl.ds((at - azimuth) * NPAD + base, 8), :]
                    grad_cos = plus(grad_cos, up * poly)
                    grad_sin = plus(grad_sin, down * poly)
                if degree > azimuth:
                    ratio = norm_of(degree, azimuth) / norm_of(degree, azimuth + 1)
                    slope = ratio * table[degree, azimuth + 1]
                    if azimuth:
                        grad_z = plus(grad_z, slope * (up * cosines[azimuth] + down * sines[azimuth]))
                    else:
                        grad_z = plus(grad_z, slope * up)
            if azimuth == 1:
                grad_x, grad_y = grad_cos, grad_sin
            elif azimuth > 1:
                below_cos, below_sin = cosines[azimuth - 1], sines[azimuth - 1]
                grad_x = grad_x + float(azimuth) * (grad_cos * below_cos + grad_sin * below_sin)
                grad_y = grad_y + float(azimuth) * (grad_sin * below_cos - grad_cos * below_sin)
        dot_u = grad_x * unit[0] + grad_y * unit[1] + grad_z * unit[2]
        live = weight > 0.0
        out = []
        for axis, grad in enumerate((grad_x, grad_y, grad_z)):
            value = (grad - dot_u * unit[axis]) * inv + grad_r * unit[axis]
            out.append(jnp.where(live, value, 0.0))
        values = out + feat_grads
        for at, value in enumerate(values):
            val_ref[pl.ds(at * NPAD + base, 8), :] = value
        return tuple(total + value for total, value in zip(own, out))

    own = lax.fori_loop(0, blocks, finish, (zero, zero, zero))
    own_ref[...] = jnp.concatenate(
        [jnp.sum(total, axis=0, keepdims=True) for total in own] + [jnp.zeros((5, TILE), f32)], axis=0
    )

    used = 3 if layer == 1 else NVAL
    sub = lax.broadcasted_iota(jnp.int32, (TILE, TILE), 0)
    windows = lax.div(row_high - row_low + WROWS, WROWS)

    def window(window_at, carry):
        row_base = row_low + window_at * WROWS

        def slot_block(block_at, acc):
            base = pl.multiple_of(block_at * 8, 8)
            index = idx_ref[pl.ds(base, 8), :]
            hi = lax.shift_right_logical(index, 7)
            lo = lax.bitwise_and(index, 127)
            tops, lows = [], []
            for value_at in range(used):
                value = val_ref[pl.ds(value_at * NPAD + base, 8), :]
                for row in range(WROWS):
                    tops.append(jnp.where(hi == row_base + row, value, 0.0))
            stacked = jnp.stack(tops, axis=0)
            ones, left = [], []
            for part in range(8):
                line = jnp.broadcast_to(lo[part : part + 1, :], (TILE, TILE))
                ones.append(jnp.where(line == sub, 1.0, 0.0).astype(bf16))
                left.append(stacked[:, part, :])
            left = jnp.concatenate(left, axis=1)
            ones = jnp.concatenate(ones, axis=1)
            high = left.astype(bf16)
            rest = (left - high.astype(f32)).astype(bf16)
            dims = (((1,), (1,)), ((), ()))
            acc = acc + lax.dot_general(high, ones, dims, preferred_element_type=f32)
            return acc + lax.dot_general(rest, ones, dims, preferred_element_type=f32)

        acc = lax.fori_loop(0, blocks, slot_block, jnp.zeros((used * WROWS, TILE), f32))
        for value_at in range(used):
            at = value_at * 32 + row_base
            win_ref[pl.ds(at, WROWS), :] = (
                win_ref[pl.ds(at, WROWS), :] + acc[value_at * WROWS : (value_at + 1) * WROWS]
            )
        return carry

    lax.fori_loop(0, windows, window, 0)


def backward_call(layer, counts, rows, radial, table, centres, index, weight, grad_dens):
    atoms = centres.shape[1]
    return pl.pallas_call(
        partial(backward_kernel, layer),
        out_shape=(
            jax.ShapeDtypeStruct((NVAL * 32, TILE), f32),
            jax.ShapeDtypeStruct((8, atoms), f32),
            jax.ShapeDtypeStruct((NMAX * NRAD * 8, TILE), f32),
        ),
        grid=(atoms // TILE,),
        in_specs=[
            smem_spec(),
            smem_spec(),
            smem_spec(),
            whole_spec(table.shape),
            tile_spec(8),
            tile_spec(NPAD),
            tile_spec(NPAD),
            tile_spec(DENS),
        ],
        out_specs=(
            whole_spec((NVAL * 32, TILE)),
            tile_spec(8),
            whole_spec((NMAX * NRAD * 8, TILE)),
        ),
        scratch_shapes=[
            pltpu.VMEM((CH * NPAD, TILE), f32),
            pltpu.VMEM((LM * NPAD, TILE), f32),
            pltpu.VMEM((CH * NPAD, TILE), f32),
            pltpu.VMEM((LM * NPAD, TILE), f32),
            pltpu.VMEM((NVAL * NPAD, TILE), f32),
        ],
        compiler_params=pltpu.CompilerParams(vmem_limit_bytes=48 << 20),
        name="backward_%d" % layer,
    )(counts, rows, radial, table, centres, index, weight, grad_dens)


def feature_map(invariants, mixing):
    inverse_rms = lax.rsqrt(jnp.mean(invariants * invariants, axis=0) + norm_eps)
    return jnp.einsum("qk,qa->ka", mixing, invariants, precision=highest) * inverse_rms


def small_solve(matrix, vector):
    order_n = matrix.shape[0]
    rows_now = [matrix[row_at] for row_at in range(order_n)]
    rights_now = [vector[row_at] for row_at in range(order_n)]
    for pivot_at in range(order_n):
        for below_at in range(pivot_at + 1, order_n):
            ratio_now = rows_now[below_at][pivot_at] / rows_now[pivot_at][pivot_at]
            rows_now[below_at] = rows_now[below_at] - ratio_now * rows_now[pivot_at]
            rights_now[below_at] = rights_now[below_at] - ratio_now * rights_now[pivot_at]
    answer = [None] * order_n
    for row_at in range(order_n - 1, -1, -1):
        running = rights_now[row_at]
        for later_at in range(row_at + 1, order_n):
            running = running - rows_now[row_at][later_at] * answer[later_at]
        answer[row_at] = running / rows_now[row_at][row_at]
    return jnp.stack(answer)


def contract(dens_in, coupling):
    factors = jnp.einsum("vdq,da->vqa", coupling, dens_in, preferred_element_type=f32)
    product = reduce(
        lambda earlier, later: earlier * later,
        [factors[index_v] for index_v in range(factors.shape[0])],
    )
    return (factors, product)


def contract_back(factors, upstream, coupling):
    partials = []
    for factor_at in range(factors.shape[0]):
        others = upstream
        for partner in range(factors.shape[0]):
            if partner != factor_at:
                others = others * factors[partner]
        partials.append(others)
    rounded = jnp.stack(partials).astype(bf16)
    return jnp.einsum("vdq,vqa->da", coupling, rounded, preferred_element_type=f32)


def as_rows(values, atoms):
    return values.reshape(values.shape[0] * (atoms // TILE), TILE)


def per_device(
    positions,
    species,
    neighbours,
    slot_counts,
    structure,
    target_energy,
    radial_one,
    coupling_one,
    coefficient_one,
    mixing,
    radial_two,
    coupling_two,
    coefficient_two,
):
    atoms = positions.shape[2]
    tiles = atoms // TILE
    centres = positions[:, 0, :]
    own_species = species[0]
    onehot = (own_species[None, :] == jnp.arange(SPECIES, dtype=jnp.int32)[:, None]).astype(f32)
    site = jnp.concatenate([centres, own_species.astype(f32)[None, :]], axis=0)
    site_left, site_right = shift_pair(site, "dom")
    site_ext = jnp.stack([site_left, site, site_right], axis=1)
    table_one = site_ext.reshape(4 * 3 * tiles, TILE)

    index = neighbours[:, 0, :] - (lax.axis_index("dom") - 1) * atoms
    live = jnp.arange(NBR, dtype=jnp.int32)[:, None] < slot_counts[0][None, :]
    own_row = jnp.broadcast_to(
        (jnp.arange(atoms, dtype=jnp.int32) // TILE + tiles)[None, :], (NBR, atoms)
    )
    block_row = jnp.where(live, index // TILE, own_row)
    counts = jnp.max(slot_counts[0].reshape(tiles, TILE), axis=1)
    row_low = jnp.min(block_row.reshape(NBR, tiles, TILE), axis=(0, 2))
    row_high = jnp.max(block_row.reshape(NBR, tiles, TILE), axis=(0, 2))
    rows = jnp.stack([row_low, row_high])
    pad = ((0, NPAD - NBR), (0, 0))
    index = jnp.pad(jnp.where(live, index, 0), pad)
    weight = jnp.pad(jnp.where(live, density_scale, 0.0).astype(f32), pad)
    centres8 = jnp.pad(centres, ((0, 5), (0, 0)))

    dens_one = density_call(1, counts, rows, radial_one, table_one, centres8, index, weight)
    factors_one, invariants_one = contract(dens_one, coupling_one)
    chosen_one = jnp.dot(coefficient_one.T, onehot, precision=highest)
    energy_one = jnp.sum(invariants_one * chosen_one, axis=0)
    features, features_back = jax.vjp(feature_map, invariants_one, mixing)
    feat_left, feat_right = shift_pair(features, "dom")
    feat_ext = jnp.stack([feat_left, features, feat_right], axis=1)
    table_two = jnp.concatenate(
        [table_one[: 3 * 3 * tiles], feat_ext.reshape(SPECIES * 3 * tiles, TILE)], axis=0
    )
    dens_two = density_call(2, counts, rows, radial_two, table_two, centres8, index, weight)
    factors_two, invariants_two = contract(dens_two, coupling_two)
    chosen_two = jnp.dot(coefficient_two.T, onehot, precision=highest)
    site_energy = energy_one + jnp.sum(invariants_two * chosen_two, axis=0)
    structure_ids = structure[0]
    slots_total = target_energy.shape[1]
    energy_part = jax.ops.segment_sum(site_energy, structure_ids, num_segments=slots_total)
    count_part = jax.ops.segment_sum(onehot.T, structure_ids, num_segments=slots_total)
    energy_sum, species_count = lax.psum((energy_part, count_part), "dom")
    atom_total = jnp.maximum(jnp.sum(species_count, axis=1), 1.0)
    fraction = species_count / atom_total[:, None]
    gram_part = jnp.dot(fraction.T, fraction, precision=highest)
    right_part = jnp.dot(fraction.T, target_energy[0], precision=highest)
    gram_matrix, right_side = lax.psum((gram_part, right_part), "grp")
    offsets = small_solve(gram_matrix + ridge_weight * jnp.eye(SPECIES, dtype=f32), right_side)
    energies = energy_sum / atom_total + jnp.dot(fraction, offsets, precision=highest)

    def unpack(window, own):
        spread = window.reshape(NVAL, 32, TILE)[:, : 3 * tiles].reshape(NVAL, 3, atoms)
        return spread

    grad_dens_two = contract_back(factors_two, chosen_two, coupling_two)
    window_two, own_two, rgr_two = backward_call(
        2, counts, rows, radial_two, table_two, centres8, index, weight, grad_dens_two
    )
    spread_two = unpack(window_two, own_two)
    feat_spread = spread_two[3:]
    from_right = lax.ppermute(
        feat_spread[:, 0], "dom", [(i + 1, i) for i in range(lax.axis_size("dom") - 1)]
    )
    from_left = lax.ppermute(
        feat_spread[:, 2], "dom", [(i, i + 1) for i in range(lax.axis_size("dom") - 1)]
    )
    grad_features = feat_spread[:, 1] + from_right + from_left
    coefficient_second = jnp.dot(onehot, invariants_two.T, precision=highest)
    grad_invariants, mixing_gradient = features_back(grad_features)
    grad_dens_one = contract_back(factors_one, chosen_one + grad_invariants, coupling_one)
    window_one, own_one, rgr_one = backward_call(
        1, counts, rows, radial_one, table_one, centres8, index, weight, grad_dens_one
    )
    spread_one = unpack(window_one, own_one)
    coefficient_first = jnp.dot(onehot, invariants_one.T, precision=highest)
    pos_spread = spread_one[:3] + spread_two[:3]
    pos_right = lax.ppermute(
        pos_spread[:, 0], "dom", [(i + 1, i) for i in range(lax.axis_size("dom") - 1)]
    )
    pos_left = lax.ppermute(
        pos_spread[:, 2], "dom", [(i, i + 1) for i in range(lax.axis_size("dom") - 1)]
    )
    forces = (own_one[:3] + own_two[:3]) - pos_spread[:, 1] - pos_right - pos_left

    def radial_sum(partial_grad):
        return jnp.sum(partial_grad.reshape(NMAX, NRAD, 8 * TILE), axis=2)

    radial_first, coefficient_first, mixing_gradient, radial_second, coefficient_second = lax.psum(
        (
            radial_sum(rgr_one),
            coefficient_first,
            mixing_gradient,
            radial_sum(rgr_two),
            coefficient_second,
        ),
        ("dom", "grp"),
    )
    return (
        energies[None, :],
        offsets,
        forces[:, None, :],
        radial_first,
        coefficient_first,
        mixing_gradient,
        radial_second,
        coefficient_second,
    )


def solution(mesh):
    in_specs = (
        P(None, "grp", "dom"),
        P("grp", "dom"),
        P(None, "grp", "dom"),
        P("grp", "dom"),
        P("grp", "dom"),
        P("grp", None),
        P(),
        P(),
        P(),
        P(),
        P(),
        P(),
        P(),
    )
    out_specs = (P("grp", None), P(), P(None, "grp", "dom"), P(), P(), P(), P(), P())
    return jax.shard_map(
        per_device, mesh=mesh, in_specs=in_specs, out_specs=out_specs, check_vma=False
    )
```

```python
from functools import partial, reduce
import math

import jax
import jax.numpy as jnp
from jax import lax
from jax.experimental import pallas as pl
from jax.experimental.pallas import tpu as pltpu
from jax.sharding import PartitionSpec as P

NRAD = 12
NMAX = 10
LMAX = 6
LM = 49
SPECIES = 4
CH = SPECIES * NMAX
DENS = CH * LM
NBR = 48
NPAD = 64
TILE = 128
LBLK = 7
WROWS = 4
NVAL = 7
SLOTS = 4

cutoff_radius = 5.0
density_scale = 0.17
norm_eps = 1e-05
ridge_weight = 0.1
highest = lax.Precision.HIGHEST
f32 = jnp.float32
bf16 = jnp.bfloat16


def shift_pair(cells, axis):
    count = lax.axis_size(axis)
    ends = count - 1
    left = lax.ppermute(cells, axis, [(i, i + 1) for i in range(ends)])
    right = lax.ppermute(cells, axis, [(i + 1, i) for i in range(ends)])
    return left, right


def double_factorial(number):
    result = 1.0
    while number > 1:
        result = result * number
        number = number - 2
    return result


def norm_of(degree, azimuth):
    value = math.sqrt(
        (2 * degree + 1)
        / (4 * math.pi)
        * math.factorial(degree - azimuth)
        / math.factorial(degree + azimuth)
    )
    return value * (math.sqrt(2.0) if azimuth else 1.0)


def scaled_legendre(coord_z):
    table = {}
    for azimuth in range(LMAX + 1):
        table[azimuth, azimuth] = norm_of(azimuth, azimuth) * double_factorial(2 * azimuth - 1)
        if azimuth + 1 <= LMAX:
            ratio = norm_of(azimuth + 1, azimuth) / norm_of(azimuth, azimuth)
            table[azimuth + 1, azimuth] = coord_z * (
                (2 * azimuth + 1) * ratio * table[azimuth, azimuth]
            )
        for degree in range(azimuth + 2, LMAX + 1):
            gap = degree - azimuth
            first = (2 * degree - 1) / gap * norm_of(degree, azimuth) / norm_of(degree - 1, azimuth)
            second = (
                (degree + azimuth - 1) / gap * norm_of(degree, azimuth) / norm_of(degree - 2, azimuth)
            )
            table[degree, azimuth] = (first * coord_z) * table[degree - 1, azimuth] - (
                second * table[degree - 2, azimuth]
            )
    return table


def azimuth_powers(coord_x, coord_y):
    cosines = [None, coord_x]
    sines = [None, coord_y]
    for _ in range(2, LMAX + 1):
        cosines.append(cosines[-1] * coord_x - sines[-1] * coord_y)
        sines.append(sines[-1] * coord_x + cosines[-2] * coord_y)
    return cosines, sines


LANE_GATHER = lax.GatherDimensionNumbers(
    offset_dims=(),
    collapsed_slice_dims=(1,),
    start_index_map=(1,),
    operand_batching_dims=(0,),
    start_indices_batching_dims=(0,),
)


def lane_gather(line, lo):
    return lax.gather(
        line,
        lo[..., None],
        LANE_GATHER,
        slice_sizes=(1, 1),
        mode=lax.GatherScatterMode.PROMISE_IN_BOUNDS,
    )


def prepare_kernel(first_ref, cnt_ref, nbr_ref, idx_ref, wt_ref, info_ref, key_ref, pos_ref):
    tile = pl.program_id(0)
    limit = cnt_ref[...]
    iota = lax.broadcasted_iota(jnp.int32, (NBR, TILE), 0)
    live = iota < limit
    index = nbr_ref[...] - first_ref[0]
    key = jnp.where(live, index, -1 - iota)
    key_ref[...] = key
    keys = [key[8 * b : 8 * b + 8] for b in range(NBR // 8)]
    sub = lax.broadcasted_iota(jnp.int32, (8, TILE), 0)
    blocks = NBR // 8
    total = [jnp.zeros((8, TILE), jnp.int32) for _ in range(blocks)]
    early = [jnp.zeros((8, TILE), jnp.int32) for _ in range(blocks)]
    for other in range(NBR):
        line = jnp.broadcast_to(key_ref[other : other + 1, :], (8, TILE))
        for b in range(blocks):
            same = jnp.where(keys[b] == line, 1, 0)
            total[b] = total[b] + same
            if other < 8 * b:
                early[b] = early[b] + same
            elif other < 8 * b + 7:
                early[b] = early[b] + jnp.where(sub > other - 8 * b, same, 0)
    packed, first = [], []
    for b in range(blocks):
        alive = sub + 8 * b < limit
        first.append(jnp.where(alive & (early[b] == 0), 1, 0))
        packed.append(total[b] * 4096 + keys[b])
    for b in range(blocks):
        pos_ref[8 * b : 8 * b + 8, :] = first[b]
    place = [jnp.zeros((8, TILE), jnp.int32) for _ in range(blocks)]
    running = jnp.zeros((1, TILE), jnp.int32)
    lines = []
    for slot in range(NBR):
        flag = pos_ref[slot : slot + 1, :]
        lines.append(jnp.where(flag == 1, running, -1))
        running = running + flag
    for b in range(blocks):
        key_ref[8 * b : 8 * b + 8, :] = packed[b]
    out = place
    for slot in range(NBR):
        where_to = jnp.broadcast_to(lines[slot], (8, TILE))
        line = jnp.broadcast_to(key_ref[slot : slot + 1, :], (8, TILE))
        for b in range(slot // 8 + 1):
            out[b] = jnp.where(where_to == sub + 8 * b, line, out[b])
    zero = jnp.zeros((8, TILE), jnp.int32)
    for b in range(NPAD // 8):
        word = out[b] if b < blocks else zero
        idx_ref[8 * b : 8 * b + 8, :] = lax.bitwise_and(word, 4095)
        wt_ref[8 * b : 8 * b + 8, :] = density_scale * lax.shift_right_logical(word, 12).astype(f32)
    used = jnp.max(running)
    info_ref[0, tile] = lax.div(used + 3, 4) * 4
    row = lax.shift_right_arithmetic(index, 7)
    info_ref[1, tile] = jnp.min(jnp.where(live, row, 1 << 20))
    info_ref[2, tile] = jnp.max(jnp.where(live, row, -1))


def prepare_call(first, limits, neighbours):
    atoms = neighbours.shape[1]
    return pl.pallas_call(
        prepare_kernel,
        out_shape=(
            jax.ShapeDtypeStruct((NPAD, atoms), jnp.int32),
            jax.ShapeDtypeStruct((NPAD, atoms), f32),
            jax.ShapeDtypeStruct((3, atoms // TILE), jnp.int32),
        ),
        grid=(atoms // TILE,),
        in_specs=[smem_spec(), tile_spec(1), tile_spec(NBR)],
        out_specs=(tile_spec(NPAD), tile_spec(NPAD), smem_spec()),
        scratch_shapes=[pltpu.VMEM((NBR, TILE), jnp.int32), pltpu.VMEM((NBR, TILE), jnp.int32)],
        name="prepare",
    )(first, limits, neighbours)


def fetch(tab_ref, names, hi, lo, row_low, row_high):
    def body(row, values):
        hit = hi == row
        out = []
        for name, value in zip(names, values):
            line = jnp.broadcast_to(tab_ref[pl.ds(name * 24 + row, 1), :], (8, TILE))
            got = lane_gather(line, lo)
            out.append(jnp.where(hit, got, value))
        return tuple(out)

    zero = jnp.zeros((8, TILE), f32)
    return lax.fori_loop(row_low, row_high + 1, body, tuple(zero for _ in names))


def edge_block(layer, tab_ref, cen_ref, idx_ref, wt_ref, block_at, row_low, row_high):
    base = pl.multiple_of(block_at * 8, 8)
    index = idx_ref[pl.ds(base, 8), :]
    weight = wt_ref[pl.ds(base, 8), :]
    hi = lax.shift_right_logical(index, 7)
    lo = lax.bitwise_and(index, 127)
    names = (0, 1, 2, 3) if layer == 1 else (0, 1, 2, 3, 4, 5, 6)
    values = fetch(tab_ref, names, hi, lo, row_low, row_high)
    live = weight > 0.0
    deltas = []
    for axis in range(3):
        centre = jnp.broadcast_to(cen_ref[pl.ds(axis, 1), :], (8, TILE))
        deltas.append(jnp.where(live, values[axis] - centre, 1.0))
    dist = jnp.sqrt(deltas[0] * deltas[0] + deltas[1] * deltas[1] + deltas[2] * deltas[2])
    inv = 1.0 / dist
    unit = [delta * inv for delta in deltas]
    if layer == 1:
        chan = [jnp.where(values[3] == float(c), 1.0, 0.0) for c in range(SPECIES)]
    else:
        chan = list(values[3:])
    return hi, lo, weight, dist, inv, unit, chan


def radial_terms(dist, rad_ref, with_slope):
    scaled = dist * (2.0 / cutoff_radius) - 1.0
    inside = dist < cutoff_radius
    angle = dist * (math.pi / cutoff_radius)
    cutoff = jnp.where(inside, 0.5 * (jnp.cos(angle) + 1.0), 0.0)
    cheb = [None, scaled]
    twice = 2.0 * scaled
    cheb.append(twice * scaled - 1.0)
    for _ in range(3, NRAD):
        cheb.append(twice * cheb[-1] - cheb[-2])
    basis = [cutoff] + [cutoff * cheb[p] for p in range(1, NRAD)]
    radial = []
    for n in range(NMAX):
        total = basis[0] * rad_ref[n, 0]
        for p in range(1, NRAD):
            total = total + basis[p] * rad_ref[n, p]
        radial.append(total)
    if not with_slope:
        return basis, radial, None
    slope_cut = jnp.where(inside, (-0.5 * math.pi / cutoff_radius) * jnp.sin(angle), 0.0)
    grad_scaled = cutoff * (2.0 / cutoff_radius)
    second = [None, None, twice]
    second[1] = jnp.ones_like(scaled)
    for _ in range(3, NRAD):
        second.append(twice * second[-1] - second[-2])
    slopes = [slope_cut, slope_cut * scaled + grad_scaled]
    for p in range(2, NRAD):
        slopes.append(slope_cut * cheb[p] + grad_scaled * (float(p) * second[p]))
    return basis, radial, slopes


def harmonic_list(unit):
    table = scaled_legendre(unit[2])
    cosines, sines = azimuth_powers(unit[0], unit[1])
    columns = []
    for degree in range(LMAX + 1):
        for signed in range(-degree, degree + 1):
            azimuth = abs(signed)
            poly = table[degree, azimuth]
            if signed == 0:
                columns.append(poly)
            elif signed > 0:
                columns.append(poly * cosines[azimuth])
            else:
                columns.append(poly * sines[azimuth])
    columns[0] = jnp.full_like(unit[2], columns[0])
    return columns


def density_kernel(layer, info_ref, rad_ref, tab_ref, cen_ref, idx_ref, wt_ref, out_ref,
                   x_ref, y_ref, d_ref):
    tile = pl.program_id(0)
    count = info_ref[0, tile]
    row_low, row_high = info_ref[1, tile], info_ref[2, tile]
    blocks = lax.div(count + 7, 8)

    def edges(block_at, carry):
        base = pl.multiple_of(block_at * 8, 8)
        hi, lo, weight, dist, inv, unit, chan = edge_block(
            layer, tab_ref, cen_ref, idx_ref, wt_ref, block_at, row_low, row_high
        )
        _, radial, _ = radial_terms(dist, rad_ref, False)
        for c in range(SPECIES):
            scale = chan[c] * weight
            for n in range(NMAX):
                x_ref[pl.ds(base * CH + (c * NMAX + n), 8, stride=CH), :] = scale * radial[n]
        for at, column in enumerate(harmonic_list(unit)):
            y_ref[pl.ds(at * NPAD + base, 8), :] = column
        return carry

    lax.fori_loop(0, blocks, edges, 0)
    groups = lax.div(count, SLOTS)

    def lm_block(block_at, carry):
        first = block_at * LBLK

        def slots(group, acc):
            acc = list(acc)
            for part in range(SLOTS):
                slot = group * SLOTS + part
                rows = [
                    x_ref[pl.ds(pl.multiple_of(slot * CH + 8 * j, 8), 8), :] for j in range(CH // 8)
                ]
                for at in range(LBLK):
                    line = jnp.broadcast_to(
                        y_ref[pl.ds((first + at) * NPAD + slot, 1), :], (8, TILE)
                    )
                    for j in range(CH // 8):
                        acc[at * (CH // 8) + j] = acc[at * (CH // 8) + j] + rows[j] * line
            return tuple(acc)

        zero = jnp.zeros((8, TILE), f32)
        acc = lax.fori_loop(0, groups, slots, tuple(zero for _ in range(LBLK * (CH // 8))))
        for at in range(LBLK):
            for j in range(CH // 8):
                d_ref[pl.ds(8 * j * LM + first + at, 8, stride=LM), :] = acc[at * (CH // 8) + j]
        return carry

    lax.fori_loop(0, LM // LBLK, lm_block, 0)
    out_ref[...] = d_ref[...].astype(bf16)


def smem_spec():
    return pl.BlockSpec(memory_space=pltpu.SMEM)


def tile_spec(rows):
    return pl.BlockSpec((rows, TILE), lambda i: (0, i))


def whole_spec(shape):
    return pl.BlockSpec(shape, lambda i: tuple(0 for _ in shape))


def density_call(layer, info, radial, table, centres, index, weight):
    atoms = centres.shape[1]
    return pl.pallas_call(
        partial(density_kernel, layer),
        out_shape=jax.ShapeDtypeStruct((DENS, atoms), bf16),
        grid=(atoms // TILE,),
        in_specs=[
            smem_spec(),
            smem_spec(),
            whole_spec(table.shape),
            tile_spec(8),
            tile_spec(NPAD),
            tile_spec(NPAD),
        ],
        out_specs=tile_spec(DENS),
        scratch_shapes=[
            pltpu.VMEM((NPAD * CH, TILE), f32),
            pltpu.VMEM((LM * NPAD, TILE), f32),
            pltpu.VMEM((DENS, TILE), f32),
        ],
        compiler_params=pltpu.CompilerParams(vmem_limit_bytes=48 << 20),
        name="density_%d" % layer,
    )(info, radial, table, centres, index, weight)


def backward_kernel(layer, info_ref, rad_ref, tab_ref, cen_ref, idx_ref, wt_ref, dd_ref,
                    win_ref, own_ref, rgr_ref, x_ref, y_ref, gx_ref, gy_ref, val_ref):
    tile = pl.program_id(0)
    count = info_ref[0, tile]
    row_low, row_high = info_ref[1, tile], info_ref[2, tile]
    blocks = lax.div(count + 7, 8)
    chunks = lax.div(count + 31, 32)

    @pl.when(tile == 0)
    def _():
        win_ref[...] = jnp.zeros_like(win_ref)
        rgr_ref[...] = jnp.zeros_like(rgr_ref)

    def edges(block_at, carry):
        base = pl.multiple_of(block_at * 8, 8)
        hi, lo, weight, dist, inv, unit, chan = edge_block(
            layer, tab_ref, cen_ref, idx_ref, wt_ref, block_at, row_low, row_high
        )
        _, radial, _ = radial_terms(dist, rad_ref, False)
        if layer == 1:
            for n in range(NMAX):
                x_ref[pl.ds(n * NPAD + base, 8), :] = weight * radial[n]
            x_ref[pl.ds(NMAX * NPAD + base, 8), :] = chan[1] + chan[3]
            x_ref[pl.ds((NMAX + 1) * NPAD + base, 8), :] = chan[2] + chan[3]
        else:
            for c in range(SPECIES):
                scale = chan[c] * weight
                for n in range(NMAX):
                    x_ref[pl.ds((c * NMAX + n) * NPAD + base, 8), :] = scale * radial[n]
        for at, column in enumerate(harmonic_list(unit)):
            y_ref[pl.ds(at * NPAD + base, 8), :] = column
        return carry

    lax.fori_loop(0, chunks * 4, edges, 0)

    zero = jnp.zeros((8, TILE), f32)

    def chunk_body(chunk, carry):
        start = pl.multiple_of(chunk * 32, 32)

        def m_block(block_at, inner):
            def over_lm(step, acc):
                acc = list(acc)
                for part in range(LBLK):
                    lm = step * LBLK + part
                    cols = [
                        y_ref[pl.ds(pl.multiple_of(lm * NPAD + start + 8 * kb, 8), 8), :]
                        for kb in range(4)
                    ]
                    for i in range(8):
                        line = jnp.broadcast_to(
                            dd_ref[pl.ds((block_at * 8 + i) * LM + lm, 1), :], (8, TILE)
                        )
                        for kb in range(4):
                            acc[i * 4 + kb] = acc[i * 4 + kb] + line * cols[kb]
                return tuple(acc)

            acc = lax.fori_loop(0, LM // LBLK, over_lm, tuple(zero for _ in range(32)))
            for i in range(8):
                for kb in range(4):
                    at = pl.multiple_of((block_at * 8 + i) * NPAD + start + 8 * kb, 8)
                    gx_ref[pl.ds(at, 8), :] = acc[i * 4 + kb]
            return inner

        lax.fori_loop(0, CH // 8, m_block, 0)

        def lm_block(block_at, inner):
            def over_m(step, acc):
                acc = list(acc)
                for part in range(8):
                    m = step * 8 + part
                    cols = [
                        x_ref[pl.ds(pl.multiple_of(m * NPAD + start + 8 * kb, 8), 8), :]
                        for kb in range(4)
                    ]
                    for i in range(LBLK):
                        line = jnp.broadcast_to(
                            dd_ref[pl.ds(m * LM + block_at * LBLK + i, 1), :], (8, TILE)
                        )
                        for kb in range(4):
                            acc[i * 4 + kb] = acc[i * 4 + kb] + line * cols[kb]
                return tuple(acc)

            acc = lax.fori_loop(0, CH // 8, over_m, tuple(zero for _ in range(LBLK * 4)))
            for i in range(LBLK):
                for kb in range(4):
                    at = pl.multiple_of((block_at * LBLK + i) * NPAD + start + 8 * kb, 8)
                    gy_ref[pl.ds(at, 8), :] = acc[i * 4 + kb]
            return inner

        lax.fori_loop(0, LM // LBLK, lm_block, 0)
        return carry

    def species_chunk(chunk, carry):
        start = pl.multiple_of(chunk * 32, 32)
        for n in range(NMAX):
            for kb in range(4):
                gx_ref[pl.ds(pl.multiple_of(n * NPAD + start + 8 * kb, 8), 8), :] = zero

        def lm_block(block_at, inner):
            def over_n(n, acc):
                acc = list(acc)
                bits = []
                for which in range(2):
                    at = (NMAX + which) * NPAD + start
                    bits.append([x_ref[pl.ds(pl.multiple_of(at + 8 * kb, 8), 8), :] > 0.5 for kb in range(4)])
                scaled, sums = [], []
                for kb in range(4):
                    at = pl.multiple_of(n * NPAD + start + 8 * kb, 8)
                    scaled.append(x_ref[pl.ds(at, 8), :])
                    sums.append(gx_ref[pl.ds(at, 8), :])
                for i in range(LBLK):
                    lines = [
                        jnp.broadcast_to(
                            dd_ref[pl.ds((c * NMAX + n) * LM + block_at * LBLK + i, 1), :], (8, TILE)
                        )
                        for c in range(SPECIES)
                    ]
                    for kb in range(4):
                        even = jnp.where(bits[0][kb], lines[1], lines[0])
                        odd = jnp.where(bits[0][kb], lines[3], lines[2])
                        grad = jnp.where(bits[1][kb], odd, even)
                        at = (block_at * LBLK + i) * NPAD + start + 8 * kb
                        col = y_ref[pl.ds(pl.multiple_of(at, 8), 8), :]
                        acc[i * 4 + kb] = acc[i * 4 + kb] + grad * scaled[kb]
                        sums[kb] = sums[kb] + grad * col
                for kb in range(4):
                    at = pl.multiple_of(n * NPAD + start + 8 * kb, 8)
                    gx_ref[pl.ds(at, 8), :] = sums[kb]
                return tuple(acc)

            acc = lax.fori_loop(0, NMAX, over_n, tuple(zero for _ in range(LBLK * 4)))
            for i in range(LBLK):
                for kb in range(4):
                    at = pl.multiple_of((block_at * LBLK + i) * NPAD + start + 8 * kb, 8)
                    gy_ref[pl.ds(at, 8), :] = acc[i * 4 + kb]
            return inner

        lax.fori_loop(0, LM // LBLK, lm_block, 0)
        return carry

    lax.fori_loop(0, chunks, species_chunk if layer == 1 else chunk_body, 0)

    def finish(block_at, own):
        base = pl.multiple_of(block_at * 8, 8)
        hi, lo, weight, dist, inv, unit, chan = edge_block(
            layer, tab_ref, cen_ref, idx_ref, wt_ref, block_at, row_low, row_high
        )
        basis, radial, slopes = radial_terms(dist, rad_ref, True)
        feat_grads = []
        radial_grads = [None] * NMAX
        if layer == 1:
            radial_grads = [gx_ref[pl.ds(n * NPAD + base, 8), :] for n in range(NMAX)]
        for c in range(SPECIES if layer == 2 else 0):
            total = None
            for n in range(NMAX):
                grad = gx_ref[pl.ds((c * NMAX + n) * NPAD + base, 8), :]
                term = grad * radial[n]
                total = term if total is None else total + term
                piece = grad * chan[c]
                radial_grads[n] = piece if c == 0 else radial_grads[n] + piece
            feat_grads.append(total * weight)
        grad_r = None
        radial_grads = [grad * weight for grad in radial_grads]
        for p in range(NRAD):
            total = None
            for n in range(NMAX):
                at = (n * NRAD + p) * 8
                rgr_ref[pl.ds(at, 8), :] = rgr_ref[pl.ds(at, 8), :] + radial_grads[n] * basis[p]
                term = radial_grads[n] * rad_ref[n, p]
                total = term if total is None else total + term
            term = total * slopes[p]
            grad_r = term if grad_r is None else grad_r + term
        table = scaled_legendre(unit[2])
        cosines, sines = azimuth_powers(unit[0], unit[1])
        grad_x = grad_y = grad_z = None

        def plus(total, term):
            return term if total is None else total + term

        for azimuth in range(LMAX + 1):
            grad_cos = grad_sin = None
            for degree in range(azimuth, LMAX + 1):
                at = degree * degree + degree
                up = gy_ref[pl.ds((at + azimuth) * NPAD + base, 8), :]
                poly = table[degree, azimuth]
                if azimuth:
                    down = gy_ref[pl.ds((at - azimuth) * NPAD + base, 8), :]
                    grad_cos = plus(grad_cos, up * poly)
                    grad_sin = plus(grad_sin, down * poly)
                if degree > azimuth:
                    ratio = norm_of(degree, azimuth) / norm_of(degree, azimuth + 1)
                    slope = ratio * table[degree, azimuth + 1]
                    if azimuth:
                        grad_z = plus(grad_z, slope * (up * cosines[azimuth] + down * sines[azimuth]))
                    else:
                        grad_z = plus(grad_z, slope * up)
            if azimuth == 1:
                grad_x, grad_y = grad_cos, grad_sin
            elif azimuth > 1:
                below_cos, below_sin = cosines[azimuth - 1], sines[azimuth - 1]
                grad_x = grad_x + float(azimuth) * (grad_cos * below_cos + grad_sin * below_sin)
                grad_y = grad_y + float(azimuth) * (grad_sin * below_cos - grad_cos * below_sin)
        dot_u = grad_x * unit[0] + grad_y * unit[1] + grad_z * unit[2]
        live = weight > 0.0
        out = []
        for axis, grad in enumerate((grad_x, grad_y, grad_z)):
            value = (grad - dot_u * unit[axis]) * inv + grad_r * unit[axis]
            out.append(jnp.where(live, value, 0.0))
        values = out + feat_grads
        for at, value in enumerate(values):
            val_ref[pl.ds(at * NPAD + base, 8), :] = value
        return tuple(total + value for total, value in zip(own, out))

    own = lax.fori_loop(0, blocks, finish, (zero, zero, zero))
    own_ref[...] = jnp.concatenate(
        [jnp.sum(total, axis=0, keepdims=True) for total in own] + [jnp.zeros((5, TILE), f32)], axis=0
    )

    used = 3 if layer == 1 else NVAL
    sub = lax.broadcasted_iota(jnp.int32, (TILE, TILE), 0)
    windows = lax.div(row_high - row_low + WROWS, WROWS)

    def window(window_at, carry):
        row_base = row_low + window_at * WROWS

        def slot_block(block_at, acc):
            base = pl.multiple_of(block_at * 8, 8)
            index = idx_ref[pl.ds(base, 8), :]
            hi = lax.shift_right_logical(index, 7)
            lo = lax.bitwise_and(index, 127)
            tops, lows = [], []
            for value_at in range(used):
                value = val_ref[pl.ds(value_at * NPAD + base, 8), :]
                for row in range(WROWS):
                    tops.append(jnp.where(hi == row_base + row, value, 0.0))
            stacked = jnp.stack(tops, axis=0)
            ones, left = [], []
            for part in range(8):
                line = jnp.broadcast_to(lo[part : part + 1, :], (TILE, TILE))
                ones.append(jnp.where(line == sub, 1.0, 0.0).astype(bf16))
                left.append(stacked[:, part, :])
            left = jnp.concatenate(left, axis=1)
            ones = jnp.concatenate(ones, axis=1)
            high = left.astype(bf16)
            rest = (left - high.astype(f32)).astype(bf16)
            dims = (((1,), (1,)), ((), ()))
            acc = acc + lax.dot_general(high, ones, dims, preferred_element_type=f32)
            return acc + lax.dot_general(rest, ones, dims, preferred_element_type=f32)

        acc = lax.fori_loop(0, blocks, slot_block, jnp.zeros((used * WROWS, TILE), f32))
        for value_at in range(used):
            at = value_at * 32 + row_base
            win_ref[pl.ds(at, WROWS), :] = (
                win_ref[pl.ds(at, WROWS), :] + acc[value_at * WROWS : (value_at + 1) * WROWS]
            )
        return carry

    lax.fori_loop(0, windows, window, 0)


def backward_call(layer, info, radial, table, centres, index, weight, grad_dens):
    atoms = centres.shape[1]
    return pl.pallas_call(
        partial(backward_kernel, layer),
        out_shape=(
            jax.ShapeDtypeStruct((NVAL * 32, TILE), f32),
            jax.ShapeDtypeStruct((8, atoms), f32),
            jax.ShapeDtypeStruct((NMAX * NRAD * 8, TILE), f32),
        ),
        grid=(atoms // TILE,),
        in_specs=[
            smem_spec(),
            smem_spec(),
            whole_spec(table.shape),
            tile_spec(8),
            tile_spec(NPAD),
            tile_spec(NPAD),
            tile_spec(DENS),
        ],
        out_specs=(
            whole_spec((NVAL * 32, TILE)),
            tile_spec(8),
            whole_spec((NMAX * NRAD * 8, TILE)),
        ),
        scratch_shapes=[
            pltpu.VMEM((CH * NPAD, TILE), f32),
            pltpu.VMEM((LM * NPAD, TILE), f32),
            pltpu.VMEM((CH * NPAD, TILE), f32),
            pltpu.VMEM((LM * NPAD, TILE), f32),
            pltpu.VMEM((NVAL * NPAD, TILE), f32),
        ],
        compiler_params=pltpu.CompilerParams(vmem_limit_bytes=48 << 20),
        name="backward_%d" % layer,
    )(info, radial, table, centres, index, weight, grad_dens)


def feature_map(invariants, mixing):
    inverse_rms = lax.rsqrt(jnp.mean(invariants * invariants, axis=0) + norm_eps)
    return jnp.einsum("qk,qa->ka", mixing, invariants, precision=highest) * inverse_rms


def small_solve(matrix, vector):
    order_n = matrix.shape[0]
    rows_now = [matrix[row_at] for row_at in range(order_n)]
    rights_now = [vector[row_at] for row_at in range(order_n)]
    for pivot_at in range(order_n):
        for below_at in range(pivot_at + 1, order_n):
            ratio_now = rows_now[below_at][pivot_at] / rows_now[pivot_at][pivot_at]
            rows_now[below_at] = rows_now[below_at] - ratio_now * rows_now[pivot_at]
            rights_now[below_at] = rights_now[below_at] - ratio_now * rights_now[pivot_at]
    answer = [None] * order_n
    for row_at in range(order_n - 1, -1, -1):
        running = rights_now[row_at]
        for later_at in range(row_at + 1, order_n):
            running = running - rows_now[row_at][later_at] * answer[later_at]
        answer[row_at] = running / rows_now[row_at][row_at]
    return jnp.stack(answer)


def contract(dens_in, coupling):
    factors = jnp.einsum("vdq,da->vqa", coupling, dens_in, preferred_element_type=f32)
    product = reduce(
        lambda earlier, later: earlier * later,
        [factors[index_v] for index_v in range(factors.shape[0])],
    )
    return (factors, product)


def contract_back(factors, upstream, coupling):
    partials = []
    for factor_at in range(factors.shape[0]):
        others = upstream
        for partner in range(factors.shape[0]):
            if partner != factor_at:
                others = others * factors[partner]
        partials.append(others)
    rounded = jnp.stack(partials).astype(bf16)
    return jnp.einsum("vdq,vqa->da", coupling, rounded, preferred_element_type=f32)


def as_rows(values, atoms):
    return values.reshape(values.shape[0] * (atoms // TILE), TILE)


def per_device(
    positions,
    species,
    neighbours,
    slot_counts,
    structure,
    target_energy,
    radial_one,
    coupling_one,
    coefficient_one,
    mixing,
    radial_two,
    coupling_two,
    coefficient_two,
):
    atoms = positions.shape[2]
    tiles = atoms // TILE
    centres = positions[:, 0, :]
    own_species = species[0]
    onehot = (own_species[None, :] == jnp.arange(SPECIES, dtype=jnp.int32)[:, None]).astype(f32)
    site = jnp.concatenate([centres, own_species.astype(f32)[None, :]], axis=0)
    site_left, site_right = shift_pair(site, "dom")
    site_ext = jnp.stack([site_left, site, site_right], axis=1)
    table_one = site_ext.reshape(4 * 3 * tiles, TILE)

    first = ((lax.axis_index("dom") - 1) * atoms).astype(jnp.int32).reshape(1)
    index, weight, info = prepare_call(first, slot_counts, neighbours[:, 0, :])
    centres8 = jnp.pad(centres, ((0, 5), (0, 0)))

    dens_one = density_call(1, info, radial_one, table_one, centres8, index, weight)
    factors_one, invariants_one = contract(dens_one, coupling_one)
    chosen_one = jnp.dot(coefficient_one.T, onehot, precision=highest)
    energy_one = jnp.sum(invariants_one * chosen_one, axis=0)
    features, features_back = jax.vjp(feature_map, invariants_one, mixing)
    feat_left, feat_right = shift_pair(features, "dom")
    feat_ext = jnp.stack([feat_left, features, feat_right], axis=1)
    table_two = jnp.concatenate(
        [table_one[: 3 * 3 * tiles], feat_ext.reshape(SPECIES * 3 * tiles, TILE)], axis=0
    )
    dens_two = density_call(2, info, radial_two, table_two, centres8, index, weight)
    factors_two, invariants_two = contract(dens_two, coupling_two)
    chosen_two = jnp.dot(coefficient_two.T, onehot, precision=highest)
    site_energy = energy_one + jnp.sum(invariants_two * chosen_two, axis=0)
    structure_ids = structure[0]
    slots_total = target_energy.shape[1]
    energy_part = jax.ops.segment_sum(site_energy, structure_ids, num_segments=slots_total)
    count_part = jax.ops.segment_sum(onehot.T, structure_ids, num_segments=slots_total)
    energy_sum, species_count = lax.psum((energy_part, count_part), "dom")
    atom_total = jnp.maximum(jnp.sum(species_count, axis=1), 1.0)
    fraction = species_count / atom_total[:, None]
    gram_part = jnp.dot(fraction.T, fraction, precision=highest)
    right_part = jnp.dot(fraction.T, target_energy[0], precision=highest)
    gram_matrix, right_side = lax.psum((gram_part, right_part), "grp")
    offsets = small_solve(gram_matrix + ridge_weight * jnp.eye(SPECIES, dtype=f32), right_side)
    energies = energy_sum / atom_total + jnp.dot(fraction, offsets, precision=highest)

    def unpack(window, own):
        spread = window.reshape(NVAL, 32, TILE)[:, : 3 * tiles].reshape(NVAL, 3, atoms)
        return spread

    grad_dens_two = contract_back(factors_two, chosen_two, coupling_two)
    window_two, own_two, rgr_two = backward_call(
        2, info, radial_two, table_two, centres8, index, weight, grad_dens_two
    )
    spread_two = unpack(window_two, own_two)
    feat_spread = spread_two[3:]
    from_right = lax.ppermute(
        feat_spread[:, 0], "dom", [(i + 1, i) for i in range(lax.axis_size("dom") - 1)]
    )
    from_left = lax.ppermute(
        feat_spread[:, 2], "dom", [(i, i + 1) for i in range(lax.axis_size("dom") - 1)]
    )
    grad_features = feat_spread[:, 1] + from_right + from_left
    coefficient_second = jnp.dot(onehot, invariants_two.T, precision=highest)
    grad_invariants, mixing_gradient = features_back(grad_features)
    grad_dens_one = contract_back(factors_one, chosen_one + grad_invariants, coupling_one)
    window_one, own_one, rgr_one = backward_call(
        1, info, radial_one, table_one, centres8, index, weight, grad_dens_one
    )
    spread_one = unpack(window_one, own_one)
    coefficient_first = jnp.dot(onehot, invariants_one.T, precision=highest)
    pos_spread = spread_one[:3] + spread_two[:3]
    pos_right = lax.ppermute(
        pos_spread[:, 0], "dom", [(i + 1, i) for i in range(lax.axis_size("dom") - 1)]
    )
    pos_left = lax.ppermute(
        pos_spread[:, 2], "dom", [(i, i + 1) for i in range(lax.axis_size("dom") - 1)]
    )
    forces = (own_one[:3] + own_two[:3]) - pos_spread[:, 1] - pos_right - pos_left

    def radial_sum(partial_grad):
        return jnp.sum(partial_grad.reshape(NMAX, NRAD, 8 * TILE), axis=2)

    radial_first, coefficient_first, mixing_gradient, radial_second, coefficient_second = lax.psum(
        (
            radial_sum(rgr_one),
            coefficient_first,
            mixing_gradient,
            radial_sum(rgr_two),
            coefficient_second,
        ),
        ("dom", "grp"),
    )
    return (
        energies[None, :],
        offsets,
        forces[:, None, :],
        radial_first,
        coefficient_first,
        mixing_gradient,
        radial_second,
        coefficient_second,
    )


def solution(mesh):
    in_specs = (
        P(None, "grp", "dom"),
        P("grp", "dom"),
        P(None, "grp", "dom"),
        P("grp", "dom"),
        P("grp", "dom"),
        P("grp", None),
        P(),
        P(),
        P(),
        P(),
        P(),
        P(),
        P(),
    )
    out_specs = (P("grp", None), P(), P(None, "grp", "dom"), P(), P(), P(), P(), P())
    return jax.shard_map(
        per_device, mesh=mesh, in_specs=in_specs, out_specs=out_specs, check_vma=False
    )
```

```python
from functools import partial, reduce
import math

import jax
import jax.numpy as jnp
from jax import lax
from jax.experimental import pallas as pl
from jax.experimental.pallas import tpu as pltpu
from jax.sharding import PartitionSpec as P

NRAD = 12
NMAX = 10
LMAX = 6
LM = 49
SPECIES = 4
CH = SPECIES * NMAX
DENS = CH * LM
NBR = 48
NPAD = 64
TILE = 128
LBLK = 7
WROWS = 4
NVAL = 7
SLOTS = 4

cutoff_radius = 5.0
density_scale = 0.17
norm_eps = 1e-05
ridge_weight = 0.1
highest = lax.Precision.HIGHEST
f32 = jnp.float32
MESH = pl.DeviceIdType.MESH
bf16 = jnp.bfloat16


def log2_of(count):
    steps = count.bit_length() - 1
    assert count == 1 << steps
    return steps


def neighbour_flags(me, count):
    return me > 0, me < count - 1


def greet(partners, flags):
    barrier = pltpu.get_barrier_semaphore()
    for partner, flag in zip(partners, flags):
        if flag is None:
            pl.semaphore_signal(barrier, inc=1, device_id=partner, device_id_type=MESH)
        else:

            @pl.when(flag)
            def _(partner=partner):
                pl.semaphore_signal(barrier, inc=1, device_id=partner, device_id_type=MESH)

    present = sum(1 for flag in flags if flag is None)
    for flag in flags:
        if flag is not None:
            present = present + jnp.where(flag, 1, 0)
    pl.semaphore_wait(barrier, present)


class SidePair:
    def __init__(self, to_left, to_right, got_ref, send_sem, recv_sem):
        count = lax.axis_size("dom")
        me = lax.axis_index("dom")
        self.partners = ({"dom": me - 1}, {"dom": me + 1})
        self.flags = neighbour_flags(me, count)
        self.got = got_ref
        self.copies = [
            pltpu.make_async_remote_copy(
                src_ref=source,
                dst_ref=got_ref.at[1 - side],
                send_sem=send_sem.at[side],
                recv_sem=recv_sem.at[1 - side],
                device_id=self.partners[side],
                device_id_type=MESH,
            )
            for side, source in enumerate((to_left, to_right))
        ]

    def start(self):
        for side in range(2):
            pl.when(self.flags[side])(self.copies[side].start)

    def wait(self):
        for side in range(2):

            @pl.when(self.flags[side])
            def _(side=side):
                self.copies[side].wait_send()
                self.copies[1 - side].wait_recv()

    def received(self, side):
        return jnp.where(self.flags[side], self.got[side], 0.0)


def spread_kernel(values, x_ref, out_ref, got_ref, send_sem, recv_sem):
    pair = SidePair(x_ref, x_ref, got_ref, send_sem, recv_sem)
    greet(pair.partners, pair.flags)
    pair.start()
    rows = x_ref.shape[0] // values
    for value in range(values):
        at = value * 3 * rows
        out_ref[at + rows : at + 2 * rows, :] = x_ref[value * rows : (value + 1) * rows, :]
    pair.wait()
    for side in range(2):
        block = pair.received(side)
        for value in range(values):
            at = value * 3 * rows + 2 * side * rows
            out_ref[at : at + rows, :] = block[value * rows : (value + 1) * rows]


def comm_params(which):
    return pltpu.CompilerParams(collective_id=which, has_side_effects=True)


def vmem_spec():
    return pl.BlockSpec(memory_space=pltpu.VMEM)


def spread_call(which, values, cells):
    rows = cells.shape[0]
    return pl.pallas_call(
        partial(spread_kernel, values),
        out_shape=jax.ShapeDtypeStruct((rows * 3, TILE), f32),
        in_specs=[vmem_spec()],
        out_specs=vmem_spec(),
        scratch_shapes=[
            pltpu.VMEM((2, rows, TILE), f32),
            pltpu.SemaphoreType.DMA((2,)),
            pltpu.SemaphoreType.DMA((2,)),
        ],
        compiler_params=comm_params(which),
        name="spread_%d" % which,
    )(cells)


def collect_kernel(rows, win_ref, out_ref, got_ref, send_sem, recv_sem):
    pair = SidePair(
        win_ref.at[:, 0:rows], win_ref.at[:, 2 * rows : 3 * rows], got_ref, send_sem, recv_sem
    )
    greet(pair.partners, pair.flags)
    pair.start()
    pair.wait()
    out_ref[...] = win_ref[:, rows : 2 * rows] + pair.received(0) + pair.received(1)


def collect_call(which, rows, window):
    values = window.shape[0]
    return pl.pallas_call(
        partial(collect_kernel, rows),
        out_shape=jax.ShapeDtypeStruct((values, rows, TILE), f32),
        in_specs=[vmem_spec()],
        out_specs=vmem_spec(),
        scratch_shapes=[
            pltpu.VMEM((2, values, rows, TILE), f32),
            pltpu.SemaphoreType.DMA((2,)),
            pltpu.SemaphoreType.DMA((2,)),
        ],
        compiler_params=comm_params(which),
        name="collect_%d" % which,
    )(window)


def finish_kernel(rows, sums_at, per_group, win_ref, own_ref, pay_ref, force_ref, sum_ref, energy_ref,
                  offset_ref, got_ref, came_ref, send_sem, recv_sem, step_send, step_recv):
    pair = SidePair(
        win_ref.at[:, 0:rows], win_ref.at[:, 2 * rows : 3 * rows], got_ref, send_sem, recv_sem
    )
    partners = []
    for axis in ("dom", "grp"):
        me = lax.axis_index(axis)
        for bit in range(log2_of(lax.axis_size(axis))):
            half = 1 << bit
            partners.append({axis: me + half - 2 * half * lax.rem(lax.div(me, half), 2)})
    greet(list(pair.partners) + partners, list(pair.flags) + [None] * len(partners))
    pair.start()
    for step, partner in enumerate(partners):
        source = pay_ref if step == 0 else sum_ref
        copy = pltpu.make_async_remote_copy(
            src_ref=source,
            dst_ref=came_ref.at[step],
            send_sem=step_send.at[step],
            recv_sem=step_recv.at[step],
            device_id=partner,
            device_id_type=MESH,
        )
        copy.start()
        copy.wait()
        sum_ref[...] = source[...] + came_ref[step]
    pair.wait()
    force_ref[...] = (
        own_ref[...] - win_ref[:, rows : 2 * rows] - pair.received(0) - pair.received(1)
    )

    groups = lax.axis_size("grp")
    gram = [[None] * SPECIES for _ in range(SPECIES)]
    right = [None] * SPECIES

    def fractions(base):
        counts = [
            sum_ref[pl.ds(base + (1 + c) * per_group, per_group), :] for c in range(SPECIES)
        ]
        size = jnp.maximum(counts[0] + counts[1] + counts[2] + counts[3], 1.0)
        return [count / size for count in counts], size

    def gather_sum(total, value):
        part = jnp.sum(jnp.sum(value, axis=0, keepdims=True), axis=1, keepdims=True)
        return part if total is None else total + part

    stride = (SPECIES + 2) * per_group
    for group in range(groups):
        base = sums_at + group * stride
        frac, _ = fractions(base)
        target = sum_ref[pl.ds(base + (1 + SPECIES) * per_group, per_group), :]
        for c in range(SPECIES):
            right[c] = gather_sum(right[c], frac[c] * target)
            for d in range(c, SPECIES):
                gram[c][d] = gather_sum(gram[c][d], frac[c] * frac[d])
    matrix = [
        [gram[min(c, d)][max(c, d)] + (ridge_weight if c == d else 0.0) for d in range(SPECIES)]
        for c in range(SPECIES)
    ]
    for pivot in range(SPECIES):
        for below in range(pivot + 1, SPECIES):
            ratio = matrix[below][pivot] / matrix[pivot][pivot]
            matrix[below] = [b - ratio * a for a, b in zip(matrix[pivot], matrix[below])]
            right[below] = right[below] - ratio * right[pivot]
    answer = [None] * SPECIES
    for row in range(SPECIES - 1, -1, -1):
        running = right[row]
        for later in range(row + 1, SPECIES):
            running = running - matrix[row][later] * answer[later]
        answer[row] = running / matrix[row][row]
    mine = sums_at + lax.axis_index("grp") * stride
    frac, size = fractions(mine)
    energy = sum_ref[pl.ds(mine, per_group), :] / size
    for c in range(SPECIES):
        energy = energy + frac[c] * answer[c]
    energy_ref[...] = energy
    offset_ref[...] = jnp.concatenate(
        [jnp.broadcast_to(value, (1, TILE)) for value in answer] + [jnp.zeros((4, TILE), f32)], axis=0
    )


def finish_call(which, mesh_steps, rows, sums_at, per_group, window, own, payload):
    size = payload.shape[0]
    return pl.pallas_call(
        partial(finish_kernel, rows, sums_at, per_group),
        out_shape=(
            jax.ShapeDtypeStruct((3, rows, TILE), f32),
            jax.ShapeDtypeStruct((size, TILE), f32),
            jax.ShapeDtypeStruct((per_group, TILE), f32),
            jax.ShapeDtypeStruct((8, TILE), f32),
        ),
        in_specs=[vmem_spec()] * 3,
        out_specs=(vmem_spec(),) * 4,
        scratch_shapes=[
            pltpu.VMEM((2, 3, rows, TILE), f32),
            pltpu.VMEM((mesh_steps, size, TILE), f32),
            pltpu.SemaphoreType.DMA((2,)),
            pltpu.SemaphoreType.DMA((2,)),
            pltpu.SemaphoreType.DMA((mesh_steps,)),
            pltpu.SemaphoreType.DMA((mesh_steps,)),
        ],
        compiler_params=comm_params(which),
        name="finish_%d" % which,
    )(window, own, payload)


def double_factorial(number):
    result = 1.0
    while number > 1:
        result = result * number
        number = number - 2
    return result


def norm_of(degree, azimuth):
    value = math.sqrt(
        (2 * degree + 1)
        / (4 * math.pi)
        * math.factorial(degree - azimuth)
        / math.factorial(degree + azimuth)
    )
    return value * (math.sqrt(2.0) if azimuth else 1.0)


def scaled_legendre(coord_z):
    table = {}
    for azimuth in range(LMAX + 1):
        table[azimuth, azimuth] = norm_of(azimuth, azimuth) * double_factorial(2 * azimuth - 1)
        if azimuth + 1 <= LMAX:
            ratio = norm_of(azimuth + 1, azimuth) / norm_of(azimuth, azimuth)
            table[azimuth + 1, azimuth] = coord_z * (
                (2 * azimuth + 1) * ratio * table[azimuth, azimuth]
            )
        for degree in range(azimuth + 2, LMAX + 1):
            gap = degree - azimuth
            first = (2 * degree - 1) / gap * norm_of(degree, azimuth) / norm_of(degree - 1, azimuth)
            second = (
                (degree + azimuth - 1) / gap * norm_of(degree, azimuth) / norm_of(degree - 2, azimuth)
            )
            table[degree, azimuth] = (first * coord_z) * table[degree - 1, azimuth] - (
                second * table[degree - 2, azimuth]
            )
    return table


def azimuth_powers(coord_x, coord_y):
    cosines = [None, coord_x]
    sines = [None, coord_y]
    for _ in range(2, LMAX + 1):
        cosines.append(cosines[-1] * coord_x - sines[-1] * coord_y)
        sines.append(sines[-1] * coord_x + cosines[-2] * coord_y)
    return cosines, sines


LANE_GATHER = lax.GatherDimensionNumbers(
    offset_dims=(),
    collapsed_slice_dims=(1,),
    start_index_map=(1,),
    operand_batching_dims=(0,),
    start_indices_batching_dims=(0,),
)


def lane_gather(line, lo):
    return lax.gather(
        line,
        lo[..., None],
        LANE_GATHER,
        slice_sizes=(1, 1),
        mode=lax.GatherScatterMode.PROMISE_IN_BOUNDS,
    )


def prepare_kernel(first_ref, cnt_ref, nbr_ref, idx_ref, wt_ref, info_ref, key_ref, pos_ref):
    tile = pl.program_id(0)
    limit = cnt_ref[...]
    iota = lax.broadcasted_iota(jnp.int32, (NBR, TILE), 0)
    live = iota < limit
    index = nbr_ref[...] - first_ref[0]
    key = jnp.where(live, index, -1 - iota)
    key_ref[...] = key
    keys = [key[8 * b : 8 * b + 8] for b in range(NBR // 8)]
    sub = lax.broadcasted_iota(jnp.int32, (8, TILE), 0)
    blocks = NBR // 8
    total = [jnp.zeros((8, TILE), jnp.int32) for _ in range(blocks)]
    early = [jnp.zeros((8, TILE), jnp.int32) for _ in range(blocks)]
    for other in range(NBR):
        line = jnp.broadcast_to(key_ref[other : other + 1, :], (8, TILE))
        for b in range(blocks):
            same = jnp.where(keys[b] == line, 1, 0)
            total[b] = total[b] + same
            if other < 8 * b:
                early[b] = early[b] + same
            elif other < 8 * b + 7:
                early[b] = early[b] + jnp.where(sub > other - 8 * b, same, 0)
    packed, first = [], []
    for b in range(blocks):
        alive = sub + 8 * b < limit
        first.append(jnp.where(alive & (early[b] == 0), 1, 0))
        packed.append(total[b] * 4096 + keys[b])
    for b in range(blocks):
        pos_ref[8 * b : 8 * b + 8, :] = first[b]
    place = [jnp.zeros((8, TILE), jnp.int32) for _ in range(blocks)]
    running = jnp.zeros((1, TILE), jnp.int32)
    lines = []
    for slot in range(NBR):
        flag = pos_ref[slot : slot + 1, :]
        lines.append(jnp.where(flag == 1, running, -1))
        running = running + flag
    for b in range(blocks):
        key_ref[8 * b : 8 * b + 8, :] = packed[b]
    out = place
    for slot in range(NBR):
        where_to = jnp.broadcast_to(lines[slot], (8, TILE))
        line = jnp.broadcast_to(key_ref[slot : slot + 1, :], (8, TILE))
        for b in range(slot // 8 + 1):
            out[b] = jnp.where(where_to == sub + 8 * b, line, out[b])
    zero = jnp.zeros((8, TILE), jnp.int32)
    for b in range(NPAD // 8):
        word = out[b] if b < blocks else zero
        idx_ref[8 * b : 8 * b + 8, :] = lax.bitwise_and(word, 4095)
        wt_ref[8 * b : 8 * b + 8, :] = density_scale * lax.shift_right_logical(word, 12).astype(f32)
    used = jnp.max(running)
    info_ref[0, tile] = lax.div(used + 3, 4) * 4
    row = lax.shift_right_arithmetic(index, 7)
    info_ref[1, tile] = jnp.min(jnp.where(live, row, 1 << 20))
    info_ref[2, tile] = jnp.max(jnp.where(live, row, -1))


def prepare_call(first, limits, neighbours):
    atoms = neighbours.shape[1]
    return pl.pallas_call(
        prepare_kernel,
        out_shape=(
            jax.ShapeDtypeStruct((NPAD, atoms), jnp.int32),
            jax.ShapeDtypeStruct((NPAD, atoms), f32),
            jax.ShapeDtypeStruct((3, atoms // TILE), jnp.int32),
        ),
        grid=(atoms // TILE,),
        in_specs=[smem_spec(), tile_spec(1), tile_spec(NBR)],
        out_specs=(tile_spec(NPAD), tile_spec(NPAD), smem_spec()),
        scratch_shapes=[pltpu.VMEM((NBR, TILE), jnp.int32), pltpu.VMEM((NBR, TILE), jnp.int32)],
        name="prepare",
    )(first, limits, neighbours)


def fetch(tab_ref, names, hi, lo, row_low, row_high):
    def body(row, values):
        hit = hi == row
        out = []
        for name, value in zip(names, values):
            line = jnp.broadcast_to(tab_ref[pl.ds(name * 24 + row, 1), :], (8, TILE))
            got = lane_gather(line, lo)
            out.append(jnp.where(hit, got, value))
        return tuple(out)

    zero = jnp.zeros((8, TILE), f32)
    return lax.fori_loop(row_low, row_high + 1, body, tuple(zero for _ in names))


def edge_block(layer, tab_ref, cen_ref, idx_ref, wt_ref, block_at, row_low, row_high):
    base = pl.multiple_of(block_at * 8, 8)
    index = idx_ref[pl.ds(base, 8), :]
    weight = wt_ref[pl.ds(base, 8), :]
    hi = lax.shift_right_logical(index, 7)
    lo = lax.bitwise_and(index, 127)
    names = (0, 1, 2, 3) if layer == 1 else (0, 1, 2, 3, 4, 5, 6)
    values = fetch(tab_ref, names, hi, lo, row_low, row_high)
    live = weight > 0.0
    deltas = []
    for axis in range(3):
        centre = jnp.broadcast_to(cen_ref[pl.ds(axis, 1), :], (8, TILE))
        deltas.append(jnp.where(live, values[axis] - centre, 1.0))
    dist = jnp.sqrt(deltas[0] * deltas[0] + deltas[1] * deltas[1] + deltas[2] * deltas[2])
    inv = 1.0 / dist
    unit = [delta * inv for delta in deltas]
    if layer == 1:
        chan = [jnp.where(values[3] == float(c), 1.0, 0.0) for c in range(SPECIES)]
    else:
        chan = list(values[3:])
    return hi, lo, weight, dist, inv, unit, chan


def radial_terms(dist, rad_ref, with_slope):
    scaled = dist * (2.0 / cutoff_radius) - 1.0
    inside = dist < cutoff_radius
    angle = dist * (math.pi / cutoff_radius)
    cutoff = jnp.where(inside, 0.5 * (jnp.cos(angle) + 1.0), 0.0)
    cheb = [None, scaled]
    twice = 2.0 * scaled
    cheb.append(twice * scaled - 1.0)
    for _ in range(3, NRAD):
        cheb.append(twice * cheb[-1] - cheb[-2])
    basis = [cutoff] + [cutoff * cheb[p] for p in range(1, NRAD)]
    radial = []
    for n in range(NMAX):
        total = basis[0] * rad_ref[n, 0]
        for p in range(1, NRAD):
            total = total + basis[p] * rad_ref[n, p]
        radial.append(total)
    if not with_slope:
        return basis, radial, None
    slope_cut = jnp.where(inside, (-0.5 * math.pi / cutoff_radius) * jnp.sin(angle), 0.0)
    grad_scaled = cutoff * (2.0 / cutoff_radius)
    second = [None, None, twice]
    second[1] = jnp.ones_like(scaled)
    for _ in range(3, NRAD):
        second.append(twice * second[-1] - second[-2])
    slopes = [slope_cut, slope_cut * scaled + grad_scaled]
    for p in range(2, NRAD):
        slopes.append(slope_cut * cheb[p] + grad_scaled * (float(p) * second[p]))
    return basis, radial, slopes


def harmonic_list(unit):
    table = scaled_legendre(unit[2])
    cosines, sines = azimuth_powers(unit[0], unit[1])
    columns = []
    for degree in range(LMAX + 1):
        for signed in range(-degree, degree + 1):
            azimuth = abs(signed)
            poly = table[degree, azimuth]
            if signed == 0:
                columns.append(poly)
            elif signed > 0:
                columns.append(poly * cosines[azimuth])
            else:
                columns.append(poly * sines[azimuth])
    columns[0] = jnp.full_like(unit[2], columns[0])
    return columns


def density_kernel(layer, info_ref, rad_ref, tab_ref, cen_ref, idx_ref, wt_ref, out_ref,
                   x_ref, y_ref, d_ref):
    tile = pl.program_id(0)
    count = info_ref[0, tile]
    row_low, row_high = info_ref[1, tile], info_ref[2, tile]
    blocks = lax.div(count + 7, 8)

    def edges(block_at, carry):
        base = pl.multiple_of(block_at * 8, 8)
        hi, lo, weight, dist, inv, unit, chan = edge_block(
            layer, tab_ref, cen_ref, idx_ref, wt_ref, block_at, row_low, row_high
        )
        _, radial, _ = radial_terms(dist, rad_ref, False)
        for c in range(SPECIES):
            scale = chan[c] * weight
            for n in range(NMAX):
                x_ref[pl.ds(base * CH + (c * NMAX + n), 8, stride=CH), :] = scale * radial[n]
        for at, column in enumerate(harmonic_list(unit)):
            y_ref[pl.ds(at * NPAD + base, 8), :] = column
        return carry

    lax.fori_loop(0, blocks, edges, 0)
    groups = lax.div(count, SLOTS)

    def lm_block(block_at, carry):
        first = block_at * LBLK

        def slots(group, acc):
            acc = list(acc)
            for part in range(SLOTS):
                slot = group * SLOTS + part
                rows = [
                    x_ref[pl.ds(pl.multiple_of(slot * CH + 8 * j, 8), 8), :] for j in range(CH // 8)
                ]
                for at in range(LBLK):
                    line = jnp.broadcast_to(
                        y_ref[pl.ds((first + at) * NPAD + slot, 1), :], (8, TILE)
                    )
                    for j in range(CH // 8):
                        acc[at * (CH // 8) + j] = acc[at * (CH // 8) + j] + rows[j] * line
            return tuple(acc)

        zero = jnp.zeros((8, TILE), f32)
        acc = lax.fori_loop(0, groups, slots, tuple(zero for _ in range(LBLK * (CH // 8))))
        for at in range(LBLK):
            for j in range(CH // 8):
                d_ref[pl.ds(8 * j * LM + first + at, 8, stride=LM), :] = acc[at * (CH // 8) + j]
        return carry

    lax.fori_loop(0, LM // LBLK, lm_block, 0)
    out_ref[...] = d_ref[...].astype(bf16)


def smem_spec():
    return pl.BlockSpec(memory_space=pltpu.SMEM)


def tile_spec(rows):
    return pl.BlockSpec((rows, TILE), lambda i: (0, i))


def whole_spec(shape):
    return pl.BlockSpec(shape, lambda i: tuple(0 for _ in shape))


def density_call(layer, info, radial, table, centres, index, weight):
    atoms = centres.shape[1]
    return pl.pallas_call(
        partial(density_kernel, layer),
        out_shape=jax.ShapeDtypeStruct((DENS, atoms), bf16),
        grid=(atoms // TILE,),
        in_specs=[
            smem_spec(),
            smem_spec(),
            whole_spec(table.shape),
            tile_spec(8),
            tile_spec(NPAD),
            tile_spec(NPAD),
        ],
        out_specs=tile_spec(DENS),
        scratch_shapes=[
            pltpu.VMEM((NPAD * CH, TILE), f32),
            pltpu.VMEM((LM * NPAD, TILE), f32),
            pltpu.VMEM((DENS, TILE), f32),
        ],
        compiler_params=pltpu.CompilerParams(vmem_limit_bytes=48 << 20),
        name="density_%d" % layer,
    )(info, radial, table, centres, index, weight)


def backward_kernel(layer, info_ref, rad_ref, tab_ref, cen_ref, idx_ref, wt_ref, dd_ref, win_in_ref,
                    own_in_ref, win_ref, own_ref, rgr_ref, x_ref, y_ref, gx_ref, gy_ref, val_ref):
    tile = pl.program_id(0)
    count = info_ref[0, tile]
    row_low, row_high = info_ref[1, tile], info_ref[2, tile]
    blocks = lax.div(count + 7, 8)
    chunks = lax.div(count + 31, 32)

    @pl.when(tile == 0)
    def _():
        if layer == 1:
            win_ref[...] = win_in_ref[...]
        else:
            win_ref[...] = jnp.zeros_like(win_ref)
        rgr_ref[...] = jnp.zeros_like(rgr_ref)

    def edges(block_at, carry):
        base = pl.multiple_of(block_at * 8, 8)
        hi, lo, weight, dist, inv, unit, chan = edge_block(
            layer, tab_ref, cen_ref, idx_ref, wt_ref, block_at, row_low, row_high
        )
        _, radial, _ = radial_terms(dist, rad_ref, False)
        if layer == 1:
            for n in range(NMAX):
                x_ref[pl.ds(n * NPAD + base, 8), :] = weight * radial[n]
            x_ref[pl.ds(NMAX * NPAD + base, 8), :] = chan[1] + chan[3]
            x_ref[pl.ds((NMAX + 1) * NPAD + base, 8), :] = chan[2] + chan[3]
        else:
            for c in range(SPECIES):
                scale = chan[c] * weight
                for n in range(NMAX):
                    x_ref[pl.ds((c * NMAX + n) * NPAD + base, 8), :] = scale * radial[n]
        for at, column in enumerate(harmonic_list(unit)):
            y_ref[pl.ds(at * NPAD + base, 8), :] = column
        return carry

    lax.fori_loop(0, chunks * 4, edges, 0)

    zero = jnp.zeros((8, TILE), f32)

    def chunk_body(chunk, carry):
        start = pl.multiple_of(chunk * 32, 32)

        def m_block(block_at, inner):
            def over_lm(step, acc):
                acc = list(acc)
                for part in range(LBLK):
                    lm = step * LBLK + part
                    cols = [
                        y_ref[pl.ds(pl.multiple_of(lm * NPAD + start + 8 * kb, 8), 8), :]
                        for kb in range(4)
                    ]
                    for i in range(8):
                        line = jnp.broadcast_to(
                            dd_ref[pl.ds((block_at * 8 + i) * LM + lm, 1), :], (8, TILE)
                        )
                        for kb in range(4):
                            acc[i * 4 + kb] = acc[i * 4 + kb] + line * cols[kb]
                return tuple(acc)

            acc = lax.fori_loop(0, LM // LBLK, over_lm, tuple(zero for _ in range(32)))
            for i in range(8):
                for kb in range(4):
                    at = pl.multiple_of((block_at * 8 + i) * NPAD + start + 8 * kb, 8)
                    gx_ref[pl.ds(at, 8), :] = acc[i * 4 + kb]
            return inner

        lax.fori_loop(0, CH // 8, m_block, 0)

        def lm_block(block_at, inner):
            def over_m(step, acc):
                acc = list(acc)
                for part in range(8):
                    m = step * 8 + part
                    cols = [
                        x_ref[pl.ds(pl.multiple_of(m * NPAD + start + 8 * kb, 8), 8), :]
                        for kb in range(4)
                    ]
                    for i in range(LBLK):
                        line = jnp.broadcast_to(
                            dd_ref[pl.ds(m * LM + block_at * LBLK + i, 1), :], (8, TILE)
                        )
                        for kb in range(4):
                            acc[i * 4 + kb] = acc[i * 4 + kb] + line * cols[kb]
                return tuple(acc)

            acc = lax.fori_loop(0, CH // 8, over_m, tuple(zero for _ in range(LBLK * 4)))
            for i in range(LBLK):
                for kb in range(4):
                    at = pl.multiple_of((block_at * LBLK + i) * NPAD + start + 8 * kb, 8)
                    gy_ref[pl.ds(at, 8), :] = acc[i * 4 + kb]
            return inner

        lax.fori_loop(0, LM // LBLK, lm_block, 0)
        return carry

    def species_chunk(chunk, carry):
        start = pl.multiple_of(chunk * 32, 32)
        for n in range(NMAX):
            for kb in range(4):
                gx_ref[pl.ds(pl.multiple_of(n * NPAD + start + 8 * kb, 8), 8), :] = zero

        def lm_block(block_at, inner):
            def over_n(n, acc):
                acc = list(acc)
                bits = []
                for which in range(2):
                    at = (NMAX + which) * NPAD + start
                    bits.append([x_ref[pl.ds(pl.multiple_of(at + 8 * kb, 8), 8), :] > 0.5 for kb in range(4)])
                scaled, sums = [], []
                for kb in range(4):
                    at = pl.multiple_of(n * NPAD + start + 8 * kb, 8)
                    scaled.append(x_ref[pl.ds(at, 8), :])
                    sums.append(gx_ref[pl.ds(at, 8), :])
                for i in range(LBLK):
                    lines = [
                        jnp.broadcast_to(
                            dd_ref[pl.ds((c * NMAX + n) * LM + block_at * LBLK + i, 1), :], (8, TILE)
                        )
                        for c in range(SPECIES)
                    ]
                    for kb in range(4):
                        even = jnp.where(bits[0][kb], lines[1], lines[0])
                        odd = jnp.where(bits[0][kb], lines[3], lines[2])
                        grad = jnp.where(bits[1][kb], odd, even)
                        at = (block_at * LBLK + i) * NPAD + start + 8 * kb
                        col = y_ref[pl.ds(pl.multiple_of(at, 8), 8), :]
                        acc[i * 4 + kb] = acc[i * 4 + kb] + grad * scaled[kb]
                        sums[kb] = sums[kb] + grad * col
                for kb in range(4):
                    at = pl.multiple_of(n * NPAD + start + 8 * kb, 8)
                    gx_ref[pl.ds(at, 8), :] = sums[kb]
                return tuple(acc)

            acc = lax.fori_loop(0, NMAX, over_n, tuple(zero for _ in range(LBLK * 4)))
            for i in range(LBLK):
                for kb in range(4):
                    at = pl.multiple_of((block_at * LBLK + i) * NPAD + start + 8 * kb, 8)
                    gy_ref[pl.ds(at, 8), :] = acc[i * 4 + kb]
            return inner

        lax.fori_loop(0, LM // LBLK, lm_block, 0)
        return carry

    lax.fori_loop(0, chunks, species_chunk if layer == 1 else chunk_body, 0)

    def finish(block_at, own):
        base = pl.multiple_of(block_at * 8, 8)
        hi, lo, weight, dist, inv, unit, chan = edge_block(
            layer, tab_ref, cen_ref, idx_ref, wt_ref, block_at, row_low, row_high
        )
        basis, radial, slopes = radial_terms(dist, rad_ref, True)
        feat_grads = []
        radial_grads = [None] * NMAX
        if layer == 1:
            radial_grads = [gx_ref[pl.ds(n * NPAD + base, 8), :] for n in range(NMAX)]
        for c in range(SPECIES if layer == 2 else 0):
            total = None
            for n in range(NMAX):
                grad = gx_ref[pl.ds((c * NMAX + n) * NPAD + base, 8), :]
                term = grad * radial[n]
                total = term if total is None else total + term
                piece = grad * chan[c]
                radial_grads[n] = piece if c == 0 else radial_grads[n] + piece
            feat_grads.append(total * weight)
        grad_r = None
        radial_grads = [grad * weight for grad in radial_grads]
        for p in range(NRAD):
            total = None
            for n in range(NMAX):
                at = (n * NRAD + p) * 8
                rgr_ref[pl.ds(at, 8), :] = rgr_ref[pl.ds(at, 8), :] + radial_grads[n] * basis[p]
                term = radial_grads[n] * rad_ref[n, p]
                total = term if total is None else total + term
            term = total * slopes[p]
            grad_r = term if grad_r is None else grad_r + term
        table = scaled_legendre(unit[2])
        cosines, sines = azimuth_powers(unit[0], unit[1])
        grad_x = grad_y = grad_z = None

        def plus(total, term):
            return term if total is None else total + term

        for azimuth in range(LMAX + 1):
            grad_cos = grad_sin = None
            for degree in range(azimuth, LMAX + 1):
                at = degree * degree + degree
                up = gy_ref[pl.ds((at + azimuth) * NPAD + base, 8), :]
                poly = table[degree, azimuth]
                if azimuth:
                    down = gy_ref[pl.ds((at - azimuth) * NPAD + base, 8), :]
                    grad_cos = plus(grad_cos, up * poly)
                    grad_sin = plus(grad_sin, down * poly)
                if degree > azimuth:
                    ratio = norm_of(degree, azimuth) / norm_of(degree, azimuth + 1)
                    slope = ratio * table[degree, azimuth + 1]
                    if azimuth:
                        grad_z = plus(grad_z, slope * (up * cosines[azimuth] + down * sines[azimuth]))
                    else:
                        grad_z = plus(grad_z, slope * up)
            if azimuth == 1:
                grad_x, grad_y = grad_cos, grad_sin
            elif azimuth > 1:
                below_cos, below_sin = cosines[azimuth - 1], sines[azimuth - 1]
                grad_x = grad_x + float(azimuth) * (grad_cos * below_cos + grad_sin * below_sin)
                grad_y = grad_y + float(azimuth) * (grad_sin * below_cos - grad_cos * below_sin)
        dot_u = grad_x * unit[0] + grad_y * unit[1] + grad_z * unit[2]
        live = weight > 0.0
        out = []
        for axis, grad in enumerate((grad_x, grad_y, grad_z)):
            value = (grad - dot_u * unit[axis]) * inv + grad_r * unit[axis]
            out.append(jnp.where(live, value, 0.0))
        values = out + feat_grads
        for at, value in enumerate(values):
            val_ref[pl.ds(at * NPAD + base, 8), :] = value
        return tuple(total + value for total, value in zip(own, out))

    own = lax.fori_loop(0, blocks, finish, (zero, zero, zero))
    own = jnp.concatenate(
        [jnp.sum(total, axis=0, keepdims=True) for total in own] + [jnp.zeros((5, TILE), f32)], axis=0
    )
    own_ref[...] = own + own_in_ref[...] if layer == 1 else own

    used = 3 if layer == 1 else NVAL
    sub = lax.broadcasted_iota(jnp.int32, (TILE, TILE), 0)
    windows = lax.div(row_high - row_low + WROWS, WROWS)

    def window(window_at, carry):
        row_base = row_low + window_at * WROWS

        def slot_block(block_at, acc):
            base = pl.multiple_of(block_at * 8, 8)
            index = idx_ref[pl.ds(base, 8), :]
            hi = lax.shift_right_logical(index, 7)
            lo = lax.bitwise_and(index, 127)
            tops, lows = [], []
            for value_at in range(used):
                value = val_ref[pl.ds(value_at * NPAD + base, 8), :]
                for row in range(WROWS):
                    tops.append(jnp.where(hi == row_base + row, value, 0.0))
            stacked = jnp.stack(tops, axis=0)
            ones, left = [], []
            for part in range(8):
                line = jnp.broadcast_to(lo[part : part + 1, :], (TILE, TILE))
                ones.append(jnp.where(line == sub, 1.0, 0.0).astype(bf16))
                left.append(stacked[:, part, :])
            left = jnp.concatenate(left, axis=1)
            ones = jnp.concatenate(ones, axis=1)
            high = left.astype(bf16)
            rest = (left - high.astype(f32)).astype(bf16)
            dims = (((1,), (1,)), ((), ()))
            acc = acc + lax.dot_general(high, ones, dims, preferred_element_type=f32)
            return acc + lax.dot_general(rest, ones, dims, preferred_element_type=f32)

        acc = lax.fori_loop(0, blocks, slot_block, jnp.zeros((used * WROWS, TILE), f32))
        for value_at in range(used):
            at = value_at * 32 + row_base
            win_ref[pl.ds(at, WROWS), :] = (
                win_ref[pl.ds(at, WROWS), :] + acc[value_at * WROWS : (value_at + 1) * WROWS]
            )
        return carry

    lax.fori_loop(0, windows, window, 0)


def backward_call(layer, info, radial, table, centres, index, weight, grad_dens, window_in, own_in):
    atoms = centres.shape[1]
    values = 3 if layer == 1 else NVAL
    return pl.pallas_call(
        partial(backward_kernel, layer),
        out_shape=(
            jax.ShapeDtypeStruct((values * 32, TILE), f32),
            jax.ShapeDtypeStruct((8, atoms), f32),
            jax.ShapeDtypeStruct((NMAX * NRAD * 8, TILE), f32),
        ),
        grid=(atoms // TILE,),
        in_specs=[
            smem_spec(),
            smem_spec(),
            whole_spec(table.shape),
            tile_spec(8),
            tile_spec(NPAD),
            tile_spec(NPAD),
            tile_spec(DENS),
            whole_spec(window_in.shape),
            tile_spec(8),
        ],
        out_specs=(
            whole_spec((values * 32, TILE)),
            tile_spec(8),
            whole_spec((NMAX * NRAD * 8, TILE)),
        ),
        scratch_shapes=[
            pltpu.VMEM((CH * NPAD, TILE), f32),
            pltpu.VMEM((LM * NPAD, TILE), f32),
            pltpu.VMEM((CH * NPAD, TILE), f32),
            pltpu.VMEM((LM * NPAD, TILE), f32),
            pltpu.VMEM((NVAL * NPAD, TILE), f32),
        ],
        compiler_params=pltpu.CompilerParams(vmem_limit_bytes=48 << 20),
        name="backward_%d" % layer,
    )(info, radial, table, centres, index, weight, grad_dens, window_in, own_in)


def feature_map(invariants, mixing):
    inverse_rms = lax.rsqrt(jnp.mean(invariants * invariants, axis=0) + norm_eps)
    return jnp.einsum("qk,qa->ka", mixing, invariants, precision=highest) * inverse_rms


def contract(dens_in, coupling):
    factors = jnp.einsum("vdq,da->vqa", coupling, dens_in, preferred_element_type=f32)
    product = reduce(
        lambda earlier, later: earlier * later,
        [factors[index_v] for index_v in range(factors.shape[0])],
    )
    return (factors, product)


def contract_back(factors, upstream, coupling):
    partials = []
    for factor_at in range(factors.shape[0]):
        others = upstream
        for partner in range(factors.shape[0]):
            if partner != factor_at:
                others = others * factors[partner]
        partials.append(others)
    rounded = jnp.stack(partials).astype(bf16)
    return jnp.einsum("vdq,vqa->da", coupling, rounded, preferred_element_type=f32)


def per_device(
    positions,
    species,
    neighbours,
    slot_counts,
    structure,
    target_energy,
    radial_one,
    coupling_one,
    coefficient_one,
    mixing,
    radial_two,
    coupling_two,
    coefficient_two,
):
    atoms = positions.shape[2]
    tiles = atoms // TILE
    centres = positions[:, 0, :]
    own_species = species[0]
    onehot = (own_species[None, :] == jnp.arange(SPECIES, dtype=jnp.int32)[:, None]).astype(f32)
    site = jnp.concatenate([centres, own_species.astype(f32)[None, :]], axis=0)
    table_one = spread_call(0, 4, site.reshape(4 * tiles, TILE))
    first = ((lax.axis_index("dom") - 1) * atoms).astype(jnp.int32).reshape(1)
    index, weight, info = prepare_call(first, slot_counts, neighbours[:, 0, :])
    centres8 = jnp.pad(centres, ((0, 5), (0, 0)))

    dens_one = density_call(1, info, radial_one, table_one, centres8, index, weight)
    factors_one, invariants_one = contract(dens_one, coupling_one)
    chosen_one = jnp.dot(coefficient_one.T, onehot, precision=highest)
    energy_one = jnp.sum(invariants_one * chosen_one, axis=0)
    features, features_back = jax.vjp(feature_map, invariants_one, mixing)
    feat_table = spread_call(1, SPECIES, features.reshape(SPECIES * tiles, TILE))
    table_two = jnp.concatenate([table_one[: 3 * 3 * tiles], feat_table], axis=0)
    dens_two = density_call(2, info, radial_two, table_two, centres8, index, weight)
    factors_two, invariants_two = contract(dens_two, coupling_two)
    chosen_two = jnp.dot(coefficient_two.T, onehot, precision=highest)
    site_energy = energy_one + jnp.sum(invariants_two * chosen_two, axis=0)
    structures = target_energy.shape[1]
    members = (structure[0][:, None] == jnp.arange(structures, dtype=jnp.int32)[None, :]).astype(f32)
    per_structure = jnp.dot(
        jnp.concatenate([site_energy[None, :], onehot], axis=0), members, precision=highest
    )
    target = jnp.where(lax.axis_index("dom") == 0, target_energy, 0.0)
    per_structure = jnp.concatenate([per_structure, target], axis=0)

    grad_dens_two = contract_back(factors_two, chosen_two, coupling_two)
    blank_window = jnp.zeros((8, TILE), f32)
    blank_own = jnp.zeros((8, atoms), f32)
    window_two, own_two, rgr_two = backward_call(
        2, info, radial_two, table_two, centres8, index, weight, grad_dens_two, blank_window, blank_own
    )
    window_two = window_two.reshape(NVAL, 32, TILE)
    grad_features = collect_call(2, tiles, window_two[3:]).reshape(SPECIES, atoms)
    coefficient_second = jnp.dot(onehot, invariants_two.T, precision=highest)
    grad_invariants, mixing_gradient = features_back(grad_features)
    grad_dens_one = contract_back(factors_one, chosen_one + grad_invariants, coupling_one)
    window_one, own_one, rgr_one = backward_call(
        1,
        info,
        radial_one,
        table_one,
        centres8,
        index,
        weight,
        grad_dens_one,
        window_two[:3].reshape(3 * 32, TILE),
        own_two,
    )
    coefficient_first = jnp.dot(onehot, invariants_one.T, precision=highest)

    def radial_sum(partial_grad):
        return jnp.sum(partial_grad.reshape(NMAX * NRAD, 8 * TILE), axis=1)

    groups = lax.axis_size("grp")
    mine = lax.axis_index("grp") == jnp.arange(groups, dtype=jnp.int32)
    slots = jnp.where(mine[:, None, None], per_structure[None], 0.0)
    quantum = coefficient_first.shape[1]
    wide = SPECIES * quantum
    radials = jnp.zeros((8 * TILE,), f32)
    radials = radials.at[: NMAX * NRAD].set(radial_sum(rgr_one))
    radials = radials.at[TILE : TILE + NMAX * NRAD].set(radial_sum(rgr_two))
    payload = jnp.concatenate(
        [
            radials,
            coefficient_first.reshape(-1),
            coefficient_second.reshape(-1),
            mixing_gradient.T.reshape(-1),
            slots.reshape(-1),
        ]
    )
    sums_at = 8 + 3 * wide // TILE
    steps = log2_of(lax.axis_size("dom")) + log2_of(groups)
    forces, sums, energies, offsets = finish_call(
        3,
        steps,
        tiles,
        sums_at,
        structures // TILE,
        window_one.reshape(3, 32, TILE),
        own_one[:3].reshape(3, tiles, TILE),
        payload.reshape(-1, TILE),
    )
    parts = sums[8:sums_at].reshape(3, SPECIES, quantum)
    return (
        energies.reshape(1, structures),
        offsets[:SPECIES, 0],
        forces.reshape(3, 1, atoms),
        sums[0, : NMAX * NRAD].reshape(NMAX, NRAD),
        parts[0],
        parts[2].T,
        sums[1, : NMAX * NRAD].reshape(NMAX, NRAD),
        parts[1],
    )


def solution(mesh):
    in_specs = (
        P(None, "grp", "dom"),
        P("grp", "dom"),
        P(None, "grp", "dom"),
        P("grp", "dom"),
        P("grp", "dom"),
        P("grp", None),
        P(),
        P(),
        P(),
        P(),
        P(),
        P(),
        P(),
    )
    out_specs = (P("grp", None), P(), P(None, "grp", "dom"), P(), P(), P(), P(), P())
    return jax.shard_map(
        per_device, mesh=mesh, in_specs=in_specs, out_specs=out_specs, check_vma=False
    )
```

```python
from functools import partial, reduce
import math

import jax
import jax.numpy as jnp
from jax import lax
from jax.experimental import pallas as pl
from jax.experimental.pallas import tpu as pltpu
from jax.sharding import PartitionSpec as P

NRAD = 12
NMAX = 10
LMAX = 6
LM = 49
SPECIES = 4
CH = SPECIES * NMAX
DENS = CH * LM
NBR = 48
NPAD = 64
TILE = 128
LBLK = 7
WROWS = 12
WSTEP = 40
GEO = 5
NVAL = 7
SLOTS = 4
XROW = CH + 1

cutoff_radius = 5.0
density_scale = 0.17
norm_eps = 1e-05
ridge_weight = 0.1
highest = lax.Precision.HIGHEST
f32 = jnp.float32
MESH = pl.DeviceIdType.MESH
bf16 = jnp.bfloat16


def log2_of(count):
    steps = count.bit_length() - 1
    assert count == 1 << steps
    return steps


def neighbour_flags(me, count):
    return me > 0, me < count - 1


def greet(partners, flags):
    barrier = pltpu.get_barrier_semaphore()
    for partner, flag in zip(partners, flags):
        if flag is None:
            pl.semaphore_signal(barrier, inc=1, device_id=partner, device_id_type=MESH)
        else:

            @pl.when(flag)
            def _(partner=partner):
                pl.semaphore_signal(barrier, inc=1, device_id=partner, device_id_type=MESH)

    present = sum(1 for flag in flags if flag is None)
    for flag in flags:
        if flag is not None:
            present = present + jnp.where(flag, 1, 0)
    pl.semaphore_wait(barrier, present)


class SidePair:
    def __init__(self, to_left, to_right, got_ref, send_sem, recv_sem):
        count = lax.axis_size("dom")
        me = lax.axis_index("dom")
        self.partners = ({"dom": me - 1}, {"dom": me + 1})
        self.flags = neighbour_flags(me, count)
        self.got = got_ref
        self.copies = [
            pltpu.make_async_remote_copy(
                src_ref=source,
                dst_ref=got_ref.at[1 - side],
                send_sem=send_sem.at[side],
                recv_sem=recv_sem.at[1 - side],
                device_id=self.partners[side],
                device_id_type=MESH,
            )
            for side, source in enumerate((to_left, to_right))
        ]

    def start(self):
        for side in range(2):
            pl.when(self.flags[side])(self.copies[side].start)

    def wait(self):
        for side in range(2):

            @pl.when(self.flags[side])
            def _(side=side):
                self.copies[side].wait_send()
                self.copies[1 - side].wait_recv()

    def received(self, side):
        return jnp.where(self.flags[side], self.got[side], 0.0)


def split3(value):
    high = value.astype(bf16)
    rest = value - high.astype(f32)
    middle = rest.astype(bf16)
    low = (rest - middle.astype(f32)).astype(bf16)
    return jnp.concatenate([high, middle, low], axis=0)


def reorder(value, perm_ref, contract_at):
    count = value.shape[0]
    out = lax.dot_general(
        split3(value), perm_ref[...], (((1,), (contract_at,)), ((), ())), preferred_element_type=f32
    )
    return out[:count] + (out[count : 2 * count] + out[2 * count :])


def spread_kernel(values, ordered, *refs):
    if ordered:
        x_ref, out_ref, mine_ref, got_ref, send_sem, recv_sem = refs
        flat = x_ref[...]
    else:
        x_ref, perm_ref, out_ref, mine_ref, got_ref, send_sem, recv_sem = refs
        flat = reorder(x_ref[...], perm_ref, 0)
    rows = flat.shape[1] // TILE
    for value in range(values):
        for row in range(rows):
            line = flat[value : value + 1, row * TILE : (row + 1) * TILE]
            at = value * rows + row
            mine_ref[at : at + 1, :] = line
    pair = SidePair(mine_ref, mine_ref, got_ref, send_sem, recv_sem)
    greet(pair.partners, pair.flags)
    pair.start()
    for value in range(values):
        at = value * 3 * rows
        out_ref[at + rows : at + 2 * rows, :] = mine_ref[value * rows : (value + 1) * rows, :]
    pair.wait()
    for side in range(2):
        block = pair.received(side)
        for value in range(values):
            at = value * 3 * rows + 2 * side * rows
            out_ref[at : at + rows, :] = block[value * rows : (value + 1) * rows]


def comm_params(which):
    return pltpu.CompilerParams(collective_id=which, has_side_effects=True)


def vmem_spec():
    return pl.BlockSpec(memory_space=pltpu.VMEM)


def spread_call(which, values, cells, perm=None):
    rows = values * cells.shape[1] // TILE
    operands = (cells,) if perm is None else (cells, perm)
    return pl.pallas_call(
        partial(spread_kernel, values, perm is None),
        out_shape=jax.ShapeDtypeStruct((rows * 3, TILE), f32),
        in_specs=[vmem_spec()] * len(operands),
        out_specs=vmem_spec(),
        scratch_shapes=[
            pltpu.VMEM((rows, TILE), f32),
            pltpu.VMEM((2, rows, TILE), f32),
            pltpu.SemaphoreType.DMA((2,)),
            pltpu.SemaphoreType.DMA((2,)),
        ],
        compiler_params=comm_params(which),
        name="spread_%d" % which,
    )(*operands)


def in_lanes(blocks):
    values, rows = blocks.shape[0], blocks.shape[1]
    flat = [
        jnp.concatenate([blocks[v, r : r + 1, :] for r in range(rows)], axis=1) for v in range(values)
    ]
    return jnp.concatenate(flat + [jnp.zeros((8 - values, rows * TILE), f32)], axis=0)


def collect_kernel(rows, values_at, win_ref, perm_ref, out_ref, got_ref, send_sem, recv_sem):
    pair = SidePair(
        win_ref.at[values_at:, 0:rows],
        win_ref.at[values_at:, 2 * rows : 3 * rows],
        got_ref,
        send_sem,
        recv_sem,
    )
    greet(pair.partners, pair.flags)
    pair.start()
    pair.wait()
    total = win_ref[values_at:, rows : 2 * rows] + pair.received(0) + pair.received(1)
    out_ref[...] = reorder(in_lanes(total), perm_ref, 1)


def collect_call(which, rows, values_at, window, perm):
    values = window.shape[0] - values_at
    return pl.pallas_call(
        partial(collect_kernel, rows, values_at),
        out_shape=jax.ShapeDtypeStruct((8, rows * TILE), f32),
        in_specs=[vmem_spec()] * 2,
        out_specs=vmem_spec(),
        scratch_shapes=[
            pltpu.VMEM((2, values, rows, TILE), f32),
            pltpu.SemaphoreType.DMA((2,)),
            pltpu.SemaphoreType.DMA((2,)),
        ],
        compiler_params=comm_params(which),
        name="collect_%d" % which,
    )(window, perm)


def finish_kernel(rows, sums_at, per_group, win_ref, own_ref, perm_ref, pay_ref, force_ref, sum_ref, energy_ref,
                  offset_ref, got_ref, came_ref, send_sem, recv_sem, step_send, step_recv):
    pair = SidePair(
        win_ref.at[:, 0:rows], win_ref.at[:, 2 * rows : 3 * rows], got_ref, send_sem, recv_sem
    )
    partners = []
    for axis in ("dom", "grp"):
        me = lax.axis_index(axis)
        for bit in range(log2_of(lax.axis_size(axis))):
            half = 1 << bit
            partners.append({axis: me + half - 2 * half * lax.rem(lax.div(me, half), 2)})
    greet(list(pair.partners) + partners, list(pair.flags) + [None] * len(partners))
    pair.start()
    force_ref[...] = reorder(own_ref[...], perm_ref, 0)
    for step, partner in enumerate(partners):
        source = pay_ref if step == 0 else sum_ref
        copy = pltpu.make_async_remote_copy(
            src_ref=source,
            dst_ref=came_ref.at[step],
            send_sem=step_send.at[step],
            recv_sem=step_recv.at[step],
            device_id=partner,
            device_id_type=MESH,
        )
        copy.start()
        copy.wait()
        sum_ref[...] = source[...] + came_ref[step]
    pair.wait()
    total = win_ref[:, rows : 2 * rows] + pair.received(0) + pair.received(1)
    force_ref[...] = force_ref[...] - in_lanes(total)

    groups = lax.axis_size("grp")
    gram = [[None] * SPECIES for _ in range(SPECIES)]
    right = [None] * SPECIES

    def fractions(base):
        counts = [
            sum_ref[pl.ds(base + (1 + c) * per_group, per_group), :] for c in range(SPECIES)
        ]
        size = jnp.maximum(counts[0] + counts[1] + counts[2] + counts[3], 1.0)
        return [count / size for count in counts], size

    def gather_sum(total, value):
        part = jnp.sum(jnp.sum(value, axis=0, keepdims=True), axis=1, keepdims=True)
        return part if total is None else total + part

    stride = (SPECIES + 2) * per_group
    for group in range(groups):
        base = sums_at + group * stride
        frac, _ = fractions(base)
        target = sum_ref[pl.ds(base + (1 + SPECIES) * per_group, per_group), :]
        for c in range(SPECIES):
            right[c] = gather_sum(right[c], frac[c] * target)
            for d in range(c, SPECIES):
                gram[c][d] = gather_sum(gram[c][d], frac[c] * frac[d])
    matrix = [
        [gram[min(c, d)][max(c, d)] + (ridge_weight if c == d else 0.0) for d in range(SPECIES)]
        for c in range(SPECIES)
    ]
    for pivot in range(SPECIES):
        for below in range(pivot + 1, SPECIES):
            ratio = matrix[below][pivot] / matrix[pivot][pivot]
            matrix[below] = [b - ratio * a for a, b in zip(matrix[pivot], matrix[below])]
            right[below] = right[below] - ratio * right[pivot]
    answer = [None] * SPECIES
    for row in range(SPECIES - 1, -1, -1):
        running = right[row]
        for later in range(row + 1, SPECIES):
            running = running - matrix[row][later] * answer[later]
        answer[row] = running / matrix[row][row]
    mine = sums_at + lax.axis_index("grp") * stride
    frac, size = fractions(mine)
    energy = sum_ref[pl.ds(mine, per_group), :] / size
    for c in range(SPECIES):
        energy = energy + frac[c] * answer[c]
    energy_ref[...] = energy
    offset_ref[...] = jnp.concatenate(
        [jnp.broadcast_to(value, (1, TILE)) for value in answer] + [jnp.zeros((4, TILE), f32)], axis=0
    )


def finish_call(which, mesh_steps, rows, sums_at, per_group, window, own, perm, payload):
    size = payload.shape[0]
    return pl.pallas_call(
        partial(finish_kernel, rows, sums_at, per_group),
        out_shape=(
            jax.ShapeDtypeStruct((8, rows * TILE), f32),
            jax.ShapeDtypeStruct((size, TILE), f32),
            jax.ShapeDtypeStruct((per_group, TILE), f32),
            jax.ShapeDtypeStruct((8, TILE), f32),
        ),
        in_specs=[vmem_spec()] * 4,
        out_specs=(vmem_spec(),) * 4,
        scratch_shapes=[
            pltpu.VMEM((2, 3, rows, TILE), f32),
            pltpu.VMEM((mesh_steps, size, TILE), f32),
            pltpu.SemaphoreType.DMA((2,)),
            pltpu.SemaphoreType.DMA((2,)),
            pltpu.SemaphoreType.DMA((mesh_steps,)),
            pltpu.SemaphoreType.DMA((mesh_steps,)),
        ],
        compiler_params=comm_params(which),
        name="finish_%d" % which,
    )(window, own, perm, payload)


def double_factorial(number):
    result = 1.0
    while number > 1:
        result = result * number
        number = number - 2
    return result


def norm_of(degree, azimuth):
    value = math.sqrt(
        (2 * degree + 1)
        / (4 * math.pi)
        * math.factorial(degree - azimuth)
        / math.factorial(degree + azimuth)
    )
    return value * (math.sqrt(2.0) if azimuth else 1.0)


def scaled_legendre(coord_z):
    table = {}
    for azimuth in range(LMAX + 1):
        table[azimuth, azimuth] = norm_of(azimuth, azimuth) * double_factorial(2 * azimuth - 1)
        if azimuth + 1 <= LMAX:
            ratio = norm_of(azimuth + 1, azimuth) / norm_of(azimuth, azimuth)
            table[azimuth + 1, azimuth] = coord_z * (
                (2 * azimuth + 1) * ratio * table[azimuth, azimuth]
            )
        for degree in range(azimuth + 2, LMAX + 1):
            gap = degree - azimuth
            first = (2 * degree - 1) / gap * norm_of(degree, azimuth) / norm_of(degree - 1, azimuth)
            second = (
                (degree + azimuth - 1) / gap * norm_of(degree, azimuth) / norm_of(degree - 2, azimuth)
            )
            table[degree, azimuth] = (first * coord_z) * table[degree - 1, azimuth] - (
                second * table[degree - 2, azimuth]
            )
    return table


def azimuth_powers(coord_x, coord_y):
    cosines = [None, coord_x]
    sines = [None, coord_y]
    for _ in range(2, LMAX + 1):
        cosines.append(cosines[-1] * coord_x - sines[-1] * coord_y)
        sines.append(sines[-1] * coord_x + cosines[-2] * coord_y)
    return cosines, sines


LANE_GATHER = lax.GatherDimensionNumbers(
    offset_dims=(),
    collapsed_slice_dims=(1,),
    start_index_map=(1,),
    operand_batching_dims=(0,),
    start_indices_batching_dims=(0,),
)


def lane_gather(line, lo):
    return lax.gather(
        line,
        lo[..., None],
        LANE_GATHER,
        slice_sizes=(1, 1),
        mode=lax.GatherScatterMode.PROMISE_IN_BOUNDS,
    )


def prepare_kernel(first_ref, cnt_ref, nbr_ref, site_ref, idx_ref, wt_ref, sorted_ref, perm_ref, info_ref,
                   key_ref, pos_ref, word_ref, rank_ref):
    atoms = nbr_ref.shape[1]
    tiles = atoms // TILE
    blocks = NBR // 8
    sub = lax.broadcasted_iota(jnp.int32, (8, TILE), 0)
    lane = lax.broadcasted_iota(jnp.int32, (1, TILE), 1)

    def merge(tile, carry):
        cols = pl.ds(pl.multiple_of(tile * TILE, TILE), TILE)
        limit = cnt_ref[:, cols]
        iota = lax.broadcasted_iota(jnp.int32, (NBR, TILE), 0)
        key = jnp.where(iota < limit, nbr_ref[:, cols] - first_ref[0], -1 - iota)
        key_ref[...] = key
        keys = [key[8 * b : 8 * b + 8] for b in range(blocks)]
        total = [jnp.zeros((8, TILE), jnp.int32) for _ in range(blocks)]
        early = [jnp.zeros((8, TILE), jnp.int32) for _ in range(blocks)]
        for other in range(NBR):
            line = jnp.broadcast_to(key_ref[other : other + 1, :], (8, TILE))
            for b in range(blocks):
                same = jnp.where(keys[b] == line, 1, 0)
                total[b] = total[b] + same
                if other < 8 * b:
                    early[b] = early[b] + same
                elif other < 8 * b + 7:
                    early[b] = early[b] + jnp.where(sub > other - 8 * b, same, 0)
        for b in range(blocks):
            alive = sub + 8 * b < limit
            pos_ref[8 * b : 8 * b + 8, :] = jnp.where(alive & (early[b] == 0), 1, 0)
            key_ref[8 * b : 8 * b + 8, :] = total[b] * 4096 + keys[b]
        running = jnp.zeros((1, TILE), jnp.int32)
        out = [jnp.zeros((8, TILE), jnp.int32) for _ in range(blocks)]
        for slot in range(NBR):
            flag = pos_ref[slot : slot + 1, :]
            place = jnp.broadcast_to(jnp.where(flag == 1, running, -1), (8, TILE))
            running = running + flag
            line = jnp.broadcast_to(key_ref[slot : slot + 1, :], (8, TILE))
            for b in range(slot // 8 + 1):
                out[b] = jnp.where(place == sub + 8 * b, line, out[b])
        for b in range(blocks):
            word_ref[8 * b : 8 * b + 8, cols] = out[b].astype(f32)
        order = running * atoms + (atoms - 1 - tile * TILE) - lane
        rank_ref[pl.ds(tile, 1), :] = order.astype(f32)
        return carry

    lax.fori_loop(0, tiles, merge, 0)
    orders = rank_ref[...]
    upright = jnp.transpose(orders)
    ranks = []
    for tile in range(tiles):
        row = jnp.broadcast_to(orders[tile : tile + 1], (TILE, TILE))
        total = jnp.zeros((TILE, TILE), f32)
        for other in range(tiles):
            col = jnp.broadcast_to(upright[:, other : other + 1], (TILE, TILE))
            total = total + jnp.where(col > row, 1.0, 0.0)
        ranks.append(jnp.sum(total, axis=0, keepdims=True))
    place = lax.broadcasted_iota(jnp.int32, (atoms, TILE), 0).astype(f32)
    for tile in range(tiles):
        line = jnp.broadcast_to(ranks[tile], (atoms, TILE))
        perm_ref[:, tile * TILE : (tile + 1) * TILE] = jnp.where(line == place, 1.0, 0.0).astype(bf16)
    word_ref[NBR : NBR + 8, :] = site_ref[...]
    moved = reorder(word_ref[...], perm_ref, 1)
    sorted_ref[...] = moved[NBR:]
    word = moved[:NBR].astype(jnp.int32)
    index = lax.bitwise_and(word, 4095)
    times = lax.shift_right_logical(word, 12)
    idx_ref[:NBR, :] = index
    idx_ref[NBR:, :] = jnp.zeros((NPAD - NBR, atoms), jnp.int32)
    wt_ref[:NBR, :] = density_scale * times.astype(f32)
    wt_ref[NBR:, :] = jnp.zeros((NPAD - NBR, atoms), f32)
    row = lax.shift_right_logical(index, 7)
    low = jnp.min(jnp.where(times > 0, row, 1 << 20))
    high = jnp.max(jnp.where(times > 0, row, -1))
    slots = lax.broadcasted_iota(jnp.int32, (NBR, TILE), 0) + 1
    for tile in range(tiles):
        used = times[:, tile * TILE : (tile + 1) * TILE] > 0
        info_ref[0, tile] = lax.div(jnp.max(jnp.where(used, slots, 0)) + SLOTS - 1, SLOTS) * SLOTS
        info_ref[1, tile] = low
        info_ref[2, tile] = high


def prepare_call(first, limits, neighbours, site):
    atoms = neighbours.shape[1]
    return pl.pallas_call(
        prepare_kernel,
        out_shape=(
            jax.ShapeDtypeStruct((NPAD, atoms), jnp.int32),
            jax.ShapeDtypeStruct((NPAD, atoms), f32),
            jax.ShapeDtypeStruct((8, atoms), f32),
            jax.ShapeDtypeStruct((atoms, atoms), bf16),
            jax.ShapeDtypeStruct((3, atoms // TILE), jnp.int32),
        ),
        in_specs=[smem_spec(), vmem_spec(), vmem_spec(), vmem_spec()],
        out_specs=(vmem_spec(), vmem_spec(), vmem_spec(), vmem_spec(), smem_spec()),
        scratch_shapes=[
            pltpu.VMEM((NBR, TILE), jnp.int32),
            pltpu.VMEM((NBR, TILE), jnp.int32),
            pltpu.VMEM((NBR + 8, atoms), f32),
            pltpu.VMEM((atoms // TILE, TILE), f32),
        ],
        name="prepare",
    )(first, limits, neighbours, site)


def fetch(tab_ref, values, idx_ref, put_ref, chunk, row_low, row_high):
    start = pl.multiple_of(chunk * 32, 32)
    index = [idx_ref[pl.ds(start + 8 * kb, 8), :] for kb in range(4)]
    hi = [lax.shift_right_logical(word, 7) for word in index]
    lo = [lax.bitwise_and(word, 127) for word in index]

    def body(row, found):
        found = list(found)
        hits = [word == row for word in hi]
        for value in range(values):
            line = jnp.broadcast_to(tab_ref[pl.ds(value * 24 + row, 1), :], (8, TILE))
            for kb in range(4):
                at = value * 4 + kb
                found[at] = jnp.where(hits[kb], lane_gather(line, lo[kb]), found[at])
        return tuple(found)

    zero = jnp.zeros((8, TILE), f32)
    found = lax.fori_loop(row_low, row_high + 1, body, tuple(zero for _ in range(4 * values)))
    for value in range(values):
        for kb in range(4):
            put_ref[pl.ds(pl.multiple_of(value * NPAD + start + 8 * kb, 8), 8), :] = found[value * 4 + kb]


def slot_rows(which, base):
    return pl.ds(pl.multiple_of(which * NPAD + base, 8), 8)


def geometry(layer, geo_ref, feat_ref, wt_ref, base):
    weight = wt_ref[pl.ds(base, 8), :]
    unit = [geo_ref[slot_rows(axis, base), :] for axis in range(3)]
    dist = geo_ref[slot_rows(4, base), :]
    if layer == 1:
        kind = geo_ref[slot_rows(3, base), :]
        chan = [jnp.where(kind == float(c), 1.0, 0.0) for c in range(SPECIES)]
    else:
        chan = [feat_ref[slot_rows(c, base), :] for c in range(SPECIES)]
    return weight, dist, unit, chan


def radial_terms(dist, rad_ref, with_slope):
    scaled = dist * (2.0 / cutoff_radius) - 1.0
    inside = dist < cutoff_radius
    angle = dist * (math.pi / cutoff_radius)
    cutoff = jnp.where(inside, 0.5 * (jnp.cos(angle) + 1.0), 0.0)
    cheb = [None, scaled]
    twice = 2.0 * scaled
    cheb.append(twice * scaled - 1.0)
    for _ in range(3, NRAD):
        cheb.append(twice * cheb[-1] - cheb[-2])
    basis = [cutoff] + [cutoff * cheb[p] for p in range(1, NRAD)]
    radial = []
    for n in range(NMAX):
        total = basis[0] * rad_ref[n, 0]
        for p in range(1, NRAD):
            total = total + basis[p] * rad_ref[n, p]
        radial.append(total)
    if not with_slope:
        return basis, radial, None
    slope_cut = jnp.where(inside, (-0.5 * math.pi / cutoff_radius) * jnp.sin(angle), 0.0)
    grad_scaled = cutoff * (2.0 / cutoff_radius)
    second = [None, None, twice]
    second[1] = jnp.ones_like(scaled)
    for _ in range(3, NRAD):
        second.append(twice * second[-1] - second[-2])
    slopes = [slope_cut, slope_cut * scaled + grad_scaled]
    for p in range(2, NRAD):
        slopes.append(slope_cut * cheb[p] + grad_scaled * (float(p) * second[p]))
    return basis, radial, slopes


def harmonic_list(unit):
    table = scaled_legendre(unit[2])
    cosines, sines = azimuth_powers(unit[0], unit[1])
    columns = []
    for degree in range(LMAX + 1):
        for signed in range(-degree, degree + 1):
            azimuth = abs(signed)
            poly = table[degree, azimuth]
            if signed == 0:
                columns.append(poly)
            elif signed > 0:
                columns.append(poly * cosines[azimuth])
            else:
                columns.append(poly * sines[azimuth])
    columns[0] = jnp.full_like(unit[2], columns[0])
    return columns


def density_kernel(layer, info_ref, rad_ref, tab_ref, cen_ref, idx_ref, wt_ref, *refs):
    if layer == 1:
        out_ref, geo_ref, x_ref, y_ref, d_ref = refs
        feat_ref, put_ref = None, geo_ref
    else:
        geo_ref, out_ref, feat_ref, x_ref, y_ref, d_ref = refs
        put_ref = feat_ref
    tile = pl.program_id(0)
    count = info_ref[0, tile]
    row_low, row_high = info_ref[1, tile], info_ref[2, tile]
    blocks = lax.div(count + 7, 8)

    def gather_chunk(chunk, carry):
        fetch(tab_ref, 4, idx_ref, put_ref, chunk, row_low, row_high)
        return carry

    lax.fori_loop(0, lax.div(count + 31, 32), gather_chunk, 0)

    def edges(block_at, carry):
        base = pl.multiple_of(block_at * 8, 8)
        if layer == 1:
            live = wt_ref[pl.ds(base, 8), :] > 0.0
            deltas = []
            for axis in range(3):
                centre = jnp.broadcast_to(cen_ref[pl.ds(axis, 1), :], (8, TILE))
                delta = geo_ref[slot_rows(axis, base), :] - centre
                deltas.append(jnp.where(live, delta, 1.0))
            dist = jnp.sqrt(deltas[0] * deltas[0] + deltas[1] * deltas[1] + deltas[2] * deltas[2])
            inv = 1.0 / dist
            for axis in range(3):
                geo_ref[slot_rows(axis, base), :] = deltas[axis] * inv
            geo_ref[slot_rows(4, base), :] = dist
        weight, dist, unit, chan = geometry(layer, geo_ref, feat_ref, wt_ref, base)
        _, radial, _ = radial_terms(dist, rad_ref, False)
        for c in range(SPECIES):
            scale = chan[c] * weight
            for n in range(NMAX):
                x_ref[pl.ds(base * XROW + (c * NMAX + n), 8, stride=XROW), :] = scale * radial[n]
        for at, column in enumerate(harmonic_list(unit)):
            y_ref[slot_rows(at, base), :] = column
        return carry

    lax.fori_loop(0, blocks, edges, 0)
    groups = lax.div(count, SLOTS)

    def lm_block(block_at, carry):
        first = block_at * LBLK

        def slots(group, acc):
            acc = list(acc)
            for part in range(SLOTS):
                slot = group * SLOTS + part
                rows = [x_ref[pl.ds(slot * XROW + 8 * j, 8), :] for j in range(CH // 8)]
                for at in range(LBLK):
                    line = jnp.broadcast_to(
                        y_ref[pl.ds((first + at) * NPAD + slot, 1), :], (8, TILE)
                    )
                    for j in range(CH // 8):
                        acc[at * (CH // 8) + j] = acc[at * (CH // 8) + j] + rows[j] * line
            return tuple(acc)

        zero = jnp.zeros((8, TILE), f32)
        acc = lax.fori_loop(0, groups, slots, tuple(zero for _ in range(LBLK * (CH // 8))))
        for at in range(LBLK):
            for j in range(CH // 8):
                d_ref[pl.ds(8 * j * LM + first + at, 8, stride=LM), :] = acc[at * (CH // 8) + j]
        return carry

    lax.fori_loop(0, LM // LBLK, lm_block, 0)
    out_ref[...] = d_ref[...].astype(bf16)


def smem_spec():
    return pl.BlockSpec(memory_space=pltpu.SMEM)


def tile_spec(rows):
    return pl.BlockSpec((rows, TILE), lambda i: (0, i))


def whole_spec(shape):
    return pl.BlockSpec(shape, lambda i: tuple(0 for _ in shape))


def density_call(layer, info, radial, table, centres, index, weight, geo=None):
    atoms = centres.shape[1]
    rows = GEO if layer == 1 else SPECIES
    extra = () if geo is None else (geo,)
    return pl.pallas_call(
        partial(density_kernel, layer),
        out_shape=(
            jax.ShapeDtypeStruct((DENS, atoms), bf16),
            jax.ShapeDtypeStruct((rows * NPAD, atoms), f32),
        ),
        grid=(atoms // TILE,),
        in_specs=[
            smem_spec(),
            smem_spec(),
            whole_spec(table.shape),
            tile_spec(8),
            tile_spec(NPAD),
            tile_spec(NPAD),
        ]
        + [tile_spec(GEO * NPAD)] * len(extra),
        out_specs=(tile_spec(DENS), tile_spec(rows * NPAD)),
        scratch_shapes=[
            pltpu.VMEM((NPAD * XROW + 8, TILE), f32),
            pltpu.VMEM((LM * NPAD, TILE), f32),
            pltpu.VMEM((DENS, TILE), f32),
        ],
        compiler_params=pltpu.CompilerParams(vmem_limit_bytes=48 << 20),
        name="density_%d" % layer,
    )(info, radial, table, centres, index, weight, *extra)


def backward_kernel(layer, info_ref, rad_ref, geo_ref, feat_ref, idx_ref, wt_ref, dd_ref, win_in_ref,
                    own_in_ref, win_ref, own_ref, rgr_ref, x_ref, y_ref, gx_ref, gy_ref, val_ref,
                    left_ref):
    tile = pl.program_id(0)
    count = info_ref[0, tile]
    row_low, row_high = info_ref[1, tile], info_ref[2, tile]
    blocks = lax.div(count + 7, 8)
    zero = jnp.zeros((8, TILE), f32)

    @pl.when(tile == 0)
    def _():
        if layer == 1:
            win_ref[...] = win_in_ref[: 3 * WSTEP]
        else:
            win_ref[...] = jnp.zeros_like(win_ref)
        rgr_ref[...] = jnp.zeros_like(rgr_ref)

    def line_of(at):
        return jnp.broadcast_to(dd_ref[pl.ds(at, 1), :], (8, TILE))

    def contract_slots():
        def over_lm(step, acc):
            acc = list(acc)
            for part in range(LBLK):
                lm = step * LBLK + part
                col = y_ref[pl.ds(pl.multiple_of(lm * 8, 8), 8), :]
                for m in range(CH):
                    acc[m] = acc[m] + line_of(m * LM + lm) * col
            return tuple(acc)

        acc = lax.fori_loop(0, LM // LBLK, over_lm, tuple(zero for _ in range(CH)))
        for m in range(CH):
            gx_ref[8 * m : 8 * m + 8, :] = acc[m]

        def over_m(step, acc):
            acc = list(acc)
            for part in range(4):
                m = step * 4 + part
                col = x_ref[pl.ds(pl.multiple_of(m * 8, 8), 8), :]
                for lm in range(LM):
                    acc[lm] = acc[lm] + line_of(m * LM + lm) * col
            return tuple(acc)

        acc = lax.fori_loop(0, CH // 4, over_m, tuple(zero for _ in range(LM)))
        for lm in range(LM):
            gy_ref[8 * lm : 8 * lm + 8, :] = acc[lm]

    def contract_species(kind):
        odd = (kind == 1.0) | (kind == 3.0)
        upper = kind > 1.5

        def over_n(step, acc):
            acc = list(acc)
            for part in range(2):
                n = step * 2 + part
                at = pl.multiple_of(n * 8, 8)
                scaled = x_ref[pl.ds(at, 8), :]
                sums = [None, None]
                for lm in range(LM):
                    lines = [line_of((c * NMAX + n) * LM + lm) for c in range(SPECIES)]
                    first = jnp.where(odd, lines[1], lines[0])
                    second = jnp.where(odd, lines[3], lines[2])
                    grad = jnp.where(upper, second, first)
                    acc[lm] = acc[lm] + grad * scaled
                    term = grad * y_ref[8 * lm : 8 * lm + 8, :]
                    sums[lm % 2] = term if lm < 2 else sums[lm % 2] + term
                gx_ref[pl.ds(at, 8), :] = sums[0] + sums[1]
            return tuple(acc)

        acc = lax.fori_loop(0, NMAX // 2, over_n, tuple(zero for _ in range(LM)))
        for lm in range(LM):
            gy_ref[8 * lm : 8 * lm + 8, :] = acc[lm]

    def slot_block(block_at, own):
        base = pl.multiple_of(block_at * 8, 8)
        weight, dist, unit, chan = geometry(layer, geo_ref, feat_ref, wt_ref, base)
        _, radial, _ = radial_terms(dist, rad_ref, False)
        for at, column in enumerate(harmonic_list(unit)):
            y_ref[8 * at : 8 * at + 8, :] = column
        if layer == 1:
            for n in range(NMAX):
                x_ref[8 * n : 8 * n + 8, :] = weight * radial[n]
            contract_species(geo_ref[slot_rows(3, base), :])
        else:
            for c in range(SPECIES):
                scale = chan[c] * weight
                for n in range(NMAX):
                    at = 8 * (c * NMAX + n)
                    x_ref[at : at + 8, :] = scale * radial[n]
            contract_slots()
        weight, dist, unit, chan = geometry(layer, geo_ref, feat_ref, wt_ref, base)
        inv = 1.0 / dist
        basis, radial, slopes = radial_terms(dist, rad_ref, True)
        feat_grads = []
        radial_grads = [None] * NMAX
        if layer == 1:
            radial_grads = [gx_ref[8 * n : 8 * n + 8, :] for n in range(NMAX)]
        for c in range(SPECIES if layer == 2 else 0):
            total = None
            for n in range(NMAX):
                grad = gx_ref[8 * (c * NMAX + n) : 8 * (c * NMAX + n) + 8, :]
                term = grad * radial[n]
                total = term if total is None else total + term
                piece = grad * chan[c]
                radial_grads[n] = piece if c == 0 else radial_grads[n] + piece
            feat_grads.append(total * weight)
        grad_r = None
        radial_grads = [grad * weight for grad in radial_grads]
        for p in range(NRAD):
            total = None
            for n in range(NMAX):
                at = (n * NRAD + p) * 8
                rgr_ref[pl.ds(at, 8), :] = rgr_ref[pl.ds(at, 8), :] + radial_grads[n] * basis[p]
                term = radial_grads[n] * rad_ref[n, p]
                total = term if total is None else total + term
            term = total * slopes[p]
            grad_r = term if grad_r is None else grad_r + term
        table = scaled_legendre(unit[2])
        cosines, sines = azimuth_powers(unit[0], unit[1])
        grad_x = grad_y = grad_z = None

        def plus(total, term):
            return term if total is None else total + term

        for azimuth in range(LMAX + 1):
            grad_cos = grad_sin = None
            for degree in range(azimuth, LMAX + 1):
                at = degree * degree + degree
                up = gy_ref[8 * (at + azimuth) : 8 * (at + azimuth) + 8, :]
                poly = table[degree, azimuth]
                if azimuth:
                    down = gy_ref[8 * (at - azimuth) : 8 * (at - azimuth) + 8, :]
                    grad_cos = plus(grad_cos, up * poly)
                    grad_sin = plus(grad_sin, down * poly)
                if degree > azimuth:
                    ratio = norm_of(degree, azimuth) / norm_of(degree, azimuth + 1)
                    slope = ratio * table[degree, azimuth + 1]
                    if azimuth:
                        grad_z = plus(grad_z, slope * (up * cosines[azimuth] + down * sines[azimuth]))
                    else:
                        grad_z = plus(grad_z, slope * up)
            if azimuth == 1:
                grad_x, grad_y = grad_cos, grad_sin
            elif azimuth > 1:
                below_cos, below_sin = cosines[azimuth - 1], sines[azimuth - 1]
                grad_x = grad_x + float(azimuth) * (grad_cos * below_cos + grad_sin * below_sin)
                grad_y = grad_y + float(azimuth) * (grad_sin * below_cos - grad_cos * below_sin)
        dot_u = grad_x * unit[0] + grad_y * unit[1] + grad_z * unit[2]
        live = weight > 0.0
        out = []
        for axis, grad in enumerate((grad_x, grad_y, grad_z)):
            value = (grad - dot_u * unit[axis]) * inv + grad_r * unit[axis]
            out.append(jnp.where(live, value, 0.0))
        values = out + feat_grads
        for at, value in enumerate(values):
            val_ref[slot_rows(at, base), :] = value
        return tuple(total + value for total, value in zip(own, out))


    own = lax.fori_loop(0, blocks, slot_block, (zero, zero, zero))
    own = jnp.concatenate(
        [jnp.sum(total, axis=0, keepdims=True) for total in own] + [jnp.zeros((5, TILE), f32)], axis=0
    )
    own_ref[...] = own + own_in_ref[...] if layer == 1 else own

    used = 3 if layer == 1 else NVAL
    height = used * WROWS
    step_rows = height + 1
    sub = lax.broadcasted_iota(jnp.int32, (TILE, TILE), 0)
    windows = lax.div(row_high - row_low + WROWS, WROWS)

    def window(window_at, carry):
        row_base = row_low + window_at * WROWS

        def scatter(block_at, acc):
            base = pl.multiple_of(block_at * 8, 8)
            index = idx_ref[pl.ds(base, 8), :]
            hi = lax.shift_right_logical(index, 7)
            lo = lax.bitwise_and(index, 127)
            for row in range(WROWS):
                hit = hi == row_base + row
                for value_at in range(used):
                    value = val_ref[slot_rows(value_at, base), :]
                    left_ref[pl.ds(value_at * WROWS + row, 8, stride=step_rows), :] = jnp.where(
                        hit, value, 0.0
                    )
            ones, left = [], []
            for part in range(8):
                line = jnp.broadcast_to(lo[part : part + 1, :], (TILE, TILE))
                ones.append(jnp.where(line == sub, 1.0, 0.0).astype(bf16))
                left.append(left_ref[part * step_rows : part * step_rows + height, :])
            left = jnp.concatenate(left, axis=1)
            ones = jnp.concatenate(ones, axis=1)
            high = left.astype(bf16)
            rest = (left - high.astype(f32)).astype(bf16)
            dims = (((1,), (1,)), ((), ()))
            acc = acc + lax.dot_general(high, ones, dims, preferred_element_type=f32)
            return acc + lax.dot_general(rest, ones, dims, preferred_element_type=f32)

        acc = lax.fori_loop(0, blocks, scatter, jnp.zeros((height, TILE), f32))
        for value_at in range(used):
            at = value_at * WSTEP + row_base
            win_ref[pl.ds(at, WROWS), :] = (
                win_ref[pl.ds(at, WROWS), :] + acc[value_at * WROWS : (value_at + 1) * WROWS]
            )
        return carry

    lax.fori_loop(0, windows, window, 0)


def backward_call(layer, info, radial, geo, feat, index, weight, grad_dens, window_in, own_in):
    atoms = index.shape[1]
    values = 3 if layer == 1 else NVAL
    return pl.pallas_call(
        partial(backward_kernel, layer),
        out_shape=(
            jax.ShapeDtypeStruct((values * WSTEP, TILE), f32),
            jax.ShapeDtypeStruct((8, atoms), f32),
            jax.ShapeDtypeStruct((NMAX * NRAD * 8, TILE), f32),
        ),
        grid=(atoms // TILE,),
        in_specs=[
            smem_spec(),
            smem_spec(),
            tile_spec(GEO * NPAD),
            tile_spec(feat.shape[0]),
            tile_spec(NPAD),
            tile_spec(NPAD),
            tile_spec(DENS),
            whole_spec(window_in.shape),
            tile_spec(8),
        ],
        out_specs=(
            whole_spec((values * WSTEP, TILE)),
            tile_spec(8),
            whole_spec((NMAX * NRAD * 8, TILE)),
        ),
        scratch_shapes=[
            pltpu.VMEM((CH * 8, TILE), f32),
            pltpu.VMEM((LM * 8, TILE), f32),
            pltpu.VMEM((CH * 8, TILE), f32),
            pltpu.VMEM((LM * 8, TILE), f32),
            pltpu.VMEM((NVAL * NPAD, TILE), f32),
            pltpu.VMEM((8 * (NVAL * WROWS + 1), TILE), f32),
        ],
        compiler_params=pltpu.CompilerParams(vmem_limit_bytes=48 << 20),
        name="backward_%d" % layer,
    )(info, radial, geo, feat, index, weight, grad_dens, window_in, own_in)


def feature_map(invariants, mixing):
    inverse_rms = lax.rsqrt(jnp.mean(invariants * invariants, axis=0) + norm_eps)
    return jnp.einsum("qk,qa->ka", mixing, invariants, precision=highest) * inverse_rms


def contract(dens_in, coupling):
    factors = jnp.einsum("vdq,da->vqa", coupling, dens_in, preferred_element_type=f32)
    product = reduce(
        lambda earlier, later: earlier * later,
        [factors[index_v] for index_v in range(factors.shape[0])],
    )
    return (factors, product)


def contract_back(factors, upstream, coupling):
    partials = []
    for factor_at in range(factors.shape[0]):
        others = upstream
        for partner in range(factors.shape[0]):
            if partner != factor_at:
                others = others * factors[partner]
        partials.append(others)
    rounded = jnp.stack(partials).astype(bf16)
    return jnp.einsum("vdq,vqa->da", coupling, rounded, preferred_element_type=f32)


def per_device(
    positions,
    species,
    neighbours,
    slot_counts,
    structure,
    target_energy,
    radial_one,
    coupling_one,
    coefficient_one,
    mixing,
    radial_two,
    coupling_two,
    coefficient_two,
):
    atoms = positions.shape[2]
    tiles = atoms // TILE
    site = jnp.concatenate(
        [
            positions[:, 0, :],
            species.astype(f32),
            structure.astype(f32),
            jnp.zeros((3, atoms), f32),
        ],
        axis=0,
    )
    table_one = spread_call(0, 4, site)
    first = ((lax.axis_index("dom") - 1) * atoms).astype(jnp.int32).reshape(1)
    index, weight, ordered, perm, info = prepare_call(first, slot_counts, neighbours[:, 0, :], site)
    onehot = (ordered[3:4] == jnp.arange(SPECIES, dtype=f32)[:, None]).astype(f32)

    dens_one, geo = density_call(1, info, radial_one, table_one, ordered, index, weight)
    factors_one, invariants_one = contract(dens_one, coupling_one)
    chosen_one = jnp.dot(coefficient_one.T, onehot, precision=highest)
    energy_one = jnp.sum(invariants_one * chosen_one, axis=0)
    features, features_back = jax.vjp(feature_map, invariants_one, mixing)
    features8 = jnp.pad(features, ((0, 8 - SPECIES), (0, 0)))
    table_two = spread_call(1, SPECIES, features8, perm)
    dens_two, feat = density_call(2, info, radial_two, table_two, ordered, index, weight, geo)
    factors_two, invariants_two = contract(dens_two, coupling_two)
    chosen_two = jnp.dot(coefficient_two.T, onehot, precision=highest)
    site_energy = energy_one + jnp.sum(invariants_two * chosen_two, axis=0)
    structures = target_energy.shape[1]
    members = (ordered[4][:, None] == jnp.arange(structures, dtype=f32)[None, :]).astype(f32)
    per_structure = jnp.dot(
        jnp.concatenate([site_energy[None, :], onehot], axis=0), members, precision=highest
    )
    target = jnp.where(lax.axis_index("dom") == 0, target_energy, 0.0)
    per_structure = jnp.concatenate([per_structure, target], axis=0)

    grad_dens_two = contract_back(factors_two, chosen_two, coupling_two)
    blank_window = jnp.zeros((8, TILE), f32)
    blank_own = jnp.zeros((8, atoms), f32)
    window_two, own_two, rgr_two = backward_call(
        2, info, radial_two, geo, feat, index, weight, grad_dens_two, blank_window, blank_own
    )
    grad_features = collect_call(
        2, tiles, 3, window_two.reshape(NVAL, WSTEP, TILE), perm
    )[:SPECIES]
    coefficient_second = jnp.dot(onehot, invariants_two.T, precision=highest)
    grad_invariants, mixing_gradient = features_back(grad_features)
    grad_dens_one = contract_back(factors_one, chosen_one + grad_invariants, coupling_one)
    window_one, own_one, rgr_one = backward_call(
        1, info, radial_one, geo, blank_own, index, weight, grad_dens_one, window_two, own_two
    )
    coefficient_first = jnp.dot(onehot, invariants_one.T, precision=highest)

    def radial_sum(partial_grad):
        return jnp.sum(partial_grad.reshape(NMAX * NRAD, 8 * TILE), axis=1)

    groups = lax.axis_size("grp")
    mine = lax.axis_index("grp") == jnp.arange(groups, dtype=jnp.int32)
    slots = jnp.where(mine[:, None, None], per_structure[None], 0.0)
    quantum = coefficient_first.shape[1]
    wide = SPECIES * quantum
    radials = jnp.zeros((8 * TILE,), f32)
    radials = radials.at[: NMAX * NRAD].set(radial_sum(rgr_one))
    radials = radials.at[TILE : TILE + NMAX * NRAD].set(radial_sum(rgr_two))
    payload = jnp.concatenate(
        [
            radials,
            coefficient_first.reshape(-1),
            coefficient_second.reshape(-1),
            mixing_gradient.T.reshape(-1),
            slots.reshape(-1),
        ]
    )
    sums_at = 8 + 3 * wide // TILE
    steps = log2_of(lax.axis_size("dom")) + log2_of(groups)
    forces, sums, energies, offsets = finish_call(
        3,
        steps,
        tiles,
        sums_at,
        structures // TILE,
        window_one.reshape(3, WSTEP, TILE),
        own_one,
        perm,
        payload.reshape(-1, TILE),
    )
    parts = sums[8:sums_at].reshape(3, SPECIES, quantum)
    return (
        energies.reshape(1, structures),
        offsets[:SPECIES, 0],
        forces[:3].reshape(3, 1, atoms),
        sums[0, : NMAX * NRAD].reshape(NMAX, NRAD),
        parts[0],
        parts[2].T,
        sums[1, : NMAX * NRAD].reshape(NMAX, NRAD),
        parts[1],
    )


def solution(mesh):
    in_specs = (
        P(None, "grp", "dom"),
        P("grp", "dom"),
        P(None, "grp", "dom"),
        P("grp", "dom"),
        P("grp", "dom"),
        P("grp", None),
        P(),
        P(),
        P(),
        P(),
        P(),
        P(),
        P(),
    )
    out_specs = (P("grp", None), P(), P(None, "grp", "dom"), P(), P(), P(), P(), P())
    return jax.shard_map(
        per_device, mesh=mesh, in_specs=in_specs, out_specs=out_specs, check_vma=False
    )
```

```python
from functools import partial
import math

import jax
import jax.numpy as jnp
from jax import lax
from jax.experimental import pallas as pl
from jax.experimental.pallas import tpu as pltpu
from jax.sharding import PartitionSpec as P

NRAD = 12
NMAX = 10
LMAX = 6
LM = 49
SPECIES = 4
CH = SPECIES * NMAX
DENS = CH * LM
NBR = 48
NPAD = 64
TILE = 128
LBLK = 7
WROWS = 12
WSTEP = 40
GEO = 5
QB = 128
DROWS = 400
NVAL = 7
SLOTS = 4
XROW = CH + 1

cutoff_radius = 5.0
density_scale = 0.17
norm_eps = 1e-05
ridge_weight = 0.1
highest = lax.Precision.HIGHEST
f32 = jnp.float32
MESH = pl.DeviceIdType.MESH
bf16 = jnp.bfloat16


def log2_of(count):
    steps = count.bit_length() - 1
    assert count == 1 << steps
    return steps


def neighbour_flags(me, count):
    return me > 0, me < count - 1


def greet(partners, flags):
    barrier = pltpu.get_barrier_semaphore()
    for partner, flag in zip(partners, flags):
        if flag is None:
            pl.semaphore_signal(barrier, inc=1, device_id=partner, device_id_type=MESH)
        else:

            @pl.when(flag)
            def _(partner=partner):
                pl.semaphore_signal(barrier, inc=1, device_id=partner, device_id_type=MESH)

    present = sum(1 for flag in flags if flag is None)
    for flag in flags:
        if flag is not None:
            present = present + jnp.where(flag, 1, 0)
    pl.semaphore_wait(barrier, present)


class SidePair:
    def __init__(self, to_left, to_right, got_ref, send_sem, recv_sem):
        count = lax.axis_size("dom")
        me = lax.axis_index("dom")
        self.partners = ({"dom": me - 1}, {"dom": me + 1})
        self.flags = neighbour_flags(me, count)
        self.got = got_ref
        self.copies = [
            pltpu.make_async_remote_copy(
                src_ref=source,
                dst_ref=got_ref.at[1 - side],
                send_sem=send_sem.at[side],
                recv_sem=recv_sem.at[1 - side],
                device_id=self.partners[side],
                device_id_type=MESH,
            )
            for side, source in enumerate((to_left, to_right))
        ]

    def start(self):
        for side in range(2):
            pl.when(self.flags[side])(self.copies[side].start)

    def wait(self):
        for side in range(2):

            @pl.when(self.flags[side])
            def _(side=side):
                self.copies[side].wait_send()
                self.copies[1 - side].wait_recv()

    def received(self, side):
        return jnp.where(self.flags[side], self.got[side], 0.0)


def split3(value):
    high = value.astype(bf16)
    rest = value - high.astype(f32)
    middle = rest.astype(bf16)
    low = (rest - middle.astype(f32)).astype(bf16)
    return jnp.concatenate([high, middle, low], axis=0)


def reorder(value, perm_ref, contract_at):
    count = value.shape[0]
    out = lax.dot_general(
        split3(value), perm_ref[...], (((1,), (contract_at,)), ((), ())), preferred_element_type=f32
    )
    return out[:count] + (out[count : 2 * count] + out[2 * count :])


def spread_kernel(values, ordered, *refs):
    if ordered:
        x_ref, out_ref, mine_ref, got_ref, send_sem, recv_sem = refs
        flat = x_ref[...]
    else:
        x_ref, perm_ref, out_ref, mine_ref, got_ref, send_sem, recv_sem = refs
        flat = reorder(x_ref[...], perm_ref, 0)
    rows = flat.shape[1] // TILE
    for value in range(values):
        for row in range(rows):
            line = flat[value : value + 1, row * TILE : (row + 1) * TILE]
            at = value * rows + row
            mine_ref[at : at + 1, :] = line
    pair = SidePair(mine_ref, mine_ref, got_ref, send_sem, recv_sem)
    greet(pair.partners, pair.flags)
    pair.start()
    for value in range(values):
        at = value * 3 * rows
        out_ref[at + rows : at + 2 * rows, :] = mine_ref[value * rows : (value + 1) * rows, :]
    pair.wait()
    for side in range(2):
        block = pair.received(side)
        for value in range(values):
            at = value * 3 * rows + 2 * side * rows
            out_ref[at : at + rows, :] = block[value * rows : (value + 1) * rows]


def comm_params(which):
    return pltpu.CompilerParams(collective_id=which, has_side_effects=True)


def vmem_spec():
    return pl.BlockSpec(memory_space=pltpu.VMEM)


def spread_call(which, values, cells, perm=None):
    rows = values * cells.shape[1] // TILE
    operands = (cells,) if perm is None else (cells, perm)
    return pl.pallas_call(
        partial(spread_kernel, values, perm is None),
        out_shape=jax.ShapeDtypeStruct((rows * 3, TILE), f32),
        in_specs=[vmem_spec()] * len(operands),
        out_specs=vmem_spec(),
        scratch_shapes=[
            pltpu.VMEM((rows, TILE), f32),
            pltpu.VMEM((2, rows, TILE), f32),
            pltpu.SemaphoreType.DMA((2,)),
            pltpu.SemaphoreType.DMA((2,)),
        ],
        compiler_params=comm_params(which),
        name="spread_%d" % which,
    )(*operands)


def in_lanes(blocks):
    values, rows = blocks.shape[0], blocks.shape[1]
    flat = [
        jnp.concatenate([blocks[v, r : r + 1, :] for r in range(rows)], axis=1) for v in range(values)
    ]
    return jnp.concatenate(flat + [jnp.zeros((8 - values, rows * TILE), f32)], axis=0)


def collect_kernel(rows, values_at, win_ref, perm_ref, out_ref, got_ref, send_sem, recv_sem):
    pair = SidePair(
        win_ref.at[values_at:, 0:rows],
        win_ref.at[values_at:, 2 * rows : 3 * rows],
        got_ref,
        send_sem,
        recv_sem,
    )
    greet(pair.partners, pair.flags)
    pair.start()
    pair.wait()
    total = win_ref[values_at:, rows : 2 * rows] + pair.received(0) + pair.received(1)
    out_ref[...] = reorder(in_lanes(total), perm_ref, 1)


def collect_call(which, rows, values_at, window, perm):
    values = window.shape[0] - values_at
    return pl.pallas_call(
        partial(collect_kernel, rows, values_at),
        out_shape=jax.ShapeDtypeStruct((8, rows * TILE), f32),
        in_specs=[vmem_spec()] * 2,
        out_specs=vmem_spec(),
        scratch_shapes=[
            pltpu.VMEM((2, values, rows, TILE), f32),
            pltpu.SemaphoreType.DMA((2,)),
            pltpu.SemaphoreType.DMA((2,)),
        ],
        compiler_params=comm_params(which),
        name="collect_%d" % which,
    )(window, perm)


def finish_kernel(rows, sums_at, per_group, win_ref, own_ref, perm_ref, pay_ref, force_ref, sum_ref, energy_ref,
                  offset_ref, got_ref, came_ref, send_sem, recv_sem, step_send, step_recv):
    pair = SidePair(
        win_ref.at[:, 0:rows], win_ref.at[:, 2 * rows : 3 * rows], got_ref, send_sem, recv_sem
    )
    partners = []
    for axis in ("dom", "grp"):
        me = lax.axis_index(axis)
        for bit in range(log2_of(lax.axis_size(axis))):
            half = 1 << bit
            partners.append({axis: me + half - 2 * half * lax.rem(lax.div(me, half), 2)})
    greet(list(pair.partners) + partners, list(pair.flags) + [None] * len(partners))
    pair.start()
    force_ref[...] = reorder(own_ref[...], perm_ref, 0)
    for step, partner in enumerate(partners):
        source = pay_ref if step == 0 else sum_ref
        copy = pltpu.make_async_remote_copy(
            src_ref=source,
            dst_ref=came_ref.at[step],
            send_sem=step_send.at[step],
            recv_sem=step_recv.at[step],
            device_id=partner,
            device_id_type=MESH,
        )
        copy.start()
        copy.wait()
        sum_ref[...] = source[...] + came_ref[step]
    pair.wait()
    total = win_ref[:, rows : 2 * rows] + pair.received(0) + pair.received(1)
    force_ref[...] = force_ref[...] - in_lanes(total)

    groups = lax.axis_size("grp")
    gram = [[None] * SPECIES for _ in range(SPECIES)]
    right = [None] * SPECIES

    def fractions(base):
        counts = [
            sum_ref[pl.ds(base + (1 + c) * per_group, per_group), :] for c in range(SPECIES)
        ]
        size = jnp.maximum(counts[0] + counts[1] + counts[2] + counts[3], 1.0)
        return [count / size for count in counts], size

    def gather_sum(total, value):
        part = jnp.sum(jnp.sum(value, axis=0, keepdims=True), axis=1, keepdims=True)
        return part if total is None else total + part

    stride = (SPECIES + 2) * per_group
    for group in range(groups):
        base = sums_at + group * stride
        frac, _ = fractions(base)
        target = sum_ref[pl.ds(base + (1 + SPECIES) * per_group, per_group), :]
        for c in range(SPECIES):
            right[c] = gather_sum(right[c], frac[c] * target)
            for d in range(c, SPECIES):
                gram[c][d] = gather_sum(gram[c][d], frac[c] * frac[d])
    matrix = [
        [gram[min(c, d)][max(c, d)] + (ridge_weight if c == d else 0.0) for d in range(SPECIES)]
        for c in range(SPECIES)
    ]
    for pivot in range(SPECIES):
        for below in range(pivot + 1, SPECIES):
            ratio = matrix[below][pivot] / matrix[pivot][pivot]
            matrix[below] = [b - ratio * a for a, b in zip(matrix[pivot], matrix[below])]
            right[below] = right[below] - ratio * right[pivot]
    answer = [None] * SPECIES
    for row in range(SPECIES - 1, -1, -1):
        running = right[row]
        for later in range(row + 1, SPECIES):
            running = running - matrix[row][later] * answer[later]
        answer[row] = running / matrix[row][row]
    mine = sums_at + lax.axis_index("grp") * stride
    frac, size = fractions(mine)
    energy = sum_ref[pl.ds(mine, per_group), :] / size
    for c in range(SPECIES):
        energy = energy + frac[c] * answer[c]
    energy_ref[...] = energy
    offset_ref[...] = jnp.concatenate(
        [jnp.broadcast_to(value, (1, TILE)) for value in answer] + [jnp.zeros((4, TILE), f32)], axis=0
    )


def finish_call(which, mesh_steps, rows, sums_at, per_group, window, own, perm, payload):
    size = payload.shape[0]
    return pl.pallas_call(
        partial(finish_kernel, rows, sums_at, per_group),
        out_shape=(
            jax.ShapeDtypeStruct((8, rows * TILE), f32),
            jax.ShapeDtypeStruct((size, TILE), f32),
            jax.ShapeDtypeStruct((per_group, TILE), f32),
            jax.ShapeDtypeStruct((8, TILE), f32),
        ),
        in_specs=[vmem_spec()] * 4,
        out_specs=(vmem_spec(),) * 4,
        scratch_shapes=[
            pltpu.VMEM((2, 3, rows, TILE), f32),
            pltpu.VMEM((mesh_steps, size, TILE), f32),
            pltpu.SemaphoreType.DMA((2,)),
            pltpu.SemaphoreType.DMA((2,)),
            pltpu.SemaphoreType.DMA((mesh_steps,)),
            pltpu.SemaphoreType.DMA((mesh_steps,)),
        ],
        compiler_params=comm_params(which),
        name="finish_%d" % which,
    )(window, own, perm, payload)


def double_factorial(number):
    result = 1.0
    while number > 1:
        result = result * number
        number = number - 2
    return result


def norm_of(degree, azimuth):
    value = math.sqrt(
        (2 * degree + 1)
        / (4 * math.pi)
        * math.factorial(degree - azimuth)
        / math.factorial(degree + azimuth)
    )
    return value * (math.sqrt(2.0) if azimuth else 1.0)


def scaled_legendre(coord_z):
    table = {}
    for azimuth in range(LMAX + 1):
        table[azimuth, azimuth] = norm_of(azimuth, azimuth) * double_factorial(2 * azimuth - 1)
        if azimuth + 1 <= LMAX:
            ratio = norm_of(azimuth + 1, azimuth) / norm_of(azimuth, azimuth)
            table[azimuth + 1, azimuth] = coord_z * (
                (2 * azimuth + 1) * ratio * table[azimuth, azimuth]
            )
        for degree in range(azimuth + 2, LMAX + 1):
            gap = degree - azimuth
            first = (2 * degree - 1) / gap * norm_of(degree, azimuth) / norm_of(degree - 1, azimuth)
            second = (
                (degree + azimuth - 1) / gap * norm_of(degree, azimuth) / norm_of(degree - 2, azimuth)
            )
            table[degree, azimuth] = (first * coord_z) * table[degree - 1, azimuth] - (
                second * table[degree - 2, azimuth]
            )
    return table


def azimuth_powers(coord_x, coord_y):
    cosines = [None, coord_x]
    sines = [None, coord_y]
    for _ in range(2, LMAX + 1):
        cosines.append(cosines[-1] * coord_x - sines[-1] * coord_y)
        sines.append(sines[-1] * coord_x + cosines[-2] * coord_y)
    return cosines, sines


LANE_GATHER = lax.GatherDimensionNumbers(
    offset_dims=(),
    collapsed_slice_dims=(1,),
    start_index_map=(1,),
    operand_batching_dims=(0,),
    start_indices_batching_dims=(0,),
)


def lane_gather(line, lo):
    return lax.gather(
        line,
        lo[..., None],
        LANE_GATHER,
        slice_sizes=(1, 1),
        mode=lax.GatherScatterMode.PROMISE_IN_BOUNDS,
    )


def prepare_kernel(first_ref, cnt_ref, nbr_ref, site_ref, idx_ref, wt_ref, sorted_ref, perm_ref, info_ref,
                   key_ref, pos_ref, word_ref, rank_ref):
    atoms = nbr_ref.shape[1]
    tiles = atoms // TILE
    blocks = NBR // 8
    sub = lax.broadcasted_iota(jnp.int32, (8, TILE), 0)
    lane = lax.broadcasted_iota(jnp.int32, (1, TILE), 1)

    def merge(tile, carry):
        cols = pl.ds(pl.multiple_of(tile * TILE, TILE), TILE)
        limit = cnt_ref[:, cols]
        iota = lax.broadcasted_iota(jnp.int32, (NBR, TILE), 0)
        key = jnp.where(iota < limit, nbr_ref[:, cols] - first_ref[0], -1 - iota)
        key_ref[...] = key
        keys = [key[8 * b : 8 * b + 8] for b in range(blocks)]
        total = [jnp.zeros((8, TILE), jnp.int32) for _ in range(blocks)]
        early = [jnp.zeros((8, TILE), jnp.int32) for _ in range(blocks)]
        for other in range(NBR):
            line = jnp.broadcast_to(key_ref[other : other + 1, :], (8, TILE))
            for b in range(blocks):
                same = jnp.where(keys[b] == line, 1, 0)
                total[b] = total[b] + same
                if other < 8 * b:
                    early[b] = early[b] + same
                elif other < 8 * b + 7:
                    early[b] = early[b] + jnp.where(sub > other - 8 * b, same, 0)
        for b in range(blocks):
            alive = sub + 8 * b < limit
            pos_ref[8 * b : 8 * b + 8, :] = jnp.where(alive & (early[b] == 0), 1, 0)
            key_ref[8 * b : 8 * b + 8, :] = total[b] * 4096 + keys[b]
        running = jnp.zeros((1, TILE), jnp.int32)
        out = [jnp.zeros((8, TILE), jnp.int32) for _ in range(blocks)]
        for slot in range(NBR):
            flag = pos_ref[slot : slot + 1, :]
            place = jnp.broadcast_to(jnp.where(flag == 1, running, -1), (8, TILE))
            running = running + flag
            line = jnp.broadcast_to(key_ref[slot : slot + 1, :], (8, TILE))
            for b in range(slot // 8 + 1):
                out[b] = jnp.where(place == sub + 8 * b, line, out[b])
        for b in range(blocks):
            word_ref[8 * b : 8 * b + 8, cols] = out[b].astype(f32)
        order = running * atoms + (atoms - 1 - tile * TILE) - lane
        rank_ref[pl.ds(tile, 1), :] = order.astype(f32)
        return carry

    lax.fori_loop(0, tiles, merge, 0)
    orders = rank_ref[...]
    upright = jnp.transpose(orders)
    ranks = []
    for tile in range(tiles):
        row = jnp.broadcast_to(orders[tile : tile + 1], (TILE, TILE))
        total = jnp.zeros((TILE, TILE), f32)
        for other in range(tiles):
            col = jnp.broadcast_to(upright[:, other : other + 1], (TILE, TILE))
            total = total + jnp.where(col > row, 1.0, 0.0)
        ranks.append(jnp.sum(total, axis=0, keepdims=True))
    place = lax.broadcasted_iota(jnp.int32, (atoms, TILE), 0).astype(f32)
    for tile in range(tiles):
        line = jnp.broadcast_to(ranks[tile], (atoms, TILE))
        perm_ref[:, tile * TILE : (tile + 1) * TILE] = jnp.where(line == place, 1.0, 0.0).astype(bf16)
    word_ref[NBR : NBR + 8, :] = site_ref[...]
    moved = reorder(word_ref[...], perm_ref, 1)
    sorted_ref[...] = moved[NBR:]
    word = moved[:NBR].astype(jnp.int32)
    index = lax.bitwise_and(word, 4095)
    times = lax.shift_right_logical(word, 12)
    idx_ref[:NBR, :] = index
    idx_ref[NBR:, :] = jnp.zeros((NPAD - NBR, atoms), jnp.int32)
    wt_ref[:NBR, :] = density_scale * times.astype(f32)
    wt_ref[NBR:, :] = jnp.zeros((NPAD - NBR, atoms), f32)
    row = lax.shift_right_logical(index, 7)
    low = jnp.min(jnp.where(times > 0, row, 1 << 20))
    high = jnp.max(jnp.where(times > 0, row, -1))
    slots = lax.broadcasted_iota(jnp.int32, (NBR, TILE), 0) + 1
    for tile in range(tiles):
        used = times[:, tile * TILE : (tile + 1) * TILE] > 0
        info_ref[0, tile] = lax.div(jnp.max(jnp.where(used, slots, 0)) + SLOTS - 1, SLOTS) * SLOTS
        info_ref[1, tile] = low
        info_ref[2, tile] = high


def prepare_call(first, limits, neighbours, site):
    atoms = neighbours.shape[1]
    return pl.pallas_call(
        prepare_kernel,
        out_shape=(
            jax.ShapeDtypeStruct((NPAD, atoms), jnp.int32),
            jax.ShapeDtypeStruct((NPAD, atoms), f32),
            jax.ShapeDtypeStruct((8, atoms), f32),
            jax.ShapeDtypeStruct((atoms, atoms), bf16),
            jax.ShapeDtypeStruct((3, atoms // TILE), jnp.int32),
        ),
        in_specs=[smem_spec(), vmem_spec(), vmem_spec(), vmem_spec()],
        out_specs=(vmem_spec(), vmem_spec(), vmem_spec(), vmem_spec(), smem_spec()),
        scratch_shapes=[
            pltpu.VMEM((NBR, TILE), jnp.int32),
            pltpu.VMEM((NBR, TILE), jnp.int32),
            pltpu.VMEM((NBR + 8, atoms), f32),
            pltpu.VMEM((atoms // TILE, TILE), f32),
        ],
        name="prepare",
    )(first, limits, neighbours, site)


def fetch(tab_ref, values, idx_ref, put_ref, chunk, row_low, row_high):
    start = pl.multiple_of(chunk * 32, 32)
    index = [idx_ref[pl.ds(start + 8 * kb, 8), :] for kb in range(4)]
    hi = [lax.shift_right_logical(word, 7) for word in index]
    lo = [lax.bitwise_and(word, 127) for word in index]

    def body(row, found):
        found = list(found)
        hits = [word == row for word in hi]
        for value in range(values):
            line = jnp.broadcast_to(tab_ref[pl.ds(value * 24 + row, 1), :], (8, TILE))
            for kb in range(4):
                at = value * 4 + kb
                found[at] = jnp.where(hits[kb], lane_gather(line, lo[kb]), found[at])
        return tuple(found)

    zero = jnp.zeros((8, TILE), f32)
    found = lax.fori_loop(row_low, row_high + 1, body, tuple(zero for _ in range(4 * values)))
    for value in range(values):
        for kb in range(4):
            put_ref[pl.ds(pl.multiple_of(value * NPAD + start + 8 * kb, 8), 8), :] = found[value * 4 + kb]


def slot_rows(which, base):
    return pl.ds(pl.multiple_of(which * NPAD + base, 8), 8)


def geometry(layer, geo_ref, feat_ref, wt_ref, base):
    weight = wt_ref[pl.ds(base, 8), :]
    unit = [geo_ref[slot_rows(axis, base), :] for axis in range(3)]
    dist = geo_ref[slot_rows(4, base), :]
    if layer == 1:
        kind = geo_ref[slot_rows(3, base), :]
        chan = [jnp.where(kind == float(c), 1.0, 0.0) for c in range(SPECIES)]
    else:
        chan = [feat_ref[slot_rows(c, base), :] for c in range(SPECIES)]
    return weight, dist, unit, chan


def radial_terms(dist, rad_ref, with_slope):
    scaled = dist * (2.0 / cutoff_radius) - 1.0
    inside = dist < cutoff_radius
    angle = dist * (math.pi / cutoff_radius)
    cutoff = jnp.where(inside, 0.5 * (jnp.cos(angle) + 1.0), 0.0)
    cheb = [None, scaled]
    twice = 2.0 * scaled
    cheb.append(twice * scaled - 1.0)
    for _ in range(3, NRAD):
        cheb.append(twice * cheb[-1] - cheb[-2])
    basis = [cutoff] + [cutoff * cheb[p] for p in range(1, NRAD)]
    radial = []
    for n in range(NMAX):
        total = basis[0] * rad_ref[n, 0]
        for p in range(1, NRAD):
            total = total + basis[p] * rad_ref[n, p]
        radial.append(total)
    if not with_slope:
        return basis, radial, None
    slope_cut = jnp.where(inside, (-0.5 * math.pi / cutoff_radius) * jnp.sin(angle), 0.0)
    grad_scaled = cutoff * (2.0 / cutoff_radius)
    second = [None, None, twice]
    second[1] = jnp.ones_like(scaled)
    for _ in range(3, NRAD):
        second.append(twice * second[-1] - second[-2])
    slopes = [slope_cut, slope_cut * scaled + grad_scaled]
    for p in range(2, NRAD):
        slopes.append(slope_cut * cheb[p] + grad_scaled * (float(p) * second[p]))
    return basis, radial, slopes


def harmonic_list(unit):
    table = scaled_legendre(unit[2])
    cosines, sines = azimuth_powers(unit[0], unit[1])
    columns = []
    for degree in range(LMAX + 1):
        for signed in range(-degree, degree + 1):
            azimuth = abs(signed)
            poly = table[degree, azimuth]
            if signed == 0:
                columns.append(poly)
            elif signed > 0:
                columns.append(poly * cosines[azimuth])
            else:
                columns.append(poly * sines[azimuth])
    columns[0] = jnp.full_like(unit[2], columns[0])
    return columns


def density_kernel(layer, info_ref, rad_ref, tab_ref, cen_ref, idx_ref, wt_ref, *refs):
    if layer == 1:
        out_ref, geo_ref, x_ref, y_ref, d_ref = refs
        feat_ref, put_ref = None, geo_ref
    else:
        geo_ref, out_ref, feat_ref, x_ref, y_ref, d_ref = refs
        put_ref = feat_ref
    tile = pl.program_id(0)
    count = info_ref[0, tile]
    row_low, row_high = info_ref[1, tile], info_ref[2, tile]
    blocks = lax.div(count + 7, 8)

    def gather_chunk(chunk, carry):
        fetch(tab_ref, 4, idx_ref, put_ref, chunk, row_low, row_high)
        return carry

    lax.fori_loop(0, lax.div(count + 31, 32), gather_chunk, 0)

    def edges(block_at, carry):
        base = pl.multiple_of(block_at * 8, 8)
        if layer == 1:
            live = wt_ref[pl.ds(base, 8), :] > 0.0
            deltas = []
            for axis in range(3):
                centre = jnp.broadcast_to(cen_ref[pl.ds(axis, 1), :], (8, TILE))
                delta = geo_ref[slot_rows(axis, base), :] - centre
                deltas.append(jnp.where(live, delta, 1.0))
            dist = jnp.sqrt(deltas[0] * deltas[0] + deltas[1] * deltas[1] + deltas[2] * deltas[2])
            inv = 1.0 / dist
            for axis in range(3):
                geo_ref[slot_rows(axis, base), :] = deltas[axis] * inv
            geo_ref[slot_rows(4, base), :] = dist
        weight, dist, unit, chan = geometry(layer, geo_ref, feat_ref, wt_ref, base)
        _, radial, _ = radial_terms(dist, rad_ref, False)
        for c in range(SPECIES):
            scale = chan[c] * weight
            for n in range(NMAX):
                x_ref[pl.ds(base * XROW + (c * NMAX + n), 8, stride=XROW), :] = scale * radial[n]
        for at, column in enumerate(harmonic_list(unit)):
            y_ref[slot_rows(at, base), :] = column
        return carry

    lax.fori_loop(0, blocks, edges, 0)
    groups = lax.div(count, SLOTS)

    def lm_block(block_at, carry):
        first = block_at * LBLK

        def slots(group, acc):
            acc = list(acc)
            for part in range(SLOTS):
                slot = group * SLOTS + part
                rows = [x_ref[pl.ds(slot * XROW + 8 * j, 8), :] for j in range(CH // 8)]
                for at in range(LBLK):
                    line = jnp.broadcast_to(
                        y_ref[pl.ds((first + at) * NPAD + slot, 1), :], (8, TILE)
                    )
                    for j in range(CH // 8):
                        acc[at * (CH // 8) + j] = acc[at * (CH // 8) + j] + rows[j] * line
            return tuple(acc)

        zero = jnp.zeros((8, TILE), f32)
        acc = lax.fori_loop(0, groups, slots, tuple(zero for _ in range(LBLK * (CH // 8))))
        for at in range(LBLK):
            for j in range(CH // 8):
                d_ref[pl.ds(8 * j * LM + first + at, 8, stride=LM), :] = acc[at * (CH // 8) + j]
        return carry

    lax.fori_loop(0, LM // LBLK, lm_block, 0)
    out_ref[...] = d_ref[...].astype(bf16)


def smem_spec():
    return pl.BlockSpec(memory_space=pltpu.SMEM)


def tile_spec(rows):
    return pl.BlockSpec((rows, TILE), lambda i: (0, i))


def whole_spec(shape):
    return pl.BlockSpec(shape, lambda i: tuple(0 for _ in shape))


def density_call(layer, info, radial, table, centres, index, weight, geo=None):
    atoms = centres.shape[1]
    rows = GEO if layer == 1 else SPECIES
    extra = () if geo is None else (geo,)
    return pl.pallas_call(
        partial(density_kernel, layer),
        out_shape=(
            jax.ShapeDtypeStruct((DENS, atoms), bf16),
            jax.ShapeDtypeStruct((rows * NPAD, atoms), f32),
        ),
        grid=(atoms // TILE,),
        in_specs=[
            smem_spec(),
            smem_spec(),
            whole_spec(table.shape),
            tile_spec(8),
            tile_spec(NPAD),
            tile_spec(NPAD),
        ]
        + [tile_spec(GEO * NPAD)] * len(extra),
        out_specs=(tile_spec(DENS), tile_spec(rows * NPAD)),
        scratch_shapes=[
            pltpu.VMEM((NPAD * XROW + 8, TILE), f32),
            pltpu.VMEM((LM * NPAD, TILE), f32),
            pltpu.VMEM((DENS, TILE), f32),
        ],
        compiler_params=pltpu.CompilerParams(vmem_limit_bytes=48 << 20),
        name="density_%d" % layer,
    )(info, radial, table, centres, index, weight, *extra)


def backward_kernel(layer, info_ref, rad_ref, geo_ref, feat_ref, idx_ref, wt_ref, dd_ref, win_in_ref,
                    own_in_ref, win_ref, own_ref, rgr_ref, x_ref, y_ref, gx_ref, gy_ref, val_ref,
                    left_ref):
    tile = pl.program_id(0)
    count = info_ref[0, tile]
    row_low, row_high = info_ref[1, tile], info_ref[2, tile]
    blocks = lax.div(count + 7, 8)
    zero = jnp.zeros((8, TILE), f32)

    @pl.when(tile == 0)
    def _():
        if layer == 1:
            win_ref[...] = win_in_ref[: 3 * WSTEP]
        else:
            win_ref[...] = jnp.zeros_like(win_ref)
        rgr_ref[...] = jnp.zeros_like(rgr_ref)

    def line_of(at):
        return jnp.broadcast_to(dd_ref[pl.ds(at, 1), :], (8, TILE))

    def contract_slots():
        def over_lm(step, acc):
            acc = list(acc)
            for part in range(LBLK):
                lm = step * LBLK + part
                col = y_ref[pl.ds(pl.multiple_of(lm * 8, 8), 8), :]
                for m in range(CH):
                    acc[m] = acc[m] + line_of(m * LM + lm) * col
            return tuple(acc)

        acc = lax.fori_loop(0, LM // LBLK, over_lm, tuple(zero for _ in range(CH)))
        for m in range(CH):
            gx_ref[8 * m : 8 * m + 8, :] = acc[m]

        def over_m(step, acc):
            acc = list(acc)
            for part in range(4):
                m = step * 4 + part
                col = x_ref[pl.ds(pl.multiple_of(m * 8, 8), 8), :]
                for lm in range(LM):
                    acc[lm] = acc[lm] + line_of(m * LM + lm) * col
            return tuple(acc)

        acc = lax.fori_loop(0, CH // 4, over_m, tuple(zero for _ in range(LM)))
        for lm in range(LM):
            gy_ref[8 * lm : 8 * lm + 8, :] = acc[lm]

    def contract_species(kind):
        odd = (kind == 1.0) | (kind == 3.0)
        upper = kind > 1.5

        def over_n(step, acc):
            acc = list(acc)
            for part in range(2):
                n = step * 2 + part
                at = pl.multiple_of(n * 8, 8)
                scaled = x_ref[pl.ds(at, 8), :]
                sums = [None, None]
                for lm in range(LM):
                    lines = [line_of((c * NMAX + n) * LM + lm) for c in range(SPECIES)]
                    first = jnp.where(odd, lines[1], lines[0])
                    second = jnp.where(odd, lines[3], lines[2])
                    grad = jnp.where(upper, second, first)
                    acc[lm] = acc[lm] + grad * scaled
                    term = grad * y_ref[8 * lm : 8 * lm + 8, :]
                    sums[lm % 2] = term if lm < 2 else sums[lm % 2] + term
                gx_ref[pl.ds(at, 8), :] = sums[0] + sums[1]
            return tuple(acc)

        acc = lax.fori_loop(0, NMAX // 2, over_n, tuple(zero for _ in range(LM)))
        for lm in range(LM):
            gy_ref[8 * lm : 8 * lm + 8, :] = acc[lm]

    def slot_block(block_at, own):
        base = pl.multiple_of(block_at * 8, 8)
        weight, dist, unit, chan = geometry(layer, geo_ref, feat_ref, wt_ref, base)
        _, radial, _ = radial_terms(dist, rad_ref, False)
        for at, column in enumerate(harmonic_list(unit)):
            y_ref[8 * at : 8 * at + 8, :] = column
        if layer == 1:
            for n in range(NMAX):
                x_ref[8 * n : 8 * n + 8, :] = weight * radial[n]
            contract_species(geo_ref[slot_rows(3, base), :])
        else:
            for c in range(SPECIES):
                scale = chan[c] * weight
                for n in range(NMAX):
                    at = 8 * (c * NMAX + n)
                    x_ref[at : at + 8, :] = scale * radial[n]
            contract_slots()
        weight, dist, unit, chan = geometry(layer, geo_ref, feat_ref, wt_ref, base)
        inv = 1.0 / dist
        basis, radial, slopes = radial_terms(dist, rad_ref, True)
        feat_grads = []
        radial_grads = [None] * NMAX
        if layer == 1:
            radial_grads = [gx_ref[8 * n : 8 * n + 8, :] for n in range(NMAX)]
        for c in range(SPECIES if layer == 2 else 0):
            total = None
            for n in range(NMAX):
                grad = gx_ref[8 * (c * NMAX + n) : 8 * (c * NMAX + n) + 8, :]
                term = grad * radial[n]
                total = term if total is None else total + term
                piece = grad * chan[c]
                radial_grads[n] = piece if c == 0 else radial_grads[n] + piece
            feat_grads.append(total * weight)
        grad_r = None
        radial_grads = [grad * weight for grad in radial_grads]
        for p in range(NRAD):
            total = None
            for n in range(NMAX):
                at = (n * NRAD + p) * 8
                rgr_ref[pl.ds(at, 8), :] = rgr_ref[pl.ds(at, 8), :] + radial_grads[n] * basis[p]
                term = radial_grads[n] * rad_ref[n, p]
                total = term if total is None else total + term
            term = total * slopes[p]
            grad_r = term if grad_r is None else grad_r + term
        table = scaled_legendre(unit[2])
        cosines, sines = azimuth_powers(unit[0], unit[1])
        grad_x = grad_y = grad_z = None

        def plus(total, term):
            return term if total is None else total + term

        for azimuth in range(LMAX + 1):
            grad_cos = grad_sin = None
            for degree in range(azimuth, LMAX + 1):
                at = degree * degree + degree
                up = gy_ref[8 * (at + azimuth) : 8 * (at + azimuth) + 8, :]
                poly = table[degree, azimuth]
                if azimuth:
                    down = gy_ref[8 * (at - azimuth) : 8 * (at - azimuth) + 8, :]
                    grad_cos = plus(grad_cos, up * poly)
                    grad_sin = plus(grad_sin, down * poly)
                if degree > azimuth:
                    ratio = norm_of(degree, azimuth) / norm_of(degree, azimuth + 1)
                    slope = ratio * table[degree, azimuth + 1]
                    if azimuth:
                        grad_z = plus(grad_z, slope * (up * cosines[azimuth] + down * sines[azimuth]))
                    else:
                        grad_z = plus(grad_z, slope * up)
            if azimuth == 1:
                grad_x, grad_y = grad_cos, grad_sin
            elif azimuth > 1:
                below_cos, below_sin = cosines[azimuth - 1], sines[azimuth - 1]
                grad_x = grad_x + float(azimuth) * (grad_cos * below_cos + grad_sin * below_sin)
                grad_y = grad_y + float(azimuth) * (grad_sin * below_cos - grad_cos * below_sin)
        dot_u = grad_x * unit[0] + grad_y * unit[1] + grad_z * unit[2]
        live = weight > 0.0
        out = []
        for axis, grad in enumerate((grad_x, grad_y, grad_z)):
            value = (grad - dot_u * unit[axis]) * inv + grad_r * unit[axis]
            out.append(jnp.where(live, value, 0.0))
        values = out + feat_grads
        for at, value in enumerate(values):
            val_ref[slot_rows(at, base), :] = value
        return tuple(total + value for total, value in zip(own, out))


    own = lax.fori_loop(0, blocks, slot_block, (zero, zero, zero))
    own = jnp.concatenate(
        [jnp.sum(total, axis=0, keepdims=True) for total in own] + [jnp.zeros((5, TILE), f32)], axis=0
    )
    own_ref[...] = own + own_in_ref[...] if layer == 1 else own

    used = 3 if layer == 1 else NVAL
    height = used * WROWS
    step_rows = height + 1
    sub = lax.broadcasted_iota(jnp.int32, (TILE, TILE), 0)
    windows = lax.div(row_high - row_low + WROWS, WROWS)

    def window(window_at, carry):
        row_base = row_low + window_at * WROWS

        def scatter(block_at, acc):
            base = pl.multiple_of(block_at * 8, 8)
            index = idx_ref[pl.ds(base, 8), :]
            hi = lax.shift_right_logical(index, 7)
            lo = lax.bitwise_and(index, 127)
            for row in range(WROWS):
                hit = hi == row_base + row
                for value_at in range(used):
                    value = val_ref[slot_rows(value_at, base), :]
                    left_ref[pl.ds(value_at * WROWS + row, 8, stride=step_rows), :] = jnp.where(
                        hit, value, 0.0
                    )
            ones, left = [], []
            for part in range(8):
                line = jnp.broadcast_to(lo[part : part + 1, :], (TILE, TILE))
                ones.append(jnp.where(line == sub, 1.0, 0.0).astype(bf16))
                left.append(left_ref[part * step_rows : part * step_rows + height, :])
            left = jnp.concatenate(left, axis=1)
            ones = jnp.concatenate(ones, axis=1)
            high = left.astype(bf16)
            rest = (left - high.astype(f32)).astype(bf16)
            dims = (((1,), (1,)), ((), ()))
            acc = acc + lax.dot_general(high, ones, dims, preferred_element_type=f32)
            return acc + lax.dot_general(rest, ones, dims, preferred_element_type=f32)

        acc = lax.fori_loop(0, blocks, scatter, jnp.zeros((height, TILE), f32))
        for value_at in range(used):
            at = value_at * WSTEP + row_base
            win_ref[pl.ds(at, WROWS), :] = (
                win_ref[pl.ds(at, WROWS), :] + acc[value_at * WROWS : (value_at + 1) * WROWS]
            )
        return carry

    lax.fori_loop(0, windows, window, 0)


def backward_call(layer, info, radial, geo, feat, index, weight, grad_dens, window_in, own_in):
    atoms = index.shape[1]
    values = 3 if layer == 1 else NVAL
    return pl.pallas_call(
        partial(backward_kernel, layer),
        out_shape=(
            jax.ShapeDtypeStruct((values * WSTEP, TILE), f32),
            jax.ShapeDtypeStruct((8, atoms), f32),
            jax.ShapeDtypeStruct((NMAX * NRAD * 8, TILE), f32),
        ),
        grid=(atoms // TILE,),
        in_specs=[
            smem_spec(),
            smem_spec(),
            tile_spec(GEO * NPAD),
            tile_spec(feat.shape[0]),
            tile_spec(NPAD),
            tile_spec(NPAD),
            tile_spec(DENS),
            whole_spec(window_in.shape),
            tile_spec(8),
        ],
        out_specs=(
            whole_spec((values * WSTEP, TILE)),
            tile_spec(8),
            whole_spec((NMAX * NRAD * 8, TILE)),
        ),
        scratch_shapes=[
            pltpu.VMEM((CH * 8, TILE), f32),
            pltpu.VMEM((LM * 8, TILE), f32),
            pltpu.VMEM((CH * 8, TILE), f32),
            pltpu.VMEM((LM * 8, TILE), f32),
            pltpu.VMEM((NVAL * NPAD, TILE), f32),
            pltpu.VMEM((8 * (NVAL * WROWS + 1), TILE), f32),
        ],
        compiler_params=pltpu.CompilerParams(vmem_limit_bytes=48 << 20),
        name="backward_%d" % layer,
    )(info, radial, geo, feat, index, weight, grad_dens, window_in, own_in)


def tn_dot(left, right):
    return lax.dot_general(left, right, (((0,), (0,)), ((), ())), preferred_element_type=f32)


def nt_dot(left, right):
    return lax.dot_general(left, right, (((1,), (1,)), ((), ())), preferred_element_type=f32)


def padded_rows(value):
    return jnp.concatenate([value, jnp.zeros((8 - value.shape[0], value.shape[1]), f32)], axis=0)


def onehot_rows(species):
    kind = lax.broadcasted_iota(jnp.int32, (8, species.shape[1]), 0).astype(f32)
    return jnp.where(kind == species, 1.0, 0.0).astype(bf16)


def combine(parts):
    total = parts[2][0:8]
    total = total + (parts[1][8:16] + parts[0][16:24])
    total = total + (parts[1][0:8] + parts[0][8:16])
    return total + parts[0][0:8]


def by_atoms(rows24, chunk):
    wide = nt_dot(rows24, split3(chunk))
    return [wide[:, j * QB : (j + 1) * QB] for j in range(3)]


def contract_one_kernel(dens_ref, coup_ref, coef_ref, mix_ref, site_ref, factor_ref, energy_ref, feat_ref,
                        aux_ref, grad_ref, b_ref, ch_ref, row_ref):
    factor_at = pl.program_id(0)
    quantum, atoms = b_ref.shape
    half = quantum // 2
    for part in range(2):
        rows = slice(part * half, (part + 1) * half)
        value = tn_dot(coup_ref[0, :, rows], dens_ref[...])
        factor_ref[0, rows, :] = value

        @pl.when(factor_at == 0)
        def _(value=value, rows=rows):
            b_ref[rows, :] = value

        @pl.when(factor_at > 0)
        def _(value=value, rows=rows):
            b_ref[rows, :] = b_ref[rows, :] * value

    @pl.when(factor_at == pl.num_programs(0) - 1)
    def _():
        onehot = onehot_rows(site_ref[3:4, :])
        row_ref[0:24, :] = split3(padded_rows(coef_ref[...]))
        row_ref[24:48, :] = split3(mix_ref[...])
        triple = jnp.concatenate([onehot] * 3, axis=0)

        def chunk_body(chunk, mixed):
            cols = pl.ds(pl.multiple_of(chunk * QB, QB), QB)
            ch_ref[...] = tn_dot(row_ref[0:24, cols], triple)
            pieces = split3(b_ref[cols, :])
            left = row_ref[24:48, cols]
            parts = [
                jnp.dot(left, pieces[j * QB : (j + 1) * QB], preferred_element_type=f32) for j in range(3)
            ]
            wide = nt_dot(onehot, pieces)
            grad_ref[:, cols] = wide[:, 2 * QB :] + wide[:, QB : 2 * QB] + wide[:, :QB]

            def rows_body(step, sums):
                at = pl.multiple_of(step * 8, 8)
                value = b_ref[pl.ds(pl.multiple_of(chunk * QB + step * 8, 8), 8), :]
                return sums[0] + value * ch_ref[pl.ds(at, 8), :], sums[1] + value * value

            energy, square = lax.fori_loop(0, QB // 8, rows_body, mixed[1:])
            return mixed[0] + combine(parts), energy, square

        zero = jnp.zeros((8, atoms), f32)
        mixed, energy, square = lax.fori_loop(0, quantum // QB, chunk_body, (zero, zero, zero))
        energy_ref[...] = jnp.broadcast_to(jnp.sum(energy, axis=0, keepdims=True), (8, atoms))
        mean = jnp.sum(square, axis=0, keepdims=True) * (1.0 / quantum)
        scale = lax.rsqrt(mean + norm_eps)
        feat_ref[...] = mixed * scale
        aux_ref[0:8, :] = mixed
        aux_ref[8:16, :] = jnp.broadcast_to(scale, (8, atoms))


def contract_one_call(dens, coupling, coefficient, mixing_rows, ordered):
    factors, depth, quantum = coupling.shape
    atoms = dens.shape[1]
    return pl.pallas_call(
        contract_one_kernel,
        out_shape=(
            jax.ShapeDtypeStruct((factors, quantum, atoms), f32),
            jax.ShapeDtypeStruct((8, atoms), f32),
            jax.ShapeDtypeStruct((8, atoms), f32),
            jax.ShapeDtypeStruct((16, atoms), f32),
            jax.ShapeDtypeStruct((8, quantum), f32),
        ),
        grid=(factors,),
        in_specs=[
            whole_spec((depth, atoms)),
            pl.BlockSpec((1, depth, quantum), lambda v: (v, 0, 0)),
            whole_spec(coefficient.shape),
            whole_spec(mixing_rows.shape),
            whole_spec(ordered.shape),
        ],
        out_specs=(
            pl.BlockSpec((1, quantum, atoms), lambda v: (v, 0, 0)),
            whole_spec((8, atoms)),
            whole_spec((8, atoms)),
            whole_spec((16, atoms)),
            whole_spec((8, quantum)),
        ),
        scratch_shapes=[
            pltpu.VMEM((quantum, atoms), f32),
            pltpu.VMEM((QB, atoms), f32),
            pltpu.VMEM((48, quantum), bf16),
        ],
        compiler_params=pltpu.CompilerParams(vmem_limit_bytes=48 << 20),
        name="contract_1",
    )(dens, coupling, coefficient, mixing_rows, ordered)


def factor_grads(values, upstream):
    low_pair, high_pair = values[0] * values[1], values[2] * values[3]
    first, second = upstream * high_pair, upstream * low_pair
    return first * values[1], first * values[0], second * values[3], second * values[2]


def contract_two_kernel(dens_ref, coef_ref, site_ref, coup_ref, out_ref, energy_ref, grad_ref,
                        cv_ref, f_ref, g_ref, ch_ref, row_ref, sem):
    step = pl.program_id(0)
    factors, quantum, atoms = f_ref.shape
    depth = dens_ref.shape[0]
    half = quantum // 2

    def load(at):
        return pltpu.make_async_copy(coup_ref.at[at], cv_ref.at[at, 0:depth], sem.at[at])

    @pl.when(step == 0)
    def _():
        for at in range(factors):
            load(at).start()
        onehot = onehot_rows(site_ref[3:4, :])
        row_ref[...] = split3(padded_rows(coef_ref[...]))
        triple = jnp.concatenate([onehot] * 3, axis=0)

        def factor_body(at, carry):
            load(at).wait()
            for part in range(2):
                rows = slice(part * half, (part + 1) * half)
                f_ref[at, rows, :] = tn_dot(cv_ref[at, 0:depth, rows], dens_ref[...])
            return carry

        lax.fori_loop(0, factors, factor_body, 0)

        def chunk_body(chunk, energy):
            cols = pl.ds(pl.multiple_of(chunk * QB, QB), QB)
            ch_ref[...] = tn_dot(row_ref[:, cols], triple)

            def rows_body(small, total):
                at = pl.multiple_of(small * 16, 16)
                rows = pl.ds(pl.multiple_of(chunk * QB + small * 16, 16), 16)
                values = [f_ref[v, rows, :] for v in range(factors)]
                upstream = ch_ref[pl.ds(at, 16), :]
                grads = factor_grads(values, upstream)
                for v in range(factors):
                    g_ref[v, rows, :] = grads[v].astype(bf16)
                product = values[0] * values[1] * values[2] * values[3]
                f_ref[0, rows, :] = product
                term = product * upstream
                return total + term[:8] + term[8:]

            energy = lax.fori_loop(0, QB // 16, rows_body, energy)
            wide = nt_dot(onehot, split3(f_ref[0, cols, :]))
            grad_ref[:, cols] = wide[:, 2 * QB :] + wide[:, QB : 2 * QB] + wide[:, :QB]
            return energy

        energy = lax.fori_loop(0, quantum // QB, chunk_body, jnp.zeros((8, atoms), f32))
        energy_ref[...] = jnp.broadcast_to(jnp.sum(energy, axis=0, keepdims=True), (8, atoms))

    rows = pl.ds(pl.multiple_of(step * DROWS, 16), DROWS)
    total = None
    for at in range(factors):
        part = jnp.dot(cv_ref[at, rows, :], g_ref[at], preferred_element_type=f32)
        total = part if total is None else total + part
    out_ref[...] = total


def contract_two_call(dens, coupling, coefficient, ordered):
    factors, depth, quantum = coupling.shape
    atoms = dens.shape[1]
    steps = pl.cdiv(depth, DROWS)
    return pl.pallas_call(
        contract_two_kernel,
        out_shape=(
            jax.ShapeDtypeStruct((steps * DROWS, atoms), f32),
            jax.ShapeDtypeStruct((8, atoms), f32),
            jax.ShapeDtypeStruct((8, quantum), f32),
        ),
        grid=(steps,),
        in_specs=[
            pl.BlockSpec((depth, atoms), lambda i: (0, 0), pipeline_mode=pl.Buffered(1)),
            whole_spec(coefficient.shape),
            whole_spec(ordered.shape),
            pl.BlockSpec(memory_space=pl.ANY),
        ],
        out_specs=(
            pl.BlockSpec((DROWS, atoms), lambda i: (i, 0)),
            whole_spec((8, atoms)),
            whole_spec((8, quantum)),
        ),
        scratch_shapes=[
            pltpu.VMEM((factors, steps * DROWS, quantum), bf16),
            pltpu.VMEM((factors, quantum, atoms), f32),
            pltpu.VMEM((factors, quantum, atoms), bf16),
            pltpu.VMEM((QB, atoms), f32),
            pltpu.VMEM((24, quantum), bf16),
            pltpu.SemaphoreType.DMA((factors,)),
        ],
        compiler_params=pltpu.CompilerParams(vmem_limit_bytes=48 << 20),
        name="contract_2",
    )(dens, coefficient, ordered, coupling)


def contract_back_kernel(coup_ref, coef_ref, mix_ref, site_ref, gfeat_ref, aux_ref, factor_ref, out_ref,
                         grad_ref, f_ref, g_ref, ch_ref, row_ref, sem):
    step = pl.program_id(0)
    factors, quantum, atoms = f_ref.shape
    chunks = quantum // QB

    def load(chunk):
        rows = pl.ds(pl.multiple_of(chunk * QB, QB), QB)
        return pltpu.make_async_copy(factor_ref.at[:, rows, :], f_ref.at[:, rows, :], sem.at[chunk])

    @pl.when(step == 0)
    def _():
        for chunk in range(chunks):
            load(chunk).start()
        onehot = onehot_rows(site_ref[3:4, :])
        scale = aux_ref[8:9, :]
        gfeat = gfeat_ref[...]
        dot = jnp.sum(aux_ref[0:8, :] * gfeat, axis=0, keepdims=True)
        shrink = jnp.broadcast_to(scale * scale * scale * dot * (1.0 / quantum), (8, atoms))
        scaled = split3(scale * gfeat)
        high, middle, low = scaled[0:8], scaled[8:16], scaled[16:24]
        mix = split3(mix_ref[...])
        row_ref[0:24, :] = split3(padded_rows(coef_ref[...]))
        for at, piece in enumerate((0, 0, 0, 1, 1, 2)):
            row_ref[24 + 8 * at : 32 + 8 * at, :] = mix[8 * piece : 8 * piece + 8]
        right = jnp.concatenate([onehot] * 3 + [high, middle, low, high, middle, high], axis=0)

        def chunk_body(chunk, carry):
            load(chunk).wait()
            cols = pl.ds(pl.multiple_of(chunk * QB, QB), QB)
            ch_ref[...] = tn_dot(row_ref[:, cols], right)

            def rows_body(small, inner):
                at = pl.multiple_of(small * 16, 16)
                rows = pl.ds(pl.multiple_of(chunk * QB + small * 16, 16), 16)
                values = [f_ref[v, rows, :] for v in range(factors)]
                product = values[0] * values[1] * values[2] * values[3]
                both = jnp.concatenate([shrink, shrink], axis=0)
                upstream = ch_ref[pl.ds(at, 16), :] - both * product
                grads = factor_grads(values, upstream)
                for v in range(factors):
                    g_ref[v, rows, :] = grads[v].astype(bf16)
                f_ref[0, rows, :] = product
                return inner

            lax.fori_loop(0, QB // 16, rows_body, 0)
            grad_ref[:, cols] = combine(by_atoms(scaled, f_ref[0, cols, :]))
            return carry

        lax.fori_loop(0, chunks, chunk_body, 0)

    total = None
    for at in range(factors):
        part = jnp.dot(coup_ref[at], g_ref[at], preferred_element_type=f32)
        total = part if total is None else total + part
    out_ref[...] = total


def contract_back_call(coupling, coefficient, mixing_rows, ordered, gfeat, aux, factor):
    factors, depth, quantum = coupling.shape
    atoms = ordered.shape[1]
    rows = depth // 5
    return pl.pallas_call(
        contract_back_kernel,
        out_shape=(
            jax.ShapeDtypeStruct((depth, atoms), f32),
            jax.ShapeDtypeStruct((8, quantum), f32),
        ),
        grid=(5,),
        in_specs=[
            pl.BlockSpec((factors, rows, quantum), lambda i: (0, i, 0)),
            whole_spec(coefficient.shape),
            whole_spec(mixing_rows.shape),
            whole_spec(ordered.shape),
            whole_spec(gfeat.shape),
            whole_spec(aux.shape),
            pl.BlockSpec(memory_space=pl.ANY),
        ],
        out_specs=(pl.BlockSpec((rows, atoms), lambda i: (i, 0)), whole_spec((8, quantum))),
        scratch_shapes=[
            pltpu.VMEM((factors, quantum, atoms), f32),
            pltpu.VMEM((factors, quantum, atoms), bf16),
            pltpu.VMEM((QB, atoms), f32),
            pltpu.VMEM((72, quantum), bf16),
            pltpu.SemaphoreType.DMA((quantum // QB,)),
        ],
        compiler_params=pltpu.CompilerParams(vmem_limit_bytes=48 << 20),
        name="contract_back_1",
    )(coupling, coefficient, mixing_rows, ordered, gfeat, aux, factor)


def per_device(
    positions,
    species,
    neighbours,
    slot_counts,
    structure,
    target_energy,
    radial_one,
    coupling_one,
    coefficient_one,
    mixing,
    radial_two,
    coupling_two,
    coefficient_two,
):
    atoms = positions.shape[2]
    tiles = atoms // TILE
    site = jnp.concatenate(
        [
            positions[:, 0, :],
            species.astype(f32),
            structure.astype(f32),
            jnp.zeros((3, atoms), f32),
        ],
        axis=0,
    )
    table_one = spread_call(0, 4, site)
    first = ((lax.axis_index("dom") - 1) * atoms).astype(jnp.int32).reshape(1)
    index, weight, ordered, perm, info = prepare_call(first, slot_counts, neighbours[:, 0, :], site)
    onehot = (ordered[3:4] == jnp.arange(SPECIES, dtype=f32)[:, None]).astype(f32)
    mixing_rows = jnp.pad(mixing.T, ((0, 8 - SPECIES), (0, 0)))

    dens_one, geo = density_call(1, info, radial_one, table_one, ordered, index, weight)
    factors_one, energy_one, features, aux, coefficient_first = contract_one_call(
        dens_one, coupling_one, coefficient_one, mixing_rows, ordered
    )
    table_two = spread_call(1, SPECIES, features, perm)
    dens_two, feat = density_call(2, info, radial_two, table_two, ordered, index, weight, geo)
    grad_dens_two, energy_two, coefficient_second = contract_two_call(
        dens_two, coupling_two, coefficient_two, ordered
    )
    site_energy = energy_one[0] + energy_two[0]
    structures = target_energy.shape[1]
    members = (ordered[4][:, None] == jnp.arange(structures, dtype=f32)[None, :]).astype(f32)
    per_structure = jnp.dot(
        jnp.concatenate([site_energy[None, :], onehot], axis=0), members, precision=highest
    )
    target = jnp.where(lax.axis_index("dom") == 0, target_energy, 0.0)
    per_structure = jnp.concatenate([per_structure, target], axis=0)

    blank_window = jnp.zeros((8, TILE), f32)
    blank_own = jnp.zeros((8, atoms), f32)
    window_two, own_two, rgr_two = backward_call(
        2, info, radial_two, geo, feat, index, weight, grad_dens_two, blank_window, blank_own
    )
    grad_features = collect_call(2, tiles, 3, window_two.reshape(NVAL, WSTEP, TILE), perm)
    grad_dens_one, mixing_gradient = contract_back_call(
        coupling_one, coefficient_one, mixing_rows, ordered, grad_features, aux, factors_one
    )
    window_one, own_one, rgr_one = backward_call(
        1, info, radial_one, geo, blank_own, index, weight, grad_dens_one, window_two, own_two
    )

    def radial_sum(partial_grad):
        return jnp.sum(partial_grad.reshape(NMAX * NRAD, 8 * TILE), axis=1)

    groups = lax.axis_size("grp")
    mine = lax.axis_index("grp") == jnp.arange(groups, dtype=jnp.int32)
    slots = jnp.where(mine[:, None, None], per_structure[None], 0.0)
    quantum = coefficient_first.shape[1]
    wide = SPECIES * quantum
    radials = jnp.zeros((8 * TILE,), f32)
    radials = radials.at[: NMAX * NRAD].set(radial_sum(rgr_one))
    radials = radials.at[TILE : TILE + NMAX * NRAD].set(radial_sum(rgr_two))
    payload = jnp.concatenate(
        [
            radials,
            coefficient_first[:SPECIES].reshape(-1),
            coefficient_second[:SPECIES].reshape(-1),
            mixing_gradient[:SPECIES].reshape(-1),
            slots.reshape(-1),
        ]
    )
    sums_at = 8 + 3 * wide // TILE
    steps = log2_of(lax.axis_size("dom")) + log2_of(groups)
    forces, sums, energies, offsets = finish_call(
        3,
        steps,
        tiles,
        sums_at,
        structures // TILE,
        window_one.reshape(3, WSTEP, TILE),
        own_one,
        perm,
        payload.reshape(-1, TILE),
    )
    parts = sums[8:sums_at].reshape(3, SPECIES, quantum)
    return (
        energies.reshape(1, structures),
        offsets[:SPECIES, 0],
        forces[:3].reshape(3, 1, atoms),
        sums[0, : NMAX * NRAD].reshape(NMAX, NRAD),
        parts[0],
        parts[2].T,
        sums[1, : NMAX * NRAD].reshape(NMAX, NRAD),
        parts[1],
    )


def solution(mesh):
    in_specs = (
        P(None, "grp", "dom"),
        P("grp", "dom"),
        P(None, "grp", "dom"),
        P("grp", "dom"),
        P("grp", "dom"),
        P("grp", None),
        P(),
        P(),
        P(),
        P(),
        P(),
        P(),
        P(),
    )
    out_specs = (P("grp", None), P(), P(None, "grp", "dom"), P(), P(), P(), P(), P())
    return jax.shard_map(
        per_device, mesh=mesh, in_specs=in_specs, out_specs=out_specs, check_vma=False
    )
```

```python
from functools import partial
import math

import jax
import jax.numpy as jnp
from jax import lax
from jax.experimental import pallas as pl
from jax.experimental.pallas import tpu as pltpu
from jax.sharding import PartitionSpec as P

NRAD = 12
NMAX = 10
LMAX = 6
LM = 49
SPECIES = 4
CH = SPECIES * NMAX
DENS = CH * LM
NBR = 48
NPAD = 64
TILE = 128
LBLK = 7
WROWS = 12
WSTEP = 40
GEO = 5
QB = 128
VMEM_ALL = 67043328
DROWS = 400
NVAL = 7
SLOTS = 4
XROW = CH + 1

cutoff_radius = 5.0
density_scale = 0.17
norm_eps = 1e-05
ridge_weight = 0.1
highest = lax.Precision.HIGHEST
f32 = jnp.float32
MESH = pl.DeviceIdType.MESH
bf16 = jnp.bfloat16


def log2_of(count):
    steps = count.bit_length() - 1
    assert count == 1 << steps
    return steps


def neighbour_flags(me, count):
    return me > 0, me < count - 1


def greet(partners, flags):
    barrier = pltpu.get_barrier_semaphore()
    for partner, flag in zip(partners, flags):
        if flag is None:
            pl.semaphore_signal(barrier, inc=1, device_id=partner, device_id_type=MESH)
        else:

            @pl.when(flag)
            def _(partner=partner):
                pl.semaphore_signal(barrier, inc=1, device_id=partner, device_id_type=MESH)

    present = sum(1 for flag in flags if flag is None)
    for flag in flags:
        if flag is not None:
            present = present + jnp.where(flag, 1, 0)
    pl.semaphore_wait(barrier, present)


class SidePair:
    def __init__(self, to_left, to_right, got_ref, send_sem, recv_sem):
        count = lax.axis_size("dom")
        me = lax.axis_index("dom")
        self.partners = ({"dom": me - 1}, {"dom": me + 1})
        self.flags = neighbour_flags(me, count)
        self.got = got_ref
        self.copies = [
            pltpu.make_async_remote_copy(
                src_ref=source,
                dst_ref=got_ref.at[1 - side],
                send_sem=send_sem.at[side],
                recv_sem=recv_sem.at[1 - side],
                device_id=self.partners[side],
                device_id_type=MESH,
            )
            for side, source in enumerate((to_left, to_right))
        ]

    def start(self):
        for side in range(2):
            pl.when(self.flags[side])(self.copies[side].start)

    def wait(self):
        for side in range(2):

            @pl.when(self.flags[side])
            def _(side=side):
                self.copies[side].wait_send()
                self.copies[1 - side].wait_recv()

    def received(self, side):
        return jnp.where(self.flags[side], self.got[side], 0.0)


def split3(value):
    high = value.astype(bf16)
    rest = value - high.astype(f32)
    middle = rest.astype(bf16)
    low = (rest - middle.astype(f32)).astype(bf16)
    return jnp.concatenate([high, middle, low], axis=0)


def reorder(value, perm_ref, contract_at):
    count = value.shape[0]
    out = lax.dot_general(
        split3(value), perm_ref[...], (((1,), (contract_at,)), ((), ())), preferred_element_type=f32
    )
    return out[:count] + (out[count : 2 * count] + out[2 * count :])


def site_rows(pos_ref, kind_ref, part_ref):
    atoms = kind_ref.shape[1]
    rows = [pos_ref[axis] for axis in range(3)]
    rows = rows + [kind_ref[...].astype(f32), part_ref[...].astype(f32)]
    return jnp.concatenate(rows + [jnp.zeros((3, atoms), f32)], axis=0)


def spread_kernel(values, ordered, *refs):
    if ordered:
        pos_ref, kind_ref, part_ref, out_ref, mine_ref, got_ref, send_sem, recv_sem = refs
        flat = site_rows(pos_ref, kind_ref, part_ref)
    else:
        x_ref, perm_ref, out_ref, mine_ref, got_ref, send_sem, recv_sem = refs
        flat = reorder(x_ref[...], perm_ref, 0)
    rows = flat.shape[1] // TILE
    for value in range(values):
        for row in range(rows):
            line = flat[value : value + 1, row * TILE : (row + 1) * TILE]
            at = value * rows + row
            mine_ref[at : at + 1, :] = line
    pair = SidePair(mine_ref, mine_ref, got_ref, send_sem, recv_sem)
    greet(pair.partners, pair.flags)
    pair.start()
    for value in range(values):
        at = value * 3 * rows
        out_ref[at + rows : at + 2 * rows, :] = mine_ref[value * rows : (value + 1) * rows, :]
    pair.wait()
    for side in range(2):
        block = pair.received(side)
        for value in range(values):
            at = value * 3 * rows + 2 * side * rows
            out_ref[at : at + rows, :] = block[value * rows : (value + 1) * rows]


def comm_params(which):
    return pltpu.CompilerParams(collective_id=which, has_side_effects=True, vmem_limit_bytes=VMEM_ALL)


def vmem_spec():
    return pl.BlockSpec(memory_space=pltpu.VMEM)


def spread_call(which, values, raw, operands):
    rows = values * operands[-1].shape[1] // TILE
    return pl.pallas_call(
        partial(spread_kernel, values, raw),
        out_shape=jax.ShapeDtypeStruct((rows * 3, TILE), f32),
        in_specs=[vmem_spec()] * len(operands),
        out_specs=vmem_spec(),
        scratch_shapes=[
            pltpu.VMEM((rows, TILE), f32),
            pltpu.VMEM((2, rows, TILE), f32),
            pltpu.SemaphoreType.DMA((2,)),
            pltpu.SemaphoreType.DMA((2,)),
        ],
        compiler_params=comm_params(which),
        name="spread_%d" % which,
    )(*operands)


def in_lanes(blocks):
    values, rows = blocks.shape[0], blocks.shape[1]
    flat = [
        jnp.concatenate([blocks[v, r : r + 1, :] for r in range(rows)], axis=1) for v in range(values)
    ]
    return jnp.concatenate(flat + [jnp.zeros((8 - values, rows * TILE), f32)], axis=0)


def collect_kernel(rows, values_at, win_ref, perm_ref, out_ref, got_ref, send_sem, recv_sem):
    pair = SidePair(
        win_ref.at[values_at:, 0:rows],
        win_ref.at[values_at:, 2 * rows : 3 * rows],
        got_ref,
        send_sem,
        recv_sem,
    )
    greet(pair.partners, pair.flags)
    pair.start()
    pair.wait()
    total = win_ref[values_at:, rows : 2 * rows] + pair.received(0) + pair.received(1)
    out_ref[...] = reorder(in_lanes(total), perm_ref, 1)


def collect_call(which, rows, values_at, window, perm):
    values = window.shape[0] - values_at
    return pl.pallas_call(
        partial(collect_kernel, rows, values_at),
        out_shape=jax.ShapeDtypeStruct((8, rows * TILE), f32),
        in_specs=[vmem_spec()] * 2,
        out_specs=vmem_spec(),
        scratch_shapes=[
            pltpu.VMEM((2, values, rows, TILE), f32),
            pltpu.SemaphoreType.DMA((2,)),
            pltpu.SemaphoreType.DMA((2,)),
        ],
        compiler_params=comm_params(which),
        name="collect_%d" % which,
    )(window, perm)


def lane_sums(value):
    wide = nt_dot(jnp.ones((8, TILE), bf16), split3(value))
    rows = value.shape[0]
    total = wide[0:1, 2 * rows :] + wide[0:1, rows : 2 * rows] + wide[0:1, :rows]
    return jnp.concatenate([total, jnp.zeros((1, TILE - rows), f32)], axis=1)


def finish_kernel(rows, win_ref, own_ref, perm_ref, first_ref, second_ref, mix_ref, one_ref, two_ref, part_ref,
                  target_ref, force_ref, sum_ref, group_ref, got_ref, pay_ref, pay_group_ref, came_ref,
                  came_group_ref, send_sem, recv_sem, step_send, step_recv, group_send, group_recv):
    pair = SidePair(
        win_ref.at[:, 0:rows], win_ref.at[:, 2 * rows : 3 * rows], got_ref, send_sem, recv_sem
    )
    partners = []
    for axis in ("dom", "grp"):
        me = lax.axis_index(axis)
        for bit in range(log2_of(lax.axis_size(axis))):
            half = 1 << bit
            partners.append({axis: me + half - 2 * half * lax.rem(lax.div(me, half), 2)})
    width = pay_ref.shape[1]
    for at, ref in enumerate((first_ref, second_ref, mix_ref)):
        pay_ref[4 * at : 4 * at + 4, :] = ref[0:4, :]
    tail = [lane_sums(one_ref[...]), lane_sums(two_ref[...]), jnp.zeros((1, width - 2 * TILE), f32)]
    pay_ref[12:13, :] = jnp.concatenate(tail, axis=1)
    pay_ref[13:16, :] = jnp.zeros((3, width), f32)
    lead = lax.axis_index("dom") == 0
    mine = lax.axis_index("grp")
    target = jnp.where(lead, target_ref[...], 0.0)
    block = part_ref[...]
    block = jnp.concatenate([block[0:5], target, block[6:8]], axis=0)
    for group in range(lax.axis_size("grp")):
        pay_group_ref[8 * group : 8 * group + 8, :] = jnp.where(mine == group, block, 0.0)
    greet(list(pair.partners) + partners, list(pair.flags) + [None] * len(partners))
    pair.start()
    force_ref[...] = reorder(own_ref[...], perm_ref, 0)
    for step, partner in enumerate(partners):
        copies = []
        for source, total, came, send, recv in (
            (pay_ref, sum_ref, came_ref, step_send, step_recv),
            (pay_group_ref, group_ref, came_group_ref, group_send, group_recv),
        ):
            now = source if step == 0 else total
            copy = pltpu.make_async_remote_copy(
                src_ref=now,
                dst_ref=came.at[step],
                send_sem=send.at[step],
                recv_sem=recv.at[step],
                device_id=partner,
                device_id_type=MESH,
            )
            copy.start()
            copies.append((copy, now, total, came))
        for copy, now, total, came in copies:
            copy.wait()
            total[...] = now[...] + came[step]
    pair.wait()
    total = win_ref[:, rows : 2 * rows] + pair.received(0) + pair.received(1)
    force_ref[...] = force_ref[...] - in_lanes(total)


def finish_call(which, mesh_steps, groups, rows, operands):
    width, structures = operands[3].shape[1], operands[9].shape[1]
    return pl.pallas_call(
        partial(finish_kernel, rows),
        out_shape=(
            jax.ShapeDtypeStruct((8, rows * TILE), f32),
            jax.ShapeDtypeStruct((16, width), f32),
            jax.ShapeDtypeStruct((8 * groups, structures), f32),
        ),
        in_specs=[vmem_spec()] * 10,
        out_specs=(vmem_spec(),) * 3,
        scratch_shapes=[
            pltpu.VMEM((2, 3, rows, TILE), f32),
            pltpu.VMEM((16, width), f32),
            pltpu.VMEM((8 * groups, structures), f32),
            pltpu.VMEM((mesh_steps, 16, width), f32),
            pltpu.VMEM((mesh_steps, 8 * groups, structures), f32),
            pltpu.SemaphoreType.DMA((2,)),
            pltpu.SemaphoreType.DMA((2,)),
            pltpu.SemaphoreType.DMA((mesh_steps,)),
            pltpu.SemaphoreType.DMA((mesh_steps,)),
            pltpu.SemaphoreType.DMA((mesh_steps,)),
            pltpu.SemaphoreType.DMA((mesh_steps,)),
        ],
        compiler_params=comm_params(which),
        name="finish_%d" % which,
    )(*operands)


def tail_kernel(mine_ref, all_force_ref, sum_ref, group_ref, energy_ref, offset_ref, force_ref, one_ref,
                first_ref, mix_ref, two_ref, second_ref):
    groups = group_ref.shape[0] // 8

    def fractions(rows):
        counts = [rows[1 + c : 2 + c, :] for c in range(SPECIES)]
        size = jnp.maximum(counts[0] + counts[1] + counts[2] + counts[3], 1.0)
        return [count / size for count in counts], size

    gram = [[None] * SPECIES for _ in range(SPECIES)]
    right = [None] * SPECIES
    energy = None
    own_frac = [None] * SPECIES

    def plus(total, value):
        return value if total is None else total + value

    for group in range(groups):
        rows = group_ref[8 * group : 8 * group + 8, :]
        frac, size = fractions(rows)
        mine = jnp.where(mine_ref[0] == group, 1.0, 0.0)
        energy = plus(energy, mine * (rows[0:1] / size))
        for c in range(SPECIES):
            own_frac[c] = plus(own_frac[c], mine * frac[c])
            right[c] = plus(right[c], frac[c] * rows[5:6])
            for d in range(c, SPECIES):
                gram[c][d] = plus(gram[c][d], frac[c] * frac[d])

    def whole(value):
        return jnp.sum(value, axis=1, keepdims=True)

    right = [whole(value) for value in right]
    upper = [[None if value is None else whole(value) for value in row] for row in gram]
    matrix = [
        [upper[min(c, d)][max(c, d)] + (ridge_weight if c == d else 0.0) for d in range(SPECIES)]
        for c in range(SPECIES)
    ]
    for pivot in range(SPECIES):
        for below in range(pivot + 1, SPECIES):
            ratio = matrix[below][pivot] / matrix[pivot][pivot]
            matrix[below] = [b - ratio * a for a, b in zip(matrix[pivot], matrix[below])]
            right[below] = right[below] - ratio * right[pivot]
    answer = [None] * SPECIES
    for row in range(SPECIES - 1, -1, -1):
        running = right[row]
        for later in range(row + 1, SPECIES):
            running = running - matrix[row][later] * answer[later]
        answer[row] = running / matrix[row][row]
    for c in range(SPECIES):
        energy = energy + own_frac[c] * answer[c]
    energy_ref[...] = energy
    offset_ref[...] = jnp.concatenate(answer, axis=1)
    for axis in range(3):
        force_ref[axis] = all_force_ref[axis : axis + 1, :]
    first_ref[...] = sum_ref[0:4, :]
    second_ref[...] = sum_ref[4:8, :]
    mix_ref[...] = sum_ref[8:12, :]
    for n in range(NMAX):
        one_ref[n : n + 1, :] = sum_ref[12:13, n * NRAD : (n + 1) * NRAD]
        two_ref[n : n + 1, :] = sum_ref[12:13, TILE + n * NRAD : TILE + (n + 1) * NRAD]


def tail_call(mine, forces, sums, groups):
    width, structures, atoms = sums.shape[1], groups.shape[1], forces.shape[1]
    shapes = (
        (1, structures),
        (1, SPECIES),
        (3, 1, atoms),
        (NMAX, NRAD),
        (SPECIES, width),
        (SPECIES, width),
        (NMAX, NRAD),
        (SPECIES, width),
    )
    return pl.pallas_call(
        tail_kernel,
        out_shape=tuple(jax.ShapeDtypeStruct(shape, f32) for shape in shapes),
        in_specs=[smem_spec()] + [vmem_spec()] * 3,
        out_specs=(vmem_spec(),) * len(shapes),
        compiler_params=pltpu.CompilerParams(vmem_limit_bytes=VMEM_ALL),
        name="tail",
    )(mine, forces, sums, groups)


def double_factorial(number):
    result = 1.0
    while number > 1:
        result = result * number
        number = number - 2
    return result


def norm_of(degree, azimuth):
    value = math.sqrt(
        (2 * degree + 1)
        / (4 * math.pi)
        * math.factorial(degree - azimuth)
        / math.factorial(degree + azimuth)
    )
    return value * (math.sqrt(2.0) if azimuth else 1.0)


def scaled_legendre(coord_z):
    table = {}
    for azimuth in range(LMAX + 1):
        table[azimuth, azimuth] = norm_of(azimuth, azimuth) * double_factorial(2 * azimuth - 1)
        if azimuth + 1 <= LMAX:
            ratio = norm_of(azimuth + 1, azimuth) / norm_of(azimuth, azimuth)
            table[azimuth + 1, azimuth] = coord_z * (
                (2 * azimuth + 1) * ratio * table[azimuth, azimuth]
            )
        for degree in range(azimuth + 2, LMAX + 1):
            gap = degree - azimuth
            first = (2 * degree - 1) / gap * norm_of(degree, azimuth) / norm_of(degree - 1, azimuth)
            second = (
                (degree + azimuth - 1) / gap * norm_of(degree, azimuth) / norm_of(degree - 2, azimuth)
            )
            table[degree, azimuth] = (first * coord_z) * table[degree - 1, azimuth] - (
                second * table[degree - 2, azimuth]
            )
    return table


def azimuth_powers(coord_x, coord_y):
    cosines = [None, coord_x]
    sines = [None, coord_y]
    for _ in range(2, LMAX + 1):
        cosines.append(cosines[-1] * coord_x - sines[-1] * coord_y)
        sines.append(sines[-1] * coord_x + cosines[-2] * coord_y)
    return cosines, sines


LANE_GATHER = lax.GatherDimensionNumbers(
    offset_dims=(),
    collapsed_slice_dims=(1,),
    start_index_map=(1,),
    operand_batching_dims=(0,),
    start_indices_batching_dims=(0,),
)


def lane_gather(line, lo):
    return lax.gather(
        line,
        lo[..., None],
        LANE_GATHER,
        slice_sizes=(1, 1),
        mode=lax.GatherScatterMode.PROMISE_IN_BOUNDS,
    )


def prepare_kernel(first_ref, cnt_ref, nbr_ref, spot_ref, kind_ref, part_ref, idx_ref, wt_ref, sorted_ref, perm_ref, info_ref,
                   key_ref, pos_ref, word_ref, rank_ref):
    atoms = nbr_ref.shape[2]
    tiles = atoms // TILE
    blocks = NBR // 8
    sub = lax.broadcasted_iota(jnp.int32, (8, TILE), 0)
    lane = lax.broadcasted_iota(jnp.int32, (1, TILE), 1)

    def merge(tile, carry):
        cols = pl.ds(pl.multiple_of(tile * TILE, TILE), TILE)
        limit = cnt_ref[:, cols]
        iota = lax.broadcasted_iota(jnp.int32, (NBR, TILE), 0)
        key = jnp.where(iota < limit, nbr_ref[:, 0, cols] - first_ref[0], -1 - iota)
        key_ref[...] = key
        keys = [key[8 * b : 8 * b + 8] for b in range(blocks)]
        total = [jnp.zeros((8, TILE), jnp.int32) for _ in range(blocks)]
        early = [jnp.zeros((8, TILE), jnp.int32) for _ in range(blocks)]
        for other in range(NBR):
            line = jnp.broadcast_to(key_ref[other : other + 1, :], (8, TILE))
            for b in range(blocks):
                same = jnp.where(keys[b] == line, 1, 0)
                total[b] = total[b] + same
                if other < 8 * b:
                    early[b] = early[b] + same
                elif other < 8 * b + 7:
                    early[b] = early[b] + jnp.where(sub > other - 8 * b, same, 0)
        for b in range(blocks):
            alive = sub + 8 * b < limit
            pos_ref[8 * b : 8 * b + 8, :] = jnp.where(alive & (early[b] == 0), 1, 0)
            key_ref[8 * b : 8 * b + 8, :] = total[b] * 4096 + keys[b]
        running = jnp.zeros((1, TILE), jnp.int32)
        out = [jnp.zeros((8, TILE), jnp.int32) for _ in range(blocks)]
        for slot in range(NBR):
            flag = pos_ref[slot : slot + 1, :]
            place = jnp.broadcast_to(jnp.where(flag == 1, running, -1), (8, TILE))
            running = running + flag
            line = jnp.broadcast_to(key_ref[slot : slot + 1, :], (8, TILE))
            for b in range(slot // 8 + 1):
                out[b] = jnp.where(place == sub + 8 * b, line, out[b])
        for b in range(blocks):
            word_ref[8 * b : 8 * b + 8, cols] = out[b].astype(f32)
        order = running * atoms + (atoms - 1 - tile * TILE) - lane
        rank_ref[pl.ds(tile, 1), :] = order.astype(f32)
        return carry

    lax.fori_loop(0, tiles, merge, 0)
    orders = rank_ref[...]
    upright = jnp.transpose(orders)
    ranks = []
    for tile in range(tiles):
        row = jnp.broadcast_to(orders[tile : tile + 1], (TILE, TILE))
        total = jnp.zeros((TILE, TILE), f32)
        for other in range(tiles):
            col = jnp.broadcast_to(upright[:, other : other + 1], (TILE, TILE))
            total = total + jnp.where(col > row, 1.0, 0.0)
        ranks.append(jnp.sum(total, axis=0, keepdims=True))
    place = lax.broadcasted_iota(jnp.int32, (atoms, TILE), 0).astype(f32)
    for tile in range(tiles):
        line = jnp.broadcast_to(ranks[tile], (atoms, TILE))
        perm_ref[:, tile * TILE : (tile + 1) * TILE] = jnp.where(line == place, 1.0, 0.0).astype(bf16)
    word_ref[NBR : NBR + 8, :] = site_rows(spot_ref, kind_ref, part_ref)
    moved = reorder(word_ref[...], perm_ref, 1)
    sorted_ref[...] = moved[NBR:]
    word = moved[:NBR].astype(jnp.int32)
    index = lax.bitwise_and(word, 4095)
    times = lax.shift_right_logical(word, 12)
    idx_ref[:NBR, :] = index
    idx_ref[NBR:, :] = jnp.zeros((NPAD - NBR, atoms), jnp.int32)
    wt_ref[:NBR, :] = density_scale * times.astype(f32)
    wt_ref[NBR:, :] = jnp.zeros((NPAD - NBR, atoms), f32)
    row = lax.shift_right_logical(index, 7)
    low = jnp.min(jnp.where(times > 0, row, 1 << 20))
    high = jnp.max(jnp.where(times > 0, row, -1))
    slots = lax.broadcasted_iota(jnp.int32, (NBR, TILE), 0) + 1
    for tile in range(tiles):
        used = times[:, tile * TILE : (tile + 1) * TILE] > 0
        info_ref[0, tile] = lax.div(jnp.max(jnp.where(used, slots, 0)) + SLOTS - 1, SLOTS) * SLOTS
        info_ref[1, tile] = low
        info_ref[2, tile] = high


def prepare_call(first, limits, neighbours, positions, species, structure):
    atoms = neighbours.shape[2]
    return pl.pallas_call(
        prepare_kernel,
        out_shape=(
            jax.ShapeDtypeStruct((NPAD, atoms), jnp.int32),
            jax.ShapeDtypeStruct((NPAD, atoms), f32),
            jax.ShapeDtypeStruct((8, atoms), f32),
            jax.ShapeDtypeStruct((atoms, atoms), bf16),
            jax.ShapeDtypeStruct((3, atoms // TILE), jnp.int32),
        ),
        in_specs=[smem_spec()] + [vmem_spec()] * 5,
        out_specs=(vmem_spec(), vmem_spec(), vmem_spec(), vmem_spec(), smem_spec()),
        scratch_shapes=[
            pltpu.VMEM((NBR, TILE), jnp.int32),
            pltpu.VMEM((NBR, TILE), jnp.int32),
            pltpu.VMEM((NBR + 8, atoms), f32),
            pltpu.VMEM((atoms // TILE, TILE), f32),
        ],
        compiler_params=pltpu.CompilerParams(vmem_limit_bytes=VMEM_ALL),
        name="prepare",
    )(first, limits, neighbours, positions, species, structure)


def fetch(tab_ref, values, idx_ref, put_ref, chunk, row_low, row_high):
    start = pl.multiple_of(chunk * 32, 32)
    index = [idx_ref[pl.ds(start + 8 * kb, 8), :] for kb in range(4)]
    hi = [lax.shift_right_logical(word, 7) for word in index]
    lo = [lax.bitwise_and(word, 127) for word in index]

    def body(row, found):
        found = list(found)
        hits = [word == row for word in hi]
        for value in range(values):
            line = jnp.broadcast_to(tab_ref[pl.ds(value * 24 + row, 1), :], (8, TILE))
            for kb in range(4):
                at = value * 4 + kb
                found[at] = jnp.where(hits[kb], lane_gather(line, lo[kb]), found[at])
        return tuple(found)

    zero = jnp.zeros((8, TILE), f32)
    found = lax.fori_loop(row_low, row_high + 1, body, tuple(zero for _ in range(4 * values)))
    for value in range(values):
        for kb in range(4):
            put_ref[pl.ds(pl.multiple_of(value * NPAD + start + 8 * kb, 8), 8), :] = found[value * 4 + kb]


def slot_rows(which, base):
    return pl.ds(pl.multiple_of(which * NPAD + base, 8), 8)


def geometry(layer, geo_ref, feat_ref, wt_ref, base):
    weight = wt_ref[pl.ds(base, 8), :]
    unit = [geo_ref[slot_rows(axis, base), :] for axis in range(3)]
    dist = geo_ref[slot_rows(4, base), :]
    if layer == 1:
        kind = geo_ref[slot_rows(3, base), :]
        chan = [jnp.where(kind == float(c), 1.0, 0.0) for c in range(SPECIES)]
    else:
        chan = [feat_ref[slot_rows(c, base), :] for c in range(SPECIES)]
    return weight, dist, unit, chan


def radial_terms(dist, rad_ref, with_slope):
    scaled = dist * (2.0 / cutoff_radius) - 1.0
    inside = dist < cutoff_radius
    angle = dist * (math.pi / cutoff_radius)
    cutoff = jnp.where(inside, 0.5 * (jnp.cos(angle) + 1.0), 0.0)
    cheb = [None, scaled]
    twice = 2.0 * scaled
    cheb.append(twice * scaled - 1.0)
    for _ in range(3, NRAD):
        cheb.append(twice * cheb[-1] - cheb[-2])
    basis = [cutoff] + [cutoff * cheb[p] for p in range(1, NRAD)]
    radial = []
    for n in range(NMAX):
        total = basis[0] * rad_ref[n, 0]
        for p in range(1, NRAD):
            total = total + basis[p] * rad_ref[n, p]
        radial.append(total)
    if not with_slope:
        return basis, radial, None
    slope_cut = jnp.where(inside, (-0.5 * math.pi / cutoff_radius) * jnp.sin(angle), 0.0)
    grad_scaled = cutoff * (2.0 / cutoff_radius)
    second = [None, None, twice]
    second[1] = jnp.ones_like(scaled)
    for _ in range(3, NRAD):
        second.append(twice * second[-1] - second[-2])
    slopes = [slope_cut, slope_cut * scaled + grad_scaled]
    for p in range(2, NRAD):
        slopes.append(slope_cut * cheb[p] + grad_scaled * (float(p) * second[p]))
    return basis, radial, slopes


def harmonic_list(unit):
    table = scaled_legendre(unit[2])
    cosines, sines = azimuth_powers(unit[0], unit[1])
    columns = []
    for degree in range(LMAX + 1):
        for signed in range(-degree, degree + 1):
            azimuth = abs(signed)
            poly = table[degree, azimuth]
            if signed == 0:
                columns.append(poly)
            elif signed > 0:
                columns.append(poly * cosines[azimuth])
            else:
                columns.append(poly * sines[azimuth])
    columns[0] = jnp.full_like(unit[2], columns[0])
    return columns


def density_kernel(layer, info_ref, rad_ref, tab_ref, cen_ref, idx_ref, wt_ref, *refs):
    if layer == 1:
        out_ref, geo_ref, x_ref, y_ref, d_ref = refs
        feat_ref, put_ref = None, geo_ref
    else:
        geo_ref, out_ref, feat_ref, x_ref, y_ref, d_ref = refs
        put_ref = feat_ref
    tile = pl.program_id(0)
    count = info_ref[0, tile]
    row_low, row_high = info_ref[1, tile], info_ref[2, tile]
    blocks = lax.div(count + 7, 8)

    def gather_chunk(chunk, carry):
        fetch(tab_ref, 4, idx_ref, put_ref, chunk, row_low, row_high)
        return carry

    lax.fori_loop(0, lax.div(count + 31, 32), gather_chunk, 0)

    def edges(block_at, carry):
        base = pl.multiple_of(block_at * 8, 8)
        if layer == 1:
            live = wt_ref[pl.ds(base, 8), :] > 0.0
            deltas = []
            for axis in range(3):
                centre = jnp.broadcast_to(cen_ref[pl.ds(axis, 1), :], (8, TILE))
                delta = geo_ref[slot_rows(axis, base), :] - centre
                deltas.append(jnp.where(live, delta, 1.0))
            dist = jnp.sqrt(deltas[0] * deltas[0] + deltas[1] * deltas[1] + deltas[2] * deltas[2])
            inv = 1.0 / dist
            for axis in range(3):
                geo_ref[slot_rows(axis, base), :] = deltas[axis] * inv
            geo_ref[slot_rows(4, base), :] = dist
        weight, dist, unit, chan = geometry(layer, geo_ref, feat_ref, wt_ref, base)
        _, radial, _ = radial_terms(dist, rad_ref, False)
        for c in range(SPECIES):
            scale = chan[c] * weight
            for n in range(NMAX):
                x_ref[pl.ds(base * XROW + (c * NMAX + n), 8, stride=XROW), :] = scale * radial[n]
        for at, column in enumerate(harmonic_list(unit)):
            y_ref[slot_rows(at, base), :] = column
        return carry

    lax.fori_loop(0, blocks, edges, 0)
    groups = lax.div(count, SLOTS)

    def lm_block(block_at, carry):
        first = block_at * LBLK

        def slots(group, acc):
            acc = list(acc)
            for part in range(SLOTS):
                slot = group * SLOTS + part
                rows = [x_ref[pl.ds(slot * XROW + 8 * j, 8), :] for j in range(CH // 8)]
                for at in range(LBLK):
                    line = jnp.broadcast_to(
                        y_ref[pl.ds((first + at) * NPAD + slot, 1), :], (8, TILE)
                    )
                    for j in range(CH // 8):
                        acc[at * (CH // 8) + j] = acc[at * (CH // 8) + j] + rows[j] * line
            return tuple(acc)

        zero = jnp.zeros((8, TILE), f32)
        acc = lax.fori_loop(0, groups, slots, tuple(zero for _ in range(LBLK * (CH // 8))))
        for at in range(LBLK):
            for j in range(CH // 8):
                d_ref[pl.ds(8 * j * LM + first + at, 8, stride=LM), :] = acc[at * (CH // 8) + j]
        return carry

    lax.fori_loop(0, LM // LBLK, lm_block, 0)
    out_ref[...] = d_ref[...].astype(bf16)


def smem_spec():
    return pl.BlockSpec(memory_space=pltpu.SMEM)


def tile_spec(rows):
    return pl.BlockSpec((rows, TILE), lambda i: (0, i))


def whole_spec(shape):
    return pl.BlockSpec(shape, lambda i: tuple(0 for _ in shape))


def density_call(layer, info, radial, table, centres, index, weight, geo=None):
    atoms = centres.shape[1]
    rows = GEO if layer == 1 else SPECIES
    extra = () if geo is None else (geo,)
    return pl.pallas_call(
        partial(density_kernel, layer),
        out_shape=(
            jax.ShapeDtypeStruct((DENS, atoms), bf16),
            jax.ShapeDtypeStruct((rows * NPAD, atoms), f32),
        ),
        grid=(atoms // TILE,),
        in_specs=[
            smem_spec(),
            smem_spec(),
            whole_spec(table.shape),
            tile_spec(8),
            tile_spec(NPAD),
            tile_spec(NPAD),
        ]
        + [tile_spec(GEO * NPAD)] * len(extra),
        out_specs=(tile_spec(DENS), tile_spec(rows * NPAD)),
        scratch_shapes=[
            pltpu.VMEM((NPAD * XROW + 8, TILE), f32),
            pltpu.VMEM((LM * NPAD, TILE), f32),
            pltpu.VMEM((DENS, TILE), f32),
        ],
        compiler_params=pltpu.CompilerParams(vmem_limit_bytes=VMEM_ALL),
        name="density_%d" % layer,
    )(info, radial, table, centres, index, weight, *extra)


def backward_kernel(layer, info_ref, rad_ref, geo_ref, feat_ref, idx_ref, wt_ref, dd_ref, win_in_ref,
                    own_in_ref, win_ref, own_ref, rad_out_ref, rgr_ref, x_ref, y_ref, gx_ref, gy_ref, val_ref,
                    left_ref):
    tile = pl.program_id(0)
    count = info_ref[0, tile]
    row_low, row_high = info_ref[1, tile], info_ref[2, tile]
    blocks = lax.div(count + 7, 8)
    zero = jnp.zeros((8, TILE), f32)

    @pl.when(tile == 0)
    def _():
        if layer == 1:
            win_ref[...] = win_in_ref[: 3 * WSTEP]
        else:
            win_ref[...] = jnp.zeros_like(win_ref)
        rgr_ref[...] = jnp.zeros_like(rgr_ref)

    def line_of(at):
        return jnp.broadcast_to(dd_ref[pl.ds(at, 1), :], (8, TILE))

    def contract_slots():
        def over_lm(step, acc):
            acc = list(acc)
            for part in range(LBLK):
                lm = step * LBLK + part
                col = y_ref[pl.ds(pl.multiple_of(lm * 8, 8), 8), :]
                for m in range(CH):
                    acc[m] = acc[m] + line_of(m * LM + lm) * col
            return tuple(acc)

        acc = lax.fori_loop(0, LM // LBLK, over_lm, tuple(zero for _ in range(CH)))
        for m in range(CH):
            gx_ref[8 * m : 8 * m + 8, :] = acc[m]

        def over_m(step, acc):
            acc = list(acc)
            for part in range(4):
                m = step * 4 + part
                col = x_ref[pl.ds(pl.multiple_of(m * 8, 8), 8), :]
                for lm in range(LM):
                    acc[lm] = acc[lm] + line_of(m * LM + lm) * col
            return tuple(acc)

        acc = lax.fori_loop(0, CH // 4, over_m, tuple(zero for _ in range(LM)))
        for lm in range(LM):
            gy_ref[8 * lm : 8 * lm + 8, :] = acc[lm]

    def contract_species(kind):
        odd = (kind == 1.0) | (kind == 3.0)
        upper = kind > 1.5

        def over_n(step, acc):
            acc = list(acc)
            for part in range(2):
                n = step * 2 + part
                at = pl.multiple_of(n * 8, 8)
                scaled = x_ref[pl.ds(at, 8), :]
                sums = [None, None]
                for lm in range(LM):
                    lines = [line_of((c * NMAX + n) * LM + lm) for c in range(SPECIES)]
                    first = jnp.where(odd, lines[1], lines[0])
                    second = jnp.where(odd, lines[3], lines[2])
                    grad = jnp.where(upper, second, first)
                    acc[lm] = acc[lm] + grad * scaled
                    term = grad * y_ref[8 * lm : 8 * lm + 8, :]
                    sums[lm % 2] = term if lm < 2 else sums[lm % 2] + term
                gx_ref[pl.ds(at, 8), :] = sums[0] + sums[1]
            return tuple(acc)

        acc = lax.fori_loop(0, NMAX // 2, over_n, tuple(zero for _ in range(LM)))
        for lm in range(LM):
            gy_ref[8 * lm : 8 * lm + 8, :] = acc[lm]

    def slot_block(block_at, own):
        base = pl.multiple_of(block_at * 8, 8)
        weight, dist, unit, chan = geometry(layer, geo_ref, feat_ref, wt_ref, base)
        _, radial, _ = radial_terms(dist, rad_ref, False)
        for at, column in enumerate(harmonic_list(unit)):
            y_ref[8 * at : 8 * at + 8, :] = column
        if layer == 1:
            for n in range(NMAX):
                x_ref[8 * n : 8 * n + 8, :] = weight * radial[n]
            contract_species(geo_ref[slot_rows(3, base), :])
        else:
            for c in range(SPECIES):
                scale = chan[c] * weight
                for n in range(NMAX):
                    at = 8 * (c * NMAX + n)
                    x_ref[at : at + 8, :] = scale * radial[n]
            contract_slots()
        weight, dist, unit, chan = geometry(layer, geo_ref, feat_ref, wt_ref, base)
        inv = 1.0 / dist
        basis, radial, slopes = radial_terms(dist, rad_ref, True)
        feat_grads = []
        radial_grads = [None] * NMAX
        if layer == 1:
            radial_grads = [gx_ref[8 * n : 8 * n + 8, :] for n in range(NMAX)]
        for c in range(SPECIES if layer == 2 else 0):
            total = None
            for n in range(NMAX):
                grad = gx_ref[8 * (c * NMAX + n) : 8 * (c * NMAX + n) + 8, :]
                term = grad * radial[n]
                total = term if total is None else total + term
                piece = grad * chan[c]
                radial_grads[n] = piece if c == 0 else radial_grads[n] + piece
            feat_grads.append(total * weight)
        grad_r = None
        radial_grads = [grad * weight for grad in radial_grads]
        for p in range(NRAD):
            total = None
            for n in range(NMAX):
                at = (n * NRAD + p) * 8
                rgr_ref[pl.ds(at, 8), :] = rgr_ref[pl.ds(at, 8), :] + radial_grads[n] * basis[p]
                term = radial_grads[n] * rad_ref[n, p]
                total = term if total is None else total + term
            term = total * slopes[p]
            grad_r = term if grad_r is None else grad_r + term
        table = scaled_legendre(unit[2])
        cosines, sines = azimuth_powers(unit[0], unit[1])
        grad_x = grad_y = grad_z = None

        def plus(total, term):
            return term if total is None else total + term

        for azimuth in range(LMAX + 1):
            grad_cos = grad_sin = None
            for degree in range(azimuth, LMAX + 1):
                at = degree * degree + degree
                up = gy_ref[8 * (at + azimuth) : 8 * (at + azimuth) + 8, :]
                poly = table[degree, azimuth]
                if azimuth:
                    down = gy_ref[8 * (at - azimuth) : 8 * (at - azimuth) + 8, :]
                    grad_cos = plus(grad_cos, up * poly)
                    grad_sin = plus(grad_sin, down * poly)
                if degree > azimuth:
                    ratio = norm_of(degree, azimuth) / norm_of(degree, azimuth + 1)
                    slope = ratio * table[degree, azimuth + 1]
                    if azimuth:
                        grad_z = plus(grad_z, slope * (up * cosines[azimuth] + down * sines[azimuth]))
                    else:
                        grad_z = plus(grad_z, slope * up)
            if azimuth == 1:
                grad_x, grad_y = grad_cos, grad_sin
            elif azimuth > 1:
                below_cos, below_sin = cosines[azimuth - 1], sines[azimuth - 1]
                grad_x = grad_x + float(azimuth) * (grad_cos * below_cos + grad_sin * below_sin)
                grad_y = grad_y + float(azimuth) * (grad_sin * below_cos - grad_cos * below_sin)
        dot_u = grad_x * unit[0] + grad_y * unit[1] + grad_z * unit[2]
        live = weight > 0.0
        out = []
        for axis, grad in enumerate((grad_x, grad_y, grad_z)):
            value = (grad - dot_u * unit[axis]) * inv + grad_r * unit[axis]
            out.append(jnp.where(live, value, 0.0))
        values = out + feat_grads
        for at, value in enumerate(values):
            val_ref[slot_rows(at, base), :] = value
        return tuple(total + value for total, value in zip(own, out))


    own = lax.fori_loop(0, blocks, slot_block, (zero, zero, zero))
    own = jnp.concatenate(
        [jnp.sum(total, axis=0, keepdims=True) for total in own] + [jnp.zeros((5, TILE), f32)], axis=0
    )
    own_ref[...] = own + own_in_ref[...] if layer == 1 else own

    used = 3 if layer == 1 else NVAL
    height = used * WROWS
    step_rows = height + 1
    sub = lax.broadcasted_iota(jnp.int32, (TILE, TILE), 0)
    windows = lax.div(row_high - row_low + WROWS, WROWS)

    def window(window_at, carry):
        row_base = row_low + window_at * WROWS

        def scatter(block_at, acc):
            base = pl.multiple_of(block_at * 8, 8)
            index = idx_ref[pl.ds(base, 8), :]
            hi = lax.shift_right_logical(index, 7)
            lo = lax.bitwise_and(index, 127)
            for row in range(WROWS):
                hit = hi == row_base + row
                for value_at in range(used):
                    value = val_ref[slot_rows(value_at, base), :]
                    left_ref[pl.ds(value_at * WROWS + row, 8, stride=step_rows), :] = jnp.where(
                        hit, value, 0.0
                    )
            ones, left = [], []
            for part in range(8):
                line = jnp.broadcast_to(lo[part : part + 1, :], (TILE, TILE))
                ones.append(jnp.where(line == sub, 1.0, 0.0).astype(bf16))
                left.append(left_ref[part * step_rows : part * step_rows + height, :])
            left = jnp.concatenate(left, axis=1)
            ones = jnp.concatenate(ones, axis=1)
            high = left.astype(bf16)
            rest = (left - high.astype(f32)).astype(bf16)
            dims = (((1,), (1,)), ((), ()))
            acc = acc + lax.dot_general(high, ones, dims, preferred_element_type=f32)
            return acc + lax.dot_general(rest, ones, dims, preferred_element_type=f32)

        acc = lax.fori_loop(0, blocks, scatter, jnp.zeros((height, TILE), f32))
        for value_at in range(used):
            at = value_at * WSTEP + row_base
            win_ref[pl.ds(at, WROWS), :] = (
                win_ref[pl.ds(at, WROWS), :] + acc[value_at * WROWS : (value_at + 1) * WROWS]
            )
        return carry

    lax.fori_loop(0, windows, window, 0)

    @pl.when(tile == pl.num_programs(0) - 1)
    def _():
        for at in range(NMAX * NRAD):
            rad_out_ref[at : at + 1, :] = jnp.sum(rgr_ref[8 * at : 8 * at + 8, :], axis=0, keepdims=True)


def backward_call(layer, info, radial, geo, feat, index, weight, grad_dens, window_in, own_in):
    atoms = index.shape[1]
    values = 3 if layer == 1 else NVAL
    return pl.pallas_call(
        partial(backward_kernel, layer),
        out_shape=(
            jax.ShapeDtypeStruct((values * WSTEP, TILE), f32),
            jax.ShapeDtypeStruct((8, atoms), f32),
            jax.ShapeDtypeStruct((NMAX * NRAD, TILE), f32),
        ),
        grid=(atoms // TILE,),
        in_specs=[
            smem_spec(),
            smem_spec(),
            tile_spec(GEO * NPAD),
            tile_spec(feat.shape[0]),
            tile_spec(NPAD),
            tile_spec(NPAD),
            tile_spec(DENS),
            whole_spec(window_in.shape),
            tile_spec(8),
        ],
        out_specs=(
            whole_spec((values * WSTEP, TILE)),
            tile_spec(8),
            whole_spec((NMAX * NRAD, TILE)),
        ),
        scratch_shapes=[
            pltpu.VMEM((NMAX * NRAD * 8, TILE), f32),
            pltpu.VMEM((CH * 8, TILE), f32),
            pltpu.VMEM((LM * 8, TILE), f32),
            pltpu.VMEM((CH * 8, TILE), f32),
            pltpu.VMEM((LM * 8, TILE), f32),
            pltpu.VMEM((NVAL * NPAD, TILE), f32),
            pltpu.VMEM((8 * (NVAL * WROWS + 1), TILE), f32),
        ],
        compiler_params=pltpu.CompilerParams(vmem_limit_bytes=VMEM_ALL),
        name="backward_%d" % layer,
    )(info, radial, geo, feat, index, weight, grad_dens, window_in, own_in)


def tn_dot(left, right):
    return lax.dot_general(left, right, (((0,), (0,)), ((), ())), preferred_element_type=f32)


def nt_dot(left, right):
    return lax.dot_general(left, right, (((1,), (1,)), ((), ())), preferred_element_type=f32)


def padded_rows(value):
    return jnp.concatenate([value, jnp.zeros((8 - value.shape[0], value.shape[1]), f32)], axis=0)


def onehot_rows(species):
    kind = lax.broadcasted_iota(jnp.int32, (8, species.shape[1]), 0).astype(f32)
    return jnp.where(kind == species, 1.0, 0.0).astype(bf16)


def combine(parts):
    total = parts[2][0:8]
    total = total + (parts[1][8:16] + parts[0][16:24])
    total = total + (parts[1][0:8] + parts[0][8:16])
    return total + parts[0][0:8]


def by_atoms(rows24, chunk):
    wide = nt_dot(rows24, split3(chunk))
    return [wide[:, j * QB : (j + 1) * QB] for j in range(3)]


def contract_one_kernel(dens_ref, coup_ref, coef_ref, mix_ref, site_ref, factor_ref, energy_ref, feat_ref,
                        aux_ref, grad_ref, b_ref, ch_ref, row_ref):
    factor_at = pl.program_id(0)
    quantum, atoms = b_ref.shape
    half = quantum // 2
    for part in range(2):
        rows = slice(part * half, (part + 1) * half)
        value = tn_dot(coup_ref[0, :, rows], dens_ref[...])
        factor_ref[0, rows, :] = value

        @pl.when(factor_at == 0)
        def _(value=value, rows=rows):
            b_ref[rows, :] = value

        @pl.when(factor_at > 0)
        def _(value=value, rows=rows):
            b_ref[rows, :] = b_ref[rows, :] * value

    @pl.when(factor_at == pl.num_programs(0) - 1)
    def _():
        onehot = onehot_rows(site_ref[3:4, :])
        row_ref[0:24, :] = split3(padded_rows(coef_ref[...]))
        row_ref[24:48, :] = split3(padded_rows(mix_ref[...]))
        triple = jnp.concatenate([onehot] * 3, axis=0)

        def chunk_body(chunk, mixed):
            cols = pl.ds(pl.multiple_of(chunk * QB, QB), QB)
            ch_ref[...] = tn_dot(row_ref[0:24, cols], triple)
            pieces = split3(b_ref[cols, :])
            left = row_ref[24:48, cols]
            parts = [
                jnp.dot(left, pieces[j * QB : (j + 1) * QB], preferred_element_type=f32) for j in range(3)
            ]
            wide = nt_dot(onehot, pieces)
            grad_ref[:, cols] = wide[:, 2 * QB :] + wide[:, QB : 2 * QB] + wide[:, :QB]

            def rows_body(step, sums):
                at = pl.multiple_of(step * 8, 8)
                value = b_ref[pl.ds(pl.multiple_of(chunk * QB + step * 8, 8), 8), :]
                return sums[0] + value * ch_ref[pl.ds(at, 8), :], sums[1] + value * value

            energy, square = lax.fori_loop(0, QB // 8, rows_body, mixed[1:])
            return mixed[0] + combine(parts), energy, square

        zero = jnp.zeros((8, atoms), f32)
        mixed, energy, square = lax.fori_loop(0, quantum // QB, chunk_body, (zero, zero, zero))
        energy_ref[...] = jnp.broadcast_to(jnp.sum(energy, axis=0, keepdims=True), (8, atoms))
        mean = jnp.sum(square, axis=0, keepdims=True) * (1.0 / quantum)
        scale = lax.rsqrt(mean + norm_eps)
        feat_ref[...] = mixed * scale
        aux_ref[0:8, :] = mixed
        aux_ref[8:16, :] = jnp.broadcast_to(scale, (8, atoms))


def contract_one_call(dens, coupling, coefficient, mixing_rows, ordered):
    factors, depth, quantum = coupling.shape
    atoms = dens.shape[1]
    return pl.pallas_call(
        contract_one_kernel,
        out_shape=(
            jax.ShapeDtypeStruct((factors, quantum, atoms), f32),
            jax.ShapeDtypeStruct((8, atoms), f32),
            jax.ShapeDtypeStruct((8, atoms), f32),
            jax.ShapeDtypeStruct((16, atoms), f32),
            jax.ShapeDtypeStruct((8, quantum), f32),
        ),
        grid=(factors,),
        in_specs=[
            whole_spec((depth, atoms)),
            pl.BlockSpec((1, depth, quantum), lambda v: (v, 0, 0)),
            whole_spec(coefficient.shape),
            whole_spec(mixing_rows.shape),
            whole_spec(ordered.shape),
        ],
        out_specs=(
            pl.BlockSpec((1, quantum, atoms), lambda v: (v, 0, 0)),
            whole_spec((8, atoms)),
            whole_spec((8, atoms)),
            whole_spec((16, atoms)),
            whole_spec((8, quantum)),
        ),
        scratch_shapes=[
            pltpu.VMEM((quantum, atoms), f32),
            pltpu.VMEM((QB, atoms), f32),
            pltpu.VMEM((48, quantum), bf16),
        ],
        compiler_params=pltpu.CompilerParams(vmem_limit_bytes=VMEM_ALL),
        name="contract_1",
    )(dens, coupling, coefficient, mixing_rows, ordered)


def factor_grads(values, upstream):
    low_pair, high_pair = values[0] * values[1], values[2] * values[3]
    first, second = upstream * high_pair, upstream * low_pair
    return first * values[1], first * values[0], second * values[3], second * values[2]


def contract_two_kernel(dens_ref, coef_ref, site_ref, before_ref, coup_ref, out_ref, part_ref, grad_ref,
                        cv_ref, f_ref, g_ref, ch_ref, row_ref, sem):
    step = pl.program_id(0)
    factors, quantum, atoms = f_ref.shape
    depth = dens_ref.shape[0]
    half = quantum // 2

    def load(at):
        return pltpu.make_async_copy(coup_ref.at[at], cv_ref.at[at, 0:depth], sem.at[at])

    @pl.when(step == 0)
    def _():
        for at in range(factors):
            load(at).start()
        onehot = onehot_rows(site_ref[3:4, :])
        row_ref[...] = split3(padded_rows(coef_ref[...]))
        triple = jnp.concatenate([onehot] * 3, axis=0)

        def factor_body(at, carry):
            load(at).wait()
            for part in range(2):
                rows = slice(part * half, (part + 1) * half)
                f_ref[at, rows, :] = tn_dot(cv_ref[at, 0:depth, rows], dens_ref[...])
            return carry

        lax.fori_loop(0, factors, factor_body, 0)

        def chunk_body(chunk, energy):
            cols = pl.ds(pl.multiple_of(chunk * QB, QB), QB)
            ch_ref[...] = tn_dot(row_ref[:, cols], triple)

            def rows_body(small, total):
                at = pl.multiple_of(small * 16, 16)
                rows = pl.ds(pl.multiple_of(chunk * QB + small * 16, 16), 16)
                values = [f_ref[v, rows, :] for v in range(factors)]
                upstream = ch_ref[pl.ds(at, 16), :]
                grads = factor_grads(values, upstream)
                for v in range(factors):
                    g_ref[v, rows, :] = grads[v].astype(bf16)
                product = values[0] * values[1] * values[2] * values[3]
                f_ref[0, rows, :] = product
                term = product * upstream
                return total + term[:8] + term[8:]

            energy = lax.fori_loop(0, QB // 16, rows_body, energy)
            wide = nt_dot(onehot, split3(f_ref[0, cols, :]))
            grad_ref[:, cols] = wide[:, 2 * QB :] + wide[:, QB : 2 * QB] + wide[:, :QB]
            return energy

        energy = lax.fori_loop(0, quantum // QB, chunk_body, jnp.zeros((8, atoms), f32))
        energy = jnp.sum(energy, axis=0, keepdims=True) + before_ref[0:1, :]
        kinds = [jnp.where(site_ref[3:4, :] == float(c), 1.0, 0.0) for c in range(SPECIES)]
        rows8 = split3(jnp.concatenate([energy] + kinds + [jnp.zeros((3, atoms), f32)], axis=0))
        owner = site_ref[4:5, :]

        def structure_body(chunk, carry):
            cols = pl.ds(pl.multiple_of(chunk * TILE, TILE), TILE)
            ids = lax.broadcasted_iota(jnp.int32, (TILE, atoms), 0) + chunk * TILE
            members = jnp.where(ids.astype(f32) == owner, 1.0, 0.0).astype(bf16)
            wide = nt_dot(rows8, members)
            part_ref[:, cols] = wide[16:24] + wide[8:16] + wide[0:8]
            return carry

        lax.fori_loop(0, part_ref.shape[1] // TILE, structure_body, 0)

    rows = pl.ds(pl.multiple_of(step * DROWS, 16), DROWS)
    total = None
    for at in range(factors):
        part = jnp.dot(cv_ref[at, rows, :], g_ref[at], preferred_element_type=f32)
        total = part if total is None else total + part
    out_ref[...] = total


def contract_two_call(dens, coupling, coefficient, ordered, energy_one, structures):
    factors, depth, quantum = coupling.shape
    atoms = dens.shape[1]
    steps = pl.cdiv(depth, DROWS)
    return pl.pallas_call(
        contract_two_kernel,
        out_shape=(
            jax.ShapeDtypeStruct((steps * DROWS, atoms), f32),
            jax.ShapeDtypeStruct((8, structures), f32),
            jax.ShapeDtypeStruct((8, quantum), f32),
        ),
        grid=(steps,),
        in_specs=[
            pl.BlockSpec((depth, atoms), lambda i: (0, 0), pipeline_mode=pl.Buffered(1)),
            whole_spec(coefficient.shape),
            whole_spec(ordered.shape),
            whole_spec(energy_one.shape),
            pl.BlockSpec(memory_space=pl.ANY),
        ],
        out_specs=(
            pl.BlockSpec((DROWS, atoms), lambda i: (i, 0)),
            whole_spec((8, structures)),
            whole_spec((8, quantum)),
        ),
        scratch_shapes=[
            pltpu.VMEM((factors, steps * DROWS, quantum), bf16),
            pltpu.VMEM((factors, quantum, atoms), f32),
            pltpu.VMEM((factors, quantum, atoms), bf16),
            pltpu.VMEM((QB, atoms), f32),
            pltpu.VMEM((24, quantum), bf16),
            pltpu.SemaphoreType.DMA((factors,)),
        ],
        compiler_params=pltpu.CompilerParams(vmem_limit_bytes=VMEM_ALL),
        name="contract_2",
    )(dens, coefficient, ordered, energy_one, coupling)


def contract_back_kernel(coup_ref, coef_ref, mix_ref, site_ref, gfeat_ref, aux_ref, factor_ref, out_ref,
                         grad_ref, f_ref, g_ref, ch_ref, row_ref, sem):
    step = pl.program_id(0)
    factors, quantum, atoms = f_ref.shape
    chunks = quantum // QB

    def load(chunk):
        rows = pl.ds(pl.multiple_of(chunk * QB, QB), QB)
        return pltpu.make_async_copy(factor_ref.at[:, rows, :], f_ref.at[:, rows, :], sem.at[chunk])

    @pl.when(step == 0)
    def _():
        for chunk in range(chunks):
            load(chunk).start()
        onehot = onehot_rows(site_ref[3:4, :])
        scale = aux_ref[8:9, :]
        gfeat = gfeat_ref[...]
        dot = jnp.sum(aux_ref[0:8, :] * gfeat, axis=0, keepdims=True)
        shrink = jnp.broadcast_to(scale * scale * scale * dot * (1.0 / quantum), (8, atoms))
        scaled = split3(scale * gfeat)
        high, middle, low = scaled[0:8], scaled[8:16], scaled[16:24]
        mix = split3(padded_rows(mix_ref[...]))
        row_ref[0:24, :] = split3(padded_rows(coef_ref[...]))
        for at, piece in enumerate((0, 0, 0, 1, 1, 2)):
            row_ref[24 + 8 * at : 32 + 8 * at, :] = mix[8 * piece : 8 * piece + 8]
        right = jnp.concatenate([onehot] * 3 + [high, middle, low, high, middle, high], axis=0)

        def chunk_body(chunk, carry):
            load(chunk).wait()
            cols = pl.ds(pl.multiple_of(chunk * QB, QB), QB)
            ch_ref[...] = tn_dot(row_ref[:, cols], right)

            def rows_body(small, inner):
                at = pl.multiple_of(small * 16, 16)
                rows = pl.ds(pl.multiple_of(chunk * QB + small * 16, 16), 16)
                values = [f_ref[v, rows, :] for v in range(factors)]
                product = values[0] * values[1] * values[2] * values[3]
                both = jnp.concatenate([shrink, shrink], axis=0)
                upstream = ch_ref[pl.ds(at, 16), :] - both * product
                grads = factor_grads(values, upstream)
                for v in range(factors):
                    g_ref[v, rows, :] = grads[v].astype(bf16)
                f_ref[0, rows, :] = product
                return inner

            lax.fori_loop(0, QB // 16, rows_body, 0)
            grad_ref[:, cols] = combine(by_atoms(scaled, f_ref[0, cols, :]))
            return carry

        lax.fori_loop(0, chunks, chunk_body, 0)

    total = None
    for at in range(factors):
        part = jnp.dot(coup_ref[at], g_ref[at], preferred_element_type=f32)
        total = part if total is None else total + part
    out_ref[...] = total


def contract_back_call(coupling, coefficient, mixing_rows, ordered, gfeat, aux, factor):
    factors, depth, quantum = coupling.shape
    atoms = ordered.shape[1]
    rows = depth // 5
    return pl.pallas_call(
        contract_back_kernel,
        out_shape=(
            jax.ShapeDtypeStruct((depth, atoms), f32),
            jax.ShapeDtypeStruct((8, quantum), f32),
        ),
        grid=(5,),
        in_specs=[
            pl.BlockSpec((factors, rows, quantum), lambda i: (0, i, 0)),
            whole_spec(coefficient.shape),
            whole_spec(mixing_rows.shape),
            whole_spec(ordered.shape),
            whole_spec(gfeat.shape),
            whole_spec(aux.shape),
            pl.BlockSpec(memory_space=pl.ANY),
        ],
        out_specs=(pl.BlockSpec((rows, atoms), lambda i: (i, 0)), whole_spec((8, quantum))),
        scratch_shapes=[
            pltpu.VMEM((factors, quantum, atoms), f32),
            pltpu.VMEM((factors, quantum, atoms), bf16),
            pltpu.VMEM((QB, atoms), f32),
            pltpu.VMEM((72, quantum), bf16),
            pltpu.SemaphoreType.DMA((quantum // QB,)),
        ],
        compiler_params=pltpu.CompilerParams(vmem_limit_bytes=VMEM_ALL),
        name="contract_back_1",
    )(coupling, coefficient, mixing_rows, ordered, gfeat, aux, factor)


def per_device(
    positions,
    species,
    neighbours,
    slot_counts,
    structure,
    target_energy,
    radial_one,
    coupling_one,
    coefficient_one,
    mixing,
    radial_two,
    coupling_two,
    coefficient_two,
):
    atoms = positions.shape[2]
    tiles = atoms // TILE
    structures = target_energy.shape[1]
    table_one = spread_call(0, 4, True, (positions, species, structure))
    first = ((lax.axis_index("dom") - 1) * atoms).astype(jnp.int32).reshape(1)
    index, weight, ordered, perm, info = prepare_call(
        first, slot_counts, neighbours, positions, species, structure
    )
    mixing_rows = mixing.T

    dens_one, geo = density_call(1, info, radial_one, table_one, ordered, index, weight)
    factors_one, energy_one, features, aux, coefficient_first = contract_one_call(
        dens_one, coupling_one, coefficient_one, mixing_rows, ordered
    )
    table_two = spread_call(1, SPECIES, False, (features, perm))
    dens_two, feat = density_call(2, info, radial_two, table_two, ordered, index, weight, geo)
    grad_dens_two, per_structure, coefficient_second = contract_two_call(
        dens_two, coupling_two, coefficient_two, ordered, energy_one, structures
    )
    window_two, own_two, radial_second = backward_call(
        2, info, radial_two, geo, feat, index, weight, grad_dens_two, table_two, ordered
    )
    grad_features = collect_call(2, tiles, 3, window_two.reshape(NVAL, WSTEP, TILE), perm)
    grad_dens_one, mixing_gradient = contract_back_call(
        coupling_one, coefficient_one, mixing_rows, ordered, grad_features, aux, factors_one
    )
    window_one, own_one, radial_first = backward_call(
        1, info, radial_one, geo, ordered, index, weight, grad_dens_one, window_two, own_two
    )
    groups = lax.axis_size("grp")
    steps = log2_of(lax.axis_size("dom")) + log2_of(groups)
    forces, sums, group_sums = finish_call(
        3,
        steps,
        groups,
        tiles,
        (
            window_one.reshape(3, WSTEP, TILE),
            own_one,
            perm,
            coefficient_first,
            coefficient_second,
            mixing_gradient,
            radial_first,
            radial_second,
            per_structure,
            target_energy,
        ),
    )
    mine = lax.axis_index("grp").astype(jnp.int32).reshape(1)
    outputs = list(tail_call(mine, forces, sums, group_sums))
    outputs[1] = outputs[1].reshape(SPECIES)
    outputs[5] = outputs[5].T
    return tuple(outputs)


def solution(mesh):
    in_specs = (
        P(None, "grp", "dom"),
        P("grp", "dom"),
        P(None, "grp", "dom"),
        P("grp", "dom"),
        P("grp", "dom"),
        P("grp", None),
        P(),
        P(),
        P(),
        P(),
        P(),
        P(),
        P(),
    )
    out_specs = (P("grp", None), P(), P(None, "grp", "dom"), P(), P(), P(), P(), P())
    return jax.shard_map(
        per_device, mesh=mesh, in_specs=in_specs, out_specs=out_specs, check_vma=False
    )
```

```python
from functools import partial
import math

import jax
import jax.numpy as jnp
from jax import lax
from jax.experimental import pallas as pl
from jax.experimental.pallas import tpu as pltpu
from jax.sharding import PartitionSpec as P

NRAD = 12
NMAX = 10
LMAX = 6
LM = 49
SPECIES = 4
CH = SPECIES * NMAX
DENS = CH * LM
NBR = 48
NPAD = 64
TILE = 128
LBLK = 7
WROWS = 12
WSTEP = 40
GEO = 5
QB = 128
FROWS = 16
VMEM_ALL = 67043328
DROWS = 400
NVAL = 7
SLOTS = 4
XROW = CH + 1

cutoff_radius = 5.0
density_scale = 0.17
norm_eps = 1e-05
ridge_weight = 0.1
highest = lax.Precision.HIGHEST
f32 = jnp.float32
MESH = pl.DeviceIdType.MESH
bf16 = jnp.bfloat16


def log2_of(count):
    steps = count.bit_length() - 1
    assert count == 1 << steps
    return steps


def neighbour_flags(me, count):
    return me > 0, me < count - 1


def greet(partners, flags):
    barrier = pltpu.get_barrier_semaphore()
    for partner, flag in zip(partners, flags):
        if flag is None:
            pl.semaphore_signal(barrier, inc=1, device_id=partner, device_id_type=MESH)
        else:

            @pl.when(flag)
            def _(partner=partner):
                pl.semaphore_signal(barrier, inc=1, device_id=partner, device_id_type=MESH)

    present = sum(1 for flag in flags if flag is None)
    for flag in flags:
        if flag is not None:
            present = present + jnp.where(flag, 1, 0)
    pl.semaphore_wait(barrier, present)


class SidePair:
    def __init__(self, to_left, to_right, got_ref, send_sem, recv_sem):
        count = lax.axis_size("dom")
        me = lax.axis_index("dom")
        self.partners = ({"dom": me - 1}, {"dom": me + 1})
        self.flags = neighbour_flags(me, count)
        self.got = got_ref
        self.copies = [
            pltpu.make_async_remote_copy(
                src_ref=source,
                dst_ref=got_ref.at[1 - side],
                send_sem=send_sem.at[side],
                recv_sem=recv_sem.at[1 - side],
                device_id=self.partners[side],
                device_id_type=MESH,
            )
            for side, source in enumerate((to_left, to_right))
        ]

    def start(self):
        for side in range(2):
            pl.when(self.flags[side])(self.copies[side].start)

    def wait(self):
        for side in range(2):

            @pl.when(self.flags[side])
            def _(side=side):
                self.copies[side].wait_send()
                self.copies[1 - side].wait_recv()

    def received(self, side):
        return jnp.where(self.flags[side], self.got[side], 0.0)


def split3(value):
    high = value.astype(bf16)
    rest = value - high.astype(f32)
    middle = rest.astype(bf16)
    low = (rest - middle.astype(f32)).astype(bf16)
    return jnp.concatenate([high, middle, low], axis=0)


def reorder(value, perm_ref, contract_at):
    count = value.shape[0]
    out = lax.dot_general(
        split3(value), perm_ref[...], (((1,), (contract_at,)), ((), ())), preferred_element_type=f32
    )
    return out[:count] + (out[count : 2 * count] + out[2 * count :])


def site_rows(pos_ref, kind_ref, part_ref):
    atoms = kind_ref.shape[1]
    rows = [pos_ref[axis] for axis in range(3)]
    rows = rows + [kind_ref[...].astype(f32), part_ref[...].astype(f32)]
    return jnp.concatenate(rows + [jnp.zeros((3, atoms), f32)], axis=0)


def spread_kernel(values, ordered, *refs):
    if ordered:
        pos_ref, kind_ref, part_ref, out_ref, mine_ref, got_ref, send_sem, recv_sem = refs
        flat = site_rows(pos_ref, kind_ref, part_ref)
    else:
        x_ref, perm_ref, out_ref, mine_ref, got_ref, send_sem, recv_sem = refs
        flat = reorder(x_ref[...], perm_ref, 0)
    rows = flat.shape[1] // TILE
    for value in range(values):
        for row in range(rows):
            line = flat[value : value + 1, row * TILE : (row + 1) * TILE]
            at = value * rows + row
            mine_ref[at : at + 1, :] = line
    pair = SidePair(mine_ref, mine_ref, got_ref, send_sem, recv_sem)
    greet(pair.partners, pair.flags)
    pair.start()
    for value in range(values):
        at = value * 3 * rows
        out_ref[at + rows : at + 2 * rows, :] = mine_ref[value * rows : (value + 1) * rows, :]
    pair.wait()
    for side in range(2):
        block = pair.received(side)
        for value in range(values):
            at = value * 3 * rows + 2 * side * rows
            out_ref[at : at + rows, :] = block[value * rows : (value + 1) * rows]


def comm_params(which):
    return pltpu.CompilerParams(collective_id=which, has_side_effects=True, vmem_limit_bytes=VMEM_ALL)


def vmem_spec():
    return pl.BlockSpec(memory_space=pltpu.VMEM)


def spread_call(which, values, raw, operands):
    rows = values * operands[-1].shape[1] // TILE
    return pl.pallas_call(
        partial(spread_kernel, values, raw),
        out_shape=jax.ShapeDtypeStruct((rows * 3, TILE), f32),
        in_specs=[vmem_spec()] * len(operands),
        out_specs=vmem_spec(),
        scratch_shapes=[
            pltpu.VMEM((rows, TILE), f32),
            pltpu.VMEM((2, rows, TILE), f32),
            pltpu.SemaphoreType.DMA((2,)),
            pltpu.SemaphoreType.DMA((2,)),
        ],
        compiler_params=comm_params(which),
        name="spread_%d" % which,
    )(*operands)


def in_lanes(blocks):
    values, rows = blocks.shape[0], blocks.shape[1]
    flat = [
        jnp.concatenate([blocks[v, r : r + 1, :] for r in range(rows)], axis=1) for v in range(values)
    ]
    return jnp.concatenate(flat + [jnp.zeros((8 - values, rows * TILE), f32)], axis=0)


def collect_kernel(rows, values_at, win_ref, perm_ref, out_ref, got_ref, send_sem, recv_sem):
    pair = SidePair(
        win_ref.at[values_at:, 0:rows],
        win_ref.at[values_at:, 2 * rows : 3 * rows],
        got_ref,
        send_sem,
        recv_sem,
    )
    greet(pair.partners, pair.flags)
    pair.start()
    pair.wait()
    total = win_ref[values_at:, rows : 2 * rows] + pair.received(0) + pair.received(1)
    out_ref[...] = reorder(in_lanes(total), perm_ref, 1)


def collect_call(which, rows, values_at, window, perm):
    values = window.shape[0] - values_at
    return pl.pallas_call(
        partial(collect_kernel, rows, values_at),
        out_shape=jax.ShapeDtypeStruct((8, rows * TILE), f32),
        in_specs=[vmem_spec()] * 2,
        out_specs=vmem_spec(),
        scratch_shapes=[
            pltpu.VMEM((2, values, rows, TILE), f32),
            pltpu.SemaphoreType.DMA((2,)),
            pltpu.SemaphoreType.DMA((2,)),
        ],
        compiler_params=comm_params(which),
        name="collect_%d" % which,
    )(window, perm)


def lane_sums(value):
    wide = nt_dot(jnp.ones((8, TILE), bf16), split3(value))
    rows = value.shape[0]
    total = wide[0:1, 2 * rows :] + wide[0:1, rows : 2 * rows] + wide[0:1, :rows]
    return jnp.concatenate([total, jnp.zeros((1, TILE - rows), f32)], axis=1)


def exchange_rounds():
    rounds = []
    for axis in ("dom", "grp"):
        me = lax.axis_index(axis)
        bits = log2_of(lax.axis_size(axis))

        def flip(places):
            other = me
            for bit in places:
                half = 1 << bit
                other = other + half - 2 * half * lax.rem(lax.div(me, half), 2)
            return {axis: other}

        for bit in range(0, bits, 2):
            if bit + 1 < bits:
                rounds.append([flip((bit,)), flip((bit + 1,)), flip((bit, bit + 1))])
            else:
                rounds.append([flip((bit,))])
    return rounds


def finish_kernel(rows, win_ref, own_ref, perm_ref, first_ref, second_ref, mix_ref, one_ref, two_ref, part_ref,
                  target_ref, force_ref, sum_ref, group_ref, got_ref, pay_ref, pay_group_ref, came_ref,
                  came_group_ref, send_sem, recv_sem, step_send, step_recv, group_send, group_recv):
    pair = SidePair(
        win_ref.at[:, 0:rows], win_ref.at[:, 2 * rows : 3 * rows], got_ref, send_sem, recv_sem
    )
    rounds = exchange_rounds()
    partners = [partner for group in rounds for partner in group]
    width = pay_ref.shape[1]
    for at, ref in enumerate((first_ref, second_ref, mix_ref)):
        pay_ref[4 * at : 4 * at + 4, :] = ref[0:4, :]
    tail = [lane_sums(one_ref[...]), lane_sums(two_ref[...]), jnp.zeros((1, width - 2 * TILE), f32)]
    pay_ref[12:13, :] = jnp.concatenate(tail, axis=1)
    pay_ref[13:16, :] = jnp.zeros((3, width), f32)
    lead = lax.axis_index("dom") == 0
    mine = lax.axis_index("grp")
    target = jnp.where(lead, target_ref[...], 0.0)
    block = part_ref[...]
    block = jnp.concatenate([block[0:5], target, block[6:8]], axis=0)
    for group in range(lax.axis_size("grp")):
        pay_group_ref[8 * group : 8 * group + 8, :] = jnp.where(mine == group, block, 0.0)
    greet(list(pair.partners) + partners, list(pair.flags) + [None] * len(partners))
    pair.start()
    at = 0
    for turn, group in enumerate(rounds):
        copies = []
        for partner in group:
            for source, total, came, send, recv in (
                (pay_ref, sum_ref, came_ref, step_send, step_recv),
                (pay_group_ref, group_ref, came_group_ref, group_send, group_recv),
            ):
                copy = pltpu.make_async_remote_copy(
                    src_ref=source if turn == 0 else total,
                    dst_ref=came.at[at],
                    send_sem=send.at[at],
                    recv_sem=recv.at[at],
                    device_id=partner,
                    device_id_type=MESH,
                )
                copy.start()
                copies.append(copy)
            at = at + 1
        if turn == 0:
            force_ref[...] = reorder(own_ref[...], perm_ref, 0)
        for copy in copies:
            copy.wait()
        for source, total, came in (
            (pay_ref, sum_ref, came_ref),
            (pay_group_ref, group_ref, came_group_ref),
        ):
            value = (source if turn == 0 else total)[...] + came[at - len(group)]
            if len(group) == 3:
                value = value + (came[at - 2] + came[at - 1])
            total[...] = value
    pair.wait()
    total = win_ref[:, rows : 2 * rows] + pair.received(0) + pair.received(1)
    force_ref[...] = force_ref[...] - in_lanes(total)


def finish_call(which, mesh_steps, groups, rows, operands):
    width, structures = operands[3].shape[1], operands[9].shape[1]
    return pl.pallas_call(
        partial(finish_kernel, rows),
        out_shape=(
            jax.ShapeDtypeStruct((8, rows * TILE), f32),
            jax.ShapeDtypeStruct((16, width), f32),
            jax.ShapeDtypeStruct((8 * groups, structures), f32),
        ),
        in_specs=[vmem_spec()] * 10,
        out_specs=(vmem_spec(),) * 3,
        scratch_shapes=[
            pltpu.VMEM((2, 3, rows, TILE), f32),
            pltpu.VMEM((16, width), f32),
            pltpu.VMEM((8 * groups, structures), f32),
            pltpu.VMEM((mesh_steps, 16, width), f32),
            pltpu.VMEM((mesh_steps, 8 * groups, structures), f32),
            pltpu.SemaphoreType.DMA((2,)),
            pltpu.SemaphoreType.DMA((2,)),
            pltpu.SemaphoreType.DMA((mesh_steps,)),
            pltpu.SemaphoreType.DMA((mesh_steps,)),
            pltpu.SemaphoreType.DMA((mesh_steps,)),
            pltpu.SemaphoreType.DMA((mesh_steps,)),
        ],
        compiler_params=comm_params(which),
        name="finish_%d" % which,
    )(*operands)


def tail_kernel(mine_ref, all_force_ref, sum_ref, group_ref, energy_ref, offset_ref, force_ref, one_ref,
                first_ref, mix_ref, two_ref, second_ref):
    groups = group_ref.shape[0] // 8

    def fractions(rows):
        counts = [rows[1 + c : 2 + c, :] for c in range(SPECIES)]
        size = jnp.maximum(counts[0] + counts[1] + counts[2] + counts[3], 1.0)
        return [count / size for count in counts], size

    gram = [[None] * SPECIES for _ in range(SPECIES)]
    right = [None] * SPECIES
    energy = None
    own_frac = [None] * SPECIES

    def plus(total, value):
        return value if total is None else total + value

    for group in range(groups):
        rows = group_ref[8 * group : 8 * group + 8, :]
        frac, size = fractions(rows)
        mine = jnp.where(mine_ref[0] == group, 1.0, 0.0)
        energy = plus(energy, mine * (rows[0:1] / size))
        for c in range(SPECIES):
            own_frac[c] = plus(own_frac[c], mine * frac[c])
            right[c] = plus(right[c], frac[c] * rows[5:6])
            for d in range(c, SPECIES):
                gram[c][d] = plus(gram[c][d], frac[c] * frac[d])

    def whole(value):
        return jnp.sum(value, axis=1, keepdims=True)

    right = [whole(value) for value in right]
    upper = [[None if value is None else whole(value) for value in row] for row in gram]
    matrix = [
        [upper[min(c, d)][max(c, d)] + (ridge_weight if c == d else 0.0) for d in range(SPECIES)]
        for c in range(SPECIES)
    ]
    for pivot in range(SPECIES):
        for below in range(pivot + 1, SPECIES):
            ratio = matrix[below][pivot] / matrix[pivot][pivot]
            matrix[below] = [b - ratio * a for a, b in zip(matrix[pivot], matrix[below])]
            right[below] = right[below] - ratio * right[pivot]
    answer = [None] * SPECIES
    for row in range(SPECIES - 1, -1, -1):
        running = right[row]
        for later in range(row + 1, SPECIES):
            running = running - matrix[row][later] * answer[later]
        answer[row] = running / matrix[row][row]
    for c in range(SPECIES):
        energy = energy + own_frac[c] * answer[c]
    energy_ref[...] = energy
    offset_ref[...] = jnp.concatenate(answer, axis=1)
    for axis in range(3):
        force_ref[axis] = all_force_ref[axis : axis + 1, :]
    first_ref[...] = sum_ref[0:4, :]
    second_ref[...] = sum_ref[4:8, :]
    mix_ref[...] = sum_ref[8:12, :]
    for n in range(NMAX):
        one_ref[n : n + 1, :] = sum_ref[12:13, n * NRAD : (n + 1) * NRAD]
        two_ref[n : n + 1, :] = sum_ref[12:13, TILE + n * NRAD : TILE + (n + 1) * NRAD]


def tail_call(mine, forces, sums, groups):
    width, structures, atoms = sums.shape[1], groups.shape[1], forces.shape[1]
    shapes = (
        (1, structures),
        (1, SPECIES),
        (3, 1, atoms),
        (NMAX, NRAD),
        (SPECIES, width),
        (SPECIES, width),
        (NMAX, NRAD),
        (SPECIES, width),
    )
    return pl.pallas_call(
        tail_kernel,
        out_shape=tuple(jax.ShapeDtypeStruct(shape, f32) for shape in shapes),
        in_specs=[smem_spec()] + [vmem_spec()] * 3,
        out_specs=(vmem_spec(),) * len(shapes),
        compiler_params=pltpu.CompilerParams(vmem_limit_bytes=VMEM_ALL),
        name="tail",
    )(mine, forces, sums, groups)


def double_factorial(number):
    result = 1.0
    while number > 1:
        result = result * number
        number = number - 2
    return result


def norm_of(degree, azimuth):
    value = math.sqrt(
        (2 * degree + 1)
        / (4 * math.pi)
        * math.factorial(degree - azimuth)
        / math.factorial(degree + azimuth)
    )
    return value * (math.sqrt(2.0) if azimuth else 1.0)


def scaled_legendre(coord_z):
    table = {}
    for azimuth in range(LMAX + 1):
        table[azimuth, azimuth] = norm_of(azimuth, azimuth) * double_factorial(2 * azimuth - 1)
        if azimuth + 1 <= LMAX:
            ratio = norm_of(azimuth + 1, azimuth) / norm_of(azimuth, azimuth)
            table[azimuth + 1, azimuth] = coord_z * (
                (2 * azimuth + 1) * ratio * table[azimuth, azimuth]
            )
        for degree in range(azimuth + 2, LMAX + 1):
            gap = degree - azimuth
            first = (2 * degree - 1) / gap * norm_of(degree, azimuth) / norm_of(degree - 1, azimuth)
            second = (
                (degree + azimuth - 1) / gap * norm_of(degree, azimuth) / norm_of(degree - 2, azimuth)
            )
            table[degree, azimuth] = (first * coord_z) * table[degree - 1, azimuth] - (
                second * table[degree - 2, azimuth]
            )
    return table


def azimuth_powers(coord_x, coord_y):
    cosines = [None, coord_x]
    sines = [None, coord_y]
    for _ in range(2, LMAX + 1):
        cosines.append(cosines[-1] * coord_x - sines[-1] * coord_y)
        sines.append(sines[-1] * coord_x + cosines[-2] * coord_y)
    return cosines, sines


LANE_GATHER = lax.GatherDimensionNumbers(
    offset_dims=(),
    collapsed_slice_dims=(1,),
    start_index_map=(1,),
    operand_batching_dims=(0,),
    start_indices_batching_dims=(0,),
)


def lane_gather(line, lo):
    return lax.gather(
        line,
        lo[..., None],
        LANE_GATHER,
        slice_sizes=(1, 1),
        mode=lax.GatherScatterMode.PROMISE_IN_BOUNDS,
    )


def prepare_kernel(first_ref, cnt_ref, nbr_ref, spot_ref, kind_ref, part_ref, idx_ref, wt_ref, sorted_ref, perm_ref, info_ref,
                   key_ref, pos_ref, word_ref, rank_ref):
    atoms = nbr_ref.shape[2]
    tiles = atoms // TILE
    blocks = NBR // 8
    sub = lax.broadcasted_iota(jnp.int32, (8, TILE), 0)
    lane = lax.broadcasted_iota(jnp.int32, (1, TILE), 1)

    def merge(tile, carry):
        cols = pl.ds(pl.multiple_of(tile * TILE, TILE), TILE)
        limit = cnt_ref[:, cols]
        iota = lax.broadcasted_iota(jnp.int32, (NBR, TILE), 0)
        key = jnp.where(iota < limit, nbr_ref[:, 0, cols] - first_ref[0], -1 - iota)
        key_ref[...] = key
        keys = [key[8 * b : 8 * b + 8] for b in range(blocks)]
        total = [jnp.zeros((8, TILE), jnp.int32) for _ in range(blocks)]
        early = [jnp.zeros((8, TILE), jnp.int32) for _ in range(blocks)]
        for other in range(NBR):
            line = jnp.broadcast_to(key_ref[other : other + 1, :], (8, TILE))
            for b in range(blocks):
                same = jnp.where(keys[b] == line, 1, 0)
                total[b] = total[b] + same
                if other < 8 * b:
                    early[b] = early[b] + same
                elif other < 8 * b + 7:
                    early[b] = early[b] + jnp.where(sub > other - 8 * b, same, 0)
        for b in range(blocks):
            alive = sub + 8 * b < limit
            pos_ref[8 * b : 8 * b + 8, :] = jnp.where(alive & (early[b] == 0), 1, 0)
            key_ref[8 * b : 8 * b + 8, :] = total[b] * 4096 + keys[b]
        running = jnp.zeros((1, TILE), jnp.int32)
        out = [jnp.zeros((8, TILE), jnp.int32) for _ in range(blocks)]
        for slot in range(NBR):
            flag = pos_ref[slot : slot + 1, :]
            place = jnp.broadcast_to(jnp.where(flag == 1, running, -1), (8, TILE))
            running = running + flag
            line = jnp.broadcast_to(key_ref[slot : slot + 1, :], (8, TILE))
            for b in range(slot // 8 + 1):
                out[b] = jnp.where(place == sub + 8 * b, line, out[b])
        for b in range(blocks):
            word_ref[8 * b : 8 * b + 8, cols] = out[b].astype(f32)
        order = running * atoms + (atoms - 1 - tile * TILE) - lane
        rank_ref[pl.ds(tile, 1), :] = order.astype(f32)
        return carry

    lax.fori_loop(0, tiles, merge, 0)
    orders = rank_ref[...]
    upright = jnp.transpose(orders)
    ranks = []
    for tile in range(tiles):
        row = jnp.broadcast_to(orders[tile : tile + 1], (TILE, TILE))
        total = jnp.zeros((TILE, TILE), f32)
        for other in range(tiles):
            col = jnp.broadcast_to(upright[:, other : other + 1], (TILE, TILE))
            total = total + jnp.where(col > row, 1.0, 0.0)
        ranks.append(jnp.sum(total, axis=0, keepdims=True))
    place = lax.broadcasted_iota(jnp.int32, (atoms, TILE), 0).astype(f32)
    for tile in range(tiles):
        line = jnp.broadcast_to(ranks[tile], (atoms, TILE))
        perm_ref[:, tile * TILE : (tile + 1) * TILE] = jnp.where(line == place, 1.0, 0.0).astype(bf16)
    word_ref[NBR : NBR + 8, :] = site_rows(spot_ref, kind_ref, part_ref)
    moved = reorder(word_ref[...], perm_ref, 1)
    sorted_ref[...] = moved[NBR:]
    word = moved[:NBR].astype(jnp.int32)
    index = lax.bitwise_and(word, 4095)
    times = lax.shift_right_logical(word, 12)
    idx_ref[:NBR, :] = index
    idx_ref[NBR:, :] = jnp.zeros((NPAD - NBR, atoms), jnp.int32)
    wt_ref[:NBR, :] = density_scale * times.astype(f32)
    wt_ref[NBR:, :] = jnp.zeros((NPAD - NBR, atoms), f32)
    row = lax.shift_right_logical(index, 7)
    low = jnp.min(jnp.where(times > 0, row, 1 << 20))
    high = jnp.max(jnp.where(times > 0, row, -1))
    slots = lax.broadcasted_iota(jnp.int32, (NBR, TILE), 0) + 1
    for tile in range(tiles):
        used = times[:, tile * TILE : (tile + 1) * TILE] > 0
        info_ref[0, tile] = lax.div(jnp.max(jnp.where(used, slots, 0)) + SLOTS - 1, SLOTS) * SLOTS
        info_ref[1, tile] = low
        info_ref[2, tile] = high


def prepare_call(first, limits, neighbours, positions, species, structure):
    atoms = neighbours.shape[2]
    return pl.pallas_call(
        prepare_kernel,
        out_shape=(
            jax.ShapeDtypeStruct((NPAD, atoms), jnp.int32),
            jax.ShapeDtypeStruct((NPAD, atoms), f32),
            jax.ShapeDtypeStruct((8, atoms), f32),
            jax.ShapeDtypeStruct((atoms, atoms), bf16),
            jax.ShapeDtypeStruct((3, atoms // TILE), jnp.int32),
        ),
        in_specs=[smem_spec()] + [vmem_spec()] * 5,
        out_specs=(vmem_spec(), vmem_spec(), vmem_spec(), vmem_spec(), smem_spec()),
        scratch_shapes=[
            pltpu.VMEM((NBR, TILE), jnp.int32),
            pltpu.VMEM((NBR, TILE), jnp.int32),
            pltpu.VMEM((NBR + 8, atoms), f32),
            pltpu.VMEM((atoms // TILE, TILE), f32),
        ],
        compiler_params=pltpu.CompilerParams(vmem_limit_bytes=VMEM_ALL),
        name="prepare",
    )(first, limits, neighbours, positions, species, structure)


def window_starts(row_low, row_high):
    start = jnp.minimum(row_low, 24 - FROWS)
    return start, lax.div(row_high - start, FROWS) + 1


def load_window(tab_ref, left_ref, values, exact, start):
    for value in range(values):
        pieces = split3(tab_ref[pl.ds(value * 24 + start, FROWS), :])
        for piece in range(3 if exact else 2):
            at = (piece * values + value) * FROWS
            left_ref[at : at + FROWS, :] = pieces[piece * FROWS : (piece + 1) * FROWS]


def fetch(left_ref, values, exact, idx_ref, put_ref, base, start):
    index = idx_ref[pl.ds(base, 8), :]
    hi = lax.shift_right_logical(index, 7) - start
    lo = lax.bitwise_and(index, 127)
    sub = lax.broadcasted_iota(jnp.int32, (TILE, TILE), 0)
    hits = []
    for part in range(8):
        line = jnp.broadcast_to(lo[part : part + 1, :], (TILE, TILE))
        hits.append(jnp.where(line == sub, 1.0, 0.0).astype(bf16))
    one = jnp.concatenate(hits, axis=1)
    height = values * FROWS
    pieces = 3 if exact else 2
    wide = jnp.dot(left_ref[0 : pieces * height, :], one, preferred_element_type=f32)
    got = wide[0:height] + wide[height : 2 * height]
    if exact:
        got = got + wide[2 * height :]
    line8 = lax.broadcasted_iota(jnp.int32, (8, TILE), 0)
    found = [jnp.zeros((8, TILE), f32) for _ in range(values)]
    for part in range(8):
        place = jnp.broadcast_to(hi[part : part + 1, :], (8, TILE))
        masks = [place == line8 + 8 * r for r in range(FROWS // 8)]
        for value in range(values):
            total = None
            for r, mask in enumerate(masks):
                at = value * FROWS + 8 * r
                term = jnp.where(mask, got[at : at + 8, part * TILE : (part + 1) * TILE], 0.0)
                total = term if total is None else total + term
            row = jnp.sum(total, axis=0, keepdims=True)
            found[value] = jnp.where(line8 == part, jnp.broadcast_to(row, (8, TILE)), found[value])
    inside = (hi >= 0) & (hi < FROWS)
    for value in range(values):
        rows = slot_rows(value, base)
        put_ref[rows, :] = jnp.where(inside, found[value], put_ref[rows, :])


def slot_rows(which, base):
    return pl.ds(pl.multiple_of(which * NPAD + base, 8), 8)


def geometry(layer, geo_ref, feat_ref, wt_ref, base):
    weight = wt_ref[pl.ds(base, 8), :]
    unit = [geo_ref[slot_rows(axis, base), :] for axis in range(3)]
    dist = geo_ref[slot_rows(4, base), :]
    if layer == 1:
        kind = geo_ref[slot_rows(3, base), :]
        chan = [jnp.where(kind == float(c), 1.0, 0.0) for c in range(SPECIES)]
    else:
        chan = [feat_ref[slot_rows(c, base), :] for c in range(SPECIES)]
    return weight, dist, unit, chan


def radial_terms(dist, rad_ref, with_slope):
    scaled = dist * (2.0 / cutoff_radius) - 1.0
    inside = dist < cutoff_radius
    angle = dist * (math.pi / cutoff_radius)
    cutoff = jnp.where(inside, 0.5 * (jnp.cos(angle) + 1.0), 0.0)
    cheb = [None, scaled]
    twice = 2.0 * scaled
    cheb.append(twice * scaled - 1.0)
    for _ in range(3, NRAD):
        cheb.append(twice * cheb[-1] - cheb[-2])
    basis = [cutoff] + [cutoff * cheb[p] for p in range(1, NRAD)]
    radial = []
    for n in range(NMAX):
        total = basis[0] * rad_ref[n, 0]
        for p in range(1, NRAD):
            total = total + basis[p] * rad_ref[n, p]
        radial.append(total)
    if not with_slope:
        return basis, radial, None
    slope_cut = jnp.where(inside, (-0.5 * math.pi / cutoff_radius) * jnp.sin(angle), 0.0)
    grad_scaled = cutoff * (2.0 / cutoff_radius)
    second = [None, None, twice]
    second[1] = jnp.ones_like(scaled)
    for _ in range(3, NRAD):
        second.append(twice * second[-1] - second[-2])
    slopes = [slope_cut, slope_cut * scaled + grad_scaled]
    for p in range(2, NRAD):
        slopes.append(slope_cut * cheb[p] + grad_scaled * (float(p) * second[p]))
    return basis, radial, slopes


def harmonic_list(unit):
    table = scaled_legendre(unit[2])
    cosines, sines = azimuth_powers(unit[0], unit[1])
    columns = []
    for degree in range(LMAX + 1):
        for signed in range(-degree, degree + 1):
            azimuth = abs(signed)
            poly = table[degree, azimuth]
            if signed == 0:
                columns.append(poly)
            elif signed > 0:
                columns.append(poly * cosines[azimuth])
            else:
                columns.append(poly * sines[azimuth])
    columns[0] = jnp.full_like(unit[2], columns[0])
    return columns


def density_kernel(layer, info_ref, rad_ref, tab_ref, cen_ref, idx_ref, wt_ref, *refs):
    if layer == 1:
        out_ref, geo_ref, x_ref, y_ref, d_ref, left_ref = refs
        feat_ref, put_ref = None, geo_ref
    else:
        geo_ref, out_ref, feat_ref, x_ref, y_ref, d_ref, left_ref = refs
        put_ref = feat_ref
    tile = pl.program_id(0)
    count = info_ref[0, tile]
    row_low, row_high = info_ref[1, tile], info_ref[2, tile]
    blocks = lax.div(count + 7, 8)

    start, windows = window_starts(row_low, row_high)

    def gather_window(window_at, carry):
        first_row = jnp.minimum(start + window_at * FROWS, 24 - FROWS)

        @pl.when((tile == 0) | (windows > 1))
        def _():
            load_window(tab_ref, left_ref, SPECIES, layer == 1, first_row)

        def gather_block(block_at, inner):
            base = pl.multiple_of(block_at * 8, 8)
            fetch(left_ref, SPECIES, layer == 1, idx_ref, put_ref, base, first_row)
            return inner

        return lax.fori_loop(0, blocks, gather_block, carry)

    lax.fori_loop(0, windows, gather_window, 0)

    def edges(block_at, carry):
        base = pl.multiple_of(block_at * 8, 8)
        if layer == 1:
            live = wt_ref[pl.ds(base, 8), :] > 0.0
            deltas = []
            for axis in range(3):
                centre = jnp.broadcast_to(cen_ref[pl.ds(axis, 1), :], (8, TILE))
                delta = geo_ref[slot_rows(axis, base), :] - centre
                deltas.append(jnp.where(live, delta, 1.0))
            dist = jnp.sqrt(deltas[0] * deltas[0] + deltas[1] * deltas[1] + deltas[2] * deltas[2])
            inv = 1.0 / dist
            for axis in range(3):
                geo_ref[slot_rows(axis, base), :] = deltas[axis] * inv
            geo_ref[slot_rows(4, base), :] = dist
        weight, dist, unit, chan = geometry(layer, geo_ref, feat_ref, wt_ref, base)
        _, radial, _ = radial_terms(dist, rad_ref, False)
        for c in range(SPECIES):
            scale = chan[c] * weight
            for n in range(NMAX):
                x_ref[pl.ds(base * XROW + (c * NMAX + n), 8, stride=XROW), :] = scale * radial[n]
        for at, column in enumerate(harmonic_list(unit)):
            y_ref[slot_rows(at, base), :] = column
        return carry

    lax.fori_loop(0, blocks, edges, 0)
    groups = lax.div(count, SLOTS)

    def lm_block(block_at, carry):
        first = block_at * LBLK

        def slots(group, acc):
            acc = list(acc)
            for part in range(SLOTS):
                slot = group * SLOTS + part
                rows = [x_ref[pl.ds(slot * XROW + 8 * j, 8), :] for j in range(CH // 8)]
                for at in range(LBLK):
                    line = jnp.broadcast_to(
                        y_ref[pl.ds((first + at) * NPAD + slot, 1), :], (8, TILE)
                    )
                    for j in range(CH // 8):
                        acc[at * (CH // 8) + j] = acc[at * (CH // 8) + j] + rows[j] * line
            return tuple(acc)

        zero = jnp.zeros((8, TILE), f32)
        acc = lax.fori_loop(0, groups, slots, tuple(zero for _ in range(LBLK * (CH // 8))))
        for at in range(LBLK):
            for j in range(CH // 8):
                d_ref[pl.ds(8 * j * LM + first + at, 8, stride=LM), :] = acc[at * (CH // 8) + j]
        return carry

    lax.fori_loop(0, LM // LBLK, lm_block, 0)
    out_ref[...] = d_ref[...].astype(bf16)


def smem_spec():
    return pl.BlockSpec(memory_space=pltpu.SMEM)


def tile_spec(rows):
    return pl.BlockSpec((rows, TILE), lambda i: (0, i))


def whole_spec(shape):
    return pl.BlockSpec(shape, lambda i: tuple(0 for _ in shape))


def density_call(layer, info, radial, table, centres, index, weight, geo=None):
    atoms = centres.shape[1]
    rows = GEO if layer == 1 else SPECIES
    extra = () if geo is None else (geo,)
    return pl.pallas_call(
        partial(density_kernel, layer),
        out_shape=(
            jax.ShapeDtypeStruct((DENS, atoms), bf16),
            jax.ShapeDtypeStruct((rows * NPAD, atoms), f32),
        ),
        grid=(atoms // TILE,),
        in_specs=[
            smem_spec(),
            smem_spec(),
            whole_spec(table.shape),
            tile_spec(8),
            tile_spec(NPAD),
            tile_spec(NPAD),
        ]
        + [tile_spec(GEO * NPAD)] * len(extra),
        out_specs=(tile_spec(DENS), tile_spec(rows * NPAD)),
        scratch_shapes=[
            pltpu.VMEM((NPAD * XROW + 8, TILE), f32),
            pltpu.VMEM((LM * NPAD, TILE), f32),
            pltpu.VMEM((DENS, TILE), f32),
            pltpu.VMEM((3 * SPECIES * FROWS, TILE), bf16),
        ],
        compiler_params=pltpu.CompilerParams(vmem_limit_bytes=VMEM_ALL),
        name="density_%d" % layer,
    )(info, radial, table, centres, index, weight, *extra)


def backward_kernel(layer, info_ref, rad_ref, geo_ref, feat_ref, idx_ref, wt_ref, dd_ref, win_in_ref,
                    own_in_ref, win_ref, own_ref, rad_out_ref, rgr_ref, x_ref, y_ref, gx_ref, gy_ref, val_ref,
                    left_ref):
    tile = pl.program_id(0)
    count = info_ref[0, tile]
    row_low, row_high = info_ref[1, tile], info_ref[2, tile]
    blocks = lax.div(count + 7, 8)
    zero = jnp.zeros((8, TILE), f32)

    @pl.when(tile == 0)
    def _():
        if layer == 1:
            win_ref[...] = win_in_ref[: 3 * WSTEP]
        else:
            win_ref[...] = jnp.zeros_like(win_ref)
        rgr_ref[...] = jnp.zeros_like(rgr_ref)

    def line_of(at):
        return jnp.broadcast_to(dd_ref[pl.ds(at, 1), :], (8, TILE))

    def contract_slots():
        def over_lm(step, acc):
            acc = list(acc)
            for part in range(LBLK):
                lm = step * LBLK + part
                col = y_ref[pl.ds(pl.multiple_of(lm * 8, 8), 8), :]
                for m in range(CH):
                    acc[m] = acc[m] + line_of(m * LM + lm) * col
            return tuple(acc)

        acc = lax.fori_loop(0, LM // LBLK, over_lm, tuple(zero for _ in range(CH)))
        for m in range(CH):
            gx_ref[8 * m : 8 * m + 8, :] = acc[m]

        def over_m(step, acc):
            acc = list(acc)
            for part in range(4):
                m = step * 4 + part
                col = x_ref[pl.ds(pl.multiple_of(m * 8, 8), 8), :]
                for lm in range(LM):
                    acc[lm] = acc[lm] + line_of(m * LM + lm) * col
            return tuple(acc)

        acc = lax.fori_loop(0, CH // 4, over_m, tuple(zero for _ in range(LM)))
        for lm in range(LM):
            gy_ref[8 * lm : 8 * lm + 8, :] = acc[lm]

    def contract_species(kind):
        odd = (kind == 1.0) | (kind == 3.0)
        upper = kind > 1.5

        def over_n(step, acc):
            acc = list(acc)
            for part in range(2):
                n = step * 2 + part
                at = pl.multiple_of(n * 8, 8)
                scaled = x_ref[pl.ds(at, 8), :]
                sums = [None, None]
                for lm in range(LM):
                    lines = [line_of((c * NMAX + n) * LM + lm) for c in range(SPECIES)]
                    first = jnp.where(odd, lines[1], lines[0])
                    second = jnp.where(odd, lines[3], lines[2])
                    grad = jnp.where(upper, second, first)
                    acc[lm] = acc[lm] + grad * scaled
                    term = grad * y_ref[8 * lm : 8 * lm + 8, :]
                    sums[lm % 2] = term if lm < 2 else sums[lm % 2] + term
                gx_ref[pl.ds(at, 8), :] = sums[0] + sums[1]
            return tuple(acc)

        acc = lax.fori_loop(0, NMAX // 2, over_n, tuple(zero for _ in range(LM)))
        for lm in range(LM):
            gy_ref[8 * lm : 8 * lm + 8, :] = acc[lm]

    def slot_block(block_at, own):
        base = pl.multiple_of(block_at * 8, 8)
        weight, dist, unit, chan = geometry(layer, geo_ref, feat_ref, wt_ref, base)
        _, radial, _ = radial_terms(dist, rad_ref, False)
        for at, column in enumerate(harmonic_list(unit)):
            y_ref[8 * at : 8 * at + 8, :] = column
        if layer == 1:
            for n in range(NMAX):
                x_ref[8 * n : 8 * n + 8, :] = weight * radial[n]
            contract_species(geo_ref[slot_rows(3, base), :])
        else:
            for c in range(SPECIES):
                scale = chan[c] * weight
                for n in range(NMAX):
                    at = 8 * (c * NMAX + n)
                    x_ref[at : at + 8, :] = scale * radial[n]
            contract_slots()
        weight, dist, unit, chan = geometry(layer, geo_ref, feat_ref, wt_ref, base)
        inv = 1.0 / dist
        basis, radial, slopes = radial_terms(dist, rad_ref, True)
        feat_grads = []
        radial_grads = [None] * NMAX
        if layer == 1:
            radial_grads = [gx_ref[8 * n : 8 * n + 8, :] for n in range(NMAX)]
        for c in range(SPECIES if layer == 2 else 0):
            total = None
            for n in range(NMAX):
                grad = gx_ref[8 * (c * NMAX + n) : 8 * (c * NMAX + n) + 8, :]
                term = grad * radial[n]
                total = term if total is None else total + term
                piece = grad * chan[c]
                radial_grads[n] = piece if c == 0 else radial_grads[n] + piece
            feat_grads.append(total * weight)
        grad_r = None
        radial_grads = [grad * weight for grad in radial_grads]
        for p in range(NRAD):
            total = None
            for n in range(NMAX):
                at = (n * NRAD + p) * 8
                rgr_ref[pl.ds(at, 8), :] = rgr_ref[pl.ds(at, 8), :] + radial_grads[n] * basis[p]
                term = radial_grads[n] * rad_ref[n, p]
                total = term if total is None else total + term
            term = total * slopes[p]
            grad_r = term if grad_r is None else grad_r + term
        table = scaled_legendre(unit[2])
        cosines, sines = azimuth_powers(unit[0], unit[1])
        grad_x = grad_y = grad_z = None

        def plus(total, term):
            return term if total is None else total + term

        for azimuth in range(LMAX + 1):
            grad_cos = grad_sin = None
            for degree in range(azimuth, LMAX + 1):
                at = degree * degree + degree
                up = gy_ref[8 * (at + azimuth) : 8 * (at + azimuth) + 8, :]
                poly = table[degree, azimuth]
                if azimuth:
                    down = gy_ref[8 * (at - azimuth) : 8 * (at - azimuth) + 8, :]
                    grad_cos = plus(grad_cos, up * poly)
                    grad_sin = plus(grad_sin, down * poly)
                if degree > azimuth:
                    ratio = norm_of(degree, azimuth) / norm_of(degree, azimuth + 1)
                    slope = ratio * table[degree, azimuth + 1]
                    if azimuth:
                        grad_z = plus(grad_z, slope * (up * cosines[azimuth] + down * sines[azimuth]))
                    else:
                        grad_z = plus(grad_z, slope * up)
            if azimuth == 1:
                grad_x, grad_y = grad_cos, grad_sin
            elif azimuth > 1:
                below_cos, below_sin = cosines[azimuth - 1], sines[azimuth - 1]
                grad_x = grad_x + float(azimuth) * (grad_cos * below_cos + grad_sin * below_sin)
                grad_y = grad_y + float(azimuth) * (grad_sin * below_cos - grad_cos * below_sin)
        dot_u = grad_x * unit[0] + grad_y * unit[1] + grad_z * unit[2]
        live = weight > 0.0
        out = []
        for axis, grad in enumerate((grad_x, grad_y, grad_z)):
            value = (grad - dot_u * unit[axis]) * inv + grad_r * unit[axis]
            out.append(jnp.where(live, value, 0.0))
        values = out + feat_grads
        for at, value in enumerate(values):
            val_ref[slot_rows(at, base), :] = value
        return tuple(total + value for total, value in zip(own, out))


    own = lax.fori_loop(0, blocks, slot_block, (zero, zero, zero))
    own = jnp.concatenate(
        [jnp.sum(total, axis=0, keepdims=True) for total in own] + [jnp.zeros((5, TILE), f32)], axis=0
    )
    own_ref[...] = own + own_in_ref[...] if layer == 1 else own

    used = 3 if layer == 1 else NVAL
    height = used * WROWS
    step_rows = height + 1
    sub = lax.broadcasted_iota(jnp.int32, (TILE, TILE), 0)
    windows = lax.div(row_high - row_low + WROWS, WROWS)

    def window(window_at, carry):
        row_base = row_low + window_at * WROWS

        def scatter(block_at, acc):
            base = pl.multiple_of(block_at * 8, 8)
            index = idx_ref[pl.ds(base, 8), :]
            hi = lax.shift_right_logical(index, 7)
            lo = lax.bitwise_and(index, 127)
            for row in range(WROWS):
                hit = hi == row_base + row
                for value_at in range(used):
                    value = val_ref[slot_rows(value_at, base), :]
                    left_ref[pl.ds(value_at * WROWS + row, 8, stride=step_rows), :] = jnp.where(
                        hit, value, 0.0
                    )
            ones, left = [], []
            for part in range(8):
                line = jnp.broadcast_to(lo[part : part + 1, :], (TILE, TILE))
                ones.append(jnp.where(line == sub, 1.0, 0.0).astype(bf16))
                left.append(left_ref[part * step_rows : part * step_rows + height, :])
            left = jnp.concatenate(left, axis=1)
            ones = jnp.concatenate(ones, axis=1)
            high = left.astype(bf16)
            rest = (left - high.astype(f32)).astype(bf16)
            dims = (((1,), (1,)), ((), ()))
            acc = acc + lax.dot_general(high, ones, dims, preferred_element_type=f32)
            return acc + lax.dot_general(rest, ones, dims, preferred_element_type=f32)

        acc = lax.fori_loop(0, blocks, scatter, jnp.zeros((height, TILE), f32))
        for value_at in range(used):
            at = value_at * WSTEP + row_base
            win_ref[pl.ds(at, WROWS), :] = (
                win_ref[pl.ds(at, WROWS), :] + acc[value_at * WROWS : (value_at + 1) * WROWS]
            )
        return carry

    lax.fori_loop(0, windows, window, 0)

    @pl.when(tile == pl.num_programs(0) - 1)
    def _():
        for at in range(NMAX * NRAD):
            rad_out_ref[at : at + 1, :] = jnp.sum(rgr_ref[8 * at : 8 * at + 8, :], axis=0, keepdims=True)


def backward_call(layer, info, radial, geo, feat, index, weight, grad_dens, window_in, own_in):
    atoms = index.shape[1]
    values = 3 if layer == 1 else NVAL
    return pl.pallas_call(
        partial(backward_kernel, layer),
        out_shape=(
            jax.ShapeDtypeStruct((values * WSTEP, TILE), f32),
            jax.ShapeDtypeStruct((8, atoms), f32),
            jax.ShapeDtypeStruct((NMAX * NRAD, TILE), f32),
        ),
        grid=(atoms // TILE,),
        in_specs=[
            smem_spec(),
            smem_spec(),
            tile_spec(GEO * NPAD),
            tile_spec(feat.shape[0]),
            tile_spec(NPAD),
            tile_spec(NPAD),
            tile_spec(DENS),
            whole_spec(window_in.shape),
            tile_spec(8),
        ],
        out_specs=(
            whole_spec((values * WSTEP, TILE)),
            tile_spec(8),
            whole_spec((NMAX * NRAD, TILE)),
        ),
        scratch_shapes=[
            pltpu.VMEM((NMAX * NRAD * 8, TILE), f32),
            pltpu.VMEM((CH * 8, TILE), f32),
            pltpu.VMEM((LM * 8, TILE), f32),
            pltpu.VMEM((CH * 8, TILE), f32),
            pltpu.VMEM((LM * 8, TILE), f32),
            pltpu.VMEM((NVAL * NPAD, TILE), f32),
            pltpu.VMEM((8 * (NVAL * WROWS + 1), TILE), f32),
        ],
        compiler_params=pltpu.CompilerParams(vmem_limit_bytes=VMEM_ALL),
        name="backward_%d" % layer,
    )(info, radial, geo, feat, index, weight, grad_dens, window_in, own_in)


def tn_dot(left, right):
    return lax.dot_general(left, right, (((0,), (0,)), ((), ())), preferred_element_type=f32)


def nt_dot(left, right):
    return lax.dot_general(left, right, (((1,), (1,)), ((), ())), preferred_element_type=f32)


def padded_rows(value):
    return jnp.concatenate([value, jnp.zeros((8 - value.shape[0], value.shape[1]), f32)], axis=0)


def onehot_rows(species):
    kind = lax.broadcasted_iota(jnp.int32, (8, species.shape[1]), 0).astype(f32)
    return jnp.where(kind == species, 1.0, 0.0).astype(bf16)


def combine(parts):
    total = parts[2][0:8]
    total = total + (parts[1][8:16] + parts[0][16:24])
    total = total + (parts[1][0:8] + parts[0][8:16])
    return total + parts[0][0:8]


def by_atoms(rows24, chunk):
    wide = nt_dot(rows24, split3(chunk))
    return [wide[:, j * QB : (j + 1) * QB] for j in range(3)]


def contract_one_kernel(dens_ref, coup_ref, coef_ref, mix_ref, site_ref, factor_ref, energy_ref, feat_ref,
                        aux_ref, grad_ref, b_ref, ch_ref, row_ref):
    factor_at = pl.program_id(0)
    quantum, atoms = b_ref.shape
    half = quantum // 2
    for part in range(2):
        rows = slice(part * half, (part + 1) * half)
        value = tn_dot(coup_ref[0, :, rows], dens_ref[...])
        factor_ref[0, rows, :] = value

        @pl.when(factor_at == 0)
        def _(value=value, rows=rows):
            b_ref[rows, :] = value

        @pl.when(factor_at > 0)
        def _(value=value, rows=rows):
            b_ref[rows, :] = b_ref[rows, :] * value

    @pl.when(factor_at == pl.num_programs(0) - 1)
    def _():
        onehot = onehot_rows(site_ref[3:4, :])
        row_ref[0:24, :] = split3(padded_rows(coef_ref[...]))
        row_ref[24:48, :] = split3(padded_rows(mix_ref[...]))
        triple = jnp.concatenate([onehot] * 3, axis=0)

        def chunk_body(chunk, mixed):
            cols = pl.ds(pl.multiple_of(chunk * QB, QB), QB)
            ch_ref[...] = tn_dot(row_ref[0:24, cols], triple)
            pieces = split3(b_ref[cols, :])
            left = row_ref[24:48, cols]
            parts = [
                jnp.dot(left, pieces[j * QB : (j + 1) * QB], preferred_element_type=f32) for j in range(3)
            ]
            wide = nt_dot(onehot, pieces)
            grad_ref[:, cols] = wide[:, 2 * QB :] + wide[:, QB : 2 * QB] + wide[:, :QB]

            def rows_body(step, sums):
                at = pl.multiple_of(step * 8, 8)
                value = b_ref[pl.ds(pl.multiple_of(chunk * QB + step * 8, 8), 8), :]
                return sums[0] + value * ch_ref[pl.ds(at, 8), :], sums[1] + value * value

            energy, square = lax.fori_loop(0, QB // 8, rows_body, mixed[1:])
            return mixed[0] + combine(parts), energy, square

        zero = jnp.zeros((8, atoms), f32)
        mixed, energy, square = lax.fori_loop(0, quantum // QB, chunk_body, (zero, zero, zero))
        energy_ref[...] = jnp.broadcast_to(jnp.sum(energy, axis=0, keepdims=True), (8, atoms))
        mean = jnp.sum(square, axis=0, keepdims=True) * (1.0 / quantum)
        scale = lax.rsqrt(mean + norm_eps)
        feat_ref[...] = mixed * scale
        aux_ref[0:8, :] = mixed
        aux_ref[8:16, :] = jnp.broadcast_to(scale, (8, atoms))


def contract_one_call(dens, coupling, coefficient, mixing_rows, ordered):
    factors, depth, quantum = coupling.shape
    atoms = dens.shape[1]
    return pl.pallas_call(
        contract_one_kernel,
        out_shape=(
            jax.ShapeDtypeStruct((factors, quantum, atoms), f32),
            jax.ShapeDtypeStruct((8, atoms), f32),
            jax.ShapeDtypeStruct((8, atoms), f32),
            jax.ShapeDtypeStruct((16, atoms), f32),
            jax.ShapeDtypeStruct((8, quantum), f32),
        ),
        grid=(factors,),
        in_specs=[
            whole_spec((depth, atoms)),
            pl.BlockSpec((1, depth, quantum), lambda v: (v, 0, 0)),
            whole_spec(coefficient.shape),
            whole_spec(mixing_rows.shape),
            whole_spec(ordered.shape),
        ],
        out_specs=(
            pl.BlockSpec((1, quantum, atoms), lambda v: (v, 0, 0)),
            whole_spec((8, atoms)),
            whole_spec((8, atoms)),
            whole_spec((16, atoms)),
            whole_spec((8, quantum)),
        ),
        scratch_shapes=[
            pltpu.VMEM((quantum, atoms), f32),
            pltpu.VMEM((QB, atoms), f32),
            pltpu.VMEM((48, quantum), bf16),
        ],
        compiler_params=pltpu.CompilerParams(vmem_limit_bytes=VMEM_ALL),
        name="contract_1",
    )(dens, coupling, coefficient, mixing_rows, ordered)


def factor_grads(values, upstream):
    low_pair, high_pair = values[0] * values[1], values[2] * values[3]
    first, second = upstream * high_pair, upstream * low_pair
    return first * values[1], first * values[0], second * values[3], second * values[2]


def contract_two_kernel(dens_ref, coef_ref, site_ref, before_ref, coup_ref, out_ref, part_ref, grad_ref,
                        cv_ref, f_ref, g_ref, ch_ref, row_ref, sem):
    step = pl.program_id(0)
    factors, quantum, atoms = f_ref.shape
    depth = dens_ref.shape[0]
    half = quantum // 2

    def load(at):
        return pltpu.make_async_copy(coup_ref.at[at], cv_ref.at[at, 0:depth], sem.at[at])

    @pl.when(step == 0)
    def _():
        for at in range(factors):
            load(at).start()
        onehot = onehot_rows(site_ref[3:4, :])
        row_ref[...] = split3(padded_rows(coef_ref[...]))
        triple = jnp.concatenate([onehot] * 3, axis=0)

        def factor_body(at, carry):
            load(at).wait()
            for part in range(2):
                rows = slice(part * half, (part + 1) * half)
                f_ref[at, rows, :] = tn_dot(cv_ref[at, 0:depth, rows], dens_ref[...])
            return carry

        lax.fori_loop(0, factors, factor_body, 0)

        def chunk_body(chunk, energy):
            cols = pl.ds(pl.multiple_of(chunk * QB, QB), QB)
            ch_ref[...] = tn_dot(row_ref[:, cols], triple)

            def rows_body(small, total):
                at = pl.multiple_of(small * 16, 16)
                rows = pl.ds(pl.multiple_of(chunk * QB + small * 16, 16), 16)
                values = [f_ref[v, rows, :] for v in range(factors)]
                upstream = ch_ref[pl.ds(at, 16), :]
                grads = factor_grads(values, upstream)
                for v in range(factors):
                    g_ref[v, rows, :] = grads[v].astype(bf16)
                product = values[0] * values[1] * values[2] * values[3]
                f_ref[0, rows, :] = product
                term = product * upstream
                return total + term[:8] + term[8:]

            energy = lax.fori_loop(0, QB // 16, rows_body, energy)
            wide = nt_dot(onehot, split3(f_ref[0, cols, :]))
            grad_ref[:, cols] = wide[:, 2 * QB :] + wide[:, QB : 2 * QB] + wide[:, :QB]
            return energy

        energy = lax.fori_loop(0, quantum // QB, chunk_body, jnp.zeros((8, atoms), f32))
        energy = jnp.sum(energy, axis=0, keepdims=True) + before_ref[0:1, :]
        kinds = [jnp.where(site_ref[3:4, :] == float(c), 1.0, 0.0) for c in range(SPECIES)]
        rows8 = split3(jnp.concatenate([energy] + kinds + [jnp.zeros((3, atoms), f32)], axis=0))
        owner = site_ref[4:5, :]

        def structure_body(chunk, carry):
            cols = pl.ds(pl.multiple_of(chunk * TILE, TILE), TILE)
            ids = lax.broadcasted_iota(jnp.int32, (TILE, atoms), 0) + chunk * TILE
            members = jnp.where(ids.astype(f32) == owner, 1.0, 0.0).astype(bf16)
            wide = nt_dot(rows8, members)
            part_ref[:, cols] = wide[16:24] + wide[8:16] + wide[0:8]
            return carry

        lax.fori_loop(0, part_ref.shape[1] // TILE, structure_body, 0)

    rows = pl.ds(pl.multiple_of(step * DROWS, 16), DROWS)
    total = None
    for at in range(factors):
        part = jnp.dot(cv_ref[at, rows, :], g_ref[at], preferred_element_type=f32)
        total = part if total is None else total + part
    out_ref[...] = total


def contract_two_call(dens, coupling, coefficient, ordered, energy_one, structures):
    factors, depth, quantum = coupling.shape
    atoms = dens.shape[1]
    steps = pl.cdiv(depth, DROWS)
    return pl.pallas_call(
        contract_two_kernel,
        out_shape=(
            jax.ShapeDtypeStruct((steps * DROWS, atoms), f32),
            jax.ShapeDtypeStruct((8, structures), f32),
            jax.ShapeDtypeStruct((8, quantum), f32),
        ),
        grid=(steps,),
        in_specs=[
            pl.BlockSpec((depth, atoms), lambda i: (0, 0), pipeline_mode=pl.Buffered(1)),
            whole_spec(coefficient.shape),
            whole_spec(ordered.shape),
            whole_spec(energy_one.shape),
            pl.BlockSpec(memory_space=pl.ANY),
        ],
        out_specs=(
            pl.BlockSpec((DROWS, atoms), lambda i: (i, 0)),
            whole_spec((8, structures)),
            whole_spec((8, quantum)),
        ),
        scratch_shapes=[
            pltpu.VMEM((factors, steps * DROWS, quantum), bf16),
            pltpu.VMEM((factors, quantum, atoms), f32),
            pltpu.VMEM((factors, quantum, atoms), bf16),
            pltpu.VMEM((QB, atoms), f32),
            pltpu.VMEM((24, quantum), bf16),
            pltpu.SemaphoreType.DMA((factors,)),
        ],
        compiler_params=pltpu.CompilerParams(vmem_limit_bytes=VMEM_ALL),
        name="contract_2",
    )(dens, coefficient, ordered, energy_one, coupling)


def contract_back_kernel(coup_ref, coef_ref, mix_ref, site_ref, gfeat_ref, aux_ref, factor_ref, out_ref,
                         grad_ref, f_ref, g_ref, ch_ref, row_ref, sem):
    step = pl.program_id(0)
    factors, quantum, atoms = f_ref.shape
    chunks = quantum // QB

    def load(chunk):
        rows = pl.ds(pl.multiple_of(chunk * QB, QB), QB)
        return pltpu.make_async_copy(factor_ref.at[:, rows, :], f_ref.at[:, rows, :], sem.at[chunk])

    @pl.when(step == 0)
    def _():
        for chunk in range(chunks):
            load(chunk).start()
        onehot = onehot_rows(site_ref[3:4, :])
        scale = aux_ref[8:9, :]
        gfeat = gfeat_ref[...]
        dot = jnp.sum(aux_ref[0:8, :] * gfeat, axis=0, keepdims=True)
        shrink = jnp.broadcast_to(scale * scale * scale * dot * (1.0 / quantum), (8, atoms))
        scaled = split3(scale * gfeat)
        high, middle, low = scaled[0:8], scaled[8:16], scaled[16:24]
        mix = split3(padded_rows(mix_ref[...]))
        row_ref[0:24, :] = split3(padded_rows(coef_ref[...]))
        for at, piece in enumerate((0, 0, 0, 1, 1, 2)):
            row_ref[24 + 8 * at : 32 + 8 * at, :] = mix[8 * piece : 8 * piece + 8]
        right = jnp.concatenate([onehot] * 3 + [high, middle, low, high, middle, high], axis=0)

        def chunk_body(chunk, carry):
            load(chunk).wait()
            cols = pl.ds(pl.multiple_of(chunk * QB, QB), QB)
            ch_ref[...] = tn_dot(row_ref[:, cols], right)

            def rows_body(small, inner):
                at = pl.multiple_of(small * 16, 16)
                rows = pl.ds(pl.multiple_of(chunk * QB + small * 16, 16), 16)
                values = [f_ref[v, rows, :] for v in range(factors)]
                product = values[0] * values[1] * values[2] * values[3]
                both = jnp.concatenate([shrink, shrink], axis=0)
                upstream = ch_ref[pl.ds(at, 16), :] - both * product
                grads = factor_grads(values, upstream)
                for v in range(factors):
                    g_ref[v, rows, :] = grads[v].astype(bf16)
                f_ref[0, rows, :] = product
                return inner

            lax.fori_loop(0, QB // 16, rows_body, 0)
            grad_ref[:, cols] = combine(by_atoms(scaled, f_ref[0, cols, :]))
            return carry

        lax.fori_loop(0, chunks, chunk_body, 0)

    total = None
    for at in range(factors):
        part = jnp.dot(coup_ref[at], g_ref[at], preferred_element_type=f32)
        total = part if total is None else total + part
    out_ref[...] = total


def contract_back_call(coupling, coefficient, mixing_rows, ordered, gfeat, aux, factor):
    factors, depth, quantum = coupling.shape
    atoms = ordered.shape[1]
    rows = depth // 5
    return pl.pallas_call(
        contract_back_kernel,
        out_shape=(
            jax.ShapeDtypeStruct((depth, atoms), f32),
            jax.ShapeDtypeStruct((8, quantum), f32),
        ),
        grid=(5,),
        in_specs=[
            pl.BlockSpec((factors, rows, quantum), lambda i: (0, i, 0)),
            whole_spec(coefficient.shape),
            whole_spec(mixing_rows.shape),
            whole_spec(ordered.shape),
            whole_spec(gfeat.shape),
            whole_spec(aux.shape),
            pl.BlockSpec(memory_space=pl.ANY),
        ],
        out_specs=(pl.BlockSpec((rows, atoms), lambda i: (i, 0)), whole_spec((8, quantum))),
        scratch_shapes=[
            pltpu.VMEM((factors, quantum, atoms), f32),
            pltpu.VMEM((factors, quantum, atoms), bf16),
            pltpu.VMEM((QB, atoms), f32),
            pltpu.VMEM((72, quantum), bf16),
            pltpu.SemaphoreType.DMA((quantum // QB,)),
        ],
        compiler_params=pltpu.CompilerParams(vmem_limit_bytes=VMEM_ALL),
        name="contract_back_1",
    )(coupling, coefficient, mixing_rows, ordered, gfeat, aux, factor)


def per_device(
    positions,
    species,
    neighbours,
    slot_counts,
    structure,
    target_energy,
    radial_one,
    coupling_one,
    coefficient_one,
    mixing,
    radial_two,
    coupling_two,
    coefficient_two,
):
    atoms = positions.shape[2]
    tiles = atoms // TILE
    structures = target_energy.shape[1]
    table_one = spread_call(0, 4, True, (positions, species, structure))
    first = ((lax.axis_index("dom") - 1) * atoms).astype(jnp.int32).reshape(1)
    index, weight, ordered, perm, info = prepare_call(
        first, slot_counts, neighbours, positions, species, structure
    )
    mixing_rows = mixing.T

    dens_one, geo = density_call(1, info, radial_one, table_one, ordered, index, weight)
    factors_one, energy_one, features, aux, coefficient_first = contract_one_call(
        dens_one, coupling_one, coefficient_one, mixing_rows, ordered
    )
    table_two = spread_call(1, SPECIES, False, (features, perm))
    dens_two, feat = density_call(2, info, radial_two, table_two, ordered, index, weight, geo)
    grad_dens_two, per_structure, coefficient_second = contract_two_call(
        dens_two, coupling_two, coefficient_two, ordered, energy_one, structures
    )
    window_two, own_two, radial_second = backward_call(
        2, info, radial_two, geo, feat, index, weight, grad_dens_two, table_two, ordered
    )
    grad_features = collect_call(2, tiles, 3, window_two.reshape(NVAL, WSTEP, TILE), perm)
    grad_dens_one, mixing_gradient = contract_back_call(
        coupling_one, coefficient_one, mixing_rows, ordered, grad_features, aux, factors_one
    )
    window_one, own_one, radial_first = backward_call(
        1, info, radial_one, geo, ordered, index, weight, grad_dens_one, window_two, own_two
    )
    groups = lax.axis_size("grp")
    steps = sum(len(group) for group in exchange_rounds())
    forces, sums, group_sums = finish_call(
        3,
        steps,
        groups,
        tiles,
        (
            window_one.reshape(3, WSTEP, TILE),
            own_one,
            perm,
            coefficient_first,
            coefficient_second,
            mixing_gradient,
            radial_first,
            radial_second,
            per_structure,
            target_energy,
        ),
    )
    mine = lax.axis_index("grp").astype(jnp.int32).reshape(1)
    outputs = list(tail_call(mine, forces, sums, group_sums))
    outputs[1] = outputs[1].reshape(SPECIES)
    outputs[5] = outputs[5].T
    return tuple(outputs)


def solution(mesh):
    in_specs = (
        P(None, "grp", "dom"),
        P("grp", "dom"),
        P(None, "grp", "dom"),
        P("grp", "dom"),
        P("grp", "dom"),
        P("grp", None),
        P(),
        P(),
        P(),
        P(),
        P(),
        P(),
        P(),
    )
    out_specs = (P("grp", None), P(), P(None, "grp", "dom"), P(), P(), P(), P(), P())
    return jax.shard_map(
        per_device, mesh=mesh, in_specs=in_specs, out_specs=out_specs, check_vma=False
    )
```

```python
from functools import partial
import math

import jax
import jax.numpy as jnp
from jax import lax
from jax.experimental import pallas as pl
from jax.experimental.pallas import tpu as pltpu
from jax.sharding import PartitionSpec as P

NRAD = 12
NMAX = 10
LMAX = 6
LM = 49
SPECIES = 4
CH = SPECIES * NMAX
DENS = CH * LM
NBR = 48
NPAD = 64
TILE = 128
LBLK = 7
WROWS = 12
WSTEP = 40
GEO = 5
QB = 128
FROWS = 16
VMEM_ALL = 67043328
DROWS = 400
NVAL = 7
SLOTS = 4
XROW = CH + 1

cutoff_radius = 5.0
density_scale = 0.17
norm_eps = 1e-05
ridge_weight = 0.1
highest = lax.Precision.HIGHEST
f32 = jnp.float32
MESH = pl.DeviceIdType.MESH
bf16 = jnp.bfloat16


def log2_of(count):
    steps = count.bit_length() - 1
    assert count == 1 << steps
    return steps


def neighbour_flags(me, count):
    return me > 0, me < count - 1


def greet(partners, flags):
    barrier = pltpu.get_barrier_semaphore()
    for partner, flag in zip(partners, flags):
        if flag is None:
            pl.semaphore_signal(barrier, inc=1, device_id=partner, device_id_type=MESH)
        else:

            @pl.when(flag)
            def _(partner=partner):
                pl.semaphore_signal(barrier, inc=1, device_id=partner, device_id_type=MESH)

    present = sum(1 for flag in flags if flag is None)
    for flag in flags:
        if flag is not None:
            present = present + jnp.where(flag, 1, 0)
    pl.semaphore_wait(barrier, present)


class SidePair:
    def __init__(self, to_left, to_right, got_ref, send_sem, recv_sem):
        count = lax.axis_size("dom")
        me = lax.axis_index("dom")
        self.partners = ({"dom": me - 1}, {"dom": me + 1})
        self.flags = neighbour_flags(me, count)
        self.got = got_ref
        self.copies = [
            pltpu.make_async_remote_copy(
                src_ref=source,
                dst_ref=got_ref.at[1 - side],
                send_sem=send_sem.at[side],
                recv_sem=recv_sem.at[1 - side],
                device_id=self.partners[side],
                device_id_type=MESH,
            )
            for side, source in enumerate((to_left, to_right))
        ]

    def start(self):
        for side in range(2):
            pl.when(self.flags[side])(self.copies[side].start)

    def wait(self):
        for side in range(2):

            @pl.when(self.flags[side])
            def _(side=side):
                self.copies[side].wait_send()
                self.copies[1 - side].wait_recv()

    def received(self, side):
        return jnp.where(self.flags[side], self.got[side], 0.0)


def split3(value):
    high = value.astype(bf16)
    rest = value - high.astype(f32)
    middle = rest.astype(bf16)
    low = (rest - middle.astype(f32)).astype(bf16)
    return jnp.concatenate([high, middle, low], axis=0)


def reorder(value, perm_ref, contract_at):
    count = value.shape[0]
    out = lax.dot_general(
        split3(value), perm_ref[...], (((1,), (contract_at,)), ((), ())), preferred_element_type=f32
    )
    return out[:count] + (out[count : 2 * count] + out[2 * count :])


def site_rows(pos_ref, kind_ref, part_ref):
    atoms = kind_ref.shape[1]
    rows = [pos_ref[axis] for axis in range(3)]
    rows = rows + [kind_ref[...].astype(f32), part_ref[...].astype(f32)]
    return jnp.concatenate(rows + [jnp.zeros((3, atoms), f32)], axis=0)


def begin_spread(values, flat, mine_ref, got_ref, send_sem, recv_sem):
    rows = flat.shape[1] // TILE
    for value in range(values):
        for row in range(rows):
            line = flat[value : value + 1, row * TILE : (row + 1) * TILE]
            at = value * rows + row
            mine_ref[at : at + 1, :] = line
    pair = SidePair(mine_ref, mine_ref, got_ref, send_sem, recv_sem)
    greet(pair.partners, pair.flags)
    pair.start()
    return pair


def end_spread(values, pair, out_ref, mine_ref):
    rows = mine_ref.shape[0] // values
    for value in range(values):
        at = value * 3 * rows
        out_ref[at + rows : at + 2 * rows, :] = mine_ref[value * rows : (value + 1) * rows, :]
    pair.wait()
    for side in range(2):
        block = pair.received(side)
        for value in range(values):
            at = value * 3 * rows + 2 * side * rows
            out_ref[at : at + rows, :] = block[value * rows : (value + 1) * rows]


def spread_kernel(values, x_ref, perm_ref, out_ref, mine_ref, got_ref, send_sem, recv_sem):
    flat = reorder(x_ref[...], perm_ref, 0)
    pair = begin_spread(values, flat, mine_ref, got_ref, send_sem, recv_sem)
    end_spread(values, pair, out_ref, mine_ref)


def comm_params(which):
    return pltpu.CompilerParams(collective_id=which, has_side_effects=True, vmem_limit_bytes=VMEM_ALL)


def vmem_spec():
    return pl.BlockSpec(memory_space=pltpu.VMEM)


def spread_call(which, values, operands):
    rows = values * operands[-1].shape[1] // TILE
    return pl.pallas_call(
        partial(spread_kernel, values),
        out_shape=jax.ShapeDtypeStruct((rows * 3, TILE), f32),
        in_specs=[vmem_spec()] * len(operands),
        out_specs=vmem_spec(),
        scratch_shapes=[
            pltpu.VMEM((rows, TILE), f32),
            pltpu.VMEM((2, rows, TILE), f32),
            pltpu.SemaphoreType.DMA((2,)),
            pltpu.SemaphoreType.DMA((2,)),
        ],
        compiler_params=comm_params(which),
        name="spread_%d" % which,
    )(*operands)


def in_lanes(blocks):
    values, rows = blocks.shape[0], blocks.shape[1]
    flat = [
        jnp.concatenate([blocks[v, r : r + 1, :] for r in range(rows)], axis=1) for v in range(values)
    ]
    return jnp.concatenate(flat + [jnp.zeros((8 - values, rows * TILE), f32)], axis=0)


def collect_kernel(rows, values_at, win_ref, perm_ref, out_ref, got_ref, send_sem, recv_sem):
    pair = SidePair(
        win_ref.at[values_at:, 0:rows],
        win_ref.at[values_at:, 2 * rows : 3 * rows],
        got_ref,
        send_sem,
        recv_sem,
    )
    greet(pair.partners, pair.flags)
    pair.start()
    pair.wait()
    total = win_ref[values_at:, rows : 2 * rows] + pair.received(0) + pair.received(1)
    out_ref[...] = reorder(in_lanes(total), perm_ref, 1)


def collect_call(which, rows, values_at, window, perm):
    values = window.shape[0] - values_at
    return pl.pallas_call(
        partial(collect_kernel, rows, values_at),
        out_shape=jax.ShapeDtypeStruct((8, rows * TILE), f32),
        in_specs=[vmem_spec()] * 2,
        out_specs=vmem_spec(),
        scratch_shapes=[
            pltpu.VMEM((2, values, rows, TILE), f32),
            pltpu.SemaphoreType.DMA((2,)),
            pltpu.SemaphoreType.DMA((2,)),
        ],
        compiler_params=comm_params(which),
        name="collect_%d" % which,
    )(window, perm)


def lane_sums(value):
    wide = nt_dot(jnp.ones((8, TILE), bf16), split3(value))
    rows = value.shape[0]
    total = wide[0:1, 2 * rows :] + wide[0:1, rows : 2 * rows] + wide[0:1, :rows]
    return jnp.concatenate([total, jnp.zeros((1, TILE - rows), f32)], axis=1)


def exchange_rounds():
    rounds = []
    for axis in ("dom", "grp"):
        me = lax.axis_index(axis)
        bits = log2_of(lax.axis_size(axis))

        def flip(places):
            other = me
            for bit in places:
                half = 1 << bit
                other = other + half - 2 * half * lax.rem(lax.div(me, half), 2)
            return {axis: other}

        for bit in range(0, bits, 2):
            if bit + 1 < bits:
                rounds.append([flip((bit,)), flip((bit + 1,)), flip((bit, bit + 1))])
            else:
                rounds.append([flip((bit,))])
    return rounds


def finish_kernel(rows, win_ref, own_ref, perm_ref, first_ref, second_ref, mix_ref, one_ref, two_ref, part_ref,
                  target_ref, force_ref, sum_ref, group_ref, got_ref, pay_ref, pay_group_ref, came_ref,
                  came_group_ref, send_sem, recv_sem, step_send, step_recv, group_send, group_recv):
    pair = SidePair(
        win_ref.at[:, 0:rows], win_ref.at[:, 2 * rows : 3 * rows], got_ref, send_sem, recv_sem
    )
    rounds = exchange_rounds()
    partners = [partner for group in rounds for partner in group]
    width = pay_ref.shape[1]
    for at, ref in enumerate((first_ref, second_ref, mix_ref)):
        pay_ref[4 * at : 4 * at + 4, :] = ref[0:4, :]
    tail = [lane_sums(one_ref[...]), lane_sums(two_ref[...]), jnp.zeros((1, width - 2 * TILE), f32)]
    pay_ref[12:13, :] = jnp.concatenate(tail, axis=1)
    pay_ref[13:16, :] = jnp.zeros((3, width), f32)
    lead = lax.axis_index("dom") == 0
    mine = lax.axis_index("grp")
    target = jnp.where(lead, target_ref[...], 0.0)
    block = part_ref[...]
    block = jnp.concatenate([block[0:5], target, block[6:8]], axis=0)
    for group in range(lax.axis_size("grp")):
        pay_group_ref[8 * group : 8 * group + 8, :] = jnp.where(mine == group, block, 0.0)
    greet(list(pair.partners) + partners, list(pair.flags) + [None] * len(partners))
    pair.start()
    at = 0
    for turn, group in enumerate(rounds):
        copies = []
        for partner in group:
            for source, total, came, send, recv in (
                (pay_ref, sum_ref, came_ref, step_send, step_recv),
                (pay_group_ref, group_ref, came_group_ref, group_send, group_recv),
            ):
                copy = pltpu.make_async_remote_copy(
                    src_ref=source if turn == 0 else total,
                    dst_ref=came.at[at],
                    send_sem=send.at[at],
                    recv_sem=recv.at[at],
                    device_id=partner,
                    device_id_type=MESH,
                )
                copy.start()
                copies.append(copy)
            at = at + 1
        if turn == 0:
            force_ref[...] = reorder(own_ref[...], perm_ref, 0)
        for copy in copies:
            copy.wait()
        for source, total, came in (
            (pay_ref, sum_ref, came_ref),
            (pay_group_ref, group_ref, came_group_ref),
        ):
            value = (source if turn == 0 else total)[...] + came[at - len(group)]
            if len(group) == 3:
                value = value + (came[at - 2] + came[at - 1])
            total[...] = value
    pair.wait()
    total = win_ref[:, rows : 2 * rows] + pair.received(0) + pair.received(1)
    force_ref[...] = force_ref[...] - in_lanes(total)


def finish_call(which, mesh_steps, groups, rows, operands):
    width, structures = operands[3].shape[1], operands[9].shape[1]
    return pl.pallas_call(
        partial(finish_kernel, rows),
        out_shape=(
            jax.ShapeDtypeStruct((8, rows * TILE), f32),
            jax.ShapeDtypeStruct((16, width), f32),
            jax.ShapeDtypeStruct((8 * groups, structures), f32),
        ),
        in_specs=[vmem_spec()] * 10,
        out_specs=(vmem_spec(),) * 3,
        scratch_shapes=[
            pltpu.VMEM((2, 3, rows, TILE), f32),
            pltpu.VMEM((16, width), f32),
            pltpu.VMEM((8 * groups, structures), f32),
            pltpu.VMEM((mesh_steps, 16, width), f32),
            pltpu.VMEM((mesh_steps, 8 * groups, structures), f32),
            pltpu.SemaphoreType.DMA((2,)),
            pltpu.SemaphoreType.DMA((2,)),
            pltpu.SemaphoreType.DMA((mesh_steps,)),
            pltpu.SemaphoreType.DMA((mesh_steps,)),
            pltpu.SemaphoreType.DMA((mesh_steps,)),
            pltpu.SemaphoreType.DMA((mesh_steps,)),
        ],
        compiler_params=comm_params(which),
        name="finish_%d" % which,
    )(*operands)


def tail_kernel(mine_ref, all_force_ref, sum_ref, group_ref, energy_ref, offset_ref, force_ref, one_ref,
                first_ref, mix_ref, two_ref, second_ref):
    groups = group_ref.shape[0] // 8

    def fractions(rows):
        counts = [rows[1 + c : 2 + c, :] for c in range(SPECIES)]
        size = jnp.maximum(counts[0] + counts[1] + counts[2] + counts[3], 1.0)
        return [count / size for count in counts], size

    gram = [[None] * SPECIES for _ in range(SPECIES)]
    right = [None] * SPECIES
    energy = None
    own_frac = [None] * SPECIES

    def plus(total, value):
        return value if total is None else total + value

    for group in range(groups):
        rows = group_ref[8 * group : 8 * group + 8, :]
        frac, size = fractions(rows)
        mine = jnp.where(mine_ref[0] == group, 1.0, 0.0)
        energy = plus(energy, mine * (rows[0:1] / size))
        for c in range(SPECIES):
            own_frac[c] = plus(own_frac[c], mine * frac[c])
            right[c] = plus(right[c], frac[c] * rows[5:6])
            for d in range(c, SPECIES):
                gram[c][d] = plus(gram[c][d], frac[c] * frac[d])

    def whole(value):
        return jnp.sum(value, axis=1, keepdims=True)

    right = [whole(value) for value in right]
    upper = [[None if value is None else whole(value) for value in row] for row in gram]
    matrix = [
        [upper[min(c, d)][max(c, d)] + (ridge_weight if c == d else 0.0) for d in range(SPECIES)]
        for c in range(SPECIES)
    ]
    for pivot in range(SPECIES):
        for below in range(pivot + 1, SPECIES):
            ratio = matrix[below][pivot] / matrix[pivot][pivot]
            matrix[below] = [b - ratio * a for a, b in zip(matrix[pivot], matrix[below])]
            right[below] = right[below] - ratio * right[pivot]
    answer = [None] * SPECIES
    for row in range(SPECIES - 1, -1, -1):
        running = right[row]
        for later in range(row + 1, SPECIES):
            running = running - matrix[row][later] * answer[later]
        answer[row] = running / matrix[row][row]
    for c in range(SPECIES):
        energy = energy + own_frac[c] * answer[c]
    energy_ref[...] = energy
    offset_ref[...] = jnp.concatenate(answer, axis=1)
    for axis in range(3):
        force_ref[axis] = all_force_ref[axis : axis + 1, :]
    first_ref[...] = sum_ref[0:4, :]
    second_ref[...] = sum_ref[4:8, :]
    mix_ref[...] = sum_ref[8:12, :]
    for n in range(NMAX):
        one_ref[n : n + 1, :] = sum_ref[12:13, n * NRAD : (n + 1) * NRAD]
        two_ref[n : n + 1, :] = sum_ref[12:13, TILE + n * NRAD : TILE + (n + 1) * NRAD]


def tail_call(mine, forces, sums, groups):
    width, structures, atoms = sums.shape[1], groups.shape[1], forces.shape[1]
    shapes = (
        (1, structures),
        (1, SPECIES),
        (3, 1, atoms),
        (NMAX, NRAD),
        (SPECIES, width),
        (SPECIES, width),
        (NMAX, NRAD),
        (SPECIES, width),
    )
    return pl.pallas_call(
        tail_kernel,
        out_shape=tuple(jax.ShapeDtypeStruct(shape, f32) for shape in shapes),
        in_specs=[smem_spec()] + [vmem_spec()] * 3,
        out_specs=(vmem_spec(),) * len(shapes),
        compiler_params=pltpu.CompilerParams(vmem_limit_bytes=VMEM_ALL),
        name="tail",
    )(mine, forces, sums, groups)


def double_factorial(number):
    result = 1.0
    while number > 1:
        result = result * number
        number = number - 2
    return result


def norm_of(degree, azimuth):
    value = math.sqrt(
        (2 * degree + 1)
        / (4 * math.pi)
        * math.factorial(degree - azimuth)
        / math.factorial(degree + azimuth)
    )
    return value * (math.sqrt(2.0) if azimuth else 1.0)


def scaled_legendre(coord_z):
    table = {}
    for azimuth in range(LMAX + 1):
        table[azimuth, azimuth] = norm_of(azimuth, azimuth) * double_factorial(2 * azimuth - 1)
        if azimuth + 1 <= LMAX:
            ratio = norm_of(azimuth + 1, azimuth) / norm_of(azimuth, azimuth)
            table[azimuth + 1, azimuth] = coord_z * (
                (2 * azimuth + 1) * ratio * table[azimuth, azimuth]
            )
        for degree in range(azimuth + 2, LMAX + 1):
            gap = degree - azimuth
            first = (2 * degree - 1) / gap * norm_of(degree, azimuth) / norm_of(degree - 1, azimuth)
            second = (
                (degree + azimuth - 1) / gap * norm_of(degree, azimuth) / norm_of(degree - 2, azimuth)
            )
            table[degree, azimuth] = (first * coord_z) * table[degree - 1, azimuth] - (
                second * table[degree - 2, azimuth]
            )
    return table


def azimuth_powers(coord_x, coord_y):
    cosines = [None, coord_x]
    sines = [None, coord_y]
    for _ in range(2, LMAX + 1):
        cosines.append(cosines[-1] * coord_x - sines[-1] * coord_y)
        sines.append(sines[-1] * coord_x + cosines[-2] * coord_y)
    return cosines, sines


LANE_GATHER = lax.GatherDimensionNumbers(
    offset_dims=(),
    collapsed_slice_dims=(1,),
    start_index_map=(1,),
    operand_batching_dims=(0,),
    start_indices_batching_dims=(0,),
)


def lane_gather(line, lo):
    return lax.gather(
        line,
        lo[..., None],
        LANE_GATHER,
        slice_sizes=(1, 1),
        mode=lax.GatherScatterMode.PROMISE_IN_BOUNDS,
    )


def prepare_kernel(first_ref, cnt_ref, nbr_ref, spot_ref, kind_ref, part_ref, table_ref, idx_ref, wt_ref,
                   sorted_ref, perm_ref, info_ref, mine_ref, got_ref, send_sem, recv_sem, key_ref, pos_ref,
                   word_ref, rank_ref):
    atoms = nbr_ref.shape[2]
    tiles = atoms // TILE
    blocks = NBR // 8
    sub = lax.broadcasted_iota(jnp.int32, (8, TILE), 0)
    lane = lax.broadcasted_iota(jnp.int32, (1, TILE), 1)
    site = site_rows(spot_ref, kind_ref, part_ref)
    pair = begin_spread(SPECIES, site, mine_ref, got_ref, send_sem, recv_sem)

    def merge(tile, carry):
        cols = pl.ds(pl.multiple_of(tile * TILE, TILE), TILE)
        limit = cnt_ref[:, cols]
        iota = lax.broadcasted_iota(jnp.int32, (NBR, TILE), 0)
        key = jnp.where(iota < limit, nbr_ref[:, 0, cols] - first_ref[0], -1 - iota)
        key_ref[...] = key
        keys = [key[8 * b : 8 * b + 8] for b in range(blocks)]
        total = [jnp.zeros((8, TILE), jnp.int32) for _ in range(blocks)]
        early = [jnp.zeros((8, TILE), jnp.int32) for _ in range(blocks)]
        for other in range(NBR):
            line = jnp.broadcast_to(key_ref[other : other + 1, :], (8, TILE))
            for b in range(blocks):
                same = jnp.where(keys[b] == line, 1, 0)
                total[b] = total[b] + same
                if other < 8 * b:
                    early[b] = early[b] + same
                elif other < 8 * b + 7:
                    early[b] = early[b] + jnp.where(sub > other - 8 * b, same, 0)
        for b in range(blocks):
            alive = sub + 8 * b < limit
            pos_ref[8 * b : 8 * b + 8, :] = jnp.where(alive & (early[b] == 0), 1, 0)
            key_ref[8 * b : 8 * b + 8, :] = total[b] * 4096 + keys[b]
        running = jnp.zeros((1, TILE), jnp.int32)
        out = [jnp.zeros((8, TILE), jnp.int32) for _ in range(blocks)]
        for slot in range(NBR):
            flag = pos_ref[slot : slot + 1, :]
            place = jnp.broadcast_to(jnp.where(flag == 1, running, -1), (8, TILE))
            running = running + flag
            line = jnp.broadcast_to(key_ref[slot : slot + 1, :], (8, TILE))
            for b in range(slot // 8 + 1):
                out[b] = jnp.where(place == sub + 8 * b, line, out[b])
        for b in range(blocks):
            word_ref[8 * b : 8 * b + 8, cols] = out[b].astype(f32)
        order = running * atoms + (atoms - 1 - tile * TILE) - lane
        rank_ref[pl.ds(tile, 1), :] = order.astype(f32)
        return carry

    lax.fori_loop(0, tiles, merge, 0)
    orders = rank_ref[...]
    upright = jnp.transpose(orders)
    ranks = []
    for tile in range(tiles):
        row = jnp.broadcast_to(orders[tile : tile + 1], (TILE, TILE))
        total = jnp.zeros((TILE, TILE), f32)
        for other in range(tiles):
            col = jnp.broadcast_to(upright[:, other : other + 1], (TILE, TILE))
            total = total + jnp.where(col > row, 1.0, 0.0)
        ranks.append(jnp.sum(total, axis=0, keepdims=True))
    place = lax.broadcasted_iota(jnp.int32, (atoms, TILE), 0).astype(f32)
    for tile in range(tiles):
        line = jnp.broadcast_to(ranks[tile], (atoms, TILE))
        perm_ref[:, tile * TILE : (tile + 1) * TILE] = jnp.where(line == place, 1.0, 0.0).astype(bf16)
    word_ref[NBR : NBR + 8, :] = site
    moved = reorder(word_ref[...], perm_ref, 1)
    sorted_ref[...] = moved[NBR:]
    word = moved[:NBR].astype(jnp.int32)
    index = lax.bitwise_and(word, 4095)
    times = lax.shift_right_logical(word, 12)
    idx_ref[:NBR, :] = index
    idx_ref[NBR:, :] = jnp.zeros((NPAD - NBR, atoms), jnp.int32)
    wt_ref[:NBR, :] = density_scale * times.astype(f32)
    wt_ref[NBR:, :] = jnp.zeros((NPAD - NBR, atoms), f32)
    row = lax.shift_right_logical(index, 7)
    low = jnp.min(jnp.where(times > 0, row, 1 << 20))
    high = jnp.max(jnp.where(times > 0, row, -1))
    slots = lax.broadcasted_iota(jnp.int32, (NBR, TILE), 0) + 1
    for tile in range(tiles):
        used = times[:, tile * TILE : (tile + 1) * TILE] > 0
        info_ref[0, tile] = lax.div(jnp.max(jnp.where(used, slots, 0)) + SLOTS - 1, SLOTS) * SLOTS
        info_ref[1, tile] = low
        info_ref[2, tile] = high
    end_spread(SPECIES, pair, table_ref, mine_ref)


def prepare_call(which, first, limits, neighbours, positions, species, structure):
    atoms = neighbours.shape[2]
    return pl.pallas_call(
        prepare_kernel,
        out_shape=(
            jax.ShapeDtypeStruct((SPECIES * 3 * atoms // TILE, TILE), f32),
            jax.ShapeDtypeStruct((NPAD, atoms), jnp.int32),
            jax.ShapeDtypeStruct((NPAD, atoms), f32),
            jax.ShapeDtypeStruct((8, atoms), f32),
            jax.ShapeDtypeStruct((atoms, atoms), bf16),
            jax.ShapeDtypeStruct((3, atoms // TILE), jnp.int32),
        ),
        in_specs=[smem_spec()] + [vmem_spec()] * 5,
        out_specs=(vmem_spec(),) * 5 + (smem_spec(),),
        scratch_shapes=[
            pltpu.VMEM((SPECIES * atoms // TILE, TILE), f32),
            pltpu.VMEM((2, SPECIES * atoms // TILE, TILE), f32),
            pltpu.SemaphoreType.DMA((2,)),
            pltpu.SemaphoreType.DMA((2,)),
            pltpu.VMEM((NBR, TILE), jnp.int32),
            pltpu.VMEM((NBR, TILE), jnp.int32),
            pltpu.VMEM((NBR + 8, atoms), f32),
            pltpu.VMEM((atoms // TILE, TILE), f32),
        ],
        compiler_params=comm_params(which),
        name="prepare",
    )(first, limits, neighbours, positions, species, structure)


def window_starts(row_low, row_high):
    start = jnp.minimum(row_low, 24 - FROWS)
    return start, lax.div(row_high - start, FROWS) + 1


def load_window(tab_ref, left_ref, values, exact, start):
    for value in range(values):
        pieces = split3(tab_ref[pl.ds(value * 24 + start, FROWS), :])
        for piece in range(3 if exact else 2):
            at = (piece * values + value) * FROWS
            left_ref[at : at + FROWS, :] = pieces[piece * FROWS : (piece + 1) * FROWS]


def fetch(left_ref, values, exact, idx_ref, put_ref, base, start):
    index = idx_ref[pl.ds(base, 8), :]
    hi = lax.shift_right_logical(index, 7) - start
    lo = lax.bitwise_and(index, 127)
    sub = lax.broadcasted_iota(jnp.int32, (TILE, TILE), 0)
    hits = []
    for part in range(8):
        line = jnp.broadcast_to(lo[part : part + 1, :], (TILE, TILE))
        hits.append(jnp.where(line == sub, 1.0, 0.0).astype(bf16))
    one = jnp.concatenate(hits, axis=1)
    height = values * FROWS
    pieces = 3 if exact else 2
    wide = jnp.dot(left_ref[0 : pieces * height, :], one, preferred_element_type=f32)
    got = wide[0:height] + wide[height : 2 * height]
    if exact:
        got = got + wide[2 * height :]
    line8 = lax.broadcasted_iota(jnp.int32, (8, TILE), 0)
    found = [jnp.zeros((8, TILE), f32) for _ in range(values)]
    for part in range(8):
        place = jnp.broadcast_to(hi[part : part + 1, :], (8, TILE))
        masks = [place == line8 + 8 * r for r in range(FROWS // 8)]
        for value in range(values):
            total = None
            for r, mask in enumerate(masks):
                at = value * FROWS + 8 * r
                term = jnp.where(mask, got[at : at + 8, part * TILE : (part + 1) * TILE], 0.0)
                total = term if total is None else total + term
            row = jnp.sum(total, axis=0, keepdims=True)
            found[value] = jnp.where(line8 == part, jnp.broadcast_to(row, (8, TILE)), found[value])
    inside = (hi >= 0) & (hi < FROWS)
    for value in range(values):
        rows = slot_rows(value, base)
        put_ref[rows, :] = jnp.where(inside, found[value], put_ref[rows, :])


def slot_rows(which, base):
    return pl.ds(pl.multiple_of(which * NPAD + base, 8), 8)


def geometry(layer, geo_ref, feat_ref, wt_ref, base):
    weight = wt_ref[pl.ds(base, 8), :]
    unit = [geo_ref[slot_rows(axis, base), :] for axis in range(3)]
    dist = geo_ref[slot_rows(4, base), :]
    if layer == 1:
        kind = geo_ref[slot_rows(3, base), :]
        chan = [jnp.where(kind == float(c), 1.0, 0.0) for c in range(SPECIES)]
    else:
        chan = [feat_ref[slot_rows(c, base), :] for c in range(SPECIES)]
    return weight, dist, unit, chan


def radial_terms(dist, rad_ref, with_slope):
    scaled = dist * (2.0 / cutoff_radius) - 1.0
    inside = dist < cutoff_radius
    angle = dist * (math.pi / cutoff_radius)
    cutoff = jnp.where(inside, 0.5 * (jnp.cos(angle) + 1.0), 0.0)
    cheb = [None, scaled]
    twice = 2.0 * scaled
    cheb.append(twice * scaled - 1.0)
    for _ in range(3, NRAD):
        cheb.append(twice * cheb[-1] - cheb[-2])
    basis = [cutoff] + [cutoff * cheb[p] for p in range(1, NRAD)]
    radial = []
    for n in range(NMAX):
        total = basis[0] * rad_ref[n, 0]
        for p in range(1, NRAD):
            total = total + basis[p] * rad_ref[n, p]
        radial.append(total)
    if not with_slope:
        return basis, radial, None
    slope_cut = jnp.where(inside, (-0.5 * math.pi / cutoff_radius) * jnp.sin(angle), 0.0)
    grad_scaled = cutoff * (2.0 / cutoff_radius)
    second = [None, None, twice]
    second[1] = jnp.ones_like(scaled)
    for _ in range(3, NRAD):
        second.append(twice * second[-1] - second[-2])
    slopes = [slope_cut, slope_cut * scaled + grad_scaled]
    for p in range(2, NRAD):
        slopes.append(slope_cut * cheb[p] + grad_scaled * (float(p) * second[p]))
    return basis, radial, slopes


def harmonic_list(unit):
    table = scaled_legendre(unit[2])
    cosines, sines = azimuth_powers(unit[0], unit[1])
    columns = []
    for degree in range(LMAX + 1):
        for signed in range(-degree, degree + 1):
            azimuth = abs(signed)
            poly = table[degree, azimuth]
            if signed == 0:
                columns.append(poly)
            elif signed > 0:
                columns.append(poly * cosines[azimuth])
            else:
                columns.append(poly * sines[azimuth])
    columns[0] = jnp.full_like(unit[2], columns[0])
    return columns


def density_kernel(layer, info_ref, rad_ref, tab_ref, cen_ref, idx_ref, wt_ref, *refs):
    if layer == 1:
        out_ref, geo_ref, x_ref, y_ref, d_ref, left_ref = refs
        feat_ref, put_ref = None, geo_ref
    else:
        geo_ref, out_ref, feat_ref, x_ref, y_ref, d_ref, left_ref = refs
        put_ref = feat_ref
    tile = pl.program_id(0)
    count = info_ref[0, tile]
    row_low, row_high = info_ref[1, tile], info_ref[2, tile]
    blocks = lax.div(count + 7, 8)

    start, windows = window_starts(row_low, row_high)

    def gather_window(window_at, carry):
        first_row = jnp.minimum(start + window_at * FROWS, 24 - FROWS)

        @pl.when((tile == 0) | (windows > 1))
        def _():
            load_window(tab_ref, left_ref, SPECIES, layer == 1, first_row)

        def gather_block(block_at, inner):
            base = pl.multiple_of(block_at * 8, 8)
            fetch(left_ref, SPECIES, layer == 1, idx_ref, put_ref, base, first_row)
            return inner

        return lax.fori_loop(0, blocks, gather_block, carry)

    lax.fori_loop(0, windows, gather_window, 0)

    def edges(block_at, carry):
        base = pl.multiple_of(block_at * 8, 8)
        if layer == 1:
            live = wt_ref[pl.ds(base, 8), :] > 0.0
            deltas = []
            for axis in range(3):
                centre = jnp.broadcast_to(cen_ref[pl.ds(axis, 1), :], (8, TILE))
                delta = geo_ref[slot_rows(axis, base), :] - centre
                deltas.append(jnp.where(live, delta, 1.0))
            dist = jnp.sqrt(deltas[0] * deltas[0] + deltas[1] * deltas[1] + deltas[2] * deltas[2])
            inv = 1.0 / dist
            for axis in range(3):
                geo_ref[slot_rows(axis, base), :] = deltas[axis] * inv
            geo_ref[slot_rows(4, base), :] = dist
        weight, dist, unit, chan = geometry(layer, geo_ref, feat_ref, wt_ref, base)
        _, radial, _ = radial_terms(dist, rad_ref, False)
        for c in range(SPECIES):
            scale = chan[c] * weight
            for n in range(NMAX):
                x_ref[pl.ds(base * XROW + (c * NMAX + n), 8, stride=XROW), :] = scale * radial[n]
        for at, column in enumerate(harmonic_list(unit)):
            y_ref[slot_rows(at, base), :] = column
        return carry

    lax.fori_loop(0, blocks, edges, 0)
    groups = lax.div(count, SLOTS)

    def lm_block(block_at, carry):
        first = block_at * LBLK

        def slots(group, acc):
            acc = list(acc)
            for part in range(SLOTS):
                slot = group * SLOTS + part
                rows = [x_ref[pl.ds(slot * XROW + 8 * j, 8), :] for j in range(CH // 8)]
                for at in range(LBLK):
                    line = jnp.broadcast_to(
                        y_ref[pl.ds((first + at) * NPAD + slot, 1), :], (8, TILE)
                    )
                    for j in range(CH // 8):
                        acc[at * (CH // 8) + j] = acc[at * (CH // 8) + j] + rows[j] * line
            return tuple(acc)

        zero = jnp.zeros((8, TILE), f32)
        acc = lax.fori_loop(0, groups, slots, tuple(zero for _ in range(LBLK * (CH // 8))))
        for at in range(LBLK):
            for j in range(CH // 8):
                d_ref[pl.ds(8 * j * LM + first + at, 8, stride=LM), :] = acc[at * (CH // 8) + j]
        return carry

    lax.fori_loop(0, LM // LBLK, lm_block, 0)
    out_ref[...] = d_ref[...].astype(bf16)


def smem_spec():
    return pl.BlockSpec(memory_space=pltpu.SMEM)


def tile_spec(rows):
    return pl.BlockSpec((rows, TILE), lambda i: (0, i))


def whole_spec(shape):
    return pl.BlockSpec(shape, lambda i: tuple(0 for _ in shape))


def density_call(layer, info, radial, table, centres, index, weight, geo=None):
    atoms = centres.shape[1]
    rows = GEO if layer == 1 else SPECIES
    extra = () if geo is None else (geo,)
    return pl.pallas_call(
        partial(density_kernel, layer),
        out_shape=(
            jax.ShapeDtypeStruct((DENS, atoms), bf16),
            jax.ShapeDtypeStruct((rows * NPAD, atoms), f32),
        ),
        grid=(atoms // TILE,),
        in_specs=[
            smem_spec(),
            smem_spec(),
            whole_spec(table.shape),
            tile_spec(8),
            tile_spec(NPAD),
            tile_spec(NPAD),
        ]
        + [tile_spec(GEO * NPAD)] * len(extra),
        out_specs=(tile_spec(DENS), tile_spec(rows * NPAD)),
        scratch_shapes=[
            pltpu.VMEM((NPAD * XROW + 8, TILE), f32),
            pltpu.VMEM((LM * NPAD, TILE), f32),
            pltpu.VMEM((DENS, TILE), f32),
            pltpu.VMEM((3 * SPECIES * FROWS, TILE), bf16),
        ],
        compiler_params=pltpu.CompilerParams(vmem_limit_bytes=VMEM_ALL),
        name="density_%d" % layer,
    )(info, radial, table, centres, index, weight, *extra)


def backward_kernel(layer, info_ref, rad_ref, geo_ref, feat_ref, idx_ref, wt_ref, dd_ref, win_in_ref,
                    own_in_ref, win_ref, own_ref, rad_out_ref, rgr_ref, x_ref, y_ref, gx_ref, gy_ref, val_ref,
                    left_ref):
    tile = pl.program_id(0)
    count = info_ref[0, tile]
    row_low, row_high = info_ref[1, tile], info_ref[2, tile]
    blocks = lax.div(count + 7, 8)
    zero = jnp.zeros((8, TILE), f32)

    @pl.when(tile == 0)
    def _():
        if layer == 1:
            win_ref[...] = win_in_ref[: 3 * WSTEP]
        else:
            win_ref[...] = jnp.zeros_like(win_ref)
        rgr_ref[...] = jnp.zeros_like(rgr_ref)

    def line_of(at):
        return jnp.broadcast_to(dd_ref[pl.ds(at, 1), :], (8, TILE))

    def contract_slots():
        def over_lm(step, acc):
            acc = list(acc)
            for part in range(LBLK):
                lm = step * LBLK + part
                col = y_ref[pl.ds(lm * 8, 8), :]
                for m in range(CH):
                    acc[m] = acc[m] + line_of(m * LM + lm) * col
            return tuple(acc)

        acc = tuple(zero for _ in range(CH))
        for step in range(LM // LBLK):
            acc = over_lm(step, acc)
        for m in range(CH):
            gx_ref[8 * m : 8 * m + 8, :] = acc[m]

        def over_m(step, acc):
            acc = list(acc)
            for part in range(4):
                m = step * 4 + part
                col = x_ref[pl.ds(m * 8, 8), :]
                for lm in range(LM):
                    acc[lm] = acc[lm] + line_of(m * LM + lm) * col
            return tuple(acc)

        acc = tuple(zero for _ in range(LM))
        for step in range(CH // 4):
            acc = over_m(step, acc)
        for lm in range(LM):
            gy_ref[8 * lm : 8 * lm + 8, :] = acc[lm]

    def contract_species(kind):
        odd = (kind == 1.0) | (kind == 3.0)
        upper = kind > 1.5

        def over_n(step, acc):
            acc = list(acc)
            for part in range(2):
                n = step * 2 + part
                at = n * 8
                scaled = x_ref[pl.ds(at, 8), :]
                sums = [None, None]
                for lm in range(LM):
                    lines = [line_of((c * NMAX + n) * LM + lm) for c in range(SPECIES)]
                    first = jnp.where(odd, lines[1], lines[0])
                    second = jnp.where(odd, lines[3], lines[2])
                    grad = jnp.where(upper, second, first)
                    acc[lm] = acc[lm] + grad * scaled
                    term = grad * y_ref[8 * lm : 8 * lm + 8, :]
                    sums[lm % 2] = term if lm < 2 else sums[lm % 2] + term
                gx_ref[pl.ds(at, 8), :] = sums[0] + sums[1]
            return tuple(acc)

        acc = tuple(zero for _ in range(LM))
        for step in range(NMAX // 2):
            acc = over_n(step, acc)
        for lm in range(LM):
            gy_ref[8 * lm : 8 * lm + 8, :] = acc[lm]

    def slot_block(block_at, own):
        base = pl.multiple_of(block_at * 8, 8)
        weight, dist, unit, chan = geometry(layer, geo_ref, feat_ref, wt_ref, base)
        _, radial, _ = radial_terms(dist, rad_ref, False)
        for at, column in enumerate(harmonic_list(unit)):
            y_ref[8 * at : 8 * at + 8, :] = column
        if layer == 1:
            for n in range(NMAX):
                x_ref[8 * n : 8 * n + 8, :] = weight * radial[n]
            contract_species(geo_ref[slot_rows(3, base), :])
        else:
            for c in range(SPECIES):
                scale = chan[c] * weight
                for n in range(NMAX):
                    at = 8 * (c * NMAX + n)
                    x_ref[at : at + 8, :] = scale * radial[n]
            contract_slots()
        weight, dist, unit, chan = geometry(layer, geo_ref, feat_ref, wt_ref, base)
        inv = 1.0 / dist
        basis, radial, slopes = radial_terms(dist, rad_ref, True)
        feat_grads = []
        radial_grads = [None] * NMAX
        if layer == 1:
            radial_grads = [gx_ref[8 * n : 8 * n + 8, :] for n in range(NMAX)]
        for c in range(SPECIES if layer == 2 else 0):
            total = None
            for n in range(NMAX):
                grad = gx_ref[8 * (c * NMAX + n) : 8 * (c * NMAX + n) + 8, :]
                term = grad * radial[n]
                total = term if total is None else total + term
                piece = grad * chan[c]
                radial_grads[n] = piece if c == 0 else radial_grads[n] + piece
            feat_grads.append(total * weight)
        grad_r = None
        radial_grads = [grad * weight for grad in radial_grads]
        for p in range(NRAD):
            total = None
            for n in range(NMAX):
                at = (n * NRAD + p) * 8
                rgr_ref[pl.ds(at, 8), :] = rgr_ref[pl.ds(at, 8), :] + radial_grads[n] * basis[p]
                term = radial_grads[n] * rad_ref[n, p]
                total = term if total is None else total + term
            term = total * slopes[p]
            grad_r = term if grad_r is None else grad_r + term
        table = scaled_legendre(unit[2])
        cosines, sines = azimuth_powers(unit[0], unit[1])
        grad_x = grad_y = grad_z = None

        def plus(total, term):
            return term if total is None else total + term

        for azimuth in range(LMAX + 1):
            grad_cos = grad_sin = None
            for degree in range(azimuth, LMAX + 1):
                at = degree * degree + degree
                up = gy_ref[8 * (at + azimuth) : 8 * (at + azimuth) + 8, :]
                poly = table[degree, azimuth]
                if azimuth:
                    down = gy_ref[8 * (at - azimuth) : 8 * (at - azimuth) + 8, :]
                    grad_cos = plus(grad_cos, up * poly)
                    grad_sin = plus(grad_sin, down * poly)
                if degree > azimuth:
                    ratio = norm_of(degree, azimuth) / norm_of(degree, azimuth + 1)
                    slope = ratio * table[degree, azimuth + 1]
                    if azimuth:
                        grad_z = plus(grad_z, slope * (up * cosines[azimuth] + down * sines[azimuth]))
                    else:
                        grad_z = plus(grad_z, slope * up)
            if azimuth == 1:
                grad_x, grad_y = grad_cos, grad_sin
            elif azimuth > 1:
                below_cos, below_sin = cosines[azimuth - 1], sines[azimuth - 1]
                grad_x = grad_x + float(azimuth) * (grad_cos * below_cos + grad_sin * below_sin)
                grad_y = grad_y + float(azimuth) * (grad_sin * below_cos - grad_cos * below_sin)
        dot_u = grad_x * unit[0] + grad_y * unit[1] + grad_z * unit[2]
        live = weight > 0.0
        out = []
        for axis, grad in enumerate((grad_x, grad_y, grad_z)):
            value = (grad - dot_u * unit[axis]) * inv + grad_r * unit[axis]
            out.append(jnp.where(live, value, 0.0))
        values = out + feat_grads
        for at, value in enumerate(values):
            val_ref[slot_rows(at, base), :] = value
        return tuple(total + value for total, value in zip(own, out))


    own = lax.fori_loop(0, blocks, slot_block, (zero, zero, zero))
    own = jnp.concatenate(
        [jnp.sum(total, axis=0, keepdims=True) for total in own] + [jnp.zeros((5, TILE), f32)], axis=0
    )
    own_ref[...] = own + own_in_ref[...] if layer == 1 else own

    used = 3 if layer == 1 else NVAL
    height = used * WROWS
    step_rows = height + 1
    sub = lax.broadcasted_iota(jnp.int32, (TILE, TILE), 0)
    windows = lax.div(row_high - row_low + WROWS, WROWS)

    def window(window_at, carry):
        row_base = row_low + window_at * WROWS

        def scatter(block_at, acc):
            base = pl.multiple_of(block_at * 8, 8)
            index = idx_ref[pl.ds(base, 8), :]
            hi = lax.shift_right_logical(index, 7)
            lo = lax.bitwise_and(index, 127)
            for row in range(WROWS):
                hit = hi == row_base + row
                for value_at in range(used):
                    value = val_ref[slot_rows(value_at, base), :]
                    left_ref[pl.ds(value_at * WROWS + row, 8, stride=step_rows), :] = jnp.where(
                        hit, value, 0.0
                    )
            ones, left = [], []
            for part in range(8):
                line = jnp.broadcast_to(lo[part : part + 1, :], (TILE, TILE))
                ones.append(jnp.where(line == sub, 1.0, 0.0).astype(bf16))
                left.append(left_ref[part * step_rows : part * step_rows + height, :])
            left = jnp.concatenate(left, axis=1)
            ones = jnp.concatenate(ones, axis=1)
            high = left.astype(bf16)
            rest = (left - high.astype(f32)).astype(bf16)
            dims = (((1,), (1,)), ((), ()))
            acc = acc + lax.dot_general(high, ones, dims, preferred_element_type=f32)
            return acc + lax.dot_general(rest, ones, dims, preferred_element_type=f32)

        acc = lax.fori_loop(0, blocks, scatter, jnp.zeros((height, TILE), f32))
        for value_at in range(used):
            at = value_at * WSTEP + row_base
            win_ref[pl.ds(at, WROWS), :] = (
                win_ref[pl.ds(at, WROWS), :] + acc[value_at * WROWS : (value_at + 1) * WROWS]
            )
        return carry

    lax.fori_loop(0, windows, window, 0)

    @pl.when(tile == pl.num_programs(0) - 1)
    def _():
        for at in range(NMAX * NRAD):
            rad_out_ref[at : at + 1, :] = jnp.sum(rgr_ref[8 * at : 8 * at + 8, :], axis=0, keepdims=True)


def backward_call(layer, info, radial, geo, feat, index, weight, grad_dens, window_in, own_in):
    atoms = index.shape[1]
    values = 3 if layer == 1 else NVAL
    return pl.pallas_call(
        partial(backward_kernel, layer),
        out_shape=(
            jax.ShapeDtypeStruct((values * WSTEP, TILE), f32),
            jax.ShapeDtypeStruct((8, atoms), f32),
            jax.ShapeDtypeStruct((NMAX * NRAD, TILE), f32),
        ),
        grid=(atoms // TILE,),
        in_specs=[
            smem_spec(),
            smem_spec(),
            tile_spec(GEO * NPAD),
            tile_spec(feat.shape[0]),
            tile_spec(NPAD),
            tile_spec(NPAD),
            tile_spec(DENS),
            whole_spec(window_in.shape),
            tile_spec(8),
        ],
        out_specs=(
            whole_spec((values * WSTEP, TILE)),
            tile_spec(8),
            whole_spec((NMAX * NRAD, TILE)),
        ),
        scratch_shapes=[
            pltpu.VMEM((NMAX * NRAD * 8, TILE), f32),
            pltpu.VMEM((CH * 8, TILE), f32),
            pltpu.VMEM((LM * 8, TILE), f32),
            pltpu.VMEM((CH * 8, TILE), f32),
            pltpu.VMEM((LM * 8, TILE), f32),
            pltpu.VMEM((NVAL * NPAD, TILE), f32),
            pltpu.VMEM((8 * (NVAL * WROWS + 1), TILE), f32),
        ],
        compiler_params=pltpu.CompilerParams(vmem_limit_bytes=VMEM_ALL),
        name="backward_%d" % layer,
    )(info, radial, geo, feat, index, weight, grad_dens, window_in, own_in)


def tn_dot(left, right):
    return lax.dot_general(left, right, (((0,), (0,)), ((), ())), preferred_element_type=f32)


def nt_dot(left, right):
    return lax.dot_general(left, right, (((1,), (1,)), ((), ())), preferred_element_type=f32)


def padded_rows(value):
    return jnp.concatenate([value, jnp.zeros((8 - value.shape[0], value.shape[1]), f32)], axis=0)


def onehot_rows(species):
    kind = lax.broadcasted_iota(jnp.int32, (8, species.shape[1]), 0).astype(f32)
    return jnp.where(kind == species, 1.0, 0.0).astype(bf16)


def combine(parts):
    total = parts[2][0:8]
    total = total + (parts[1][8:16] + parts[0][16:24])
    total = total + (parts[1][0:8] + parts[0][8:16])
    return total + parts[0][0:8]


def by_atoms(rows24, chunk):
    wide = nt_dot(rows24, split3(chunk))
    return [wide[:, j * QB : (j + 1) * QB] for j in range(3)]


def contract_one_kernel(dens_ref, coup_ref, coef_ref, mix_ref, site_ref, factor_ref, energy_ref, feat_ref,
                        aux_ref, grad_ref, b_ref, ch_ref, row_ref):
    factor_at = pl.program_id(0)
    quantum, atoms = b_ref.shape
    half = quantum // 2
    for part in range(2):
        rows = slice(part * half, (part + 1) * half)
        value = tn_dot(coup_ref[0, :, rows], dens_ref[...])
        factor_ref[0, rows, :] = value

        @pl.when(factor_at == 0)
        def _(value=value, rows=rows):
            b_ref[rows, :] = value

        @pl.when(factor_at > 0)
        def _(value=value, rows=rows):
            b_ref[rows, :] = b_ref[rows, :] * value

    @pl.when(factor_at == pl.num_programs(0) - 1)
    def _():
        onehot = onehot_rows(site_ref[3:4, :])
        row_ref[0:24, :] = split3(padded_rows(coef_ref[...]))
        row_ref[24:48, :] = split3(padded_rows(mix_ref[...]))
        triple = jnp.concatenate([onehot] * 3, axis=0)

        def chunk_body(chunk, mixed):
            cols = pl.ds(pl.multiple_of(chunk * QB, QB), QB)
            ch_ref[...] = tn_dot(row_ref[0:24, cols], triple)
            pieces = split3(b_ref[cols, :])
            left = row_ref[24:48, cols]
            parts = [
                jnp.dot(left, pieces[j * QB : (j + 1) * QB], preferred_element_type=f32) for j in range(3)
            ]
            wide = nt_dot(onehot, pieces)
            grad_ref[:, cols] = wide[:, 2 * QB :] + wide[:, QB : 2 * QB] + wide[:, :QB]

            def rows_body(step, sums):
                at = pl.multiple_of(step * 8, 8)
                value = b_ref[pl.ds(pl.multiple_of(chunk * QB + step * 8, 8), 8), :]
                return sums[0] + value * ch_ref[pl.ds(at, 8), :], sums[1] + value * value

            energy, square = lax.fori_loop(0, QB // 8, rows_body, mixed[1:])
            return mixed[0] + combine(parts), energy, square

        zero = jnp.zeros((8, atoms), f32)
        mixed, energy, square = lax.fori_loop(0, quantum // QB, chunk_body, (zero, zero, zero))
        energy_ref[...] = jnp.broadcast_to(jnp.sum(energy, axis=0, keepdims=True), (8, atoms))
        mean = jnp.sum(square, axis=0, keepdims=True) * (1.0 / quantum)
        scale = lax.rsqrt(mean + norm_eps)
        feat_ref[...] = mixed * scale
        aux_ref[0:8, :] = mixed
        aux_ref[8:16, :] = jnp.broadcast_to(scale, (8, atoms))


def contract_one_call(dens, coupling, coefficient, mixing_rows, ordered):
    factors, depth, quantum = coupling.shape
    atoms = dens.shape[1]
    return pl.pallas_call(
        contract_one_kernel,
        out_shape=(
            jax.ShapeDtypeStruct((factors, quantum, atoms), f32),
            jax.ShapeDtypeStruct((8, atoms), f32),
            jax.ShapeDtypeStruct((8, atoms), f32),
            jax.ShapeDtypeStruct((16, atoms), f32),
            jax.ShapeDtypeStruct((8, quantum), f32),
        ),
        grid=(factors,),
        in_specs=[
            whole_spec((depth, atoms)),
            pl.BlockSpec((1, depth, quantum), lambda v: (v, 0, 0)),
            whole_spec(coefficient.shape),
            whole_spec(mixing_rows.shape),
            whole_spec(ordered.shape),
        ],
        out_specs=(
            pl.BlockSpec((1, quantum, atoms), lambda v: (v, 0, 0)),
            whole_spec((8, atoms)),
            whole_spec((8, atoms)),
            whole_spec((16, atoms)),
            whole_spec((8, quantum)),
        ),
        scratch_shapes=[
            pltpu.VMEM((quantum, atoms), f32),
            pltpu.VMEM((QB, atoms), f32),
            pltpu.VMEM((48, quantum), bf16),
        ],
        compiler_params=pltpu.CompilerParams(vmem_limit_bytes=VMEM_ALL),
        name="contract_1",
    )(dens, coupling, coefficient, mixing_rows, ordered)


def factor_grads(values, upstream):
    low_pair, high_pair = values[0] * values[1], values[2] * values[3]
    first, second = upstream * high_pair, upstream * low_pair
    return first * values[1], first * values[0], second * values[3], second * values[2]


def contract_two_kernel(dens_ref, coef_ref, site_ref, before_ref, coup_ref, out_ref, part_ref, grad_ref,
                        cv_ref, f_ref, g_ref, ch_ref, row_ref, sem):
    step = pl.program_id(0)
    factors, quantum, atoms = f_ref.shape
    depth = dens_ref.shape[0]
    half = quantum // 2

    def load(at):
        return pltpu.make_async_copy(coup_ref.at[at], cv_ref.at[at, 0:depth], sem.at[at])

    @pl.when(step == 0)
    def _():
        for at in range(factors):
            load(at).start()
        onehot = onehot_rows(site_ref[3:4, :])
        row_ref[...] = split3(padded_rows(coef_ref[...]))
        triple = jnp.concatenate([onehot] * 3, axis=0)

        def factor_body(at, carry):
            load(at).wait()
            for part in range(2):
                rows = slice(part * half, (part + 1) * half)
                f_ref[at, rows, :] = tn_dot(cv_ref[at, 0:depth, rows], dens_ref[...])
            return carry

        lax.fori_loop(0, factors, factor_body, 0)

        def chunk_body(chunk, energy):
            cols = pl.ds(pl.multiple_of(chunk * QB, QB), QB)
            ch_ref[...] = tn_dot(row_ref[:, cols], triple)

            def rows_body(small, total):
                at = pl.multiple_of(small * 16, 16)
                rows = pl.ds(pl.multiple_of(chunk * QB + small * 16, 16), 16)
                values = [f_ref[v, rows, :] for v in range(factors)]
                upstream = ch_ref[pl.ds(at, 16), :]
                grads = factor_grads(values, upstream)
                for v in range(factors):
                    g_ref[v, rows, :] = grads[v].astype(bf16)
                product = values[0] * values[1] * values[2] * values[3]
                f_ref[0, rows, :] = product
                term = product * upstream
                return total + term[:8] + term[8:]

            energy = lax.fori_loop(0, QB // 16, rows_body, energy)
            wide = nt_dot(onehot, split3(f_ref[0, cols, :]))
            grad_ref[:, cols] = wide[:, 2 * QB :] + wide[:, QB : 2 * QB] + wide[:, :QB]
            return energy

        energy = lax.fori_loop(0, quantum // QB, chunk_body, jnp.zeros((8, atoms), f32))
        energy = jnp.sum(energy, axis=0, keepdims=True) + before_ref[0:1, :]
        kinds = [jnp.where(site_ref[3:4, :] == float(c), 1.0, 0.0) for c in range(SPECIES)]
        rows8 = split3(jnp.concatenate([energy] + kinds + [jnp.zeros((3, atoms), f32)], axis=0))
        owner = site_ref[4:5, :]

        def structure_body(chunk, carry):
            cols = pl.ds(pl.multiple_of(chunk * TILE, TILE), TILE)
            ids = lax.broadcasted_iota(jnp.int32, (TILE, atoms), 0) + chunk * TILE
            members = jnp.where(ids.astype(f32) == owner, 1.0, 0.0).astype(bf16)
            wide = nt_dot(rows8, members)
            part_ref[:, cols] = wide[16:24] + wide[8:16] + wide[0:8]
            return carry

        lax.fori_loop(0, part_ref.shape[1] // TILE, structure_body, 0)

    rows = pl.ds(pl.multiple_of(step * DROWS, 16), DROWS)
    total = None
    for at in range(factors):
        part = jnp.dot(cv_ref[at, rows, :], g_ref[at], preferred_element_type=f32)
        total = part if total is None else total + part
    out_ref[...] = total


def contract_two_call(dens, coupling, coefficient, ordered, energy_one, structures):
    factors, depth, quantum = coupling.shape
    atoms = dens.shape[1]
    steps = pl.cdiv(depth, DROWS)
    return pl.pallas_call(
        contract_two_kernel,
        out_shape=(
            jax.ShapeDtypeStruct((steps * DROWS, atoms), f32),
            jax.ShapeDtypeStruct((8, structures), f32),
            jax.ShapeDtypeStruct((8, quantum), f32),
        ),
        grid=(steps,),
        in_specs=[
            pl.BlockSpec((depth, atoms), lambda i: (0, 0), pipeline_mode=pl.Buffered(1)),
            whole_spec(coefficient.shape),
            whole_spec(ordered.shape),
            whole_spec(energy_one.shape),
            pl.BlockSpec(memory_space=pl.ANY),
        ],
        out_specs=(
            pl.BlockSpec((DROWS, atoms), lambda i: (i, 0)),
            whole_spec((8, structures)),
            whole_spec((8, quantum)),
        ),
        scratch_shapes=[
            pltpu.VMEM((factors, steps * DROWS, quantum), bf16),
            pltpu.VMEM((factors, quantum, atoms), f32),
            pltpu.VMEM((factors, quantum, atoms), bf16),
            pltpu.VMEM((QB, atoms), f32),
            pltpu.VMEM((24, quantum), bf16),
            pltpu.SemaphoreType.DMA((factors,)),
        ],
        compiler_params=pltpu.CompilerParams(vmem_limit_bytes=VMEM_ALL),
        name="contract_2",
    )(dens, coefficient, ordered, energy_one, coupling)


def contract_back_kernel(coup_ref, coef_ref, mix_ref, site_ref, gfeat_ref, aux_ref, factor_ref, out_ref,
                         grad_ref, f_ref, g_ref, ch_ref, row_ref, sem):
    step = pl.program_id(0)
    factors, quantum, atoms = f_ref.shape
    chunks = quantum // QB

    def load(chunk):
        rows = pl.ds(pl.multiple_of(chunk * QB, QB), QB)
        return pltpu.make_async_copy(factor_ref.at[:, rows, :], f_ref.at[:, rows, :], sem.at[chunk])

    @pl.when(step == 0)
    def _():
        for chunk in range(chunks):
            load(chunk).start()
        onehot = onehot_rows(site_ref[3:4, :])
        scale = aux_ref[8:9, :]
        gfeat = gfeat_ref[...]
        dot = jnp.sum(aux_ref[0:8, :] * gfeat, axis=0, keepdims=True)
        shrink = jnp.broadcast_to(scale * scale * scale * dot * (1.0 / quantum), (8, atoms))
        scaled = split3(scale * gfeat)
        high, middle, low = scaled[0:8], scaled[8:16], scaled[16:24]
        mix = split3(padded_rows(mix_ref[...]))
        row_ref[0:24, :] = split3(padded_rows(coef_ref[...]))
        for at, piece in enumerate((0, 0, 0, 1, 1, 2)):
            row_ref[24 + 8 * at : 32 + 8 * at, :] = mix[8 * piece : 8 * piece + 8]
        right = jnp.concatenate([onehot] * 3 + [high, middle, low, high, middle, high], axis=0)

        def chunk_body(chunk, carry):
            load(chunk).wait()
            cols = pl.ds(pl.multiple_of(chunk * QB, QB), QB)
            ch_ref[...] = tn_dot(row_ref[:, cols], right)

            def rows_body(small, inner):
                at = pl.multiple_of(small * 16, 16)
                rows = pl.ds(pl.multiple_of(chunk * QB + small * 16, 16), 16)
                values = [f_ref[v, rows, :] for v in range(factors)]
                product = values[0] * values[1] * values[2] * values[3]
                both = jnp.concatenate([shrink, shrink], axis=0)
                upstream = ch_ref[pl.ds(at, 16), :] - both * product
                grads = factor_grads(values, upstream)
                for v in range(factors):
                    g_ref[v, rows, :] = grads[v].astype(bf16)
                f_ref[0, rows, :] = product
                return inner

            lax.fori_loop(0, QB // 16, rows_body, 0)
            grad_ref[:, cols] = combine(by_atoms(scaled, f_ref[0, cols, :]))
            return carry

        lax.fori_loop(0, chunks, chunk_body, 0)

    total = None
    for at in range(factors):
        part = jnp.dot(coup_ref[at], g_ref[at], preferred_element_type=f32)
        total = part if total is None else total + part
    out_ref[...] = total


def contract_back_call(coupling, coefficient, mixing_rows, ordered, gfeat, aux, factor):
    factors, depth, quantum = coupling.shape
    atoms = ordered.shape[1]
    rows = depth // 5
    return pl.pallas_call(
        contract_back_kernel,
        out_shape=(
            jax.ShapeDtypeStruct((depth, atoms), f32),
            jax.ShapeDtypeStruct((8, quantum), f32),
        ),
        grid=(5,),
        in_specs=[
            pl.BlockSpec((factors, rows, quantum), lambda i: (0, i, 0)),
            whole_spec(coefficient.shape),
            whole_spec(mixing_rows.shape),
            whole_spec(ordered.shape),
            whole_spec(gfeat.shape),
            whole_spec(aux.shape),
            pl.BlockSpec(memory_space=pl.ANY),
        ],
        out_specs=(pl.BlockSpec((rows, atoms), lambda i: (i, 0)), whole_spec((8, quantum))),
        scratch_shapes=[
            pltpu.VMEM((factors, quantum, atoms), f32),
            pltpu.VMEM((factors, quantum, atoms), bf16),
            pltpu.VMEM((QB, atoms), f32),
            pltpu.VMEM((72, quantum), bf16),
            pltpu.SemaphoreType.DMA((quantum // QB,)),
        ],
        compiler_params=pltpu.CompilerParams(vmem_limit_bytes=VMEM_ALL),
        name="contract_back_1",
    )(coupling, coefficient, mixing_rows, ordered, gfeat, aux, factor)


def per_device(
    positions,
    species,
    neighbours,
    slot_counts,
    structure,
    target_energy,
    radial_one,
    coupling_one,
    coefficient_one,
    mixing,
    radial_two,
    coupling_two,
    coefficient_two,
):
    atoms = positions.shape[2]
    tiles = atoms // TILE
    structures = target_energy.shape[1]
    first = ((lax.axis_index("dom") - 1) * atoms).astype(jnp.int32).reshape(1)
    table_one, index, weight, ordered, perm, info = prepare_call(
        0, first, slot_counts, neighbours, positions, species, structure
    )
    mixing_rows = mixing.T

    dens_one, geo = density_call(1, info, radial_one, table_one, ordered, index, weight)
    factors_one, energy_one, features, aux, coefficient_first = contract_one_call(
        dens_one, coupling_one, coefficient_one, mixing_rows, ordered
    )
    table_two = spread_call(1, SPECIES, (features, perm))
    dens_two, feat = density_call(2, info, radial_two, table_two, ordered, index, weight, geo)
    grad_dens_two, per_structure, coefficient_second = contract_two_call(
        dens_two, coupling_two, coefficient_two, ordered, energy_one, structures
    )
    window_two, own_two, radial_second = backward_call(
        2, info, radial_two, geo, feat, index, weight, grad_dens_two, table_two, ordered
    )
    grad_features = collect_call(2, tiles, 3, window_two.reshape(NVAL, WSTEP, TILE), perm)
    grad_dens_one, mixing_gradient = contract_back_call(
        coupling_one, coefficient_one, mixing_rows, ordered, grad_features, aux, factors_one
    )
    window_one, own_one, radial_first = backward_call(
        1, info, radial_one, geo, ordered, index, weight, grad_dens_one, window_two, own_two
    )
    groups = lax.axis_size("grp")
    steps = sum(len(group) for group in exchange_rounds())
    forces, sums, group_sums = finish_call(
        3,
        steps,
        groups,
        tiles,
        (
            window_one.reshape(3, WSTEP, TILE),
            own_one,
            perm,
            coefficient_first,
            coefficient_second,
            mixing_gradient,
            radial_first,
            radial_second,
            per_structure,
            target_energy,
        ),
    )
    mine = lax.axis_index("grp").astype(jnp.int32).reshape(1)
    outputs = list(tail_call(mine, forces, sums, group_sums))
    outputs[1] = outputs[1].reshape(SPECIES)
    outputs[5] = outputs[5].T
    return tuple(outputs)


def solution(mesh):
    in_specs = (
        P(None, "grp", "dom"),
        P("grp", "dom"),
        P(None, "grp", "dom"),
        P("grp", "dom"),
        P("grp", "dom"),
        P("grp", None),
        P(),
        P(),
        P(),
        P(),
        P(),
        P(),
        P(),
    )
    out_specs = (P("grp", None), P(), P(None, "grp", "dom"), P(), P(), P(), P(), P())
    return jax.shard_map(
        per_device, mesh=mesh, in_specs=in_specs, out_specs=out_specs, check_vma=False
    )
```

```python
from functools import partial
import math

import jax
import jax.numpy as jnp
from jax import lax
from jax.experimental import pallas as pl
from jax.experimental.pallas import tpu as pltpu
from jax.sharding import PartitionSpec as P

NRAD = 12
NMAX = 10
LMAX = 6
LM = 49
SPECIES = 4
CH = SPECIES * NMAX
DENS = CH * LM
NBR = 48
NPAD = 64
TILE = 128
LBLK = 7
WROWS = 12
WSTEP = 40
GEO = 5
QB = 128
FROWS = 16
VMEM_ALL = 67043328
DROWS = 400
NVAL = 7
SLOTS = 4
XROW = CH + 1

cutoff_radius = 5.0
density_scale = 0.17
norm_eps = 1e-05
ridge_weight = 0.1
highest = lax.Precision.HIGHEST
f32 = jnp.float32
MESH = pl.DeviceIdType.MESH
bf16 = jnp.bfloat16


def log2_of(count):
    steps = count.bit_length() - 1
    assert count == 1 << steps
    return steps


def neighbour_flags(me, count):
    return me > 0, me < count - 1


def greet(partners, flags):
    barrier = pltpu.get_barrier_semaphore()
    for partner, flag in zip(partners, flags):
        if flag is None:
            pl.semaphore_signal(barrier, inc=1, device_id=partner, device_id_type=MESH)
        else:

            @pl.when(flag)
            def _(partner=partner):
                pl.semaphore_signal(barrier, inc=1, device_id=partner, device_id_type=MESH)

    present = sum(1 for flag in flags if flag is None)
    for flag in flags:
        if flag is not None:
            present = present + jnp.where(flag, 1, 0)
    pl.semaphore_wait(barrier, present)


class SidePair:
    def __init__(self, to_left, to_right, got_ref, send_sem, recv_sem):
        count = lax.axis_size("dom")
        me = lax.axis_index("dom")
        self.partners = ({"dom": me - 1}, {"dom": me + 1})
        self.flags = neighbour_flags(me, count)
        self.got = got_ref
        self.copies = [
            pltpu.make_async_remote_copy(
                src_ref=source,
                dst_ref=got_ref.at[1 - side],
                send_sem=send_sem.at[side],
                recv_sem=recv_sem.at[1 - side],
                device_id=self.partners[side],
                device_id_type=MESH,
            )
            for side, source in enumerate((to_left, to_right))
        ]

    def start(self):
        for side in range(2):
            pl.when(self.flags[side])(self.copies[side].start)

    def wait(self):
        for side in range(2):

            @pl.when(self.flags[side])
            def _(side=side):
                self.copies[side].wait_send()
                self.copies[1 - side].wait_recv()

    def received(self, side):
        return jnp.where(self.flags[side], self.got[side], 0.0)


def split3(value):
    high = value.astype(bf16)
    rest = value - high.astype(f32)
    middle = rest.astype(bf16)
    low = (rest - middle.astype(f32)).astype(bf16)
    return jnp.concatenate([high, middle, low], axis=0)


def reorder(value, perm_ref, contract_at):
    count = value.shape[0]
    out = lax.dot_general(
        split3(value), perm_ref[...], (((1,), (contract_at,)), ((), ())), preferred_element_type=f32
    )
    return out[:count] + (out[count : 2 * count] + out[2 * count :])


def site_rows(pos_ref, kind_ref, part_ref):
    atoms = kind_ref.shape[1]
    rows = [pos_ref[axis] for axis in range(3)]
    rows = rows + [kind_ref[...].astype(f32), part_ref[...].astype(f32)]
    return jnp.concatenate(rows + [jnp.zeros((3, atoms), f32)], axis=0)


def begin_spread(values, flat, mine_ref, got_ref, send_sem, recv_sem):
    rows = flat.shape[1] // TILE
    for value in range(values):
        for row in range(rows):
            line = flat[value : value + 1, row * TILE : (row + 1) * TILE]
            at = value * rows + row
            mine_ref[at : at + 1, :] = line
    pair = SidePair(mine_ref, mine_ref, got_ref, send_sem, recv_sem)
    greet(pair.partners, pair.flags)
    pair.start()
    return pair


def end_spread(values, pair, out_ref, mine_ref):
    rows = mine_ref.shape[0] // values
    for value in range(values):
        at = value * 3 * rows
        out_ref[at + rows : at + 2 * rows, :] = mine_ref[value * rows : (value + 1) * rows, :]
    pair.wait()
    for side in range(2):
        block = pair.received(side)
        for value in range(values):
            at = value * 3 * rows + 2 * side * rows
            out_ref[at : at + rows, :] = block[value * rows : (value + 1) * rows]


def spread_kernel(values, x_ref, perm_ref, out_ref, mine_ref, got_ref, send_sem, recv_sem):
    flat = reorder(x_ref[...], perm_ref, 0)
    pair = begin_spread(values, flat, mine_ref, got_ref, send_sem, recv_sem)
    end_spread(values, pair, out_ref, mine_ref)


def comm_params(which):
    return pltpu.CompilerParams(collective_id=which, has_side_effects=True, vmem_limit_bytes=VMEM_ALL)


def vmem_spec():
    return pl.BlockSpec(memory_space=pltpu.VMEM)


def spread_call(which, values, operands):
    rows = values * operands[-1].shape[1] // TILE
    return pl.pallas_call(
        partial(spread_kernel, values),
        out_shape=jax.ShapeDtypeStruct((rows * 3, TILE), f32),
        in_specs=[vmem_spec()] * len(operands),
        out_specs=vmem_spec(),
        scratch_shapes=[
            pltpu.VMEM((rows, TILE), f32),
            pltpu.VMEM((2, rows, TILE), f32),
            pltpu.SemaphoreType.DMA((2,)),
            pltpu.SemaphoreType.DMA((2,)),
        ],
        compiler_params=comm_params(which),
        name="spread_%d" % which,
    )(*operands)


def in_lanes(blocks):
    values, rows = blocks.shape[0], blocks.shape[1]
    flat = [
        jnp.concatenate([blocks[v, r : r + 1, :] for r in range(rows)], axis=1) for v in range(values)
    ]
    return jnp.concatenate(flat + [jnp.zeros((8 - values, rows * TILE), f32)], axis=0)


def lane_sums(value):
    wide = nt_dot(jnp.ones((8, TILE), bf16), split3(value))
    rows = value.shape[0]
    total = wide[0:1, 2 * rows :] + wide[0:1, rows : 2 * rows] + wide[0:1, :rows]
    return jnp.concatenate([total, jnp.zeros((1, TILE - rows), f32)], axis=1)


def exchange_rounds():
    rounds = []
    for axis in ("dom", "grp"):
        me = lax.axis_index(axis)
        bits = log2_of(lax.axis_size(axis))

        def flip(places):
            other = me
            for bit in places:
                half = 1 << bit
                other = other + half - 2 * half * lax.rem(lax.div(me, half), 2)
            return {axis: other}

        for bit in range(0, bits, 2):
            if bit + 1 < bits:
                rounds.append([flip((bit,)), flip((bit + 1,)), flip((bit, bit + 1))])
            else:
                rounds.append([flip((bit,))])
    return rounds


def finish_kernel(rows, win_ref, own_ref, perm_ref, first_ref, second_ref, mix_ref, one_ref, two_ref, part_ref,
                  target_ref, force_ref, sum_ref, group_ref, got_ref, pay_ref, pay_group_ref, came_ref,
                  came_group_ref, send_sem, recv_sem, step_send, step_recv, group_send, group_recv):
    pair = SidePair(
        win_ref.at[:, 0:rows], win_ref.at[:, 2 * rows : 3 * rows], got_ref, send_sem, recv_sem
    )
    rounds = exchange_rounds()
    partners = [partner for group in rounds for partner in group]
    width = pay_ref.shape[1]
    for at, ref in enumerate((first_ref, second_ref, mix_ref)):
        pay_ref[4 * at : 4 * at + 4, :] = ref[0:4, :]
    tail = [lane_sums(one_ref[...]), lane_sums(two_ref[...]), jnp.zeros((1, width - 2 * TILE), f32)]
    pay_ref[12:13, :] = jnp.concatenate(tail, axis=1)
    pay_ref[13:16, :] = jnp.zeros((3, width), f32)
    lead = lax.axis_index("dom") == 0
    mine = lax.axis_index("grp")
    target = jnp.where(lead, target_ref[...], 0.0)
    block = part_ref[...]
    block = jnp.concatenate([block[0:5], target, block[6:8]], axis=0)
    for group in range(lax.axis_size("grp")):
        pay_group_ref[8 * group : 8 * group + 8, :] = jnp.where(mine == group, block, 0.0)
    greet(list(pair.partners) + partners, list(pair.flags) + [None] * len(partners))
    pair.start()
    at = 0
    for turn, group in enumerate(rounds):
        copies = []
        for partner in group:
            for source, total, came, send, recv in (
                (pay_ref, sum_ref, came_ref, step_send, step_recv),
                (pay_group_ref, group_ref, came_group_ref, group_send, group_recv),
            ):
                copy = pltpu.make_async_remote_copy(
                    src_ref=source if turn == 0 else total,
                    dst_ref=came.at[at],
                    send_sem=send.at[at],
                    recv_sem=recv.at[at],
                    device_id=partner,
                    device_id_type=MESH,
                )
                copy.start()
                copies.append(copy)
            at = at + 1
        if turn == 0:
            force_ref[...] = reorder(own_ref[...], perm_ref, 0)
        for copy in copies:
            copy.wait()
        for source, total, came in (
            (pay_ref, sum_ref, came_ref),
            (pay_group_ref, group_ref, came_group_ref),
        ):
            value = (source if turn == 0 else total)[...] + came[at - len(group)]
            if len(group) == 3:
                value = value + (came[at - 2] + came[at - 1])
            total[...] = value
    pair.wait()
    total = win_ref[:, rows : 2 * rows] + pair.received(0) + pair.received(1)
    force_ref[...] = force_ref[...] - in_lanes(total)


def finish_call(which, mesh_steps, groups, rows, operands):
    width, structures = operands[3].shape[1], operands[9].shape[1]
    return pl.pallas_call(
        partial(finish_kernel, rows),
        out_shape=(
            jax.ShapeDtypeStruct((8, rows * TILE), f32),
            jax.ShapeDtypeStruct((16, width), f32),
            jax.ShapeDtypeStruct((8 * groups, structures), f32),
        ),
        in_specs=[vmem_spec()] * 10,
        out_specs=(vmem_spec(),) * 3,
        scratch_shapes=[
            pltpu.VMEM((2, 3, rows, TILE), f32),
            pltpu.VMEM((16, width), f32),
            pltpu.VMEM((8 * groups, structures), f32),
            pltpu.VMEM((mesh_steps, 16, width), f32),
            pltpu.VMEM((mesh_steps, 8 * groups, structures), f32),
            pltpu.SemaphoreType.DMA((2,)),
            pltpu.SemaphoreType.DMA((2,)),
            pltpu.SemaphoreType.DMA((mesh_steps,)),
            pltpu.SemaphoreType.DMA((mesh_steps,)),
            pltpu.SemaphoreType.DMA((mesh_steps,)),
            pltpu.SemaphoreType.DMA((mesh_steps,)),
        ],
        compiler_params=comm_params(which),
        name="finish_%d" % which,
    )(*operands)


def tail_kernel(mine_ref, all_force_ref, sum_ref, group_ref, energy_ref, offset_ref, force_ref, one_ref,
                first_ref, mix_ref, two_ref, second_ref):
    groups = group_ref.shape[0] // 8

    def fractions(rows):
        counts = [rows[1 + c : 2 + c, :] for c in range(SPECIES)]
        size = jnp.maximum(counts[0] + counts[1] + counts[2] + counts[3], 1.0)
        return [count / size for count in counts], size

    gram = [[None] * SPECIES for _ in range(SPECIES)]
    right = [None] * SPECIES
    energy = None
    own_frac = [None] * SPECIES

    def plus(total, value):
        return value if total is None else total + value

    for group in range(groups):
        rows = group_ref[8 * group : 8 * group + 8, :]
        frac, size = fractions(rows)
        mine = jnp.where(mine_ref[0] == group, 1.0, 0.0)
        energy = plus(energy, mine * (rows[0:1] / size))
        for c in range(SPECIES):
            own_frac[c] = plus(own_frac[c], mine * frac[c])
            right[c] = plus(right[c], frac[c] * rows[5:6])
            for d in range(c, SPECIES):
                gram[c][d] = plus(gram[c][d], frac[c] * frac[d])

    def whole(value):
        return jnp.sum(value, axis=1, keepdims=True)

    right = [whole(value) for value in right]
    upper = [[None if value is None else whole(value) for value in row] for row in gram]
    matrix = [
        [upper[min(c, d)][max(c, d)] + (ridge_weight if c == d else 0.0) for d in range(SPECIES)]
        for c in range(SPECIES)
    ]
    for pivot in range(SPECIES):
        for below in range(pivot + 1, SPECIES):
            ratio = matrix[below][pivot] / matrix[pivot][pivot]
            matrix[below] = [b - ratio * a for a, b in zip(matrix[pivot], matrix[below])]
            right[below] = right[below] - ratio * right[pivot]
    answer = [None] * SPECIES
    for row in range(SPECIES - 1, -1, -1):
        running = right[row]
        for later in range(row + 1, SPECIES):
            running = running - matrix[row][later] * answer[later]
        answer[row] = running / matrix[row][row]
    for c in range(SPECIES):
        energy = energy + own_frac[c] * answer[c]
    energy_ref[...] = energy
    offset_ref[...] = jnp.concatenate(answer, axis=1)
    for axis in range(3):
        force_ref[axis] = all_force_ref[axis : axis + 1, :]
    first_ref[...] = sum_ref[0:4, :]
    second_ref[...] = sum_ref[4:8, :]
    mix_ref[...] = sum_ref[8:12, :]
    for n in range(NMAX):
        one_ref[n : n + 1, :] = sum_ref[12:13, n * NRAD : (n + 1) * NRAD]
        two_ref[n : n + 1, :] = sum_ref[12:13, TILE + n * NRAD : TILE + (n + 1) * NRAD]


def tail_call(mine, forces, sums, groups):
    width, structures, atoms = sums.shape[1], groups.shape[1], forces.shape[1]
    shapes = (
        (1, structures),
        (1, SPECIES),
        (3, 1, atoms),
        (NMAX, NRAD),
        (SPECIES, width),
        (SPECIES, width),
        (NMAX, NRAD),
        (SPECIES, width),
    )
    return pl.pallas_call(
        tail_kernel,
        out_shape=tuple(jax.ShapeDtypeStruct(shape, f32) for shape in shapes),
        in_specs=[smem_spec()] + [vmem_spec()] * 3,
        out_specs=(vmem_spec(),) * len(shapes),
        compiler_params=pltpu.CompilerParams(vmem_limit_bytes=VMEM_ALL),
        name="tail",
    )(mine, forces, sums, groups)


def double_factorial(number):
    result = 1.0
    while number > 1:
        result = result * number
        number = number - 2
    return result


def norm_of(degree, azimuth):
    value = math.sqrt(
        (2 * degree + 1)
        / (4 * math.pi)
        * math.factorial(degree - azimuth)
        / math.factorial(degree + azimuth)
    )
    return value * (math.sqrt(2.0) if azimuth else 1.0)


def scaled_legendre(coord_z):
    table = {}
    for azimuth in range(LMAX + 1):
        table[azimuth, azimuth] = norm_of(azimuth, azimuth) * double_factorial(2 * azimuth - 1)
        if azimuth + 1 <= LMAX:
            ratio = norm_of(azimuth + 1, azimuth) / norm_of(azimuth, azimuth)
            table[azimuth + 1, azimuth] = coord_z * (
                (2 * azimuth + 1) * ratio * table[azimuth, azimuth]
            )
        for degree in range(azimuth + 2, LMAX + 1):
            gap = degree - azimuth
            first = (2 * degree - 1) / gap * norm_of(degree, azimuth) / norm_of(degree - 1, azimuth)
            second = (
                (degree + azimuth - 1) / gap * norm_of(degree, azimuth) / norm_of(degree - 2, azimuth)
            )
            table[degree, azimuth] = (first * coord_z) * table[degree - 1, azimuth] - (
                second * table[degree - 2, azimuth]
            )
    return table


def azimuth_powers(coord_x, coord_y):
    cosines = [None, coord_x]
    sines = [None, coord_y]
    for _ in range(2, LMAX + 1):
        cosines.append(cosines[-1] * coord_x - sines[-1] * coord_y)
        sines.append(sines[-1] * coord_x + cosines[-2] * coord_y)
    return cosines, sines


LANE_GATHER = lax.GatherDimensionNumbers(
    offset_dims=(),
    collapsed_slice_dims=(1,),
    start_index_map=(1,),
    operand_batching_dims=(0,),
    start_indices_batching_dims=(0,),
)


def lane_gather(line, lo):
    return lax.gather(
        line,
        lo[..., None],
        LANE_GATHER,
        slice_sizes=(1, 1),
        mode=lax.GatherScatterMode.PROMISE_IN_BOUNDS,
    )


def prepare_kernel(first_ref, cnt_ref, nbr_ref, spot_ref, kind_ref, part_ref, table_ref, idx_ref, wt_ref,
                   sorted_ref, perm_ref, info_ref, mine_ref, got_ref, send_sem, recv_sem, key_ref, pos_ref,
                   word_ref, rank_ref):
    atoms = nbr_ref.shape[2]
    tiles = atoms // TILE
    blocks = NBR // 8
    sub = lax.broadcasted_iota(jnp.int32, (8, TILE), 0)
    lane = lax.broadcasted_iota(jnp.int32, (1, TILE), 1)
    site = site_rows(spot_ref, kind_ref, part_ref)
    pair = begin_spread(SPECIES, site, mine_ref, got_ref, send_sem, recv_sem)

    def merge(tile, carry):
        cols = pl.ds(pl.multiple_of(tile * TILE, TILE), TILE)
        limit = cnt_ref[:, cols]
        iota = lax.broadcasted_iota(jnp.int32, (NBR, TILE), 0)
        key = jnp.where(iota < limit, nbr_ref[:, 0, cols] - first_ref[0], -1 - iota)
        key_ref[...] = key
        keys = [key[8 * b : 8 * b + 8] for b in range(blocks)]
        total = [jnp.zeros((8, TILE), jnp.int32) for _ in range(blocks)]
        early = [jnp.zeros((8, TILE), jnp.int32) for _ in range(blocks)]
        for other in range(NBR):
            line = jnp.broadcast_to(key_ref[other : other + 1, :], (8, TILE))
            for b in range(blocks):
                same = jnp.where(keys[b] == line, 1, 0)
                total[b] = total[b] + same
                if other < 8 * b:
                    early[b] = early[b] + same
                elif other < 8 * b + 7:
                    early[b] = early[b] + jnp.where(sub > other - 8 * b, same, 0)
        for b in range(blocks):
            alive = sub + 8 * b < limit
            pos_ref[8 * b : 8 * b + 8, :] = jnp.where(alive & (early[b] == 0), 1, 0)
            key_ref[8 * b : 8 * b + 8, :] = total[b] * 4096 + keys[b]
        running = jnp.zeros((1, TILE), jnp.int32)
        out = [jnp.zeros((8, TILE), jnp.int32) for _ in range(blocks)]
        for slot in range(NBR):
            flag = pos_ref[slot : slot + 1, :]
            place = jnp.broadcast_to(jnp.where(flag == 1, running, -1), (8, TILE))
            running = running + flag
            line = jnp.broadcast_to(key_ref[slot : slot + 1, :], (8, TILE))
            for b in range(slot // 8 + 1):
                out[b] = jnp.where(place == sub + 8 * b, line, out[b])
        for b in range(blocks):
            word_ref[8 * b : 8 * b + 8, cols] = out[b].astype(f32)
        order = running * atoms + (atoms - 1 - tile * TILE) - lane
        rank_ref[pl.ds(tile, 1), :] = order.astype(f32)
        return carry

    lax.fori_loop(0, tiles, merge, 0)
    orders = rank_ref[...]
    upright = jnp.transpose(orders)
    ranks = []
    for tile in range(tiles):
        row = jnp.broadcast_to(orders[tile : tile + 1], (TILE, TILE))
        total = jnp.zeros((TILE, TILE), f32)
        for other in range(tiles):
            col = jnp.broadcast_to(upright[:, other : other + 1], (TILE, TILE))
            total = total + jnp.where(col > row, 1.0, 0.0)
        ranks.append(jnp.sum(total, axis=0, keepdims=True))
    place = lax.broadcasted_iota(jnp.int32, (atoms, TILE), 0).astype(f32)
    for tile in range(tiles):
        line = jnp.broadcast_to(ranks[tile], (atoms, TILE))
        perm_ref[:, tile * TILE : (tile + 1) * TILE] = jnp.where(line == place, 1.0, 0.0).astype(bf16)
    word_ref[NBR : NBR + 8, :] = site
    moved = reorder(word_ref[...], perm_ref, 1)
    sorted_ref[...] = moved[NBR:]
    word = moved[:NBR].astype(jnp.int32)
    index = lax.bitwise_and(word, 4095)
    times = lax.shift_right_logical(word, 12)
    idx_ref[:NBR, :] = index
    idx_ref[NBR:, :] = jnp.zeros((NPAD - NBR, atoms), jnp.int32)
    wt_ref[:NBR, :] = density_scale * times.astype(f32)
    wt_ref[NBR:, :] = jnp.zeros((NPAD - NBR, atoms), f32)
    row = lax.shift_right_logical(index, 7)
    low = jnp.min(jnp.where(times > 0, row, 1 << 20))
    high = jnp.max(jnp.where(times > 0, row, -1))
    slots = lax.broadcasted_iota(jnp.int32, (NBR, TILE), 0) + 1
    for tile in range(tiles):
        used = times[:, tile * TILE : (tile + 1) * TILE] > 0
        info_ref[0, tile] = lax.div(jnp.max(jnp.where(used, slots, 0)) + SLOTS - 1, SLOTS) * SLOTS
        info_ref[1, tile] = low
        info_ref[2, tile] = high
    end_spread(SPECIES, pair, table_ref, mine_ref)


def prepare_call(which, first, limits, neighbours, positions, species, structure):
    atoms = neighbours.shape[2]
    return pl.pallas_call(
        prepare_kernel,
        out_shape=(
            jax.ShapeDtypeStruct((SPECIES * 3 * atoms // TILE, TILE), f32),
            jax.ShapeDtypeStruct((NPAD, atoms), jnp.int32),
            jax.ShapeDtypeStruct((NPAD, atoms), f32),
            jax.ShapeDtypeStruct((8, atoms), f32),
            jax.ShapeDtypeStruct((atoms, atoms), bf16),
            jax.ShapeDtypeStruct((3, atoms // TILE), jnp.int32),
        ),
        in_specs=[smem_spec()] + [vmem_spec()] * 5,
        out_specs=(vmem_spec(),) * 5 + (smem_spec(),),
        scratch_shapes=[
            pltpu.VMEM((SPECIES * atoms // TILE, TILE), f32),
            pltpu.VMEM((2, SPECIES * atoms // TILE, TILE), f32),
            pltpu.SemaphoreType.DMA((2,)),
            pltpu.SemaphoreType.DMA((2,)),
            pltpu.VMEM((NBR, TILE), jnp.int32),
            pltpu.VMEM((NBR, TILE), jnp.int32),
            pltpu.VMEM((NBR + 8, atoms), f32),
            pltpu.VMEM((atoms // TILE, TILE), f32),
        ],
        compiler_params=comm_params(which),
        name="prepare",
    )(first, limits, neighbours, positions, species, structure)


def window_starts(row_low, row_high):
    start = jnp.minimum(row_low, 24 - FROWS)
    return start, lax.div(row_high - start, FROWS) + 1


def load_window(tab_ref, left_ref, values, exact, start):
    for value in range(values):
        pieces = split3(tab_ref[pl.ds(value * 24 + start, FROWS), :])
        for piece in range(3 if exact else 2):
            at = (piece * values + value) * FROWS
            left_ref[at : at + FROWS, :] = pieces[piece * FROWS : (piece + 1) * FROWS]


def fetch(left_ref, values, exact, idx_ref, put_ref, base, start):
    index = idx_ref[pl.ds(base, 8), :]
    hi = lax.shift_right_logical(index, 7) - start
    lo = lax.bitwise_and(index, 127)
    sub = lax.broadcasted_iota(jnp.int32, (TILE, TILE), 0)
    hits = []
    for part in range(8):
        line = jnp.broadcast_to(lo[part : part + 1, :], (TILE, TILE))
        hits.append(jnp.where(line == sub, 1.0, 0.0).astype(bf16))
    one = jnp.concatenate(hits, axis=1)
    height = values * FROWS
    pieces = 3 if exact else 2
    wide = jnp.dot(left_ref[0 : pieces * height, :], one, preferred_element_type=f32)
    got = wide[0:height] + wide[height : 2 * height]
    if exact:
        got = got + wide[2 * height :]
    line8 = lax.broadcasted_iota(jnp.int32, (8, TILE), 0)
    found = [jnp.zeros((8, TILE), f32) for _ in range(values)]
    for part in range(8):
        place = jnp.broadcast_to(hi[part : part + 1, :], (8, TILE))
        masks = [place == line8 + 8 * r for r in range(FROWS // 8)]
        for value in range(values):
            total = None
            for r, mask in enumerate(masks):
                at = value * FROWS + 8 * r
                term = jnp.where(mask, got[at : at + 8, part * TILE : (part + 1) * TILE], 0.0)
                total = term if total is None else total + term
            row = jnp.sum(total, axis=0, keepdims=True)
            found[value] = jnp.where(line8 == part, jnp.broadcast_to(row, (8, TILE)), found[value])
    inside = (hi >= 0) & (hi < FROWS)
    for value in range(values):
        rows = slot_rows(value, base)
        put_ref[rows, :] = jnp.where(inside, found[value], put_ref[rows, :])


def slot_rows(which, base):
    return pl.ds(pl.multiple_of(which * NPAD + base, 8), 8)


def geometry(layer, geo_ref, feat_ref, wt_ref, base):
    weight = wt_ref[pl.ds(base, 8), :]
    unit = [geo_ref[slot_rows(axis, base), :] for axis in range(3)]
    dist = geo_ref[slot_rows(4, base), :]
    if layer == 1:
        kind = geo_ref[slot_rows(3, base), :]
        chan = [jnp.where(kind == float(c), 1.0, 0.0) for c in range(SPECIES)]
    else:
        chan = [feat_ref[slot_rows(c, base), :] for c in range(SPECIES)]
    return weight, dist, unit, chan


def radial_terms(dist, rad_ref, with_slope):
    scaled = dist * (2.0 / cutoff_radius) - 1.0
    inside = dist < cutoff_radius
    angle = dist * (math.pi / cutoff_radius)
    cutoff = jnp.where(inside, 0.5 * (jnp.cos(angle) + 1.0), 0.0)
    cheb = [None, scaled]
    twice = 2.0 * scaled
    cheb.append(twice * scaled - 1.0)
    for _ in range(3, NRAD):
        cheb.append(twice * cheb[-1] - cheb[-2])
    basis = [cutoff] + [cutoff * cheb[p] for p in range(1, NRAD)]
    radial = []
    for n in range(NMAX):
        total = basis[0] * rad_ref[n, 0]
        for p in range(1, NRAD):
            total = total + basis[p] * rad_ref[n, p]
        radial.append(total)
    if not with_slope:
        return basis, radial, None
    slope_cut = jnp.where(inside, (-0.5 * math.pi / cutoff_radius) * jnp.sin(angle), 0.0)
    grad_scaled = cutoff * (2.0 / cutoff_radius)
    second = [None, None, twice]
    second[1] = jnp.ones_like(scaled)
    for _ in range(3, NRAD):
        second.append(twice * second[-1] - second[-2])
    slopes = [slope_cut, slope_cut * scaled + grad_scaled]
    for p in range(2, NRAD):
        slopes.append(slope_cut * cheb[p] + grad_scaled * (float(p) * second[p]))
    return basis, radial, slopes


def harmonic_list(unit):
    table = scaled_legendre(unit[2])
    cosines, sines = azimuth_powers(unit[0], unit[1])
    columns = []
    for degree in range(LMAX + 1):
        for signed in range(-degree, degree + 1):
            azimuth = abs(signed)
            poly = table[degree, azimuth]
            if signed == 0:
                columns.append(poly)
            elif signed > 0:
                columns.append(poly * cosines[azimuth])
            else:
                columns.append(poly * sines[azimuth])
    columns[0] = jnp.full_like(unit[2], columns[0])
    return columns


def density_kernel(layer, info_ref, rad_ref, tab_ref, cen_ref, idx_ref, wt_ref, *refs):
    if layer == 1:
        out_ref, geo_ref, x_ref, y_ref, d_ref, left_ref = refs
        feat_ref, put_ref = None, geo_ref
    else:
        geo_ref, out_ref, feat_ref, x_ref, y_ref, d_ref, left_ref = refs
        put_ref = feat_ref
    tile = pl.program_id(0)
    count = info_ref[0, tile]
    row_low, row_high = info_ref[1, tile], info_ref[2, tile]
    blocks = lax.div(count + 7, 8)

    start, windows = window_starts(row_low, row_high)

    def gather_window(window_at, carry):
        first_row = jnp.minimum(start + window_at * FROWS, 24 - FROWS)

        @pl.when((tile == 0) | (windows > 1))
        def _():
            load_window(tab_ref, left_ref, SPECIES, layer == 1, first_row)

        def gather_block(block_at, inner):
            base = pl.multiple_of(block_at * 8, 8)
            fetch(left_ref, SPECIES, layer == 1, idx_ref, put_ref, base, first_row)
            return inner

        return lax.fori_loop(0, blocks, gather_block, carry)

    lax.fori_loop(0, windows, gather_window, 0)

    def edges(block_at, carry):
        base = pl.multiple_of(block_at * 8, 8)
        if layer == 1:
            live = wt_ref[pl.ds(base, 8), :] > 0.0
            deltas = []
            for axis in range(3):
                centre = jnp.broadcast_to(cen_ref[pl.ds(axis, 1), :], (8, TILE))
                delta = geo_ref[slot_rows(axis, base), :] - centre
                deltas.append(jnp.where(live, delta, 1.0))
            dist = jnp.sqrt(deltas[0] * deltas[0] + deltas[1] * deltas[1] + deltas[2] * deltas[2])
            inv = 1.0 / dist
            for axis in range(3):
                geo_ref[slot_rows(axis, base), :] = deltas[axis] * inv
            geo_ref[slot_rows(4, base), :] = dist
        weight, dist, unit, chan = geometry(layer, geo_ref, feat_ref, wt_ref, base)
        _, radial, _ = radial_terms(dist, rad_ref, False)
        for c in range(SPECIES):
            scale = chan[c] * weight
            for n in range(NMAX):
                x_ref[pl.ds(base * XROW + (c * NMAX + n), 8, stride=XROW), :] = scale * radial[n]
        for at, column in enumerate(harmonic_list(unit)):
            y_ref[slot_rows(at, base), :] = column
        return carry

    lax.fori_loop(0, blocks, edges, 0)
    groups = lax.div(count, SLOTS)

    def lm_block(block_at, carry):
        first = block_at * LBLK

        def slots(group, acc):
            acc = list(acc)
            for part in range(SLOTS):
                slot = group * SLOTS + part
                rows = [x_ref[pl.ds(slot * XROW + 8 * j, 8), :] for j in range(CH // 8)]
                for at in range(LBLK):
                    line = jnp.broadcast_to(
                        y_ref[pl.ds((first + at) * NPAD + slot, 1), :], (8, TILE)
                    )
                    for j in range(CH // 8):
                        acc[at * (CH // 8) + j] = acc[at * (CH // 8) + j] + rows[j] * line
            return tuple(acc)

        zero = jnp.zeros((8, TILE), f32)
        acc = lax.fori_loop(0, groups, slots, tuple(zero for _ in range(LBLK * (CH // 8))))
        for at in range(LBLK):
            for j in range(CH // 8):
                d_ref[pl.ds(8 * j * LM + first + at, 8, stride=LM), :] = acc[at * (CH // 8) + j]
        return carry

    lax.fori_loop(0, LM // LBLK, lm_block, 0)
    out_ref[...] = d_ref[...].astype(bf16)


def smem_spec():
    return pl.BlockSpec(memory_space=pltpu.SMEM)


def tile_spec(rows):
    return pl.BlockSpec((rows, TILE), lambda i: (0, i))


def whole_spec(shape):
    return pl.BlockSpec(shape, lambda i: tuple(0 for _ in shape))


def density_call(layer, info, radial, table, centres, index, weight, geo=None):
    atoms = centres.shape[1]
    rows = GEO if layer == 1 else SPECIES
    extra = () if geo is None else (geo,)
    return pl.pallas_call(
        partial(density_kernel, layer),
        out_shape=(
            jax.ShapeDtypeStruct((DENS, atoms), bf16),
            jax.ShapeDtypeStruct((rows * NPAD, atoms), f32),
        ),
        grid=(atoms // TILE,),
        in_specs=[
            smem_spec(),
            smem_spec(),
            whole_spec(table.shape),
            tile_spec(8),
            tile_spec(NPAD),
            tile_spec(NPAD),
        ]
        + [tile_spec(GEO * NPAD)] * len(extra),
        out_specs=(tile_spec(DENS), tile_spec(rows * NPAD)),
        scratch_shapes=[
            pltpu.VMEM((NPAD * XROW + 8, TILE), f32),
            pltpu.VMEM((LM * NPAD, TILE), f32),
            pltpu.VMEM((DENS, TILE), f32),
            pltpu.VMEM((3 * SPECIES * FROWS, TILE), bf16),
        ],
        compiler_params=pltpu.CompilerParams(vmem_limit_bytes=VMEM_ALL),
        name="density_%d" % layer,
    )(info, radial, table, centres, index, weight, *extra)


def backward_kernel(layer, info_ref, rad_ref, geo_ref, feat_ref, idx_ref, wt_ref, dd_ref, win_in_ref,
                    own_in_ref, win_ref, own_ref, rad_out_ref, rgr_ref, x_ref, y_ref, gx_ref, gy_ref, val_ref,
                    left_ref):
    tile = pl.program_id(0)
    count = info_ref[0, tile]
    row_low, row_high = info_ref[1, tile], info_ref[2, tile]
    blocks = lax.div(count + 7, 8)
    zero = jnp.zeros((8, TILE), f32)

    @pl.when(tile == 0)
    def _():
        if layer == 1:
            win_ref[...] = win_in_ref[: 3 * WSTEP]
        else:
            win_ref[...] = jnp.zeros_like(win_ref)
        rgr_ref[...] = jnp.zeros_like(rgr_ref)

    def line_of(at):
        return jnp.broadcast_to(dd_ref[pl.ds(at, 1), :], (8, TILE))

    def contract_slots():
        def over_lm(step, acc):
            acc = list(acc)
            for part in range(LBLK):
                lm = step * LBLK + part
                col = y_ref[pl.ds(lm * 8, 8), :]
                for m in range(CH):
                    acc[m] = acc[m] + line_of(m * LM + lm) * col
            return tuple(acc)

        acc = tuple(zero for _ in range(CH))
        for step in range(LM // LBLK):
            acc = over_lm(step, acc)
        for m in range(CH):
            gx_ref[8 * m : 8 * m + 8, :] = acc[m]

        def over_m(step, acc):
            acc = list(acc)
            for part in range(4):
                m = step * 4 + part
                col = x_ref[pl.ds(m * 8, 8), :]
                for lm in range(LM):
                    acc[lm] = acc[lm] + line_of(m * LM + lm) * col
            return tuple(acc)

        acc = tuple(zero for _ in range(LM))
        for step in range(CH // 4):
            acc = over_m(step, acc)
        for lm in range(LM):
            gy_ref[8 * lm : 8 * lm + 8, :] = acc[lm]

    def contract_species(kind):
        odd = (kind == 1.0) | (kind == 3.0)
        upper = kind > 1.5

        def over_n(step, acc):
            acc = list(acc)
            for part in range(2):
                n = step * 2 + part
                at = n * 8
                scaled = x_ref[pl.ds(at, 8), :]
                sums = [None, None]
                for lm in range(LM):
                    lines = [line_of((c * NMAX + n) * LM + lm) for c in range(SPECIES)]
                    first = jnp.where(odd, lines[1], lines[0])
                    second = jnp.where(odd, lines[3], lines[2])
                    grad = jnp.where(upper, second, first)
                    acc[lm] = acc[lm] + grad * scaled
                    term = grad * y_ref[8 * lm : 8 * lm + 8, :]
                    sums[lm % 2] = term if lm < 2 else sums[lm % 2] + term
                gx_ref[pl.ds(at, 8), :] = sums[0] + sums[1]
            return tuple(acc)

        acc = tuple(zero for _ in range(LM))
        for step in range(NMAX // 2):
            acc = over_n(step, acc)
        for lm in range(LM):
            gy_ref[8 * lm : 8 * lm + 8, :] = acc[lm]

    def slot_block(block_at, own):
        base = pl.multiple_of(block_at * 8, 8)
        weight, dist, unit, chan = geometry(layer, geo_ref, feat_ref, wt_ref, base)
        _, radial, _ = radial_terms(dist, rad_ref, False)
        for at, column in enumerate(harmonic_list(unit)):
            y_ref[8 * at : 8 * at + 8, :] = column
        if layer == 1:
            for n in range(NMAX):
                x_ref[8 * n : 8 * n + 8, :] = weight * radial[n]
            contract_species(geo_ref[slot_rows(3, base), :])
        else:
            for c in range(SPECIES):
                scale = chan[c] * weight
                for n in range(NMAX):
                    at = 8 * (c * NMAX + n)
                    x_ref[at : at + 8, :] = scale * radial[n]
            contract_slots()
        weight, dist, unit, chan = geometry(layer, geo_ref, feat_ref, wt_ref, base)
        inv = 1.0 / dist
        basis, radial, slopes = radial_terms(dist, rad_ref, True)
        feat_grads = []
        radial_grads = [None] * NMAX
        if layer == 1:
            radial_grads = [gx_ref[8 * n : 8 * n + 8, :] for n in range(NMAX)]
        for c in range(SPECIES if layer == 2 else 0):
            total = None
            for n in range(NMAX):
                grad = gx_ref[8 * (c * NMAX + n) : 8 * (c * NMAX + n) + 8, :]
                term = grad * radial[n]
                total = term if total is None else total + term
                piece = grad * chan[c]
                radial_grads[n] = piece if c == 0 else radial_grads[n] + piece
            feat_grads.append(total * weight)
        grad_r = None
        radial_grads = [grad * weight for grad in radial_grads]
        for p in range(NRAD):
            total = None
            for n in range(NMAX):
                at = (n * NRAD + p) * 8
                rgr_ref[pl.ds(at, 8), :] = rgr_ref[pl.ds(at, 8), :] + radial_grads[n] * basis[p]
                term = radial_grads[n] * rad_ref[n, p]
                total = term if total is None else total + term
            term = total * slopes[p]
            grad_r = term if grad_r is None else grad_r + term
        table = scaled_legendre(unit[2])
        cosines, sines = azimuth_powers(unit[0], unit[1])
        grad_x = grad_y = grad_z = None

        def plus(total, term):
            return term if total is None else total + term

        for azimuth in range(LMAX + 1):
            grad_cos = grad_sin = None
            for degree in range(azimuth, LMAX + 1):
                at = degree * degree + degree
                up = gy_ref[8 * (at + azimuth) : 8 * (at + azimuth) + 8, :]
                poly = table[degree, azimuth]
                if azimuth:
                    down = gy_ref[8 * (at - azimuth) : 8 * (at - azimuth) + 8, :]
                    grad_cos = plus(grad_cos, up * poly)
                    grad_sin = plus(grad_sin, down * poly)
                if degree > azimuth:
                    ratio = norm_of(degree, azimuth) / norm_of(degree, azimuth + 1)
                    slope = ratio * table[degree, azimuth + 1]
                    if azimuth:
                        grad_z = plus(grad_z, slope * (up * cosines[azimuth] + down * sines[azimuth]))
                    else:
                        grad_z = plus(grad_z, slope * up)
            if azimuth == 1:
                grad_x, grad_y = grad_cos, grad_sin
            elif azimuth > 1:
                below_cos, below_sin = cosines[azimuth - 1], sines[azimuth - 1]
                grad_x = grad_x + float(azimuth) * (grad_cos * below_cos + grad_sin * below_sin)
                grad_y = grad_y + float(azimuth) * (grad_sin * below_cos - grad_cos * below_sin)
        dot_u = grad_x * unit[0] + grad_y * unit[1] + grad_z * unit[2]
        live = weight > 0.0
        out = []
        for axis, grad in enumerate((grad_x, grad_y, grad_z)):
            value = (grad - dot_u * unit[axis]) * inv + grad_r * unit[axis]
            out.append(jnp.where(live, value, 0.0))
        values = out + feat_grads
        for at, value in enumerate(values):
            val_ref[slot_rows(at, base), :] = value
        return tuple(total + value for total, value in zip(own, out))


    own = lax.fori_loop(0, blocks, slot_block, (zero, zero, zero))
    own = jnp.concatenate(
        [jnp.sum(total, axis=0, keepdims=True) for total in own] + [jnp.zeros((5, TILE), f32)], axis=0
    )
    own_ref[...] = own + own_in_ref[...] if layer == 1 else own

    used = 3 if layer == 1 else NVAL
    height = used * WROWS
    step_rows = height + 1
    sub = lax.broadcasted_iota(jnp.int32, (TILE, TILE), 0)
    windows = lax.div(row_high - row_low + WROWS, WROWS)

    def window(window_at, carry):
        row_base = row_low + window_at * WROWS

        def scatter(block_at, acc):
            base = pl.multiple_of(block_at * 8, 8)
            index = idx_ref[pl.ds(base, 8), :]
            hi = lax.shift_right_logical(index, 7)
            lo = lax.bitwise_and(index, 127)
            for row in range(WROWS):
                hit = hi == row_base + row
                for value_at in range(used):
                    value = val_ref[slot_rows(value_at, base), :]
                    left_ref[pl.ds(value_at * WROWS + row, 8, stride=step_rows), :] = jnp.where(
                        hit, value, 0.0
                    )
            ones, left = [], []
            for part in range(8):
                line = jnp.broadcast_to(lo[part : part + 1, :], (TILE, TILE))
                ones.append(jnp.where(line == sub, 1.0, 0.0).astype(bf16))
                left.append(left_ref[part * step_rows : part * step_rows + height, :])
            left = jnp.concatenate(left, axis=1)
            ones = jnp.concatenate(ones, axis=1)
            high = left.astype(bf16)
            rest = (left - high.astype(f32)).astype(bf16)
            dims = (((1,), (1,)), ((), ()))
            acc = acc + lax.dot_general(high, ones, dims, preferred_element_type=f32)
            return acc + lax.dot_general(rest, ones, dims, preferred_element_type=f32)

        acc = lax.fori_loop(0, blocks, scatter, jnp.zeros((height, TILE), f32))
        for value_at in range(used):
            at = value_at * WSTEP + row_base
            win_ref[pl.ds(at, WROWS), :] = (
                win_ref[pl.ds(at, WROWS), :] + acc[value_at * WROWS : (value_at + 1) * WROWS]
            )
        return carry

    lax.fori_loop(0, windows, window, 0)

    @pl.when(tile == pl.num_programs(0) - 1)
    def _():
        for at in range(NMAX * NRAD):
            rad_out_ref[at : at + 1, :] = jnp.sum(rgr_ref[8 * at : 8 * at + 8, :], axis=0, keepdims=True)


def backward_call(layer, info, radial, geo, feat, index, weight, grad_dens, window_in, own_in):
    atoms = index.shape[1]
    values = 3 if layer == 1 else NVAL
    return pl.pallas_call(
        partial(backward_kernel, layer),
        out_shape=(
            jax.ShapeDtypeStruct((values * WSTEP, TILE), f32),
            jax.ShapeDtypeStruct((8, atoms), f32),
            jax.ShapeDtypeStruct((NMAX * NRAD, TILE), f32),
        ),
        grid=(atoms // TILE,),
        in_specs=[
            smem_spec(),
            smem_spec(),
            tile_spec(GEO * NPAD),
            tile_spec(feat.shape[0]),
            tile_spec(NPAD),
            tile_spec(NPAD),
            tile_spec(DENS),
            whole_spec(window_in.shape),
            tile_spec(8),
        ],
        out_specs=(
            whole_spec((values * WSTEP, TILE)),
            tile_spec(8),
            whole_spec((NMAX * NRAD, TILE)),
        ),
        scratch_shapes=[
            pltpu.VMEM((NMAX * NRAD * 8, TILE), f32),
            pltpu.VMEM((CH * 8, TILE), f32),
            pltpu.VMEM((LM * 8, TILE), f32),
            pltpu.VMEM((CH * 8, TILE), f32),
            pltpu.VMEM((LM * 8, TILE), f32),
            pltpu.VMEM((NVAL * NPAD, TILE), f32),
            pltpu.VMEM((8 * (NVAL * WROWS + 1), TILE), f32),
        ],
        compiler_params=pltpu.CompilerParams(vmem_limit_bytes=VMEM_ALL),
        name="backward_%d" % layer,
    )(info, radial, geo, feat, index, weight, grad_dens, window_in, own_in)


def tn_dot(left, right):
    return lax.dot_general(left, right, (((0,), (0,)), ((), ())), preferred_element_type=f32)


def nt_dot(left, right):
    return lax.dot_general(left, right, (((1,), (1,)), ((), ())), preferred_element_type=f32)


def padded_rows(value):
    return jnp.concatenate([value, jnp.zeros((8 - value.shape[0], value.shape[1]), f32)], axis=0)


def onehot_rows(species):
    kind = lax.broadcasted_iota(jnp.int32, (8, species.shape[1]), 0).astype(f32)
    return jnp.where(kind == species, 1.0, 0.0).astype(bf16)


def combine(parts):
    total = parts[2][0:8]
    total = total + (parts[1][8:16] + parts[0][16:24])
    total = total + (parts[1][0:8] + parts[0][8:16])
    return total + parts[0][0:8]


def by_atoms(rows24, chunk):
    wide = nt_dot(rows24, split3(chunk))
    return [wide[:, j * QB : (j + 1) * QB] for j in range(3)]


def contract_one_kernel(dens_ref, coup_ref, coef_ref, mix_ref, site_ref, factor_ref, energy_ref, feat_ref,
                        aux_ref, grad_ref, b_ref, ch_ref, row_ref):
    factor_at = pl.program_id(0)
    quantum, atoms = b_ref.shape
    half = quantum // 2
    for part in range(2):
        rows = slice(part * half, (part + 1) * half)
        value = tn_dot(coup_ref[0, :, rows], dens_ref[...])
        factor_ref[0, rows, :] = value

        @pl.when(factor_at == 0)
        def _(value=value, rows=rows):
            b_ref[rows, :] = value

        @pl.when(factor_at > 0)
        def _(value=value, rows=rows):
            b_ref[rows, :] = b_ref[rows, :] * value

    @pl.when(factor_at == pl.num_programs(0) - 1)
    def _():
        onehot = onehot_rows(site_ref[3:4, :])
        row_ref[0:24, :] = split3(padded_rows(coef_ref[...]))
        row_ref[24:48, :] = split3(padded_rows(mix_ref[...]))
        triple = jnp.concatenate([onehot] * 3, axis=0)

        def chunk_body(chunk, mixed):
            cols = pl.ds(pl.multiple_of(chunk * QB, QB), QB)
            ch_ref[...] = tn_dot(row_ref[0:24, cols], triple)
            pieces = split3(b_ref[cols, :])
            left = row_ref[24:48, cols]
            parts = [
                jnp.dot(left, pieces[j * QB : (j + 1) * QB], preferred_element_type=f32) for j in range(3)
            ]
            wide = nt_dot(onehot, pieces)
            grad_ref[:, cols] = wide[:, 2 * QB :] + wide[:, QB : 2 * QB] + wide[:, :QB]

            def rows_body(step, sums):
                at = pl.multiple_of(step * 8, 8)
                value = b_ref[pl.ds(pl.multiple_of(chunk * QB + step * 8, 8), 8), :]
                return sums[0] + value * ch_ref[pl.ds(at, 8), :], sums[1] + value * value

            energy, square = lax.fori_loop(0, QB // 8, rows_body, mixed[1:])
            return mixed[0] + combine(parts), energy, square

        zero = jnp.zeros((8, atoms), f32)
        mixed, energy, square = lax.fori_loop(0, quantum // QB, chunk_body, (zero, zero, zero))
        energy_ref[...] = jnp.broadcast_to(jnp.sum(energy, axis=0, keepdims=True), (8, atoms))
        mean = jnp.sum(square, axis=0, keepdims=True) * (1.0 / quantum)
        scale = lax.rsqrt(mean + norm_eps)
        feat_ref[...] = mixed * scale
        aux_ref[0:8, :] = mixed
        aux_ref[8:16, :] = jnp.broadcast_to(scale, (8, atoms))


def contract_one_call(dens, coupling, coefficient, mixing_rows, ordered):
    factors, depth, quantum = coupling.shape
    atoms = dens.shape[1]
    return pl.pallas_call(
        contract_one_kernel,
        out_shape=(
            jax.ShapeDtypeStruct((factors, quantum, atoms), f32),
            jax.ShapeDtypeStruct((8, atoms), f32),
            jax.ShapeDtypeStruct((8, atoms), f32),
            jax.ShapeDtypeStruct((16, atoms), f32),
            jax.ShapeDtypeStruct((8, quantum), f32),
        ),
        grid=(factors,),
        in_specs=[
            whole_spec((depth, atoms)),
            pl.BlockSpec((1, depth, quantum), lambda v: (v, 0, 0)),
            whole_spec(coefficient.shape),
            whole_spec(mixing_rows.shape),
            whole_spec(ordered.shape),
        ],
        out_specs=(
            pl.BlockSpec((1, quantum, atoms), lambda v: (v, 0, 0)),
            whole_spec((8, atoms)),
            whole_spec((8, atoms)),
            whole_spec((16, atoms)),
            whole_spec((8, quantum)),
        ),
        scratch_shapes=[
            pltpu.VMEM((quantum, atoms), f32),
            pltpu.VMEM((QB, atoms), f32),
            pltpu.VMEM((48, quantum), bf16),
        ],
        compiler_params=pltpu.CompilerParams(vmem_limit_bytes=VMEM_ALL),
        name="contract_1",
    )(dens, coupling, coefficient, mixing_rows, ordered)


def factor_grads(values, upstream):
    low_pair, high_pair = values[0] * values[1], values[2] * values[3]
    first, second = upstream * high_pair, upstream * low_pair
    return first * values[1], first * values[0], second * values[3], second * values[2]


def contract_two_kernel(dens_ref, coef_ref, site_ref, before_ref, coup_ref, out_ref, part_ref, grad_ref,
                        cv_ref, f_ref, g_ref, ch_ref, row_ref, sem):
    step = pl.program_id(0)
    factors, quantum, atoms = f_ref.shape
    depth = dens_ref.shape[0]
    half = quantum // 2

    def load(at):
        return pltpu.make_async_copy(coup_ref.at[at], cv_ref.at[at, 0:depth], sem.at[at])

    @pl.when(step == 0)
    def _():
        for at in range(factors):
            load(at).start()
        onehot = onehot_rows(site_ref[3:4, :])
        row_ref[...] = split3(padded_rows(coef_ref[...]))
        triple = jnp.concatenate([onehot] * 3, axis=0)

        def factor_body(at, carry):
            load(at).wait()
            for part in range(2):
                rows = slice(part * half, (part + 1) * half)
                f_ref[at, rows, :] = tn_dot(cv_ref[at, 0:depth, rows], dens_ref[...])
            return carry

        lax.fori_loop(0, factors, factor_body, 0)

        def chunk_body(chunk, energy):
            cols = pl.ds(pl.multiple_of(chunk * QB, QB), QB)
            ch_ref[...] = tn_dot(row_ref[:, cols], triple)

            def rows_body(small, total):
                at = pl.multiple_of(small * 16, 16)
                rows = pl.ds(pl.multiple_of(chunk * QB + small * 16, 16), 16)
                values = [f_ref[v, rows, :] for v in range(factors)]
                upstream = ch_ref[pl.ds(at, 16), :]
                grads = factor_grads(values, upstream)
                for v in range(factors):
                    g_ref[v, rows, :] = grads[v].astype(bf16)
                product = values[0] * values[1] * values[2] * values[3]
                f_ref[0, rows, :] = product
                term = product * upstream
                return total + term[:8] + term[8:]

            energy = lax.fori_loop(0, QB // 16, rows_body, energy)
            wide = nt_dot(onehot, split3(f_ref[0, cols, :]))
            grad_ref[:, cols] = wide[:, 2 * QB :] + wide[:, QB : 2 * QB] + wide[:, :QB]
            return energy

        energy = lax.fori_loop(0, quantum // QB, chunk_body, jnp.zeros((8, atoms), f32))
        energy = jnp.sum(energy, axis=0, keepdims=True) + before_ref[0:1, :]
        kinds = [jnp.where(site_ref[3:4, :] == float(c), 1.0, 0.0) for c in range(SPECIES)]
        rows8 = split3(jnp.concatenate([energy] + kinds + [jnp.zeros((3, atoms), f32)], axis=0))
        owner = site_ref[4:5, :]

        def structure_body(chunk, carry):
            cols = pl.ds(pl.multiple_of(chunk * TILE, TILE), TILE)
            ids = lax.broadcasted_iota(jnp.int32, (TILE, atoms), 0) + chunk * TILE
            members = jnp.where(ids.astype(f32) == owner, 1.0, 0.0).astype(bf16)
            wide = nt_dot(rows8, members)
            part_ref[:, cols] = wide[16:24] + wide[8:16] + wide[0:8]
            return carry

        lax.fori_loop(0, part_ref.shape[1] // TILE, structure_body, 0)

    rows = pl.ds(pl.multiple_of(step * DROWS, 16), DROWS)
    total = None
    for at in range(factors):
        part = jnp.dot(cv_ref[at, rows, :], g_ref[at], preferred_element_type=f32)
        total = part if total is None else total + part
    out_ref[...] = total


def contract_two_call(dens, coupling, coefficient, ordered, energy_one, structures):
    factors, depth, quantum = coupling.shape
    atoms = dens.shape[1]
    steps = pl.cdiv(depth, DROWS)
    return pl.pallas_call(
        contract_two_kernel,
        out_shape=(
            jax.ShapeDtypeStruct((steps * DROWS, atoms), f32),
            jax.ShapeDtypeStruct((8, structures), f32),
            jax.ShapeDtypeStruct((8, quantum), f32),
        ),
        grid=(steps,),
        in_specs=[
            pl.BlockSpec((depth, atoms), lambda i: (0, 0), pipeline_mode=pl.Buffered(1)),
            whole_spec(coefficient.shape),
            whole_spec(ordered.shape),
            whole_spec(energy_one.shape),
            pl.BlockSpec(memory_space=pl.ANY),
        ],
        out_specs=(
            pl.BlockSpec((DROWS, atoms), lambda i: (i, 0)),
            whole_spec((8, structures)),
            whole_spec((8, quantum)),
        ),
        scratch_shapes=[
            pltpu.VMEM((factors, steps * DROWS, quantum), bf16),
            pltpu.VMEM((factors, quantum, atoms), f32),
            pltpu.VMEM((factors, quantum, atoms), bf16),
            pltpu.VMEM((QB, atoms), f32),
            pltpu.VMEM((24, quantum), bf16),
            pltpu.SemaphoreType.DMA((factors,)),
        ],
        compiler_params=pltpu.CompilerParams(vmem_limit_bytes=VMEM_ALL),
        name="contract_2",
    )(dens, coefficient, ordered, energy_one, coupling)


def contract_back_kernel(values_at, coup_ref, coef_ref, mix_ref, site_ref, win_ref, perm_ref, aux_ref, factor_ref,
                         out_ref, grad_ref, f_ref, g_ref, ch_ref, row_ref, got_ref, sem, send_sem, recv_sem):
    step = pl.program_id(0)
    factors, quantum, atoms = f_ref.shape
    chunks = quantum // QB

    def load(chunk):
        rows = pl.ds(pl.multiple_of(chunk * QB, QB), QB)
        return pltpu.make_async_copy(factor_ref.at[:, rows, :], f_ref.at[:, rows, :], sem.at[chunk])

    @pl.when(step == 0)
    def _():
        tiles = got_ref.shape[2]
        pair = SidePair(
            win_ref.at[values_at:, 0:tiles],
            win_ref.at[values_at:, 2 * tiles : 3 * tiles],
            got_ref,
            send_sem,
            recv_sem,
        )
        greet(pair.partners, pair.flags)
        pair.start()
        for chunk in range(chunks):
            load(chunk).start()
        onehot = onehot_rows(site_ref[3:4, :])
        scale = aux_ref[8:9, :]
        pair.wait()
        total = win_ref[values_at:, tiles : 2 * tiles] + pair.received(0) + pair.received(1)
        gfeat = reorder(in_lanes(total), perm_ref, 1)
        dot = jnp.sum(aux_ref[0:8, :] * gfeat, axis=0, keepdims=True)
        shrink = jnp.broadcast_to(scale * scale * scale * dot * (1.0 / quantum), (8, atoms))
        scaled = split3(scale * gfeat)
        high, middle, low = scaled[0:8], scaled[8:16], scaled[16:24]
        mix = split3(padded_rows(mix_ref[...]))
        row_ref[0:24, :] = split3(padded_rows(coef_ref[...]))
        for at, piece in enumerate((0, 0, 0, 1, 1, 2)):
            row_ref[24 + 8 * at : 32 + 8 * at, :] = mix[8 * piece : 8 * piece + 8]
        right = jnp.concatenate([onehot] * 3 + [high, middle, low, high, middle, high], axis=0)

        def chunk_body(chunk, carry):
            load(chunk).wait()
            cols = pl.ds(pl.multiple_of(chunk * QB, QB), QB)
            ch_ref[...] = tn_dot(row_ref[:, cols], right)

            def rows_body(small, inner):
                at = pl.multiple_of(small * 16, 16)
                rows = pl.ds(pl.multiple_of(chunk * QB + small * 16, 16), 16)
                values = [f_ref[v, rows, :] for v in range(factors)]
                product = values[0] * values[1] * values[2] * values[3]
                both = jnp.concatenate([shrink, shrink], axis=0)
                upstream = ch_ref[pl.ds(at, 16), :] - both * product
                grads = factor_grads(values, upstream)
                for v in range(factors):
                    g_ref[v, rows, :] = grads[v].astype(bf16)
                f_ref[0, rows, :] = product
                return inner

            lax.fori_loop(0, QB // 16, rows_body, 0)
            grad_ref[:, cols] = combine(by_atoms(scaled, f_ref[0, cols, :]))
            return carry

        lax.fori_loop(0, chunks, chunk_body, 0)

    total = None
    for at in range(factors):
        part = jnp.dot(coup_ref[at], g_ref[at], preferred_element_type=f32)
        total = part if total is None else total + part
    out_ref[...] = total


def contract_back_call(which, values_at, coupling, coefficient, mixing_rows, ordered, window, perm, aux, factor):
    factors, depth, quantum = coupling.shape
    atoms = ordered.shape[1]
    rows = depth // 5
    return pl.pallas_call(
        partial(contract_back_kernel, values_at),
        out_shape=(
            jax.ShapeDtypeStruct((depth, atoms), f32),
            jax.ShapeDtypeStruct((8, quantum), f32),
        ),
        grid=(5,),
        in_specs=[
            pl.BlockSpec((factors, rows, quantum), lambda i: (0, i, 0)),
            whole_spec(coefficient.shape),
            whole_spec(mixing_rows.shape),
            whole_spec(ordered.shape),
            whole_spec(window.shape),
            whole_spec(perm.shape),
            whole_spec(aux.shape),
            pl.BlockSpec(memory_space=pl.ANY),
        ],
        out_specs=(pl.BlockSpec((rows, atoms), lambda i: (i, 0)), whole_spec((8, quantum))),
        scratch_shapes=[
            pltpu.VMEM((factors, quantum, atoms), f32),
            pltpu.VMEM((factors, quantum, atoms), bf16),
            pltpu.VMEM((QB, atoms), f32),
            pltpu.VMEM((72, quantum), bf16),
            pltpu.VMEM((2, window.shape[0] - values_at, atoms // TILE, TILE), f32),
            pltpu.SemaphoreType.DMA((quantum // QB,)),
            pltpu.SemaphoreType.DMA((2,)),
            pltpu.SemaphoreType.DMA((2,)),
        ],
        compiler_params=comm_params(which),
        name="contract_back_1",
    )(coupling, coefficient, mixing_rows, ordered, window, perm, aux, factor)


def per_device(
    positions,
    species,
    neighbours,
    slot_counts,
    structure,
    target_energy,
    radial_one,
    coupling_one,
    coefficient_one,
    mixing,
    radial_two,
    coupling_two,
    coefficient_two,
):
    atoms = positions.shape[2]
    tiles = atoms // TILE
    structures = target_energy.shape[1]
    first = ((lax.axis_index("dom") - 1) * atoms).astype(jnp.int32).reshape(1)
    table_one, index, weight, ordered, perm, info = prepare_call(
        0, first, slot_counts, neighbours, positions, species, structure
    )
    mixing_rows = mixing.T

    dens_one, geo = density_call(1, info, radial_one, table_one, ordered, index, weight)
    factors_one, energy_one, features, aux, coefficient_first = contract_one_call(
        dens_one, coupling_one, coefficient_one, mixing_rows, ordered
    )
    table_two = spread_call(1, SPECIES, (features, perm))
    dens_two, feat = density_call(2, info, radial_two, table_two, ordered, index, weight, geo)
    grad_dens_two, per_structure, coefficient_second = contract_two_call(
        dens_two, coupling_two, coefficient_two, ordered, energy_one, structures
    )
    window_two, own_two, radial_second = backward_call(
        2, info, radial_two, geo, feat, index, weight, grad_dens_two, table_two, ordered
    )
    grad_dens_one, mixing_gradient = contract_back_call(
        2,
        3,
        coupling_one,
        coefficient_one,
        mixing_rows,
        ordered,
        window_two.reshape(NVAL, WSTEP, TILE),
        perm,
        aux,
        factors_one,
    )
    window_one, own_one, radial_first = backward_call(
        1, info, radial_one, geo, ordered, index, weight, grad_dens_one, window_two, own_two
    )
    groups = lax.axis_size("grp")
    steps = sum(len(group) for group in exchange_rounds())
    forces, sums, group_sums = finish_call(
        3,
        steps,
        groups,
        tiles,
        (
            window_one.reshape(3, WSTEP, TILE),
            own_one,
            perm,
            coefficient_first,
            coefficient_second,
            mixing_gradient,
            radial_first,
            radial_second,
            per_structure,
            target_energy,
        ),
    )
    mine = lax.axis_index("grp").astype(jnp.int32).reshape(1)
    outputs = list(tail_call(mine, forces, sums, group_sums))
    outputs[1] = outputs[1].reshape(SPECIES)
    outputs[5] = outputs[5].T
    return tuple(outputs)


def solution(mesh):
    in_specs = (
        P(None, "grp", "dom"),
        P("grp", "dom"),
        P(None, "grp", "dom"),
        P("grp", "dom"),
        P("grp", "dom"),
        P("grp", None),
        P(),
        P(),
        P(),
        P(),
        P(),
        P(),
        P(),
    )
    out_specs = (P("grp", None), P(), P(None, "grp", "dom"), P(), P(), P(), P(), P())
    return jax.shard_map(
        per_device, mesh=mesh, in_specs=in_specs, out_specs=out_specs, check_vma=False
    )
```
